128 devices in a mesh: rep: 2 (over core), dp: 64 (over x, y, z).
Axes of the slice: x: 4, y: 4, z: 4, core: 2. Of those that a mesh axis runs over, the one named last changes fastest.
Arguments:
- x: bfloat16 [128, 2048, 896], P(('rep', 'dp')), parts along dimension 0
- dy: bfloat16 [128, 2048, 896], P(('rep', 'dp')), parts along dimension 0
- w_gate: bfloat16 [2, 896, 2560], replicated
- w_up: bfloat16 [2, 896, 2560], replicated
- w_down: bfloat16 [2, 2560, 896], replicated
- m_w_gate: float32 [2, 896, 2560], P(None, 'dp')
- m_w_up: float32 [2, 896, 2560], P(None, 'dp')
- m_w_down: float32 [2, 2560, 896], P(None, 'dp')
- v_w_gate: float32 [2, 896, 2560], P(None, 'dp')
- v_w_up: float32 [2, 896, 2560], P(None, 'dp')
- v_w_down: float32 [2, 2560, 896], P(None, 'dp')
Outputs:
- output 1: bfloat16 [4, 896, 2560], P('rep'), parts along dimension 0
- output 2: bfloat16 [4, 896, 2560], P('rep'), parts along dimension 0
- output 3: bfloat16 [4, 2560, 896], P('rep'), parts along dimension 0
- output 4: float32 [4, 896, 2560], P('rep', 'dp'), parts along dimension 0
- output 5: float32 [4, 896, 2560], P('rep', 'dp'), parts along dimension 0
- output 6: float32 [4, 2560, 896], P('rep', 'dp'), parts along dimension 0
- output 7: float32 [4, 896, 2560], P('rep', 'dp'), parts along dimension 0
- output 8: float32 [4, 896, 2560], P('rep', 'dp'), parts along dimension 0
- output 9: float32 [4, 2560, 896], P('rep', 'dp'), parts along dimension 0
There are 2 independent parts. The reference program is written for one: setup_inputs(seed, part) draws one part's arguments, and reference() takes and returns one part's arrays. A program takes and returns all parts, laid end to end along the dimension named above; an argument that names none is the same for every part.
All inputs are finite; a program needn't handle non-finite values.
Results may differ from the reference program's by a relative error of at most 0.022.
Values are sent between devices in bfloat16 or wider.
A program may use at most 1.5 GiB of HBM per device.

```python
import jax
import jax.numpy as jnp
from jax import lax

SEQUENCES = 64
TOKENS = 2048
D = 896
FF = 2560
LAYERS = 2
NAMES = ("w_gate", "w_up", "w_down")
SHAPES = {"w_gate": (LAYERS, D, FF), "w_up": (LAYERS, D, FF), "w_down": (LAYERS, FF, D)}


def bump(key, n, height):
    away = (jnp.arange(n, dtype=jnp.int32) - jax.random.randint(key, (), 0, n, jnp.int32)) % n
    return jnp.where(away < n // 8, height, 1.0)


def together(key, own, strength):
    shared = jax.random.normal(key, own.shape[1:], jnp.float32)
    return (own + strength * shared) * lax.rsqrt(1 + strength * strength)


def setup_inputs(seed: int = 0, part: int = 0) -> dict:
    kx, kdy, ka, kb, kz, kf, kh, kl, *keys = jax.random.split(jax.random.key(seed), 8 + 3 * len(NAMES))
    kx, kdy, ka, kb = (jax.random.fold_in(k, part) for k in (kx, kdy, ka, kb))
    kw, km, kv = (keys[i::3] for i in range(3))
    shape = (SEQUENCES, TOKENS, D)
    much_x, much_dy = jax.random.uniform(kz, (2,), jnp.float32, 0.0, 1.0)
    loud = 2.0 ** jax.random.uniform(jax.random.fold_in(kz, 1), (), jnp.float32, -1.0, 2.0)
    layers = 2.0 ** jax.random.uniform(kl, (LAYERS, 1, 1), jnp.float32, -1.0, 1.0)
    x = together(ka, jax.random.normal(kx, shape, jnp.float32), much_x) * bump(kf, D, 4.0)
    dy = together(kb, jax.random.normal(kdy, shape, jnp.float32), much_dy)
    drawn = {"x": x.astype(jnp.bfloat16), "dy": (loud * dy * (SEQUENCES * TOKENS) ** -0.5).astype(jnp.bfloat16)}
    for key, name in zip(kw, NAMES, strict=True):
        w = jax.random.normal(key, SHAPES[name], jnp.float32) * SHAPES[name][1] ** -0.5
        drawn[name] = (w * {"w_gate": 1.0, "w_up": bump(kh, FF, 4.0), "w_down": layers}[name]).astype(jnp.bfloat16)
    for key, name in zip(km, NAMES, strict=True):
        drawn[f"m_{name}"] = 0.1 * jax.random.normal(key, SHAPES[name], jnp.float32)
    for key, name in zip(kv, NAMES, strict=True):
        drawn[f"v_{name}"] = jax.random.uniform(key, SHAPES[name], jnp.float32, 0.005, 0.015)
    return drawn


def matmul(a, w):
    return jnp.dot(a, w, preferred_element_type=jnp.float32).astype(jnp.bfloat16)


def normed(h):
    wide = h.astype(jnp.float32)
    scale = lax.rsqrt(jnp.mean(wide**2, -1, keepdims=True) + 1e-6)
    return (wide * scale).astype(jnp.bfloat16)


def layer(h, w):
    a = normed(h)
    gate = jnp.dot(a, w["w_gate"], preferred_element_type=jnp.float32)
    up = jnp.dot(a, w["w_up"], preferred_element_type=jnp.float32)
    return h + matmul((jax.nn.silu(gate) * up).astype(jnp.bfloat16), w["w_down"])


def adamw(w, m, v, g):
    m = 0.9 * m + 0.1 * g
    v = 0.95 * v + 0.05 * g * g
    step = m * lax.rsqrt(v + 1e-8) + 0.1 * w
    return (w - 0.02 * step).astype(jnp.bfloat16), m, v


def clipped(gradients, sum_of_squares, count):
    factor = jnp.minimum(1.0, 0.5 * lax.rsqrt(sum_of_squares / count + 1e-30))
    return [g * factor for g in gradients]


def stack(weights, h):
    return lax.scan(lambda h, w: (layer(h, w), None), h, weights)[0]


def reference(x, dy, w_gate, w_up, w_down, m_w_gate, m_w_up, m_w_down, v_w_gate, v_w_up, v_w_down):
    weights = dict(zip(NAMES, (w_gate, w_up, w_down), strict=True))

    def take(so_far, sequence):
        h, by_y = sequence
        _, back = jax.vjp(lambda w: stack(w, h), weights)
        return jax.tree.map(lambda total, term: total + term.astype(jnp.float32), so_far, back(by_y)[0]), None

    none_yet = {name: jnp.zeros(w.shape, jnp.float32) for name, w in weights.items()}
    by_weights, _ = lax.scan(take, none_yet, (x, dy))
    gradients = [by_weights[name].astype(jnp.bfloat16).astype(jnp.float32) for name in NAMES]
    gradients = clipped(gradients, sum(jnp.sum(g * g) for g in gradients), sum(g.size for g in gradients))
    new = [
        adamw(w.astype(jnp.float32), m, v, g)
        for w, m, v, g in zip((w_gate, w_up, w_down), (m_w_gate, m_w_up, m_w_down), (v_w_gate, v_w_up, v_w_down), gradients, strict=True)
    ]
    return tuple(one[which] for which in range(3) for one in new)
```

```python
import functools
import jax
import jax.numpy as jnp
from jax import lax
from jax.experimental import pallas as pl
from jax.experimental.pallas import tpu as pltpu
from jax.sharding import PartitionSpec as P

MESH = pl.DeviceIdType.MESH
STRIDE = (16, 4, 1)
ORDERS = ((0, 1, 2), (0, 1, 2), (1, 2, 0), (1, 2, 0), (2, 0, 1), (2, 0, 1))
SIGNS = (1, -1, 1, -1, 1, -1)


def place():
    me = lax.axis_index("dp")
    return (me // 16, (me // 4) % 4, me % 4)


def neighbour(at, axis, step):
    there = [c for c in at]
    there[axis] = (at[axis] + step + 4) % 4
    return {"dp": there[0] * 16 + there[1] * 4 + there[2]}


def remote(src, dst, send, recv, to):
    return pltpu.make_async_remote_copy(src_ref=src, dst_ref=dst, send_sem=send, recv_sem=recv, device_id=to, device_id_type=MESH)


def enter(at):
    barrier = pltpu.get_barrier_semaphore()
    for axis in range(3):
        for step in range(1, 4):
            pl.semaphore_signal(barrier, inc=1, device_id=neighbour(at, axis, step), device_id_type=MESH)
    pl.semaphore_wait(barrier, 9)


def norm_exchange(at, buf, send, recv, total):
    for axis in range(3):
        buf[axis, 3] = total
        for off in range(1, 4):
            remote(buf.at[axis, 3], buf.at[axis, off - 1], send.at[axis], recv.at[axis, off - 1], neighbour(at, axis, off)).start()
        for off in range(1, 4):
            remote(buf.at[axis, 3], buf.at[axis, off - 1], send.at[axis], recv.at[axis, off - 1], neighbour(at, axis, off)).wait_recv()
            total = total + buf[axis, off - 1]
    return total


def rs_kernel(*refs):
    terms, (out, squares), scratch = refs[:6], refs[6:8], refs[8:]
    r1, r2, r3, own, f1, f2, sums, send1, send2, send3, recv1, recv2, recv3, load, send4, recv4 = scratch
    at = place()
    enter(at)

    def block(c, a, i):
        o = ORDERS[c]
        index = [slice(None)] * 3
        index[o[0]] = a
        index[o[1]] = i
        return terms[c].at[tuple(index)]

    def split(c):
        o, s = ORDERS[c], SIGNS[c]
        return o, s, at[o[0]], at[o[1]], at[o[2]]

    def first(c, step, j):
        o, s, p1, p2, p3 = split(c)
        i = (p2 - s * (1 + j) + 8) % 4
        src = block(c, (p1 - s + 4) % 4, i) if step == 0 else r1.at[c, step - 1, j]
        return remote(src, r1.at[c, step, j], send1.at[c], recv1.at[c, step, j], neighbour(at, o[0], s))

    def loading(c, step, j):
        o, s, p1, p2, p3 = split(c)
        i = (p2 - s * (1 + j) + 8) % 4
        return pltpu.make_async_copy(block(c, (p1 - s * (2 + step) + 12) % 4, i), own.at[c, step, j], load.at[c, step, j])

    def second(c, step, k):
        o, s, p1, p2, p3 = split(c)
        i = (p3 - s * (1 + k) + 8) % 4
        src = r1.at[c, 2, 0, i] if step == 0 else r2.at[c, step - 1, k]
        return remote(src, r2.at[c, step, k], send2.at[c], recv2.at[c, step, k], neighbour(at, o[1], s))

    def third(c, step):
        o, s, p1, p2, p3 = split(c)
        src = r2.at[c, 2, 0] if step == 0 else r3.at[c, step - 1]
        return remote(src, r3.at[c, step], send3.at[c], recv3.at[c, step], neighbour(at, o[2], s))

    for j in range(4):
        for c in range(6):
            first(c, 0, j).start()
    for step in range(3):
        for j in range(4):
            for c in range(6):
                loading(c, step, j).start()

    for step in range(3):
        for j in range(4):
            for c in range(6):
                first(c, step, j).wait_recv()
                loading(c, step, j).wait()
                for k in range(4):
                    both = r1[c, step, j, k].astype(jnp.float32) + own[c, step, j, k].astype(jnp.float32)
                    if step == 2 and j == 3:
                        f1[c, k] = both
                    r1[c, step, j, k] = both.astype(jnp.bfloat16)
                if step < 2:
                    first(c, step + 1, j).start()
                elif j == 0:
                    for k in range(4):
                        second(c, 0, k).start()
    for step in range(3):
        for k in range(4):
            for c in range(6):
                o, s, p1, p2, p3 = split(c)
                i = (p3 - s * (1 + k) + 8) % 4
                second(c, step, k).wait_recv()
                if step < 2:
                    both = r2[c, step, k].astype(jnp.float32) + r1[c, 2, step + 1, i].astype(jnp.float32)
                else:
                    both = r2[c, step, k].astype(jnp.float32) + f1[c, i]
                if step == 2 and k == 3:
                    f2[c] = both
                r2[c, step, k] = both.astype(jnp.bfloat16)
                if step < 2:
                    second(c, step + 1, k).start()
                elif k == 0:
                    third(c, 0).start()
    for step in range(3):
        for c in range(6):
            third(c, step).wait_recv()
            if step < 2:
                both = r3[c, step].astype(jnp.float32) + r2[c, 2, step + 1].astype(jnp.float32)
                r3[c, step] = both.astype(jnp.bfloat16)
                third(c, step + 1).start()
            else:
                out[c] = (r3[c, step].astype(jnp.float32) + f2[c]).astype(jnp.bfloat16)
    total = jnp.zeros((8, 128), jnp.float32)
    for c in range(6):
        g = out[c].astype(jnp.float32)
        total = total + jnp.sum((g * g).reshape(-1, 8, 128), axis=0)
    squares[...] = norm_exchange(at, sums, send4, recv4, total)

    for c in range(6):
        pltpu.make_async_copy(r1.at[c], r1.at[c], send1.at[c]).wait()
        pltpu.make_async_copy(r2.at[c], r2.at[c], send2.at[c]).wait()
        pltpu.make_async_copy(r3.at[c], r3.at[c], send3.at[c]).wait()
    for axis in range(3):
        pltpu.make_async_copy(sums.at[axis, pl.ds(0, 3)], sums.at[axis, pl.ds(0, 3)], send4.at[axis]).wait()


def reduce_scatter(terms):
    rows = terms[0].shape[3]
    bf16, f32 = jnp.bfloat16, jnp.float32
    dma = pltpu.SemaphoreType.DMA
    return pl.pallas_call(
        rs_kernel,
        out_shape=(jax.ShapeDtypeStruct((6, rows, 128), bf16), jax.ShapeDtypeStruct((8, 128), f32)),
        in_specs=[pl.BlockSpec(memory_space=pl.ANY)] * 6,
        out_specs=(pl.BlockSpec(memory_space=pltpu.VMEM), pl.BlockSpec(memory_space=pltpu.VMEM)),
        scratch_shapes=[
            pltpu.VMEM((6, 3, 4, 4, rows, 128), bf16),
            pltpu.VMEM((6, 3, 4, rows, 128), bf16),
            pltpu.VMEM((6, 3, rows, 128), bf16),
            pltpu.VMEM((6, 3, 4, 4, rows, 128), bf16),
            pltpu.VMEM((6, 4, rows, 128), f32),
            pltpu.VMEM((6, rows, 128), f32),
            pltpu.VMEM((3, 4, 8, 128), f32),
            dma((6,)), dma((6,)), dma((6,)),
            dma((6, 3, 4)), dma((6, 3, 4)), dma((6, 3)),
            dma((6, 3, 4)),
            dma((3,)), dma((3, 3)),
        ],
        compiler_params=pltpu.CompilerParams(collective_id=0, has_side_effects=True, vmem_limit_bytes=60 * 1024 * 1024),
        name="scatter",
    )(*terms)


def ag_order(latency=1.8):
    import heapq

    free, out, seen, count = {}, [], [], 0
    heap = []

    def send(t, c, phase, key, size):
        nonlocal count
        axis = ORDERS[2 * c][2 - phase]
        start = max(t, free.get(axis, 0.0))
        free[axis] = start + size
        count += 1
        heapq.heappush(heap, (start + size + latency, count, c, phase, key))

    def hold(t, c, phase, key):
        d1, d2, d3 = key
        if phase == 0 and d3 < 3:
            send(t, c, 0, (0, 0, d3 + 1), 1)
        if phase <= 1 and d2 < 3:
            send(t, c, 1, (0, d2 + 1, d3), 1)
        if d2 == 0 or phase == 2:
            if d1 < 3:
                send(t, c, 2, (d1 + 1, d2, d3), 1 if d3 is not None else 4)
        elif phase == 1:
            seen.append((c, d2))
            if seen.count((c, d2)) == 4:
                send(t, c, 2, (1, d2, None), 4)

    for c in range(3):
        hold(0.0, c, 0, (0, 0, 0))
    while heap:
        t, _, c, phase, key = heapq.heappop(heap)
        out.append((c, phase, key))
        hold(t, c, phase, key)
    return out, t


def ag_kernel(*refs):
    mine, outs, scratch = refs[0], refs[1:7], refs[7:]
    sends, recv1, recv2, recv3, recv4, local = scratch
    at = place()
    enter(at)

    def where(c, d1, d2, d3):
        o, s = ORDERS[c], SIGNS[c]
        index = [None] * 3
        for axis, d in zip(o, (d1, d2, d3), strict=True):
            index[axis] = slice(None) if d is None else (at[axis] - s * d + 4) % 4
        return outs[c].at[tuple(index)]

    def copy(c, phase, key, of_receiver):
        o, s = ORDERS[c], SIGNS[c]
        d1, d2, d3 = key
        back = [d1, d2, d3]
        if not of_receiver:
            back[2 - phase] -= 1
        place_there = where(c, *back)
        src = mine.at[c] if not of_receiver and tuple(back) == (0, 0, 0) else place_there
        if phase == 0:
            recv = recv1.at[c, d3 - 1]
        elif phase == 1:
            recv = recv2.at[c, d2 - 1, d3]
        elif d3 is not None:
            recv = recv3.at[c, d1 - 1, d3]
        else:
            recv = recv4.at[c, d1 - 1, d2 - 1]
        return remote(src, place_there, sends.at[c, phase], recv, neighbour(at, o[2 - phase], s))

    seen = []

    def hold(c, phase, key):
        d1, d2, d3 = key
        todo = []
        if phase == 0 and d3 < 3:
            todo.append((0, (0, 0, d3 + 1)))
        if phase <= 1 and d2 < 3:
            todo.append((1, (0, d2 + 1, d3)))
        if d2 == 0 or phase == 2:
            if d1 < 3:
                todo.append((2, (d1 + 1, d2, d3)))
        elif phase == 1:
            seen.append((c, d2))
            if seen.count((c, d2)) == 4:
                todo.append((2, (1, d2, None)))
        for phase, key in todo:
            copy(c, phase, key, False).start()

    for c in range(6):
        hold(c, 0, (0, 0, 0))
    for c in range(6):
        pltpu.make_async_copy(mine.at[c], where(c, 0, 0, 0), local.at[c]).start()
    for pair, phase, key in ag_order()[0]:
        for c in (2 * pair, 2 * pair + 1):
            copy(c, phase, key, True).wait_recv()
            hold(c, phase, key)
    for c in range(6):
        pltpu.make_async_copy(mine.at[c], where(c, 0, 0, 0), local.at[c]).wait()
        pltpu.make_async_copy(outs[c].at[0, 0, pl.ds(0, 3)], outs[c].at[0, 0, pl.ds(0, 3)], sends.at[c, 0]).wait()
        pltpu.make_async_copy(outs[c].at[0, pl.ds(0, 3)], outs[c].at[0, pl.ds(0, 3)], sends.at[c, 1]).wait()
        pltpu.make_async_copy(outs[c].at[pl.ds(0, 3)], outs[c].at[pl.ds(0, 3)], sends.at[c, 2]).wait()


def all_gather(mine):
    rows = mine.shape[1]
    dma = pltpu.SemaphoreType.DMA
    return pl.pallas_call(
        ag_kernel,
        out_shape=tuple(jax.ShapeDtypeStruct((4, 4, 4, rows, 128), jnp.bfloat16) for _ in range(6)),
        in_specs=[pl.BlockSpec(memory_space=pltpu.VMEM)],
        out_specs=tuple(pl.BlockSpec(memory_space=pl.ANY) for _ in range(6)),
        scratch_shapes=[dma((6, 3)), dma((6, 3)), dma((6, 3, 4)), dma((6, 3, 4)), dma((6, 3, 3)), dma((6,))],
        compiler_params=pltpu.CompilerParams(collective_id=1, has_side_effects=True),
        name="gather",
    )(mine)


NAMES = ("w_gate", "w_up", "w_down")
LANES = 128


def tiles_of(t, rows, columns):
    n = columns // LANES
    if t < 2:
        return [(0, rows, j * LANES, j * rows) for j in range(n)]
    return [(8 * i, 8, j * LANES, (i * n + j) * 8) for i in range(rows // 8) for j in range(n)]


def adam_kernel(count, g, total, *refs):
    ws, ms, vs, new, new_m, new_v, wide_g, wide_w = refs[0:3], refs[3:6], refs[6:9], refs[9], refs[10:13], refs[13:16], refs[16], refs[17]
    factor = jnp.minimum(1.0, 0.5 * lax.rsqrt(jnp.full((1, 1), jnp.sum(total[...])) / count + 1e-30))
    for t in range(3):
        for l in range(2):
            c = 2 * t + l
            wide_g[...] = g[c].astype(jnp.float32) * factor
            for row, rows, column, at in tiles_of(t, *ms[t].shape[1:]):
                here = (l, pl.ds(row, rows), pl.ds(column, LANES))
                grad = wide_g[pl.ds(at, rows), :]
                m = 0.9 * ms[t][here] + 0.1 * grad
                v = 0.95 * vs[t][here] + 0.05 * grad * grad
                w = ws[t][here].astype(jnp.float32)
                new_m[t][here] = m
                new_v[t][here] = v
                wide_w[pl.ds(at, rows), :] = w - 0.02 * (m * lax.rsqrt(v + 1e-8) + 0.1 * w)
            new[c] = wide_w[...].astype(jnp.bfloat16)


def adam(count, g, total, ws, ms, vs):
    vmem = pl.BlockSpec(memory_space=pltpu.VMEM)
    like = [jax.ShapeDtypeStruct(m.shape, jnp.float32) for m in ms]
    out = pl.pallas_call(
        functools.partial(adam_kernel, count),
        out_shape=(jax.ShapeDtypeStruct(g.shape, jnp.bfloat16), *like, *like),
        in_specs=[vmem] * 11,
        out_specs=(vmem,) * 7,
        scratch_shapes=[pltpu.VMEM(g.shape[1:], jnp.float32)] * 2,
        name="adam",
    )(g, total, *ws, *ms, *vs)
    return out[0], out[1:4], out[4:7]


def natural_kernel(*refs):
    blocks, outs, wide = refs[:6], refs[6:9], refs[9:]
    for t in range(3):
        for l in range(2):
            for z in range(4):
                block = blocks[2 * t + l][z].astype(jnp.float32)
                rows = outs[t].shape[1] // 4
                for row, n, column, at in tiles_of(t, rows, outs[t].shape[2]):
                    wide[t][pl.ds(z * rows + row, n), pl.ds(column, LANES)] = block[at : at + n]
            outs[t][l] = wide[t][...].astype(jnp.bfloat16)


def natural(blocks):
    blocks = [b.reshape(64, *b.shape[3:]) for b in blocks]
    shapes = ((2, 896, 2560), (2, 896, 2560), (2, 2560, 896))
    return pl.pallas_call(
        natural_kernel,
        grid=(16,),
        out_shape=tuple(jax.ShapeDtypeStruct(s, jnp.bfloat16) for s in shapes),
        in_specs=[pl.BlockSpec((4, 280, 128), lambda i: (i, 0, 0))] * 6,
        out_specs=tuple(pl.BlockSpec((2, s[1] // 16, s[2]), lambda i: (0, i, 0)) for s in shapes),
        scratch_shapes=[pltpu.VMEM((s[1] // 16, s[2]), jnp.float32) for s in shapes],
        name="natural",
    )(*blocks)


def matmul(a, w):
    return jnp.dot(a, w, preferred_element_type=jnp.float32).astype(jnp.bfloat16)


def normed(h):
    wide = h.astype(jnp.float32)
    scale = lax.rsqrt(jnp.mean(wide**2, -1, keepdims=True) + 1e-6)
    return (wide * scale).astype(jnp.bfloat16)


def layer(h, w):
    a = normed(h)
    gate = jnp.dot(a, w["w_gate"], preferred_element_type=jnp.float32)
    up = jnp.dot(a, w["w_up"], preferred_element_type=jnp.float32)
    return h + matmul((jax.nn.silu(gate) * up).astype(jnp.bfloat16), w["w_down"])


def stack(weights, h):
    for number in range(2):
        h = layer(h, {name: w[number] for name, w in weights.items()})
    return h


def in_blocks(t, g):
    if t < 2:
        g = g.reshape(64, 14, 20, LANES).transpose(0, 2, 1, 3)
    else:
        g = g.reshape(64, 5, 8, 7, LANES).transpose(0, 1, 3, 2, 4)
    return g.reshape(4, 4, 4, 280, LANES)


def solution(mesh):
    rep, dp = mesh.axis_names

    def step(x, dy, *arrays):
        weights, m, v = (arrays[i : i + 3] for i in (0, 3, 6))
        _, back = jax.vjp(lambda w: stack(w, x[0]), dict(zip(NAMES, weights, strict=True)))
        by_weights = back(dy[0])[0]
        terms = [in_blocks(t, by_weights[NAMES[t]][l]) for t in range(3) for l in range(2)]
        g, total = reduce_scatter(terms)
        me = lax.axis_index(dp)
        mine = [lax.dynamic_slice_in_dim(w, me * b.shape[1], b.shape[1], 1) for w, b in zip(weights, m, strict=True)]
        new, new_m, new_v = adam(sum(w.size for w in weights), g, total, mine, m, v)
        return (*natural(all_gather(new)), *new_m, *new_v)

    whole, rows, sequences = P(None, None, None), P(None, dp, None), P((rep, dp), None, None)
    return jax.shard_map(
        step,
        mesh=mesh,
        in_specs=(sequences, sequences, *[whole] * 3, *[rows] * 6),
        out_specs=(*[P(rep, None, None)] * 3, *[P(rep, dp, None)] * 6),
        check_vma=False,
    )
```

```python
import functools
import jax
import jax.numpy as jnp
from jax import lax
from jax.experimental import pallas as pl
from jax.experimental.pallas import tpu as pltpu
from jax.sharding import PartitionSpec as P

MESH = pl.DeviceIdType.MESH
STRIDE = (16, 4, 1)
ORDERS = ((0, 1, 2), (0, 1, 2), (1, 2, 0), (1, 2, 0), (2, 0, 1), (2, 0, 1))
SIGNS = (1, -1, 1, -1, 1, -1)
TAKEN = (3, 0, 4, 1, 5, 2)


def place():
    me = lax.axis_index("dp")
    return (me // 16, (me // 4) % 4, me % 4)


def neighbour(at, axis, step):
    there = [c for c in at]
    there[axis] = (at[axis] + step + 4) % 4
    return {"dp": there[0] * 16 + there[1] * 4 + there[2]}


def remote(src, dst, send, recv, to):
    return pltpu.make_async_remote_copy(src_ref=src, dst_ref=dst, send_sem=send, recv_sem=recv, device_id=to, device_id_type=MESH)


def enter(at):
    barrier = pltpu.get_barrier_semaphore()
    for axis in range(3):
        for step in range(1, 4):
            pl.semaphore_signal(barrier, inc=1, device_id=neighbour(at, axis, step), device_id_type=MESH)
    pl.semaphore_wait(barrier, 9)


def norm_exchange(at, buf, send, recv, total):
    for axis in range(3):
        buf[axis, 3] = total
        for off in range(1, 4):
            remote(buf.at[axis, 3], buf.at[axis, off - 1], send.at[axis], recv.at[axis, off - 1], neighbour(at, axis, off)).start()
        for off in range(1, 4):
            remote(buf.at[axis, 3], buf.at[axis, off - 1], send.at[axis], recv.at[axis, off - 1], neighbour(at, axis, off)).wait_recv()
            total = total + buf[axis, off - 1]
    return total


def rs_kernel(*refs):
    terms, (out, squares), scratch = [refs[0].at[m] for m in TAKEN], refs[1:3], refs[3:]
    r1, r2, r3, own, f1, f2, sums, send1, send2, send3, recv1, recv2, recv3, load, send4, recv4 = scratch
    at = place()
    enter(at)

    def block(c, a, i):
        o = ORDERS[c]
        index = [slice(None)] * 3
        index[o[0]] = a
        index[o[1]] = i
        return terms[c].at[tuple(index)]

    def split(c):
        o, s = ORDERS[c], SIGNS[c]
        return o, s, at[o[0]], at[o[1]], at[o[2]]

    def first(c, step, j):
        o, s, p1, p2, p3 = split(c)
        i = (p2 - s * (1 + j) + 8) % 4
        src = block(c, (p1 - s + 4) % 4, i) if step == 0 else r1.at[c, step - 1, j]
        return remote(src, r1.at[c, step, j], send1.at[c], recv1.at[c, step, j], neighbour(at, o[0], s))

    def loading(c, step, j):
        o, s, p1, p2, p3 = split(c)
        i = (p2 - s * (1 + j) + 8) % 4
        return pltpu.make_async_copy(block(c, (p1 - s * (2 + step) + 12) % 4, i), own.at[c, step, j], load.at[c, step, j])

    def second(c, step, k):
        o, s, p1, p2, p3 = split(c)
        i = (p3 - s * (1 + k) + 8) % 4
        src = r1.at[c, 2, 0, i] if step == 0 else r2.at[c, step - 1, k]
        return remote(src, r2.at[c, step, k], send2.at[c], recv2.at[c, step, k], neighbour(at, o[1], s))

    def third(c, step):
        o, s, p1, p2, p3 = split(c)
        src = r2.at[c, 2, 0] if step == 0 else r3.at[c, step - 1]
        return remote(src, r3.at[c, step], send3.at[c], recv3.at[c, step], neighbour(at, o[2], s))

    for j in range(4):
        for c in range(6):
            first(c, 0, j).start()
    for step in range(3):
        for j in range(4):
            for c in range(6):
                loading(c, step, j).start()

    for step in range(3):
        for j in range(4):
            for c in range(6):
                first(c, step, j).wait_recv()
                loading(c, step, j).wait()
                for k in range(4):
                    both = r1[c, step, j, k].astype(jnp.float32) + own[c, step, j, k].astype(jnp.float32)
                    if step == 2 and j == 3:
                        f1[c, k] = both
                    r1[c, step, j, k] = both.astype(jnp.bfloat16)
                if step < 2:
                    first(c, step + 1, j).start()
                elif j == 0:
                    for k in range(4):
                        second(c, 0, k).start()
    for step in range(3):
        for k in range(4):
            for c in range(6):
                o, s, p1, p2, p3 = split(c)
                i = (p3 - s * (1 + k) + 8) % 4
                second(c, step, k).wait_recv()
                if step < 2:
                    both = r2[c, step, k].astype(jnp.float32) + r1[c, 2, step + 1, i].astype(jnp.float32)
                else:
                    both = r2[c, step, k].astype(jnp.float32) + f1[c, i]
                if step == 2 and k == 3:
                    f2[c] = both
                r2[c, step, k] = both.astype(jnp.bfloat16)
                if step < 2:
                    second(c, step + 1, k).start()
                elif k == 0:
                    third(c, 0).start()
    for step in range(3):
        for c in range(6):
            third(c, step).wait_recv()
            if step < 2:
                both = r3[c, step].astype(jnp.float32) + r2[c, 2, step + 1].astype(jnp.float32)
                r3[c, step] = both.astype(jnp.bfloat16)
                third(c, step + 1).start()
            else:
                out[c] = (r3[c, step].astype(jnp.float32) + f2[c]).astype(jnp.bfloat16)
    total = jnp.zeros((8, 128), jnp.float32)
    for c in range(6):
        g = out[c].astype(jnp.float32)
        total = total + jnp.sum((g * g).reshape(-1, 8, 128), axis=0)
    squares[...] = norm_exchange(at, sums, send4, recv4, total)

    for c in range(6):
        pltpu.make_async_copy(r1.at[c], r1.at[c], send1.at[c]).wait()
        pltpu.make_async_copy(r2.at[c], r2.at[c], send2.at[c]).wait()
        pltpu.make_async_copy(r3.at[c], r3.at[c], send3.at[c]).wait()
    for axis in range(3):
        pltpu.make_async_copy(sums.at[axis, pl.ds(0, 3)], sums.at[axis, pl.ds(0, 3)], send4.at[axis]).wait()


def reduce_scatter(terms):
    rows = terms.shape[4]
    bf16, f32 = jnp.bfloat16, jnp.float32
    dma = pltpu.SemaphoreType.DMA
    return pl.pallas_call(
        rs_kernel,
        out_shape=(jax.ShapeDtypeStruct((6, rows, 128), bf16), jax.ShapeDtypeStruct((8, 128), f32)),
        in_specs=[pl.BlockSpec(memory_space=pl.ANY)],
        out_specs=(pl.BlockSpec(memory_space=pltpu.VMEM), pl.BlockSpec(memory_space=pltpu.VMEM)),
        scratch_shapes=[
            pltpu.VMEM((6, 3, 4, 4, rows, 128), bf16),
            pltpu.VMEM((6, 3, 4, rows, 128), bf16),
            pltpu.VMEM((6, 3, rows, 128), bf16),
            pltpu.VMEM((6, 3, 4, 4, rows, 128), bf16),
            pltpu.VMEM((6, 4, rows, 128), f32),
            pltpu.VMEM((6, rows, 128), f32),
            pltpu.VMEM((3, 4, 8, 128), f32),
            dma((6,)), dma((6,)), dma((6,)),
            dma((6, 3, 4)), dma((6, 3, 4)), dma((6, 3)),
            dma((6, 3, 4)),
            dma((3,)), dma((3, 3)),
        ],
        compiler_params=pltpu.CompilerParams(collective_id=0, has_side_effects=True, vmem_limit_bytes=60 * 1024 * 1024),
        name="scatter",
    )(terms)


def ag_order(latency=1.8):
    import heapq

    free, out, seen, count = {}, [], [], 0
    heap = []

    def send(t, c, phase, key, size):
        nonlocal count
        axis = ORDERS[2 * c][2 - phase]
        start = max(t, free.get(axis, 0.0))
        free[axis] = start + size
        count += 1
        heapq.heappush(heap, (start + size + latency, count, c, phase, key))

    def hold(t, c, phase, key):
        d1, d2, d3 = key
        if phase == 0 and d3 < 3:
            send(t, c, 0, (0, 0, d3 + 1), 1)
        if phase <= 1 and d2 < 3:
            send(t, c, 1, (0, d2 + 1, d3), 1)
        if d2 == 0 or phase == 2:
            if d1 < 3:
                send(t, c, 2, (d1 + 1, d2, d3), 1 if d3 is not None else 4)
        elif phase == 1:
            seen.append((c, d2))
            if seen.count((c, d2)) == 4:
                send(t, c, 2, (1, d2, None), 4)

    for c in range(3):
        hold(0.0, c, 0, (0, 0, 0))
    while heap:
        t, _, c, phase, key = heapq.heappop(heap)
        out.append((c, phase, key))
        hold(t, c, phase, key)
    return out, t


def ag_kernel(*refs):
    mine, outs, scratch = refs[0], refs[1:7], refs[7:]
    sends, recv1, recv2, recv3, recv4, local = scratch
    at = place()
    enter(at)

    def where(c, d1, d2, d3):
        o, s = ORDERS[c], SIGNS[c]
        index = [None] * 3
        for axis, d in zip(o, (d1, d2, d3), strict=True):
            index[axis] = slice(None) if d is None else (at[axis] - s * d + 4) % 4
        return outs[c].at[tuple(index)]

    def copy(c, phase, key, of_receiver):
        o, s = ORDERS[c], SIGNS[c]
        d1, d2, d3 = key
        back = [d1, d2, d3]
        if not of_receiver:
            back[2 - phase] -= 1
        place_there = where(c, *back)
        src = mine.at[c] if not of_receiver and tuple(back) == (0, 0, 0) else place_there
        if phase == 0:
            recv = recv1.at[c, d3 - 1]
        elif phase == 1:
            recv = recv2.at[c, d2 - 1, d3]
        elif d3 is not None:
            recv = recv3.at[c, d1 - 1, d3]
        else:
            recv = recv4.at[c, d1 - 1, d2 - 1]
        return remote(src, place_there, sends.at[c, phase], recv, neighbour(at, o[2 - phase], s))

    seen = []

    def hold(c, phase, key):
        d1, d2, d3 = key
        todo = []
        if phase == 0 and d3 < 3:
            todo.append((0, (0, 0, d3 + 1)))
        if phase <= 1 and d2 < 3:
            todo.append((1, (0, d2 + 1, d3)))
        if d2 == 0 or phase == 2:
            if d1 < 3:
                todo.append((2, (d1 + 1, d2, d3)))
        elif phase == 1:
            seen.append((c, d2))
            if seen.count((c, d2)) == 4:
                todo.append((2, (1, d2, None)))
        for phase, key in todo:
            copy(c, phase, key, False).start()

    for c in range(6):
        hold(c, 0, (0, 0, 0))
    for c in range(6):
        pltpu.make_async_copy(mine.at[c], where(c, 0, 0, 0), local.at[c]).start()
    for pair, phase, key in ag_order()[0]:
        for c in (2 * pair, 2 * pair + 1):
            copy(c, phase, key, True).wait_recv()
            hold(c, phase, key)
    for c in range(6):
        pltpu.make_async_copy(mine.at[c], where(c, 0, 0, 0), local.at[c]).wait()
        pltpu.make_async_copy(outs[c].at[0, 0, pl.ds(0, 3)], outs[c].at[0, 0, pl.ds(0, 3)], sends.at[c, 0]).wait()
        pltpu.make_async_copy(outs[c].at[0, pl.ds(0, 3)], outs[c].at[0, pl.ds(0, 3)], sends.at[c, 1]).wait()
        pltpu.make_async_copy(outs[c].at[pl.ds(0, 3)], outs[c].at[pl.ds(0, 3)], sends.at[c, 2]).wait()


def all_gather(mine):
    rows = mine.shape[1]
    dma = pltpu.SemaphoreType.DMA
    return pl.pallas_call(
        ag_kernel,
        out_shape=tuple(jax.ShapeDtypeStruct((4, 4, 4, rows, 128), jnp.bfloat16) for _ in range(6)),
        in_specs=[pl.BlockSpec(memory_space=pltpu.VMEM)],
        out_specs=tuple(pl.BlockSpec(memory_space=pl.ANY) for _ in range(6)),
        scratch_shapes=[dma((6, 3)), dma((6, 3)), dma((6, 3, 4)), dma((6, 3, 4)), dma((6, 3, 3)), dma((6,))],
        compiler_params=pltpu.CompilerParams(collective_id=1, has_side_effects=True),
        name="gather",
    )(mine)


NAMES = ("w_gate", "w_up", "w_down")
LANES = 128


def tiles_of(t, rows, columns):
    n = columns // LANES
    if t < 2:
        return [(0, rows, j * LANES, j * rows) for j in range(n)]
    return [(8 * i, 8, j * LANES, (i * n + j) * 8) for i in range(rows // 8) for j in range(n)]


def adam_kernel(count, g, total, *refs):
    ws, ms, vs, new, new_m, new_v, wide_g, wide_w = refs[0:3], refs[3:6], refs[6:9], refs[9], refs[10:13], refs[13:16], refs[16], refs[17]
    factor = jnp.minimum(1.0, 0.5 * lax.rsqrt(jnp.full((1, 1), jnp.sum(total[...])) / count + 1e-30))
    for t in range(3):
        for l in range(2):
            c = 2 * t + l
            wide_g[...] = g[c].astype(jnp.float32) * factor
            for row, rows, column, at in tiles_of(t, *ms[t].shape[1:]):
                here = (l, pl.ds(row, rows), pl.ds(column, LANES))
                grad = wide_g[pl.ds(at, rows), :]
                m = 0.9 * ms[t][here] + 0.1 * grad
                v = 0.95 * vs[t][here] + 0.05 * grad * grad
                w = ws[t][here].astype(jnp.float32)
                new_m[t][here] = m
                new_v[t][here] = v
                wide_w[pl.ds(at, rows), :] = w - 0.02 * (m * lax.rsqrt(v + 1e-8) + 0.1 * w)
            new[c] = wide_w[...].astype(jnp.bfloat16)


def adam(count, g, total, ws, ms, vs):
    vmem = pl.BlockSpec(memory_space=pltpu.VMEM)
    like = [jax.ShapeDtypeStruct(m.shape, jnp.float32) for m in ms]
    out = pl.pallas_call(
        functools.partial(adam_kernel, count),
        out_shape=(jax.ShapeDtypeStruct(g.shape, jnp.bfloat16), *like, *like),
        in_specs=[vmem] * 11,
        out_specs=(vmem,) * 7,
        scratch_shapes=[pltpu.VMEM(g.shape[1:], jnp.float32)] * 2,
        name="adam",
    )(g, total, *ws, *ms, *vs)
    return out[0], out[1:4], out[4:7]


def natural_kernel(*refs):
    blocks, outs, wide = refs[:6], refs[6:9], refs[9:]
    for t in range(3):
        for l in range(2):
            for z in range(4):
                block = blocks[2 * t + l][z].astype(jnp.float32)
                rows = outs[t].shape[1] // 4
                for row, n, column, at in tiles_of(t, rows, outs[t].shape[2]):
                    wide[t][pl.ds(z * rows + row, n), pl.ds(column, LANES)] = block[at : at + n]
            outs[t][l] = wide[t][...].astype(jnp.bfloat16)


def natural(blocks):
    blocks = [b.reshape(64, *b.shape[3:]) for b in blocks]
    shapes = ((2, 896, 2560), (2, 896, 2560), (2, 2560, 896))
    return pl.pallas_call(
        natural_kernel,
        grid=(16,),
        out_shape=tuple(jax.ShapeDtypeStruct(s, jnp.bfloat16) for s in shapes),
        in_specs=[pl.BlockSpec((4, 280, 128), lambda i: (i, 0, 0))] * 6,
        out_specs=tuple(pl.BlockSpec((2, s[1] // 16, s[2]), lambda i: (0, i, 0)) for s in shapes),
        scratch_shapes=[pltpu.VMEM((s[1] // 16, s[2]), jnp.float32) for s in shapes],
        name="natural",
    )(*blocks)


D, FF, TOKENS = 896, 2560, 2048
ROWS, CHUNK, TILE = 256, 512, 512
NT = (((1,), (1,)), ((), ()))


def dot(a, b):
    return jnp.dot(a, b, preferred_element_type=jnp.float32)


def dot_t(a, b):
    return lax.dot_general(a, b, NT, preferred_element_type=jnp.float32)


def scale_of(wide):
    return lax.rsqrt(jnp.mean(wide * wide, -1, keepdims=True) + 1e-6)


def rows_kernel(x, dy, *refs):
    hbm, left, right, weights, (g0, u0, sems) = refs[:3], refs[3], refs[4], refs[5:11], refs[11:]
    wg0, wu0, wd0, wg1, wu1, wd1 = weights
    first = pl.program_id(0) == 0

    def fetch(k):
        return pltpu.make_async_copy(hbm[k % 3].at[k // 3], weights[k], sems.at[k])

    @pl.when(first)
    def _():
        for k in range(6):
            fetch(k).start()

    def ready(*ks):
        @pl.when(first)
        def _():
            for k in ks:
                fetch(k).wait()

    bf16, f32 = jnp.bfloat16, jnp.float32
    a = (x[...].astype(f32) * scale_of(x[...].astype(f32))).astype(bf16)
    left[2] = a.T
    left[1] = dy[...].T
    ready(0, 1)
    for j in range(FF // CHUNK):
        ch = pl.ds(j * CHUNK, CHUNK)
        gate, up = dot(a, wg0[:, ch]), dot(a, wu0[:, ch])
        g0[:, ch], u0[:, ch] = gate, up
        right[5, :, ch] = (gate * jax.nn.sigmoid(gate) * up).astype(bf16)
    ready(2)
    h = x[...] + dot(right[5], wd0[...]).astype(bf16)
    wide = h.astype(f32)
    scale = scale_of(wide)
    a = (wide * scale).astype(bf16)
    left[0] = a.T
    ready(3, 4, 5)
    for j in range(FF // CHUNK):
        ch = pl.ds(j * CHUNK, CHUNK)
        gate, up = dot(a, wg1[:, ch]), dot(a, wu1[:, ch])
        dz = dot_t(dy[...], wd1[ch, :]).astype(bf16).astype(f32)
        s = jax.nn.sigmoid(gate)
        silu = gate * s
        right[2, :, ch] = (silu * up).astype(bf16)
        right[1, :, ch] = (dz * silu).astype(bf16)
        right[0, :, ch] = (dz * up * (s * (1 + gate * (1 - s)))).astype(bf16)
    da = dot_t(right[0], wg1[...]).astype(bf16) + dot_t(right[1], wu1[...]).astype(bf16)
    da = da.astype(f32)
    dwide = scale * (da - wide * (scale * scale * jnp.mean(da * wide, -1, keepdims=True)))
    dh = dy[...] + dwide.astype(bf16)
    left[3] = dh.T
    for j in range(FF // CHUNK):
        ch = pl.ds(j * CHUNK, CHUNK)
        dz = dot_t(dh, wd0[ch, :]).astype(bf16).astype(f32)
        gate, up = g0[:, ch], u0[:, ch]
        s = jax.nn.sigmoid(gate)
        right[4, :, ch] = (dz * (gate * s)).astype(bf16)
        right[3, :, ch] = (dz * up * (s * (1 + gate * (1 - s)))).astype(bf16)


def by_rows(x, dy, weights):
    bf16 = jnp.bfloat16
    state = pl.BlockSpec((ROWS, D), lambda i: (i, 0))
    return pl.pallas_call(
        rows_kernel,
        grid=(TOKENS // ROWS,),
        out_shape=(jax.ShapeDtypeStruct((4, D, TOKENS), bf16), jax.ShapeDtypeStruct((6, TOKENS, FF), bf16)),
        in_specs=[state, state] + [pl.BlockSpec(memory_space=pl.ANY)] * 3,
        out_specs=(pl.BlockSpec((4, D, ROWS), lambda i: (0, 0, i)), pl.BlockSpec((6, ROWS, FF), lambda i: (0, i, 0))),
        scratch_shapes=[*[pltpu.VMEM(w.shape[1:], bf16) for w in weights * 2], pltpu.VMEM((ROWS, FF), jnp.float32), pltpu.VMEM((ROWS, FF), jnp.float32), pltpu.SemaphoreType.DMA((6,))],
        compiler_params=pltpu.CompilerParams(vmem_limit_bytes=62 * 1024 * 1024),
        name="rows",
    )(x, dy, *weights)


def gate_block(acc, stage, wide):
    def group(i, _):
        rows = pl.ds(pl.multiple_of(i * 56, 8), 56)
        for c in range(4):
            piece = acc[rows, pl.ds(c * LANES, LANES)]
            for z in range(4):
                wide[z, pl.ds(14 * c, 14), :] = piece[14 * z : 14 * z + 14]
        for z in range(4):
            stage[4 * i + z] = wide[z].astype(jnp.bfloat16)
        return 0

    lax.fori_loop(0, 16, group, 0)


def down_block(acc, stage, turned):
    turned[...] = acc[...].T

    def group(i, _):
        rows = turned[pl.ds(pl.multiple_of(i * 8, 8), 8), :]
        stage[i] = jnp.concatenate([rows[:, c * LANES : (c + 1) * LANES] for c in range(7)], 0).astype(jnp.bfloat16)
        return 0

    lax.fori_loop(0, 64, group, 0)


def gradients_kernel(left, right, out, acc, stage, wide, turned, sem):
    m, h = pl.program_id(0), pl.program_id(1)
    acc[...] = dot(left[...], right[...])

    whole = out.at[m, :, pl.ds(pl.multiple_of(56 * h, 8), 56)]

    @pl.when(m + h > 0)
    def _():
        pltpu.make_async_copy(stage, whole, sem).wait()

    @pl.when(m % 3 < 2)
    def _():
        gate_block(acc, stage, wide)
        pltpu.make_async_copy(stage, whole, sem).start()

    @pl.when(m % 3 == 2)
    def _():
        down_block(acc, stage, turned)

        def put(k, _):
            i = 64 * h + k
            pltpu.make_async_copy(stage.at[k], out.at[m, i // 5, pl.ds(pl.multiple_of(i % 5 * 56, 8), 56)], sem).start()
            return 0

        lax.fori_loop(0, 64, put, 0)

    @pl.when(m + h == 9)
    def _():
        pltpu.make_async_copy(stage, whole, sem).wait()


def gradients(left, right):
    bf16, f32 = jnp.bfloat16, jnp.float32
    return pl.pallas_call(
        gradients_kernel,
        grid=(6, FF // TILE),
        out_shape=jax.ShapeDtypeStruct((6, 64, 280, LANES), bf16),
        in_specs=[
            pl.BlockSpec((None, D, TOKENS), lambda m, h: (m // 3 * 2 + m % 3 // 2, 0, 0)),
            pl.BlockSpec((None, TOKENS, TILE), lambda m, h: (m, 0, h)),
        ],
        out_specs=pl.BlockSpec(memory_space=pl.ANY),
        scratch_shapes=[
            pltpu.VMEM((D, TILE), f32),
            pltpu.VMEM((64, 56, LANES), bf16),
            pltpu.VMEM((4, 56, LANES), f32),
            pltpu.VMEM((TILE, D), f32),
            pltpu.SemaphoreType.DMA,
        ],
        compiler_params=pltpu.CompilerParams(vmem_limit_bytes=62 * 1024 * 1024),
        name="gradients",
    )(left, right)


def solution(mesh):
    rep, dp = mesh.axis_names

    def step(x, dy, *arrays):
        weights, m, v = (arrays[i : i + 3] for i in (0, 3, 6))
        left, right = by_rows(x[0], dy[0], weights)
        g, total = reduce_scatter(gradients(left, right).reshape(6, 4, 4, 4, 280, LANES))
        me = lax.axis_index(dp)
        mine = [lax.dynamic_slice_in_dim(w, me * b.shape[1], b.shape[1], 1) for w, b in zip(weights, m, strict=True)]
        new, new_m, new_v = adam(sum(w.size for w in weights), g, total, mine, m, v)
        return (*natural(all_gather(new)), *new_m, *new_v)

    whole, rows, sequences = P(None, None, None), P(None, dp, None), P((rep, dp), None, None)
    return jax.shard_map(
        step,
        mesh=mesh,
        in_specs=(sequences, sequences, *[whole] * 3, *[rows] * 6),
        out_specs=(*[P(rep, None, None)] * 3, *[P(rep, dp, None)] * 6),
        check_vma=False,
    )
```

```python
import functools
import jax
import jax.numpy as jnp
from jax import lax
from jax.experimental import pallas as pl
from jax.experimental.pallas import tpu as pltpu
from jax.sharding import PartitionSpec as P

MESH = pl.DeviceIdType.MESH
WAYS, AXES, SIDE = 6, 3, 4
STEPS = SIDE - 1
MATRICES, LAYERS, DEVICES, PLANE = 6, 2, 64, 16
LANES, SUBLANES, BLOCK = 128, 8, 280
BF16, F32 = jnp.bfloat16, jnp.float32
HBM, VMEM = pl.BlockSpec(memory_space=pl.ANY), pl.BlockSpec(memory_space=pltpu.VMEM)
DMA = pltpu.SemaphoreType.DMA
MOST_VMEM = 62 * 1024 * 1024
ORDERS = tuple(tuple((way // 2 + i) % AXES for i in range(AXES)) for way in range(WAYS))
SIGNS = (1, -1) * AXES
TAKEN = (3, 0, 4, 1, 5, 2)


def place():
    me = lax.axis_index("dp")
    return (me // PLANE, me // SIDE % SIDE, me % SIDE)


def wrap(i):
    return (i + 3 * SIDE) % SIDE


def neighbour(at, axis, step):
    there = [c for c in at]
    there[axis] = wrap(at[axis] + step)
    return {"dp": (there[0] * SIDE + there[1]) * SIDE + there[2]}


def remote(src, dst, send, recv, to):
    return pltpu.make_async_remote_copy(src_ref=src, dst_ref=dst, send_sem=send, recv_sem=recv, device_id=to, device_id_type=MESH)


def enter(at):
    barrier = pltpu.get_barrier_semaphore()
    for axis in range(AXES):
        for step in range(STEPS):
            pl.semaphore_signal(barrier, inc=1, device_id=neighbour(at, axis, step + 1), device_id_type=MESH)
    pl.semaphore_wait(barrier, AXES * STEPS)


def norm_exchange(at, buf, send, recv, total):
    for axis in range(AXES):
        buf[axis, STEPS] = total
        copies = [
            remote(buf.at[axis, STEPS], buf.at[axis, k], send.at[axis], recv.at[axis, k], neighbour(at, axis, k + 1)) for k in range(STEPS)
        ]
        for copy in copies:
            copy.start()
        for k, copy in enumerate(copies):
            copy.wait_recv()
            total = total + buf[axis, k]
    return total


def passed_on(seen, c, phase, key):
    d1, d2, d3 = key
    if phase == 0 and d3 < STEPS:
        yield 0, (0, 0, d3 + 1)
    if phase < 2 and d2 < STEPS:
        yield 1, (0, d2 + 1, d3)
    if phase == 1 and d2 > 0:
        seen.append((c, d2))
        if seen.count((c, d2)) < SIDE:
            return
        d3 = None
    if d1 < STEPS:
        yield 2, (d1 + 1, d2, d3)


def ag_order(latency=1.8):
    import heapq

    free, out, seen, heap = {}, [], [], []

    def hold(t, c, phase, key):
        for phase, key in passed_on(seen, c, phase, key):
            link = ORDERS[c][2 - phase]
            size = SIDE if key[2] is None else 1
            free[link] = max(t, free.get(link, 0)) + size
            heapq.heappush(heap, (free[link] + latency, len(out) * WAYS + len(heap), c, phase, key))

    for c in range(0, WAYS, 2):
        hold(0, c, 0, (0, 0, 0))
    while heap:
        t, _, *arrival = heapq.heappop(heap)
        out.append(arrival)
        hold(t, *arrival)
    return out


def ag_kernel(*refs):
    mine, outs, (sends, recv1, recv2, recv3, recv4, local) = refs[0], refs[1 : 1 + WAYS], refs[1 + WAYS :]
    at = place()
    enter(at)

    def where(c, key):
        index = [None] * AXES
        for axis, d in zip(ORDERS[c], key, strict=True):
            index[axis] = slice(None) if d is None else wrap(at[axis] - SIGNS[c] * d)
        return outs[c].at[tuple(index)]

    def copy(c, phase, key, of_receiver):
        d1, d2, d3 = key
        back = list(key)
        if not of_receiver:
            back[2 - phase] -= 1
        there = where(c, back)
        src = mine.at[c] if not of_receiver and not any(back) and d3 is not None else there
        if phase == 0:
            recv = recv1.at[c, d3]
        elif phase == 1:
            recv = recv2.at[c, d2, d3]
        elif d3 is not None:
            recv = recv3.at[c, d1, d3]
        else:
            recv = recv4.at[c, d1, d2]
        return remote(src, there, sends.at[c, phase], recv, neighbour(at, ORDERS[c][2 - phase], SIGNS[c]))

    seen = []

    def hold(*held):
        for phase, key in passed_on(seen, *held):
            copy(held[0], phase, key, False).start()

    own = [pltpu.make_async_copy(mine.at[c], where(c, (0, 0, 0)), local.at[c]) for c in range(WAYS)]
    for c in range(WAYS):
        hold(c, 0, (0, 0, 0))
    for copied in own:
        copied.start()
    for even, phase, key in ag_order():
        for c in (even, even + 1):
            copy(c, phase, key, True).wait_recv()
            hold(c, phase, key)
    for c in range(WAYS):
        own[c].wait()
        sent = outs[c].at[pl.ds(0, STEPS)]
        for phase in (2, 1, 0):
            pltpu.make_async_copy(sent, sent, sends.at[c, phase]).wait()
            sent = outs[c].at[(0,) * (AXES - phase) + (pl.ds(0, STEPS),)]


def all_gather(mine):
    return pl.pallas_call(
        ag_kernel,
        out_shape=tuple(jax.ShapeDtypeStruct((SIDE, SIDE, SIDE, *mine.shape[1:]), BF16) for _ in range(WAYS)),
        in_specs=[VMEM],
        out_specs=(HBM,) * WAYS,
        scratch_shapes=[DMA((WAYS, AXES)), DMA((WAYS, SIDE)), *[DMA((WAYS, SIDE, SIDE))] * 3, DMA((WAYS,))],
        compiler_params=pltpu.CompilerParams(collective_id=1, has_side_effects=True),
        name="gather",
    )(mine)


def tiles_of(t, rows, columns):
    n = columns // LANES
    if t < 2:
        return [(0, rows, j * LANES, j * rows) for j in range(n)]
    return [(8 * i, 8, j * LANES, (i * n + j) * 8) for i in range(rows // 8) for j in range(n)]


def adam_kernel(count, g, total, *refs):
    ws, ms, vs, new, new_m, new_v, wide_g, wide_w = refs[0:3], refs[3:6], refs[6:9], refs[9], refs[10:13], refs[13:16], refs[16], refs[17]
    factor = jnp.minimum(1.0, 0.5 * lax.rsqrt(jnp.full((1, 1), jnp.sum(total[...])) / count + 1e-30))
    for t in range(3):
        for l in range(2):
            c = 2 * t + l
            wide_g[...] = g[TAKEN[c]].astype(F32) * factor
            for row, rows, column, at in tiles_of(t, *ms[t].shape[1:]):
                here = (l, pl.ds(row, rows), pl.ds(column, LANES))
                grad = wide_g[pl.ds(at, rows), :]
                m = 0.9 * ms[t][here] + 0.1 * grad
                v = 0.95 * vs[t][here] + 0.05 * grad * grad
                w = ws[t][here].astype(F32)
                new_m[t][here] = m
                new_v[t][here] = v
                wide_w[pl.ds(at, rows), :] = w - 0.02 * (m * lax.rsqrt(v + 1e-8) + 0.1 * w)
            new[c] = wide_w[...].astype(BF16)


def adam(count, g, total, ws, ms, vs):
    like = [jax.ShapeDtypeStruct(m.shape, F32) for m in ms]
    out = pl.pallas_call(
        functools.partial(adam_kernel, count),
        out_shape=(jax.ShapeDtypeStruct(g.shape, BF16), *like, *like),
        in_specs=[VMEM] * 11,
        out_specs=(VMEM,) * 7,
        scratch_shapes=[pltpu.VMEM(g.shape[1:], F32)] * 2,
        name="adam",
    )(g, total, *ws, *ms, *vs)
    return out[0], out[1:4], out[4:7]


def natural_kernel(*refs):
    blocks, outs, wide = refs[:6], refs[6:9], refs[9:]
    for t in range(3):
        for l in range(2):
            for z in range(4):
                block = blocks[2 * t + l][z].astype(F32)
                rows = outs[t].shape[1] // 4
                for row, n, column, at in tiles_of(t, rows, outs[t].shape[2]):
                    wide[t][pl.ds(z * rows + row, n), pl.ds(column, LANES)] = block[at : at + n]
            outs[t][l] = wide[t][...].astype(BF16)


def natural(blocks):
    blocks = [b.reshape(64, *b.shape[3:]) for b in blocks]
    shapes = ((2, 896, 2560), (2, 896, 2560), (2, 2560, 896))
    return pl.pallas_call(
        natural_kernel,
        grid=(16,),
        out_shape=tuple(jax.ShapeDtypeStruct(s, BF16) for s in shapes),
        in_specs=[pl.BlockSpec((4, 280, 128), lambda i: (i, 0, 0))] * 6,
        out_specs=tuple(pl.BlockSpec((2, s[1] // 16, s[2]), lambda i: (0, i, 0)) for s in shapes),
        scratch_shapes=[pltpu.VMEM((s[1] // 16, s[2]), F32) for s in shapes],
        name="natural",
    )(*blocks)


D, FF, TOKENS = 896, 2560, 2048
ROWS, CHUNK, TILE = 256, 512, 512
TILES, PIECE, PLANE_ROWS = FF // TILE, BLOCK * TILE // FF, FF // SIDE
NT = (((1,), (1,)), ((), ()))


def dot(a, b):
    return jnp.dot(a, b, preferred_element_type=F32)


def dot_t(a, b):
    return lax.dot_general(a, b, NT, preferred_element_type=F32)


def scale_of(wide):
    return lax.rsqrt(jnp.mean(wide * wide, -1, keepdims=True) + 1e-6)


def rows_kernel(x, dy, *refs):
    hbm, (tall, wide, turned, deep), weights, (g0, u0, z0, sems) = refs[:3], refs[3:7], refs[7:13], refs[13:]
    wg0, wu0, wd0, wg1, wu1, wd1 = weights
    first = pl.program_id(0) == 0

    def fetch(k):
        return pltpu.make_async_copy(hbm[k % 3].at[k // 3], weights[k], sems.at[k])

    @pl.when(first)
    def _():
        for k in range(6):
            fetch(k).start()

    def ready(*ks):
        @pl.when(first)
        def _():
            for k in ks:
                fetch(k).wait()

    a = (x[...].astype(F32) * scale_of(x[...].astype(F32))).astype(BF16)
    tall[1] = a.T
    deep[0] = dy[...]
    ready(0, 1)
    for j in range(FF // CHUNK):
        ch = pl.ds(j * CHUNK, CHUNK)
        gate, up = dot(a, wg0[:, ch]), dot(a, wu0[:, ch])
        g0[:, ch], u0[:, ch] = gate, up
        z0[:, ch] = (gate * jax.nn.sigmoid(gate) * up).astype(BF16)
        turned[1, ch, :] = z0[:, ch].T
    ready(2)
    h = x[...] + dot(z0[...], wd0[...]).astype(BF16)
    h = h.astype(F32)
    scale = scale_of(h)
    a = (h * scale).astype(BF16)
    tall[0] = a.T
    ready(3, 4, 5)
    for j in range(FF // CHUNK):
        ch = pl.ds(j * CHUNK, CHUNK)
        gate, up = dot(a, wg1[:, ch]), dot(a, wu1[:, ch])
        dz = dot_t(dy[...], wd1[ch, :]).astype(BF16).astype(F32)
        s = jax.nn.sigmoid(gate)
        silu = gate * s
        turned[0, ch, :] = (silu * up).astype(BF16).T
        wide[1, :, ch] = (dz * silu).astype(BF16)
        wide[0, :, ch] = (dz * up * (s * (1 + gate * (1 - s)))).astype(BF16)
    da = dot_t(wide[0], wg1[...]).astype(BF16) + dot_t(wide[1], wu1[...]).astype(BF16)
    da = da.astype(F32)
    dwide = scale * (da - h * (scale * scale * jnp.mean(da * h, -1, keepdims=True)))
    dh = dy[...] + dwide.astype(BF16)
    deep[1] = dh
    for j in range(FF // CHUNK):
        ch = pl.ds(j * CHUNK, CHUNK)
        dz = dot_t(dh, wd0[ch, :]).astype(BF16).astype(F32)
        gate, up = g0[:, ch], u0[:, ch]
        s = jax.nn.sigmoid(gate)
        wide[3, :, ch] = (dz * (gate * s)).astype(BF16)
        wide[2, :, ch] = (dz * up * (s * (1 + gate * (1 - s)))).astype(BF16)


def by_rows(x, dy, weights):
    state = pl.BlockSpec((ROWS, D), lambda i: (i, 0))
    return pl.pallas_call(
        rows_kernel,
        grid=(TOKENS // ROWS,),
        out_shape=tuple(jax.ShapeDtypeStruct(s, BF16) for s in ((2, D, TOKENS), (4, TOKENS, FF), (2, FF, TOKENS), (2, TOKENS, D))),
        in_specs=[state, state] + [HBM] * 3,
        out_specs=(
            pl.BlockSpec((2, D, ROWS), lambda i: (0, 0, i)),
            pl.BlockSpec((4, ROWS, FF), lambda i: (0, i, 0)),
            pl.BlockSpec((2, FF, ROWS), lambda i: (0, 0, i)),
            pl.BlockSpec((2, ROWS, D), lambda i: (0, i, 0)),
        ),
        scratch_shapes=[*[pltpu.VMEM(w.shape[1:], BF16) for w in weights * 2], pltpu.VMEM((ROWS, FF), F32), pltpu.VMEM((ROWS, FF), F32), pltpu.VMEM((ROWS, FF), BF16), pltpu.SemaphoreType.DMA((6,))],
        compiler_params=pltpu.CompilerParams(vmem_limit_bytes=MOST_VMEM),
        name="rows",
    )(x, dy, *weights)


STARTS = (0, 48, 96, 144, 192, 232)
PART = 48


def gate_block(acc, stage, wide):
    def group(i, _):
        rows = pl.ds(pl.multiple_of(i * 56, 8), 56)
        for c in range(4):
            piece = acc[rows, pl.ds(c * LANES, LANES)]
            for z in range(4):
                wide[z, pl.ds(14 * c, 14), :] = piece[14 * z : 14 * z + 14]
        for z in range(4):
            stage[i // 4, i % 4, z] = wide[z].astype(BF16)
        return 0

    lax.fori_loop(0, 16, group, 0)


def down_block(acc, stage):
    def group(i, _):
        for t in range(5):
            rows = acc[pl.ds(pl.multiple_of(i * 40, 8) + 8 * t, 8), :]
            piece = jnp.concatenate([rows[:, c * LANES : (c + 1) * LANES] for c in range(7)], 0)
            stage[i // 4, i % 4, pl.ds(56 * t, 56)] = piece.astype(BF16)
        return 0

    lax.fori_loop(0, 16, group, 0)


def gradients_kernel(*refs):
    (tall, wide, turned, deep), (out, squares, terms), scratch = refs[:4], refs[4:7], refs[7:]
    (lhs, rhs, zs, dh, acc, acc2, stage, stage2, shift, r1, r2, r3, own, f1, f2, sums) = scratch[:16]
    (in_sem, rhs_sem, zs_sem, put_sem, send1, send2, send3, recv1, recv2, recv3, load, send4, recv4) = scratch[16:]
    at = place()

    def fetch_tall(l):
        return pltpu.make_async_copy(tall.at[l], lhs, in_sem.at[0])

    def fetch_deep(l):
        return pltpu.make_async_copy(deep.at[l], dh, in_sem.at[1])

    def fetch_wide(t):
        columns = pl.ds(pl.multiple_of(t % TILES * TILE, TILE), TILE)
        return pltpu.make_async_copy(wide.at[t // TILES, :, columns], rhs.at[t % 2], rhs_sem.at[t % 2])

    def fetch_turned(t):
        rows = pl.ds(pl.multiple_of(t % SIDE * PLANE_ROWS, LANES), PLANE_ROWS)
        return pltpu.make_async_copy(turned.at[t // SIDE, rows], zs.at[t % 2], zs_sem.at[t % 2])

    def put(m, h):
        return pltpu.make_async_copy(stage, terms.at[m, :, :, :, pl.ds(pl.multiple_of(PIECE * h, SUBLANES), PIECE)], put_sem.at[0])

    def put2(m, h):
        return pltpu.make_async_copy(stage2, terms.at[m, h], put_sem.at[1])

    fetch_tall(0).start()
    fetch_wide(0).start()
    fetch_deep(0).start()
    fetch_turned(0).start()
    enter(at)

    def split(c):
        o, s = ORDERS[c], SIGNS[c]
        return o, s, at[o[0]], at[o[1]], at[o[2]]

    def block(m, c, a, i):
        o = ORDERS[c]
        index = [slice(None)] * 3
        index[o[0]] = a
        if i is not None:
            index[o[1]] = i
        return terms.at[(m, *index, pl.ds(STARTS[c], PART))]

    def first(m, c, step, j, start=False):
        o, s, p1, p2, p3 = split(c)
        if start:
            src = block(m, c, wrap(p1 - s), wrap(p2 - s * (1 + j)))
        else:
            src = r1.at[c, m, (step + 2) % STEPS, j]
        return remote(src, r1.at[c, m, step, j], send1.at[c], recv1.at[c, m, step, j], neighbour(at, o[0], s))

    def loading(m, c, step):
        o, s, p1, p2, p3 = split(c)
        return pltpu.make_async_copy(block(m, c, wrap(p1 - s * (2 + step)), None), own.at[c, step], load.at[c, step])

    def second(m, c, step, start=False):
        o, s, p1, p2, p3 = split(c)
        src = r1.at[c, m, 2, 0] if start else r2.at[c, m, (step + 2) % STEPS]
        return remote(src, r2.at[c, m, step], send2.at[c], recv2.at[c, m, step], neighbour(at, o[1], s))

    def third(m, c, step, start=False):
        o, s, p1, p2, p3 = split(c)
        src = r2.at[c, m, 2, wrap(p3 - s)] if start else r3.at[c, m, (step + 2) % STEPS]
        return remote(src, r3.at[c, m, step], send3.at[c], recv3.at[c, m, step], neighbour(at, o[2], s))

    def launch(m):
        for c in range(WAYS):
            for j in range(SIDE):
                first(m, c, 0, j, True).start()
        for step in range(STEPS):
            for c in range(WAYS):
                loading(m, c, step).start()

    def on_first(m, e):
        step, j = e // SIDE, e % SIDE

        @pl.when(j == 0)
        def _():
            for c in range(WAYS):
                loading(m, c, step).wait()

        for c in range(WAYS):
            o, s, p1, p2, p3 = split(c)
            first(m, c, step, j).wait_recv()
            i = wrap(p2 - s * (1 + j))
            mine = own[c, step, i] if o[1] < o[2] else own[c, step, :, i]
            both = r1[c, m, step, j].astype(F32) + mine.astype(F32)
            r1[c, m, step, j] = both.astype(BF16)

            @pl.when(step == 2)
            def _():
                f1[c, j] = both

            @pl.when(step < 2)
            def _():
                first(m, c, step + 1, j).start()

            @pl.when(e == 8)
            def _():
                second(m, c, 0, True).start()

    def on_second(m, step):
        for c in range(WAYS):
            second(m, c, step).wait_recv()
            both = r2[c, m, step].astype(F32) + f1[c, step + 1]
            r2[c, m, step] = both.astype(BF16)

            @pl.when(step == 2)
            def _():
                f2[c] = both
                third(m, c, 0, True).start()

            @pl.when(step < 2)
            def _():
                second(m, c, step + 1).start()

    def on_third(m, step):
        for c in range(WAYS):
            o, s, p1, p2, p3 = split(c)
            third(m, c, step).wait_recv()
            both = (r3[c, m, step].astype(F32) + f2[c, wrap(p3 - s * (2 + step))]).astype(BF16)

            @pl.when(step < 2)
            def _():
                r3[c, m, step] = both
                third(m, c, step + 1).start()

            @pl.when(step == 2)
            def _():
                out[m, pl.ds(STARTS[c], PART)] = both

    def tile(i, _):
        m, h = i // TILES, i % TILES
        kind, l = m % AXES, m // AXES

        @pl.when((h == 0) & (m > 0) & (m < MATRICES + 1))
        def _():
            @pl.when(kind > 0)
            def _():
                put(0, 0).wait()

            @pl.when(kind == 0)
            def _():
                put2(0, 0).wait()

            launch(m - 1)

        @pl.when((m < MATRICES) & (kind < 2))
        def _():
            t = (2 * l + kind) * TILES + h

            @pl.when((kind == 0) & (h == 0))
            def _():
                fetch_tall(l).wait()

                @pl.when(l == 1)
                def _():
                    fetch_deep(1).start()

            fetch_wide(t).wait()

            @pl.when(t < 19)
            def _():
                fetch_wide(t + 1).start()

            acc[...] = dot(lhs[...], rhs[t % 2])

            @pl.when(h > 0)
            def _():
                put(m, h).wait()

            gate_block(acc, stage, shift)
            put(m, h).start()

        @pl.when((m < MATRICES) & (kind == 2) & (h < SIDE))
        def _():
            t = SIDE * l + h

            @pl.when(h == 0)
            def _():
                fetch_deep(l).wait()

                @pl.when(l == 0)
                def _():
                    fetch_tall(1).start()

            fetch_turned(t).wait()

            @pl.when(t < 7)
            def _():
                fetch_turned(t + 1).start()

            acc2[...] = dot(zs[t % 2], dh[...])

            @pl.when(h > 0)
            def _():
                put2(m, h).wait()

            down_block(acc2, stage2)
            put2(m, h).start()

        @pl.when((h > 0) & (h < SIDE) & (m > 2))
        def _():
            on_third(m - 3, h - 1)

        @pl.when((h > 0) & (h < SIDE) & (m > 1) & (m < MATRICES + 2))
        def _():
            on_second(m - 2, h - 1)

        @pl.when((h < SIDE) & (m > 0) & (m < MATRICES + 1))
        def _():
            lax.fori_loop(0, 3, lambda k, _: (on_first(m - 1, 3 * h + k), 0)[1], 0)

        return 0

    lax.fori_loop(0, (MATRICES + AXES) * TILES, tile, 0)

    total = jnp.zeros((SUBLANES, LANES), F32)
    for m in range(MATRICES):
        g = out[m].astype(F32)
        total = total + jnp.sum((g * g).reshape(-1, SUBLANES, LANES), axis=0)
    squares[...] = norm_exchange(at, sums, send4, recv4, total)
    for c in range(WAYS):
        for r, sem in ((r1, send1), (r2, send2), (r3, send3)):
            pltpu.make_async_copy(r.at[c], r.at[c], sem.at[c]).wait()
    for axis in range(STEPS):
        pltpu.make_async_copy(sums.at[axis, pl.ds(0, STEPS)], sums.at[axis, pl.ds(0, STEPS)], send4.at[axis]).wait()


def gradients(tall, wide, turned, deep):
    g, squares, _ = pl.pallas_call(
        gradients_kernel,
        out_shape=(
            jax.ShapeDtypeStruct((MATRICES, BLOCK, LANES), BF16),
            jax.ShapeDtypeStruct((SUBLANES, LANES), F32),
            jax.ShapeDtypeStruct((MATRICES, SIDE, SIDE, SIDE, BLOCK, LANES), BF16),
        ),
        in_specs=[HBM] * 4,
        out_specs=(VMEM, VMEM, HBM),
        scratch_shapes=[
            pltpu.VMEM((D, TOKENS), BF16),
            pltpu.VMEM((2, TOKENS, TILE), BF16),
            pltpu.VMEM((2, PLANE_ROWS, TOKENS), BF16),
            pltpu.VMEM((TOKENS, D), BF16),
            pltpu.VMEM((D, TILE), F32),
            pltpu.VMEM((PLANE_ROWS, D), F32),
            pltpu.VMEM((SIDE, SIDE, SIDE, PIECE, LANES), BF16),
            pltpu.VMEM((SIDE, SIDE, BLOCK, LANES), BF16),
            pltpu.VMEM((SIDE, PIECE, LANES), F32),
            pltpu.VMEM((WAYS, MATRICES, STEPS, SIDE, SIDE, PART, LANES), BF16),
            pltpu.VMEM((WAYS, MATRICES, STEPS, SIDE, PART, LANES), BF16),
            pltpu.VMEM((WAYS, MATRICES, STEPS, PART, LANES), BF16),
            pltpu.VMEM((WAYS, STEPS, SIDE, SIDE, PART, LANES), BF16),
            pltpu.VMEM((WAYS, SIDE, SIDE, PART, LANES), F32),
            pltpu.VMEM((WAYS, SIDE, PART, LANES), F32),
            pltpu.VMEM((AXES, SIDE, SUBLANES, LANES), F32),
            *[DMA((2,))] * 4,
            *[DMA((WAYS,))] * AXES,
            DMA((WAYS, MATRICES, STEPS, SIDE)), *[DMA((WAYS, MATRICES, STEPS))] * 2,
            DMA((WAYS, STEPS)),
            DMA((AXES,)), DMA((AXES, STEPS)),
        ],
        compiler_params=pltpu.CompilerParams(collective_id=0, has_side_effects=True, vmem_limit_bytes=MOST_VMEM),
        name="gradients",
    )(tall, wide, turned, deep)
    return g, squares


def solution(mesh):
    rep, dp = mesh.axis_names

    def step(x, dy, *arrays):
        weights, m, v = (arrays[i : i + 3] for i in (0, 3, 6))
        g, total = gradients(*by_rows(x[0], dy[0], weights))
        me = lax.axis_index(dp)
        mine = [lax.dynamic_slice_in_dim(w, me * b.shape[1], b.shape[1], 1) for w, b in zip(weights, m, strict=True)]
        new, new_m, new_v = adam(sum(w.size for w in weights), g, total, mine, m, v)
        return (*natural(all_gather(new)), *new_m, *new_v)

    whole, rows, sequences = P(None, None, None), P(None, dp, None), P((rep, dp), None, None)
    return jax.shard_map(
        step,
        mesh=mesh,
        in_specs=(sequences, sequences, *[whole] * 3, *[rows] * 6),
        out_specs=(*[P(rep, None, None)] * 3, *[P(rep, dp, None)] * 6),
        check_vma=False,
    )
```

```python
import functools
import jax
import jax.numpy as jnp
from jax import lax
from jax.experimental import pallas as pl
from jax.experimental.pallas import tpu as pltpu
from jax.sharding import PartitionSpec as P

MESH = pl.DeviceIdType.MESH
WAYS, AXES, SIDE = 6, 3, 4
STEPS = SIDE - 1
MATRICES, LAYERS, DEVICES, PLANE = 6, 2, 64, 16
LANES, SUBLANES, BLOCK = 128, 8, 280
BF16, F32 = jnp.bfloat16, jnp.float32
HBM, VMEM = pl.BlockSpec(memory_space=pl.ANY), pl.BlockSpec(memory_space=pltpu.VMEM)
DMA = pltpu.SemaphoreType.DMA
MOST_VMEM = 62 * 1024 * 1024
ORDERS = tuple(tuple((way // 2 + i) % AXES for i in range(AXES)) for way in range(WAYS))
SIGNS = (1, -1) * AXES
TAKEN = (3, 0, 4, 1, 5, 2)


def place():
    me = lax.axis_index("dp")
    return (me // PLANE, me // SIDE % SIDE, me % SIDE)


def wrap(i):
    return (i + 3 * SIDE) % SIDE


def neighbour(at, axis, step):
    there = [c for c in at]
    there[axis] = wrap(at[axis] + step)
    return {"dp": (there[0] * SIDE + there[1]) * SIDE + there[2]}


def remote(src, dst, send, recv, to):
    return pltpu.make_async_remote_copy(src_ref=src, dst_ref=dst, send_sem=send, recv_sem=recv, device_id=to, device_id_type=MESH)


def enter(at):
    barrier = pltpu.get_barrier_semaphore()
    for axis in range(AXES):
        for step in range(STEPS):
            pl.semaphore_signal(barrier, inc=1, device_id=neighbour(at, axis, step + 1), device_id_type=MESH)
    pl.semaphore_wait(barrier, AXES * STEPS)


def norm_exchange(at, buf, send, recv, total):
    for axis in range(AXES):
        buf[axis, STEPS] = total
        copies = [
            remote(buf.at[axis, STEPS], buf.at[axis, k], send.at[axis], recv.at[axis, k], neighbour(at, axis, k + 1)) for k in range(STEPS)
        ]
        for copy in copies:
            copy.start()
        for k, copy in enumerate(copies):
            copy.wait_recv()
            total = total + buf[axis, k]
    return total


def passed_on(seen, c, phase, key):
    d1, d2, d3 = key
    if phase == 0 and d3 < STEPS:
        yield 0, (0, 0, d3 + 1)
    if phase < 2 and d2 < STEPS:
        yield 1, (0, d2 + 1, d3)
    if phase == 1 and d2 > 0:
        seen.append((c, d2))
        if seen.count((c, d2)) < SIDE:
            return
        d3 = None
    if d1 < STEPS:
        yield 2, (d1 + 1, d2, d3)


def ag_order(latency=1.8):
    import heapq

    free, out, seen, heap = {}, [], [], []

    def hold(t, c, phase, key):
        for phase, key in passed_on(seen, c, phase, key):
            link = ORDERS[c][2 - phase]
            size = SIDE if key[2] is None else 1
            free[link] = max(t, free.get(link, 0)) + size
            heapq.heappush(heap, (free[link] + latency, len(out) * WAYS + len(heap), c, phase, key))

    for c in range(0, WAYS, 2):
        hold(0, c, 0, (0, 0, 0))
    while heap:
        t, _, *arrival = heapq.heappop(heap)
        out.append(arrival)
        hold(t, *arrival)
    return out


def ag_kernel(*refs):
    mine, outs, (sends, recv1, recv2, recv3, recv4, local) = refs[0], refs[1 : 1 + WAYS], refs[1 + WAYS :]
    at = place()
    enter(at)

    def where(c, key):
        index = [None] * AXES
        for axis, d in zip(ORDERS[c], key, strict=True):
            index[axis] = slice(None) if d is None else wrap(at[axis] - SIGNS[c] * d)
        return outs[c].at[tuple(index)]

    def copy(c, phase, key, of_receiver):
        d1, d2, d3 = key
        back = list(key)
        if not of_receiver:
            back[2 - phase] -= 1
        there = where(c, back)
        src = mine.at[c] if not of_receiver and not any(back) and d3 is not None else there
        if phase == 0:
            recv = recv1.at[c, d3]
        elif phase == 1:
            recv = recv2.at[c, d2, d3]
        elif d3 is not None:
            recv = recv3.at[c, d1, d3]
        else:
            recv = recv4.at[c, d1, d2]
        return remote(src, there, sends.at[c, phase], recv, neighbour(at, ORDERS[c][2 - phase], SIGNS[c]))

    seen = []

    def hold(*held):
        for phase, key in passed_on(seen, *held):
            copy(held[0], phase, key, False).start()

    own = [pltpu.make_async_copy(mine.at[c], where(c, (0, 0, 0)), local.at[c]) for c in range(WAYS)]
    for c in range(WAYS):
        hold(c, 0, (0, 0, 0))
    for copied in own:
        copied.start()
    for even, phase, key in ag_order():
        for c in (even, even + 1):
            copy(c, phase, key, True).wait_recv()
            hold(c, phase, key)
    for c in range(WAYS):
        own[c].wait()
        sent = outs[c].at[pl.ds(0, STEPS)]
        for phase in (2, 1, 0):
            pltpu.make_async_copy(sent, sent, sends.at[c, phase]).wait()
            sent = outs[c].at[(0,) * (AXES - phase) + (pl.ds(0, STEPS),)]


def all_gather(mine):
    return pl.pallas_call(
        ag_kernel,
        out_shape=(pltpu.VMEM((SIDE, SIDE, SIDE, *mine.shape[1:]), BF16),) * WAYS,
        in_specs=[VMEM],
        out_specs=(VMEM,) * WAYS,
        scratch_shapes=[DMA((WAYS, AXES)), DMA((WAYS, SIDE)), *[DMA((WAYS, SIDE, SIDE))] * 3, DMA((WAYS,))],
        compiler_params=pltpu.CompilerParams(collective_id=1, has_side_effects=True, vmem_limit_bytes=MOST_VMEM // SUBLANES),
        name="gather",
    )(mine)


def tiles_of(t, rows, columns):
    n = columns // LANES
    if t < 2:
        return [(0, rows, j * LANES, j * rows) for j in range(n)]
    return [(8 * i, 8, j * LANES, (i * n + j) * 8) for i in range(rows // 8) for j in range(n)]


def adam_kernel(count, g, total, *refs):
    ws, ms, vs, new, new_m, new_v, wide_g, wide_w = refs[0:3], refs[3:6], refs[6:9], refs[9], refs[10:13], refs[13:16], refs[16], refs[17]
    factor = jnp.minimum(1.0, 0.5 * lax.rsqrt(jnp.full((1, 1), jnp.sum(total[...])) / count + 1e-30))
    for t in range(3):
        for l in range(2):
            c = 2 * t + l
            wide_g[...] = g[TAKEN[c]].astype(F32) * factor
            for row, rows, column, at in tiles_of(t, *ms[t].shape[1:]):
                here = (l, pl.ds(row, rows), pl.ds(column, LANES))
                grad = wide_g[pl.ds(at, rows), :]
                m = 0.9 * ms[t][here] + 0.1 * grad
                v = 0.95 * vs[t][here] + 0.05 * grad * grad
                w = ws[t][here].astype(F32)
                new_m[t][here] = m
                new_v[t][here] = v
                wide_w[pl.ds(at, rows), :] = w - 0.02 * (m * lax.rsqrt(v + 1e-8) + 0.1 * w)
            new[c] = wide_w[...].astype(BF16)


def adam(count, g, total, ws, ms, vs):
    like = [jax.ShapeDtypeStruct(m.shape, F32) for m in ms]
    out = pl.pallas_call(
        functools.partial(adam_kernel, count),
        out_shape=(jax.ShapeDtypeStruct(g.shape, BF16), *like, *like),
        in_specs=[VMEM] * 11,
        out_specs=(VMEM,) * 7,
        scratch_shapes=[pltpu.VMEM(g.shape[1:], F32)] * 2,
        name="adam",
    )(g, total, *ws, *ms, *vs)
    return out[0], out[1:4], out[4:7]


def natural_kernel(*refs):
    gathered, outs, wide = refs[:MATRICES], refs[MATRICES:-AXES], refs[-AXES:]
    first = pl.program_id(0) * SIDE
    for t in range(AXES):
        for l in range(LAYERS):
            for z in range(SIDE):
                block = gathered[LAYERS * t + l][first + z].astype(F32)
                rows = outs[t].shape[1] // SIDE
                for row, n, column, at in tiles_of(t, rows, outs[t].shape[2]):
                    wide[t][pl.ds(z * rows + row, n), pl.ds(column, LANES)] = block[at : at + n]
            outs[t][l] = wide[t][...].astype(BF16)


def natural(gathered):
    shapes = (GATE, GATE, DOWN)
    return pl.pallas_call(
        natural_kernel,
        grid=(PLANE,),
        out_shape=tuple(jax.ShapeDtypeStruct((LAYERS, *s), BF16) for s in shapes),
        in_specs=[VMEM] * MATRICES,
        out_specs=tuple(pl.BlockSpec((LAYERS, s[0] // PLANE, s[1]), lambda i: (0, i, 0)) for s in shapes),
        scratch_shapes=[pltpu.VMEM((s[0] // PLANE, s[1]), F32) for s in shapes],
        compiler_params=pltpu.CompilerParams(vmem_limit_bytes=MOST_VMEM // SIDE),
        name="natural",
    )(*[g.reshape(DEVICES, BLOCK, LANES) for g in gathered])


D, FF, TOKENS = 896, 2560, 2048
GATE, DOWN = (D, FF), (FF, D)
ROWS, CHUNK, TILE = 256, 512, 512
TILES, PIECE, PLANE_ROWS = FF // TILE, BLOCK * TILE // FF, FF // SIDE
NT = (((1,), (1,)), ((), ()))


def dot(a, b):
    return jnp.dot(a, b, preferred_element_type=F32)


def dot_t(a, b):
    return lax.dot_general(a, b, NT, preferred_element_type=F32)


def scale_of(wide):
    return lax.rsqrt(jnp.mean(wide * wide, -1, keepdims=True) + 1e-6)


def rows_kernel(x, dy, *refs):
    hbm, (tall, wide, turned, deep), weights, (g0, u0, z0, sems) = refs[:3], refs[3:7], refs[7:13], refs[13:]
    wg0, wu0, wd0, wg1, wu1, wd1 = weights
    first = pl.program_id(0) == 0

    def fetch(k):
        return pltpu.make_async_copy(hbm[k % 3].at[k // 3], weights[k], sems.at[k])

    @pl.when(first)
    def _():
        for k in range(6):
            fetch(k).start()

    def ready(*ks):
        @pl.when(first)
        def _():
            for k in ks:
                fetch(k).wait()

    a = (x[...].astype(F32) * scale_of(x[...].astype(F32))).astype(BF16)
    tall[1] = a.T
    deep[0] = dy[...]
    ready(0, 1)
    for j in range(FF // CHUNK):
        ch = pl.ds(j * CHUNK, CHUNK)
        gate, up = dot(a, wg0[:, ch]), dot(a, wu0[:, ch])
        g0[:, ch], u0[:, ch] = gate, up
        z0[:, ch] = (gate * jax.nn.sigmoid(gate) * up).astype(BF16)
        turned[1, ch, :] = z0[:, ch].T
    ready(2)
    h = x[...] + dot(z0[...], wd0[...]).astype(BF16)
    h = h.astype(F32)
    scale = scale_of(h)
    a = (h * scale).astype(BF16)
    tall[0] = a.T
    ready(3, 4, 5)
    for j in range(FF // CHUNK):
        ch = pl.ds(j * CHUNK, CHUNK)
        gate, up = dot(a, wg1[:, ch]), dot(a, wu1[:, ch])
        dz = dot_t(dy[...], wd1[ch, :]).astype(BF16).astype(F32)
        s = jax.nn.sigmoid(gate)
        silu = gate * s
        turned[0, ch, :] = (silu * up).astype(BF16).T
        wide[1, :, ch] = (dz * silu).astype(BF16)
        wide[0, :, ch] = (dz * up * (s * (1 + gate * (1 - s)))).astype(BF16)
    da = dot_t(wide[0], wg1[...]).astype(BF16) + dot_t(wide[1], wu1[...]).astype(BF16)
    da = da.astype(F32)
    dwide = scale * (da - h * (scale * scale * jnp.mean(da * h, -1, keepdims=True)))
    dh = dy[...] + dwide.astype(BF16)
    deep[1] = dh
    for j in range(FF // CHUNK):
        ch = pl.ds(j * CHUNK, CHUNK)
        dz = dot_t(dh, wd0[ch, :]).astype(BF16).astype(F32)
        gate, up = g0[:, ch], u0[:, ch]
        s = jax.nn.sigmoid(gate)
        wide[3, :, ch] = (dz * (gate * s)).astype(BF16)
        wide[2, :, ch] = (dz * up * (s * (1 + gate * (1 - s)))).astype(BF16)


def by_rows(x, dy, weights):
    state = pl.BlockSpec((ROWS, D), lambda i: (i, 0))
    return pl.pallas_call(
        rows_kernel,
        grid=(TOKENS // ROWS,),
        out_shape=tuple(jax.ShapeDtypeStruct(s, BF16) for s in ((2, D, TOKENS), (4, TOKENS, FF), (2, FF, TOKENS), (2, TOKENS, D))),
        in_specs=[state, state] + [HBM] * 3,
        out_specs=(
            pl.BlockSpec((2, D, ROWS), lambda i: (0, 0, i)),
            pl.BlockSpec((4, ROWS, FF), lambda i: (0, i, 0)),
            pl.BlockSpec((2, FF, ROWS), lambda i: (0, 0, i)),
            pl.BlockSpec((2, ROWS, D), lambda i: (0, i, 0)),
        ),
        scratch_shapes=[*[pltpu.VMEM(w.shape[1:], BF16) for w in weights * 2], pltpu.VMEM((ROWS, FF), F32), pltpu.VMEM((ROWS, FF), F32), pltpu.VMEM((ROWS, FF), BF16), pltpu.SemaphoreType.DMA((6,))],
        compiler_params=pltpu.CompilerParams(vmem_limit_bytes=MOST_VMEM),
        name="rows",
    )(x, dy, *weights)


STARTS = (0, 48, 96, 144, 192, 232)
PART = 48


def gate_block(acc, stage, wide):
    def group(i, _):
        rows = pl.ds(pl.multiple_of(i * 56, 8), 56)
        for c in range(4):
            piece = acc[rows, pl.ds(c * LANES, LANES)]
            for z in range(4):
                wide[z, pl.ds(14 * c, 14), :] = piece[14 * z : 14 * z + 14]
        for z in range(4):
            stage[i // 4, i % 4, z] = wide[z].astype(BF16)
        return 0

    lax.fori_loop(0, 16, group, 0)


def down_block(acc, stage):
    def group(i, _):
        for t in range(5):
            rows = acc[pl.ds(pl.multiple_of(i * 40, 8) + 8 * t, 8), :]
            piece = jnp.concatenate([rows[:, c * LANES : (c + 1) * LANES] for c in range(7)], 0)
            stage[i // 4, i % 4, pl.ds(56 * t, 56)] = piece.astype(BF16)
        return 0

    lax.fori_loop(0, 16, group, 0)


def gradients_kernel(*refs):
    (tall, wide, turned, deep), (out, squares, terms), scratch = refs[:4], refs[4:7], refs[7:]
    (lhs, rhs, zs, dh, acc, acc2, stage, stage2, shift, r1, r2, r3, own, f1, f2, sums) = scratch[:16]
    (in_sem, rhs_sem, zs_sem, put_sem, send1, send2, send3, recv1, recv2, recv3, load, send4, recv4) = scratch[16:]
    at = place()

    def fetch_tall(l):
        return pltpu.make_async_copy(tall.at[l], lhs, in_sem.at[0])

    def fetch_deep(l):
        return pltpu.make_async_copy(deep.at[l], dh, in_sem.at[1])

    def fetch_wide(t):
        columns = pl.ds(pl.multiple_of(t % TILES * TILE, TILE), TILE)
        return pltpu.make_async_copy(wide.at[t // TILES, :, columns], rhs.at[t % 2], rhs_sem.at[t % 2])

    def fetch_turned(t):
        rows = pl.ds(pl.multiple_of(t % SIDE * PLANE_ROWS, LANES), PLANE_ROWS)
        return pltpu.make_async_copy(turned.at[t // SIDE, rows], zs.at[t % 2], zs_sem.at[t % 2])

    def put(m, h):
        return pltpu.make_async_copy(stage, terms.at[m, :, :, :, pl.ds(pl.multiple_of(PIECE * h, SUBLANES), PIECE)], put_sem.at[0])

    def put2(m, h):
        return pltpu.make_async_copy(stage2, terms.at[m, h], put_sem.at[1])

    fetch_tall(0).start()
    fetch_wide(0).start()
    fetch_deep(0).start()
    fetch_turned(0).start()
    enter(at)

    def split(c):
        o, s = ORDERS[c], SIGNS[c]
        return o, s, at[o[0]], at[o[1]], at[o[2]]

    def block(m, c, a, i):
        o = ORDERS[c]
        index = [slice(None)] * 3
        index[o[0]] = a
        if i is not None:
            index[o[1]] = i
        return terms.at[(m, *index, pl.ds(STARTS[c], PART))]

    def first(m, c, step, j, start=False):
        o, s, p1, p2, p3 = split(c)
        if start:
            src = block(m, c, wrap(p1 - s), wrap(p2 - s * (1 + j)))
        else:
            src = r1.at[c, m, (step + 2) % STEPS, j]
        return remote(src, r1.at[c, m, step, j], send1.at[c], recv1.at[c, m, step, j], neighbour(at, o[0], s))

    def loading(m, c, step):
        o, s, p1, p2, p3 = split(c)
        return pltpu.make_async_copy(block(m, c, wrap(p1 - s * (2 + step)), None), own.at[c, step], load.at[c, step])

    def second(m, c, step, start=False):
        o, s, p1, p2, p3 = split(c)
        src = r1.at[c, m, 2, 0] if start else r2.at[c, m, (step + 2) % STEPS]
        return remote(src, r2.at[c, m, step], send2.at[c], recv2.at[c, m, step], neighbour(at, o[1], s))

    def third(m, c, k):
        o, s, p1, p2, p3 = split(c)
        return remote(r2.at[c, m, 2, wrap(p3 + k + 1)], r3.at[c, m, k], send3.at[c], recv3.at[c, m, k], neighbour(at, o[2], k + 1))

    def launch(m):
        for c in range(WAYS):
            for j in range(SIDE):
                first(m, c, 0, j, True).start()
    def load_own(m):
        for step in range(STEPS):
            for c in range(WAYS):
                loading(m, c, step).start()

    def on_first(m, e):
        step, j = e // SIDE, e % SIDE

        @pl.when(j == 0)
        def _():
            for c in range(WAYS):
                loading(m, c, step).wait()

        for c in range(WAYS):
            o, s, p1, p2, p3 = split(c)
            first(m, c, step, j).wait_recv()
            i = wrap(p2 - s * (1 + j))
            mine = own[c, step, i] if o[1] < o[2] else own[c, step, :, i]
            both = r1[c, m, step, j].astype(F32) + mine.astype(F32)
            r1[c, m, step, j] = both.astype(BF16)

            @pl.when(step == 2)
            def _():
                f1[c, j] = both

            @pl.when(step < 2)
            def _():
                first(m, c, step + 1, j).start()

            @pl.when(e == 8)
            def _():
                second(m, c, 0, True).start()

    def on_second(m, step):
        for c in range(WAYS):
            second(m, c, step).wait_recv()
            both = r2[c, m, step].astype(F32) + f1[c, step + 1]
            r2[c, m, step] = both.astype(BF16)

            @pl.when(step == 2)
            def _():
                f2[c] = both
                for k in range(STEPS):
                    third(m, c, k).start()

            @pl.when(step < 2)
            def _():
                second(m, c, step + 1).start()

    def on_third(m):
        for c in range(WAYS):
            o, s, p1, p2, p3 = split(c)
            total = f2[c, p3]
            for k in range(STEPS):
                third(m, c, k).wait_recv()
                total = total + r3[c, m, k].astype(F32)
            out[m, pl.ds(STARTS[c], PART)] = total.astype(BF16)

    def tile(i, _):
        m, h = i // TILES, i % TILES
        kind, l = m % AXES, m // AXES

        @pl.when((h == 0) & (m > 0) & (m < MATRICES + 1))
        def _():
            @pl.when(kind > 0)
            def _():
                put(0, 0).wait()

            @pl.when(kind == 0)
            def _():
                put2(0, 0).wait()

            launch(m - 1)

        @pl.when((m < MATRICES) & (kind < 2))
        def _():
            t = (2 * l + kind) * TILES + h

            @pl.when((kind == 0) & (h == 0))
            def _():
                fetch_tall(l).wait()

                @pl.when(l == 1)
                def _():
                    fetch_deep(1).start()

            fetch_wide(t).wait()

            @pl.when(t < 19)
            def _():
                fetch_wide(t + 1).start()

            acc[...] = dot(lhs[...], rhs[t % 2])

            @pl.when(h > 0)
            def _():
                put(m, h).wait()

            gate_block(acc, stage, shift)
            put(m, h).start()

        @pl.when((m < MATRICES) & (kind == 2) & (h < SIDE))
        def _():
            t = SIDE * l + h

            @pl.when(h == 0)
            def _():
                fetch_deep(l).wait()

                @pl.when(l == 0)
                def _():
                    fetch_tall(1).start()

            fetch_turned(t).wait()

            @pl.when(t < 7)
            def _():
                fetch_turned(t + 1).start()

            acc2[...] = dot(zs[t % 2], dh[...])

            @pl.when(h > 0)
            def _():
                put2(m, h).wait()

            down_block(acc2, stage2)
            put2(m, h).start()

        @pl.when((h == SIDE) & (m > 1))
        def _():
            on_third(m - 2)

        @pl.when((h != 1) & (h != SIDE) & (m > 1) & (m < MATRICES + 2))
        def _():
            on_second(m - 2, (h + 1) // 2)

        ring, turn = (i - 1) // TILES - 1, (i - 1) % TILES

        @pl.when((ring >= 0) & (ring < MATRICES))
        def _():
            lax.fori_loop(TILES * turn // 2, TILES * (turn + 1) // 2, lambda e, _: (on_first(ring, e), 0)[1], 0)

        @pl.when((h == 0) & (m > 0) & (m < MATRICES + 1))
        def _():
            load_own(m - 1)

        return 0

    lax.fori_loop(0, (MATRICES + 2) * TILES, tile, 0)

    total = jnp.zeros((SUBLANES, LANES), F32)
    for m in range(MATRICES):
        g = out[m].astype(F32)
        total = total + jnp.sum((g * g).reshape(-1, SUBLANES, LANES), axis=0)
    squares[...] = norm_exchange(at, sums, send4, recv4, total)
    for c in range(WAYS):
        for r, sem in ((r1, send1), (r2, send2), (r3, send3)):
            pltpu.make_async_copy(r.at[c], r.at[c], sem.at[c]).wait()
    for axis in range(STEPS):
        pltpu.make_async_copy(sums.at[axis, pl.ds(0, STEPS)], sums.at[axis, pl.ds(0, STEPS)], send4.at[axis]).wait()


def gradients(tall, wide, turned, deep):
    g, squares, _ = pl.pallas_call(
        gradients_kernel,
        out_shape=(
            jax.ShapeDtypeStruct((MATRICES, BLOCK, LANES), BF16),
            jax.ShapeDtypeStruct((SUBLANES, LANES), F32),
            jax.ShapeDtypeStruct((MATRICES, SIDE, SIDE, SIDE, BLOCK, LANES), BF16),
        ),
        in_specs=[HBM] * 4,
        out_specs=(VMEM, VMEM, HBM),
        scratch_shapes=[
            pltpu.VMEM((D, TOKENS), BF16),
            pltpu.VMEM((2, TOKENS, TILE), BF16),
            pltpu.VMEM((2, PLANE_ROWS, TOKENS), BF16),
            pltpu.VMEM((TOKENS, D), BF16),
            pltpu.VMEM((D, TILE), F32),
            pltpu.VMEM((PLANE_ROWS, D), F32),
            pltpu.VMEM((SIDE, SIDE, SIDE, PIECE, LANES), BF16),
            pltpu.VMEM((SIDE, SIDE, BLOCK, LANES), BF16),
            pltpu.VMEM((SIDE, PIECE, LANES), F32),
            pltpu.VMEM((WAYS, MATRICES, STEPS, SIDE, SIDE, PART, LANES), BF16),
            pltpu.VMEM((WAYS, MATRICES, STEPS, SIDE, PART, LANES), BF16),
            pltpu.VMEM((WAYS, MATRICES, STEPS, PART, LANES), BF16),
            pltpu.VMEM((WAYS, STEPS, SIDE, SIDE, PART, LANES), BF16),
            pltpu.VMEM((WAYS, SIDE, SIDE, PART, LANES), F32),
            pltpu.VMEM((WAYS, SIDE, PART, LANES), F32),
            pltpu.VMEM((AXES, SIDE, SUBLANES, LANES), F32),
            *[DMA((2,))] * 4,
            *[DMA((WAYS,))] * AXES,
            DMA((WAYS, MATRICES, STEPS, SIDE)), *[DMA((WAYS, MATRICES, STEPS))] * 2,
            DMA((WAYS, STEPS)),
            DMA((AXES,)), DMA((AXES, STEPS)),
        ],
        compiler_params=pltpu.CompilerParams(collective_id=0, has_side_effects=True, vmem_limit_bytes=MOST_VMEM),
        name="gradients",
    )(tall, wide, turned, deep)
    return g, squares


def solution(mesh):
    rep, dp = mesh.axis_names

    def step(x, dy, *arrays):
        weights, m, v = (arrays[i : i + 3] for i in (0, 3, 6))
        g, total = gradients(*by_rows(x[0], dy[0], weights))
        me = lax.axis_index(dp)
        mine = [lax.dynamic_slice_in_dim(w, me * b.shape[1], b.shape[1], 1) for w, b in zip(weights, m, strict=True)]
        new, new_m, new_v = adam(sum(w.size for w in weights), g, total, mine, m, v)
        return (*natural(all_gather(new)), *new_m, *new_v)

    whole, rows, sequences = P(None, None, None), P(None, dp, None), P((rep, dp), None, None)
    return jax.shard_map(
        step,
        mesh=mesh,
        in_specs=(sequences, sequences, *[whole] * 3, *[rows] * 6),
        out_specs=(*[P(rep, None, None)] * 3, *[P(rep, dp, None)] * 6),
        check_vma=False,
    )
```

```python
import functools
import jax
import jax.numpy as jnp
from jax import lax
from jax.experimental import pallas as pl
from jax.experimental.pallas import tpu as pltpu
from jax.sharding import PartitionSpec as P

MESH = pl.DeviceIdType.MESH
WAYS, AXES, SIDE = 6, 3, 4
STEPS = SIDE - 1
MATRICES, LAYERS, DEVICES, PLANE = 6, 2, 64, 16
LANES, SUBLANES, BLOCK = 128, 8, 280
BF16, F32 = jnp.bfloat16, jnp.float32
HBM, VMEM = pl.BlockSpec(memory_space=pl.ANY), pl.BlockSpec(memory_space=pltpu.VMEM)
DMA = pltpu.SemaphoreType.DMA
MOST_VMEM = 62 * 1024 * 1024
ORDERS = tuple(tuple((way // 2 + i) % AXES for i in range(AXES)) for way in range(WAYS))
SIGNS = (1, -1) * AXES
TAKEN = (3, 0, 4, 1, 5, 2)


def place():
    me = lax.axis_index("dp")
    return (me // PLANE, me // SIDE % SIDE, me % SIDE)


def wrap(i):
    return (i + 3 * SIDE) % SIDE


def neighbour(at, axis, step):
    there = [c for c in at]
    there[axis] = wrap(at[axis] + step)
    return {"dp": (there[0] * SIDE + there[1]) * SIDE + there[2]}


def remote(src, dst, send, recv, to):
    return pltpu.make_async_remote_copy(src_ref=src, dst_ref=dst, send_sem=send, recv_sem=recv, device_id=to, device_id_type=MESH)


def enter(at):
    barrier = pltpu.get_barrier_semaphore()
    for axis in range(AXES):
        for step in range(STEPS):
            pl.semaphore_signal(barrier, inc=1, device_id=neighbour(at, axis, step + 1), device_id_type=MESH)
    pl.semaphore_wait(barrier, AXES * STEPS)


def norm_exchange(at, buf, send, recv, total):
    for axis in range(AXES):
        buf[axis, STEPS] = total
        copies = [
            remote(buf.at[axis, STEPS], buf.at[axis, k], send.at[axis], recv.at[axis, k], neighbour(at, axis, k + 1)) for k in range(STEPS)
        ]
        for copy in copies:
            copy.start()
        for k, copy in enumerate(copies):
            copy.wait_recv()
            total = total + buf[axis, k]
    return total


def passed_on(seen, c, phase, key):
    d1, d2, d3 = key
    if phase == 0 and d3 < STEPS:
        yield 0, (0, 0, d3 + 1)
    if phase < 2 and d2 < STEPS:
        yield 1, (0, d2 + 1, d3)
    if phase == 1 and d2 > 0:
        seen.append((c, d2))
        if seen.count((c, d2)) < SIDE:
            return
        d3 = None
    if d1 < STEPS:
        yield 2, (d1 + 1, d2, d3)


def ag_order(latency=1.8):
    import heapq

    free, out, seen, heap = {}, [], [], []

    def hold(t, c, phase, key):
        for phase, key in passed_on(seen, c, phase, key):
            link = ORDERS[c][2 - phase]
            size = SIDE if key[2] is None else 1
            free[link] = max(t, free.get(link, 0)) + size
            heapq.heappush(heap, (free[link] + latency, len(out) * WAYS + len(heap), c, phase, key))

    for c in range(0, WAYS, 2):
        hold(0, c, 0, (0, 0, 0))
    while heap:
        t, _, *arrival = heapq.heappop(heap)
        out.append(arrival)
        hold(t, *arrival)
    return out


def ag_kernel(*refs):
    mine, outs, (sends, recv1, recv2, recv3, recv4, local) = refs[0], refs[1 : 1 + WAYS], refs[1 + WAYS :]
    at = place()
    enter(at)

    def where(c, key):
        index = [None] * AXES
        for axis, d in zip(ORDERS[c], key, strict=True):
            index[axis] = slice(None) if d is None else wrap(at[axis] - SIGNS[c] * d)
        return outs[c].at[tuple(index)]

    def copy(c, phase, key, of_receiver):
        d1, d2, d3 = key
        back = list(key)
        if not of_receiver:
            back[2 - phase] -= 1
        there = where(c, back)
        src = mine.at[c] if not of_receiver and not any(back) and d3 is not None else there
        if phase == 0:
            recv = recv1.at[c, d3]
        elif phase == 1:
            recv = recv2.at[c, d2, d3]
        elif d3 is not None:
            recv = recv3.at[c, d1, d3]
        else:
            recv = recv4.at[c, d1, d2]
        return remote(src, there, sends.at[c, phase], recv, neighbour(at, ORDERS[c][2 - phase], SIGNS[c]))

    seen = []

    def hold(*held):
        for phase, key in passed_on(seen, *held):
            copy(held[0], phase, key, False).start()

    own = [pltpu.make_async_copy(mine.at[c], where(c, (0, 0, 0)), local.at[c]) for c in range(WAYS)]
    for c in range(WAYS):
        hold(c, 0, (0, 0, 0))
    for copied in own:
        copied.start()
    for even, phase, key in ag_order():
        for c in (even, even + 1):
            copy(c, phase, key, True).wait_recv()
            hold(c, phase, key)
    for c in range(WAYS):
        own[c].wait()
        sent = outs[c].at[pl.ds(0, STEPS)]
        for phase in (2, 1, 0):
            pltpu.make_async_copy(sent, sent, sends.at[c, phase]).wait()
            sent = outs[c].at[(0,) * (AXES - phase) + (pl.ds(0, STEPS),)]


def all_gather(mine):
    return pl.pallas_call(
        ag_kernel,
        out_shape=(pltpu.VMEM((SIDE, SIDE, SIDE, *mine.shape[1:]), BF16),) * WAYS,
        in_specs=[VMEM],
        out_specs=(VMEM,) * WAYS,
        scratch_shapes=[DMA((WAYS, AXES)), DMA((WAYS, SIDE)), *[DMA((WAYS, SIDE, SIDE))] * 3, DMA((WAYS,))],
        compiler_params=pltpu.CompilerParams(collective_id=1, has_side_effects=True, vmem_limit_bytes=MOST_VMEM // SUBLANES),
        name="gather",
    )(mine)


def tiles_of(t, rows, columns):
    n = columns // LANES
    if t < 2:
        return [(0, rows, j * LANES, j * rows) for j in range(n)]
    return [(8 * i, 8, j * LANES, (i * n + j) * 8) for i in range(rows // 8) for j in range(n)]


def adam_kernel(count, g, total, *refs):
    refs = list(refs)
    ws, ms, vs = (refs[AXES * k : AXES * (k + 1)] for k in range(3))
    new, *refs = refs[3 * AXES :]
    new_m, new_v, windows, owns = (refs[AXES * k : AXES * (k + 1)] for k in range(4))
    wide_g, wide_w, sems = refs[4 * AXES :]
    me = lax.axis_index("dp")
    taken = []
    for t in range(AXES):
        rows = windows[t].shape[1]
        first = pl.multiple_of((me // SIDE if t < 2 else me) * rows, SUBLANES)
        taken.append(pltpu.make_async_copy(ws[t].at[:, pl.ds(first, rows)], windows[t], sems.at[t]))
    for copy in taken:
        copy.start()
    factor = jnp.minimum(1.0, 0.5 * lax.rsqrt(jnp.full((1, 1), jnp.sum(total[...])) / count + 1e-30))
    for t in range(AXES):
        taken[t].wait()
        rows, columns = owns[t].shape[1:]
        if t < 2:
            for z in range(SIDE):

                @pl.when(me % SIDE == z)
                def _():
                    for l in range(LAYERS):
                        owns[t][l] = windows[t][l].astype(F32)[z * rows : (z + 1) * rows]

        for l in range(LAYERS):
            wide_g[...] = g[TAKEN[LAYERS * t + l]].astype(F32) * factor
            for row, n, column, at in tiles_of(t, rows, columns):
                lanes = pl.ds(column, LANES)
                here = (slice(None), l, lanes) if t < 2 else (l, pl.ds(row, n), lanes)
                grad = wide_g[pl.ds(at, n), :]
                m = 0.9 * ms[t][here] + 0.1 * grad
                v = 0.95 * vs[t][here] + 0.05 * grad * grad
                w = (owns if t < 2 else windows)[t][l, pl.ds(row, n), lanes].astype(F32)
                new_m[t][here] = m
                new_v[t][here] = v
                wide_w[pl.ds(at, n), :] = w - 0.02 * (m * lax.rsqrt(v + 1e-8) + 0.1 * w)
            new[LAYERS * t + l] = wide_w[...].astype(BF16)


def adam(count, g, total, ws, ms, vs):
    ms, vs = ([*(jnp.swapaxes(a, 0, 1) for a in arrays[:2]), arrays[2]] for arrays in (ms, vs))
    like = [jax.ShapeDtypeStruct(m.shape, F32) for m in ms]
    new, *moments = pl.pallas_call(
        functools.partial(adam_kernel, count),
        out_shape=(pltpu.VMEM(g.shape, BF16), *like, *like),
        in_specs=[VMEM] * 2 + [HBM] * AXES + [VMEM] * AXES * 2,
        out_specs=(VMEM,) * (1 + AXES * 2),
        scratch_shapes=[
            *[pltpu.VMEM((LAYERS, w.shape[1] // n, w.shape[2]), BF16) for w, n in zip(ws, (PLANE, PLANE, DEVICES), strict=True)],
            *[pltpu.VMEM((LAYERS, w.shape[1] // DEVICES, w.shape[2]), F32) for w in ws],
            *[pltpu.VMEM(g.shape[1:], F32)] * 2,
            DMA((AXES,)),
        ],
        compiler_params=pltpu.CompilerParams(vmem_limit_bytes=MOST_VMEM),
        name="adam",
    )(g, total, *ws, *ms, *vs)
    return new, *([*(jnp.swapaxes(a, 0, 1) for a in part[:2]), part[2]] for part in (moments[:AXES], moments[AXES:]))


def natural_kernel(*refs):
    gathered, outs, wide = refs[:MATRICES], refs[MATRICES:-AXES], refs[-AXES:]
    first = pl.program_id(0) * SIDE
    for t in range(AXES):
        for l in range(LAYERS):
            for z in range(SIDE):
                block = gathered[LAYERS * t + l][first + z].astype(F32)
                rows = outs[t].shape[1] // SIDE
                for row, n, column, at in tiles_of(t, rows, outs[t].shape[2]):
                    wide[t][pl.ds(z * rows + row, n), pl.ds(column, LANES)] = block[at : at + n]
            outs[t][l] = wide[t][...].astype(BF16)


def natural(gathered):
    shapes = (GATE, GATE, DOWN)
    return pl.pallas_call(
        natural_kernel,
        grid=(PLANE,),
        out_shape=tuple(jax.ShapeDtypeStruct((LAYERS, *s), BF16) for s in shapes),
        in_specs=[VMEM] * MATRICES,
        out_specs=tuple(pl.BlockSpec((LAYERS, s[0] // PLANE, s[1]), lambda i: (0, i, 0)) for s in shapes),
        scratch_shapes=[pltpu.VMEM((s[0] // PLANE, s[1]), F32) for s in shapes],
        compiler_params=pltpu.CompilerParams(vmem_limit_bytes=MOST_VMEM // SIDE),
        name="natural",
    )(*[g.reshape(DEVICES, BLOCK, LANES) for g in gathered])


D, FF, TOKENS = 896, 2560, 2048
GATE, DOWN = (D, FF), (FF, D)
ROWS, CHUNK, TILE = 256, 512, 512
TILES, PIECE, PLANE_ROWS = FF // TILE, BLOCK * TILE // FF, FF // SIDE
NT = (((1,), (1,)), ((), ()))


def dot(a, b):
    return jnp.dot(a, b, preferred_element_type=F32)


def dot_t(a, b):
    return lax.dot_general(a, b, NT, preferred_element_type=F32)


def scale_of(wide):
    return lax.rsqrt(jnp.mean(wide * wide, -1, keepdims=True) + 1e-6)


def rows_kernel(x, dy, *refs):
    hbm, (tall, wide, turned, deep), weights, (g0, u0, z0, sems) = refs[:3], refs[3:7], refs[7:13], refs[13:]
    wg0, wu0, wd0, wg1, wu1, wd1 = weights
    first = pl.program_id(0) == 0

    def fetch(k):
        return pltpu.make_async_copy(hbm[k % 3].at[k // 3], weights[k], sems.at[k])

    @pl.when(first)
    def _():
        for k in range(2):
            fetch(k).start()

    def ready(*ks):
        @pl.when(first)
        def _():
            for k in ks:
                fetch(k).wait()
            if 0 in ks:
                for k in range(2, MATRICES):
                    fetch(k).start()

    a = (x[...].astype(F32) * scale_of(x[...].astype(F32))).astype(BF16)
    tall[1] = a.T
    deep[0] = dy[...]
    ready(0, 1)
    for j in range(FF // CHUNK):
        ch = pl.ds(j * CHUNK, CHUNK)
        gate, up = dot(a, wg0[:, ch]), dot(a, wu0[:, ch])
        g0[:, ch], u0[:, ch] = gate, up
        z0[:, ch] = (gate * jax.nn.sigmoid(gate) * up).astype(BF16)
        turned[1, ch, :] = z0[:, ch].T
    ready(2)
    h = x[...] + dot(z0[...], wd0[...]).astype(BF16)
    h = h.astype(F32)
    scale = scale_of(h)
    a = (h * scale).astype(BF16)
    tall[0] = a.T
    ready(3, 4, 5)
    for j in range(FF // CHUNK):
        ch = pl.ds(j * CHUNK, CHUNK)
        gate, up = dot(a, wg1[:, ch]), dot(a, wu1[:, ch])
        dz = dot_t(dy[...], wd1[ch, :]).astype(BF16).astype(F32)
        s = jax.nn.sigmoid(gate)
        silu = gate * s
        turned[0, ch, :] = (silu * up).astype(BF16).T
        wide[1, :, ch] = (dz * silu).astype(BF16)
        wide[0, :, ch] = (dz * up * (s * (1 + gate * (1 - s)))).astype(BF16)
    da = dot_t(wide[0], wg1[...]).astype(BF16) + dot_t(wide[1], wu1[...]).astype(BF16)
    da = da.astype(F32)
    dwide = scale * (da - h * (scale * scale * jnp.mean(da * h, -1, keepdims=True)))
    dh = dy[...] + dwide.astype(BF16)
    deep[1] = dh
    for j in range(FF // CHUNK):
        ch = pl.ds(j * CHUNK, CHUNK)
        dz = dot_t(dh, wd0[ch, :]).astype(BF16).astype(F32)
        gate, up = g0[:, ch], u0[:, ch]
        s = jax.nn.sigmoid(gate)
        wide[3, :, ch] = (dz * (gate * s)).astype(BF16)
        wide[2, :, ch] = (dz * up * (s * (1 + gate * (1 - s)))).astype(BF16)


def by_rows(x, dy, weights):
    state = pl.BlockSpec((ROWS, D), lambda i: (i, 0))
    return pl.pallas_call(
        rows_kernel,
        grid=(TOKENS // ROWS,),
        out_shape=tuple(jax.ShapeDtypeStruct(s, BF16) for s in ((2, D, TOKENS), (4, TOKENS, FF), (2, FF, TOKENS), (2, TOKENS, D))),
        in_specs=[state, state] + [HBM] * 3,
        out_specs=(
            pl.BlockSpec((2, D, ROWS), lambda i: (0, 0, i)),
            pl.BlockSpec((4, ROWS, FF), lambda i: (0, i, 0)),
            pl.BlockSpec((2, FF, ROWS), lambda i: (0, 0, i)),
            pl.BlockSpec((2, ROWS, D), lambda i: (0, i, 0)),
        ),
        scratch_shapes=[*[pltpu.VMEM(w.shape[1:], BF16) for w in weights * 2], pltpu.VMEM((ROWS, FF), F32), pltpu.VMEM((ROWS, FF), F32), pltpu.VMEM((ROWS, FF), BF16), DMA((MATRICES,))],
        compiler_params=pltpu.CompilerParams(vmem_limit_bytes=MOST_VMEM),
        name="rows",
    )(x, dy, *weights)


STARTS = (0, 48, 96, 144, 192, 232)
PART = 48


def gate_block(acc, stage, wide):
    def group(i, _):
        rows = pl.ds(pl.multiple_of(i * 56, 8), 56)
        for c in range(4):
            piece = acc[rows, pl.ds(c * LANES, LANES)]
            for z in range(4):
                wide[z, pl.ds(14 * c, 14), :] = piece[14 * z : 14 * z + 14]
        for z in range(4):
            stage[i // 4, i % 4, z] = wide[z].astype(BF16)
        return 0

    lax.fori_loop(0, 16, group, 0)


def down_block(acc, stage):
    def group(i, _):
        for t in range(5):
            rows = acc[pl.ds(pl.multiple_of(i * 40, 8) + 8 * t, 8), :]
            piece = jnp.concatenate([rows[:, c * LANES : (c + 1) * LANES] for c in range(7)], 0)
            stage[i // 4, i % 4, pl.ds(56 * t, 56)] = piece.astype(BF16)
        return 0

    lax.fori_loop(0, 16, group, 0)


def gradients_kernel(*refs):
    (tall, wide, turned, deep), (out, squares, terms), scratch = refs[:4], refs[4:7], refs[7:]
    (lhs, rhs, zs, dh, acc, acc2, stage, stage2, shift, r1, r2, r3, own, f1, f2, sums) = scratch[:16]
    (in_sem, rhs_sem, zs_sem, put_sem, send1, send2, send3, recv1, recv2, recv3, load, send4, recv4) = scratch[16:]
    at = place()

    def fetch_tall(l):
        return pltpu.make_async_copy(tall.at[l], lhs, in_sem.at[0])

    def fetch_deep(l):
        return pltpu.make_async_copy(deep.at[l], dh, in_sem.at[1])

    def fetch_wide(t):
        columns = pl.ds(pl.multiple_of(t % TILES * TILE, TILE), TILE)
        return pltpu.make_async_copy(wide.at[t // TILES, :, columns], rhs.at[t % 2], rhs_sem.at[t % 2])

    def fetch_turned(t):
        rows = pl.ds(pl.multiple_of(t % SIDE * PLANE_ROWS, LANES), PLANE_ROWS)
        return pltpu.make_async_copy(turned.at[t // SIDE, rows], zs.at[t % 2], zs_sem.at[t % 2])

    def put(m, h):
        return pltpu.make_async_copy(stage, terms.at[m, :, :, :, pl.ds(pl.multiple_of(PIECE * h, SUBLANES), PIECE)], put_sem.at[0])

    def put2(m, h):
        return pltpu.make_async_copy(stage2, terms.at[m, h], put_sem.at[1])

    fetch_tall(0).start()
    fetch_wide(0).start()
    fetch_deep(0).start()
    fetch_turned(0).start()
    enter(at)

    def split(c):
        o, s = ORDERS[c], SIGNS[c]
        return o, s, at[o[0]], at[o[1]], at[o[2]]

    def block(m, c, a, i):
        o = ORDERS[c]
        index = [slice(None)] * 3
        index[o[0]] = a
        if i is not None:
            index[o[1]] = i
        return terms.at[(m, *index, pl.ds(STARTS[c], PART))]

    def first(m, c, step, j, start=False):
        o, s, p1, p2, p3 = split(c)
        if start:
            src = block(m, c, wrap(p1 - s), wrap(p2 - s * (1 + j)))
        else:
            src = r1.at[c, m, (step + 2) % STEPS, j]
        return remote(src, r1.at[c, m, step, j], send1.at[c], recv1.at[c, m, step, j], neighbour(at, o[0], s))

    def loading(m, c, step):
        o, s, p1, p2, p3 = split(c)
        return pltpu.make_async_copy(block(m, c, wrap(p1 - s * (2 + step)), None), own.at[c, step], load.at[c, step])

    def second(m, c, step, start=False):
        o, s, p1, p2, p3 = split(c)
        src = r1.at[c, m, 2, 0] if start else r2.at[c, m, (step + 2) % STEPS]
        return remote(src, r2.at[c, m, step], send2.at[c], recv2.at[c, m, step], neighbour(at, o[1], s))

    def third(m, c, k):
        o, s, p1, p2, p3 = split(c)
        return remote(r2.at[c, m, 2, wrap(p3 + k + 1)], r3.at[c, m, k], send3.at[c], recv3.at[c, m, k], neighbour(at, o[2], k + 1))

    def launch(m):
        for c in range(WAYS):
            for j in range(SIDE):
                first(m, c, 0, j, True).start()
    def load_own(m):
        for step in range(STEPS):
            for c in range(WAYS):
                loading(m, c, step).start()

    def on_first(m, e):
        step, j = e // SIDE, e % SIDE

        @pl.when(j == 0)
        def _():
            for c in range(WAYS):
                loading(m, c, step).wait()

        for c in range(WAYS):
            o, s, p1, p2, p3 = split(c)
            first(m, c, step, j).wait_recv()
            i = wrap(p2 - s * (1 + j))
            mine = own[c, step, i] if o[1] < o[2] else own[c, step, :, i]
            both = r1[c, m, step, j].astype(F32) + mine.astype(F32)
            r1[c, m, step, j] = both.astype(BF16)

            @pl.when(step == 2)
            def _():
                f1[c, j] = both

            @pl.when(step < 2)
            def _():
                first(m, c, step + 1, j).start()

            @pl.when(e == 8)
            def _():
                second(m, c, 0, True).start()

    def on_second(m, step):
        for c in range(WAYS):
            second(m, c, step).wait_recv()
            both = r2[c, m, step].astype(F32) + f1[c, step + 1]
            r2[c, m, step] = both.astype(BF16)

            @pl.when(step == 2)
            def _():
                f2[c] = both
                for k in range(STEPS):
                    third(m, c, k).start()

            @pl.when(step < 2)
            def _():
                second(m, c, step + 1).start()

    def on_third(m):
        for c in range(WAYS):
            o, s, p1, p2, p3 = split(c)
            total = f2[c, p3]
            for k in range(STEPS):
                third(m, c, k).wait_recv()
                total = total + r3[c, m, k].astype(F32)
            out[m, pl.ds(STARTS[c], PART)] = total.astype(BF16)

    def tile(i, _):
        m, h = i // TILES, i % TILES
        kind, l = m % AXES, m // AXES

        @pl.when((h == 0) & (m > 0) & (m < MATRICES + 1))
        def _():
            @pl.when(kind > 0)
            def _():
                put(0, 0).wait()

            @pl.when(kind == 0)
            def _():
                put2(0, 0).wait()

            launch(m - 1)

        @pl.when((m < MATRICES) & (kind < 2))
        def _():
            t = (2 * l + kind) * TILES + h

            @pl.when((kind == 0) & (h == 0))
            def _():
                fetch_tall(l).wait()

                @pl.when(l == 1)
                def _():
                    fetch_deep(1).start()

            fetch_wide(t).wait()

            @pl.when(t < 19)
            def _():
                fetch_wide(t + 1).start()

            acc[...] = dot(lhs[...], rhs[t % 2])

            @pl.when(h > 0)
            def _():
                put(m, h).wait()

            gate_block(acc, stage, shift)
            put(m, h).start()

        @pl.when((m < MATRICES) & (kind == 2) & (h < SIDE))
        def _():
            t = SIDE * l + h

            @pl.when(h == 0)
            def _():
                fetch_deep(l).wait()

                @pl.when(l == 0)
                def _():
                    fetch_tall(1).start()

            fetch_turned(t).wait()

            @pl.when(t < 7)
            def _():
                fetch_turned(t + 1).start()

            acc2[...] = dot(zs[t % 2], dh[...])

            @pl.when(h > 0)
            def _():
                put2(m, h).wait()

            down_block(acc2, stage2)
            put2(m, h).start()

        @pl.when((h == SIDE) & (m > 1))
        def _():
            on_third(m - 2)

        @pl.when((h != 1) & (h != SIDE) & (m > 1) & (m < MATRICES + 2))
        def _():
            on_second(m - 2, (h + 1) // 2)

        ring, turn = (i - 1) // TILES - 1, (i - 1) % TILES

        @pl.when((ring >= 0) & (ring < MATRICES))
        def _():
            lax.fori_loop(TILES * turn // 2, TILES * (turn + 1) // 2, lambda e, _: (on_first(ring, e), 0)[1], 0)

        @pl.when((h == 0) & (m > 0) & (m < MATRICES + 1))
        def _():
            load_own(m - 1)

        return 0

    lax.fori_loop(0, (MATRICES + 2) * TILES, tile, 0)

    total = jnp.zeros((SUBLANES, LANES), F32)
    for m in range(MATRICES):
        g = out[m].astype(F32)
        total = total + jnp.sum((g * g).reshape(-1, SUBLANES, LANES), axis=0)
    squares[...] = norm_exchange(at, sums, send4, recv4, total)
    for c in range(WAYS):
        for r, sem in ((r1, send1), (r2, send2), (r3, send3)):
            pltpu.make_async_copy(r.at[c], r.at[c], sem.at[c]).wait()
    for axis in range(STEPS):
        pltpu.make_async_copy(sums.at[axis, pl.ds(0, STEPS)], sums.at[axis, pl.ds(0, STEPS)], send4.at[axis]).wait()


def gradients(tall, wide, turned, deep):
    g, squares, _ = pl.pallas_call(
        gradients_kernel,
        out_shape=(
            jax.ShapeDtypeStruct((MATRICES, BLOCK, LANES), BF16),
            jax.ShapeDtypeStruct((SUBLANES, LANES), F32),
            jax.ShapeDtypeStruct((MATRICES, SIDE, SIDE, SIDE, BLOCK, LANES), BF16),
        ),
        in_specs=[HBM] * 4,
        out_specs=(VMEM, VMEM, HBM),
        scratch_shapes=[
            pltpu.VMEM((D, TOKENS), BF16),
            pltpu.VMEM((2, TOKENS, TILE), BF16),
            pltpu.VMEM((2, PLANE_ROWS, TOKENS), BF16),
            pltpu.VMEM((TOKENS, D), BF16),
            pltpu.VMEM((D, TILE), F32),
            pltpu.VMEM((PLANE_ROWS, D), F32),
            pltpu.VMEM((SIDE, SIDE, SIDE, PIECE, LANES), BF16),
            pltpu.VMEM((SIDE, SIDE, BLOCK, LANES), BF16),
            pltpu.VMEM((SIDE, PIECE, LANES), F32),
            pltpu.VMEM((WAYS, MATRICES, STEPS, SIDE, SIDE, PART, LANES), BF16),
            pltpu.VMEM((WAYS, MATRICES, STEPS, SIDE, PART, LANES), BF16),
            pltpu.VMEM((WAYS, MATRICES, STEPS, PART, LANES), BF16),
            pltpu.VMEM((WAYS, STEPS, SIDE, SIDE, PART, LANES), BF16),
            pltpu.VMEM((WAYS, SIDE, SIDE, PART, LANES), F32),
            pltpu.VMEM((WAYS, SIDE, PART, LANES), F32),
            pltpu.VMEM((AXES, SIDE, SUBLANES, LANES), F32),
            *[DMA((2,))] * 4,
            *[DMA((WAYS,))] * AXES,
            DMA((WAYS, MATRICES, STEPS, SIDE)), *[DMA((WAYS, MATRICES, STEPS))] * 2,
            DMA((WAYS, STEPS)),
            DMA((AXES,)), DMA((AXES, STEPS)),
        ],
        compiler_params=pltpu.CompilerParams(collective_id=0, has_side_effects=True, vmem_limit_bytes=MOST_VMEM),
        name="gradients",
    )(tall, wide, turned, deep)
    return g, squares


def solution(mesh):
    rep, dp = mesh.axis_names

    def step(x, dy, *arrays):
        weights, m, v = (arrays[i : i + 3] for i in (0, 3, 6))
        g, total = gradients(*by_rows(x[0], dy[0], weights))
        new, new_m, new_v = adam(sum(w.size for w in weights), g, total, weights, m, v)
        return (*natural(all_gather(new)), *new_m, *new_v)

    whole, rows, sequences = P(None, None, None), P(None, dp, None), P((rep, dp), None, None)
    return jax.shard_map(
        step,
        mesh=mesh,
        in_specs=(sequences, sequences, *[whole] * 3, *[rows] * 6),
        out_specs=(*[P(rep, None, None)] * 3, *[P(rep, dp, None)] * 6),
        check_vma=False,
    )
```

```python
import functools
import jax
import jax.numpy as jnp
from jax import lax
from jax.experimental import pallas as pl
from jax.experimental.pallas import tpu as pltpu
from jax.sharding import PartitionSpec as P

MESH = pl.DeviceIdType.MESH
WAYS, AXES, SIDE = 6, 3, 4
STEPS = SIDE - 1
MATRICES, LAYERS, DEVICES, PLANE = 6, 2, 64, 16
LANES, SUBLANES, BLOCK = 128, 8, 280
BF16, F32 = jnp.bfloat16, jnp.float32
HBM, VMEM = pl.BlockSpec(memory_space=pl.ANY), pl.BlockSpec(memory_space=pltpu.VMEM)
DMA = pltpu.SemaphoreType.DMA
MOST_VMEM = 62 * 1024 * 1024
ORDERS = tuple(tuple((way // 2 + i) % AXES for i in range(AXES)) for way in range(WAYS))
SIGNS = (1, -1) * AXES
TAKEN = (3, 0, 4, 1, 5, 2)


def place():
    me = lax.axis_index("dp")
    return (me // PLANE, me // SIDE % SIDE, me % SIDE)


def wrap(i):
    return (i + 3 * SIDE) % SIDE


def neighbour(at, axis, step):
    there = [c for c in at]
    there[axis] = wrap(at[axis] + step)
    return {"dp": (there[0] * SIDE + there[1]) * SIDE + there[2]}


def remote(src, dst, send, recv, to):
    return pltpu.make_async_remote_copy(src_ref=src, dst_ref=dst, send_sem=send, recv_sem=recv, device_id=to, device_id_type=MESH)


def enter(at):
    barrier = pltpu.get_barrier_semaphore()
    for axis in range(AXES):
        for step in range(STEPS):
            pl.semaphore_signal(barrier, inc=1, device_id=neighbour(at, axis, step + 1), device_id_type=MESH)
    pl.semaphore_wait(barrier, AXES * STEPS)


def norm_exchange(at, buf, send, recv, total):
    for axis in range(AXES):
        buf[axis, STEPS] = total
        copies = [
            remote(buf.at[axis, STEPS], buf.at[axis, k], send.at[axis], recv.at[axis, k], neighbour(at, axis, k + 1)) for k in range(STEPS)
        ]
        for copy in copies:
            copy.start()
        for k, copy in enumerate(copies):
            copy.wait_recv()
            total = total + buf[axis, k]
    return total


def passed_on(seen, c, phase, key):
    d1, d2, d3 = key
    if phase == 0 and d3 < STEPS:
        yield 0, (0, 0, d3 + 1)
    if phase < 2 and d2 < STEPS:
        yield 1, (0, d2 + 1, d3)
    if phase == 1 and d2 > 0:
        seen.append((c, d2))
        if seen.count((c, d2)) < SIDE:
            return
        d3 = None
    if d1 < STEPS:
        yield 2, (d1 + 1, d2, d3)


def ag_order(latency=1.8):
    import heapq

    free, out, seen, heap = {}, [], [], []

    def hold(t, c, phase, key):
        for phase, key in passed_on(seen, c, phase, key):
            link = ORDERS[c][2 - phase]
            size = SIDE if key[2] is None else 1
            free[link] = max(t, free.get(link, 0)) + size
            heapq.heappush(heap, (free[link] + latency, len(out) * WAYS + len(heap), c, phase, key))

    for c in range(0, WAYS, 2):
        hold(0, c, 0, (0, 0, 0))
    while heap:
        t, _, *arrival = heapq.heappop(heap)
        out.append(arrival)
        hold(t, *arrival)
    return out


def ag_kernel(*refs):
    mine, outs, (sends, recv1, recv2, recv3, recv4, local) = refs[0], refs[1 : 1 + WAYS], refs[1 + WAYS :]
    at = place()
    enter(at)

    def where(c, key):
        index = [None] * AXES
        for axis, d in zip(ORDERS[c], key, strict=True):
            index[axis] = slice(None) if d is None else wrap(at[axis] - SIGNS[c] * d)
        return outs[c].at[tuple(index)]

    def copy(c, phase, key, of_receiver):
        d1, d2, d3 = key
        back = list(key)
        if not of_receiver:
            back[2 - phase] -= 1
        there = where(c, back)
        src = mine.at[c] if not of_receiver and not any(back) and d3 is not None else there
        if phase == 0:
            recv = recv1.at[c, d3]
        elif phase == 1:
            recv = recv2.at[c, d2, d3]
        elif d3 is not None:
            recv = recv3.at[c, d1, d3]
        else:
            recv = recv4.at[c, d1, d2]
        return remote(src, there, sends.at[c, phase], recv, neighbour(at, ORDERS[c][2 - phase], SIGNS[c]))

    seen = []

    def hold(*held):
        for phase, key in passed_on(seen, *held):
            copy(held[0], phase, key, False).start()

    own = [pltpu.make_async_copy(mine.at[c], where(c, (0, 0, 0)), local.at[c]) for c in range(WAYS)]
    for c in range(WAYS):
        hold(c, 0, (0, 0, 0))
    for copied in own:
        copied.start()
    for even, phase, key in ag_order():
        for c in (even, even + 1):
            copy(c, phase, key, True).wait_recv()
            hold(c, phase, key)
    for c in range(WAYS):
        own[c].wait()
        sent = outs[c].at[pl.ds(0, STEPS)]
        for phase in (2, 1, 0):
            pltpu.make_async_copy(sent, sent, sends.at[c, phase]).wait()
            sent = outs[c].at[(0,) * (AXES - phase) + (pl.ds(0, STEPS),)]


def all_gather(mine):
    return pl.pallas_call(
        ag_kernel,
        out_shape=(pltpu.VMEM((SIDE, SIDE, SIDE, *mine.shape[1:]), BF16),) * WAYS,
        in_specs=[VMEM],
        out_specs=(VMEM,) * WAYS,
        scratch_shapes=[DMA((WAYS, AXES)), DMA((WAYS, SIDE)), *[DMA((WAYS, SIDE, SIDE))] * 3, DMA((WAYS,))],
        compiler_params=pltpu.CompilerParams(collective_id=1, has_side_effects=True, vmem_limit_bytes=MOST_VMEM // SUBLANES),
        name="gather",
    )(mine)


def tiles_of(t, rows, columns):
    n = columns // LANES
    if t < 2:
        return [(0, rows, j * LANES, j * rows) for j in range(n)]
    return [(8 * i, 8, j * LANES, (i * n + j) * 8) for i in range(rows // 8) for j in range(n)]


def adam_kernel(count, g, total, *refs):
    refs = list(refs)
    ws, ms, vs = (refs[AXES * k : AXES * (k + 1)] for k in range(3))
    new, *refs = refs[3 * AXES :]
    new_m, new_v, windows, owns = (refs[AXES * k : AXES * (k + 1)] for k in range(4))
    wide_g, wide_w, sems = refs[4 * AXES :]
    me = lax.axis_index("dp")
    taken = []
    for t in range(AXES):
        rows = windows[t].shape[1]
        first = pl.multiple_of((me // SIDE if t < 2 else me) * rows, SUBLANES)
        taken.append(pltpu.make_async_copy(ws[t].at[:, pl.ds(first, rows)], windows[t], sems.at[t]))
    for copy in taken:
        copy.start()
    factor = jnp.minimum(1.0, 0.5 * lax.rsqrt(jnp.full((1, 1), jnp.sum(total[...])) / count + 1e-30))
    for t in range(AXES):
        taken[t].wait()
        rows, columns = owns[t].shape[1:]
        if t < 2:
            for z in range(SIDE):

                @pl.when(me % SIDE == z)
                def _():
                    for l in range(LAYERS):
                        owns[t][l] = windows[t][l].astype(F32)[z * rows : (z + 1) * rows]

        for l in range(LAYERS):
            wide_g[...] = g[TAKEN[LAYERS * t + l]].astype(F32) * factor
            for row, n, column, at in tiles_of(t, rows, columns):
                lanes = pl.ds(column, LANES)
                here = (slice(None), l, lanes) if t < 2 else (l, pl.ds(row, n), lanes)
                grad = wide_g[pl.ds(at, n), :]
                m = 0.9 * ms[t][here] + 0.1 * grad
                v = 0.95 * vs[t][here] + 0.05 * grad * grad
                w = (owns if t < 2 else windows)[t][l, pl.ds(row, n), lanes].astype(F32)
                new_m[t][here] = m
                new_v[t][here] = v
                wide_w[pl.ds(at, n), :] = w - 0.02 * (m * lax.rsqrt(v + 1e-8) + 0.1 * w)
            new[LAYERS * t + l] = wide_w[...].astype(BF16)


def adam(count, g, total, ws, ms, vs):
    ms, vs = ([*(jnp.swapaxes(a, 0, 1) for a in arrays[:2]), arrays[2]] for arrays in (ms, vs))
    like = [jax.ShapeDtypeStruct(m.shape, F32) for m in ms]
    new, *moments = pl.pallas_call(
        functools.partial(adam_kernel, count),
        out_shape=(pltpu.VMEM(g.shape, BF16), *like, *like),
        in_specs=[VMEM] * 2 + [HBM] * AXES + [VMEM] * AXES * 2,
        out_specs=(VMEM,) * (1 + AXES * 2),
        scratch_shapes=[
            *[pltpu.VMEM((LAYERS, w.shape[1] // n, w.shape[2]), BF16) for w, n in zip(ws, (PLANE, PLANE, DEVICES), strict=True)],
            *[pltpu.VMEM((LAYERS, w.shape[1] // DEVICES, w.shape[2]), F32) for w in ws],
            *[pltpu.VMEM(g.shape[1:], F32)] * 2,
            DMA((AXES,)),
        ],
        compiler_params=pltpu.CompilerParams(vmem_limit_bytes=MOST_VMEM),
        name="adam",
    )(g, total, *ws, *ms, *vs)
    return new, *([*(jnp.swapaxes(a, 0, 1) for a in part[:2]), part[2]] for part in (moments[:AXES], moments[AXES:]))


def natural_kernel(*refs):
    gathered, outs, wide = refs[:MATRICES], refs[MATRICES:-AXES], refs[-AXES:]
    first = pl.program_id(0) * SUBLANES
    for t in range(AXES):
        for l in range(LAYERS):
            rows, columns = outs[t].shape[1:]
            for k in range(SUBLANES):
                block = gathered[LAYERS * t + l][first + k].astype(F32)
                for row, n, column, at in tiles_of(t, rows // SUBLANES, columns):
                    wide[t][pl.ds(k * rows // SUBLANES + row, n), pl.ds(column, LANES)] = block[at : at + n]
            outs[t][l] = wide[t][...].astype(BF16)


def natural(gathered):
    shapes = (GATE, GATE, DOWN)
    return pl.pallas_call(
        natural_kernel,
        grid=(SUBLANES,),
        out_shape=tuple(jax.ShapeDtypeStruct((LAYERS, *s), BF16) for s in shapes),
        in_specs=[VMEM] * MATRICES,
        out_specs=tuple(pl.BlockSpec((LAYERS, s[0] // SUBLANES, s[1]), lambda i: (0, i, 0)) for s in shapes),
        scratch_shapes=[pltpu.VMEM((s[0] // SUBLANES, s[1]), F32) for s in shapes],
        compiler_params=pltpu.CompilerParams(vmem_limit_bytes=MOST_VMEM // SIDE),
        name="natural",
    )(*[g.reshape(DEVICES, BLOCK, LANES) for g in gathered])


D, FF, TOKENS = 896, 2560, 2048
GATE, DOWN = (D, FF), (FF, D)
ROWS, CHUNK, TILE = 256, 256, 512
TILES, PIECE, PLANE_ROWS = FF // TILE, BLOCK * TILE // FF, FF // SIDE
NT = (((1,), (1,)), ((), ()))


def dot(a, b):
    return jnp.dot(a, b, preferred_element_type=F32)


def dot_t(a, b):
    return lax.dot_general(a, b, NT, preferred_element_type=F32)


def scale_of(wide):
    return lax.rsqrt(jnp.mean(wide * wide, -1, keepdims=True) + 1e-6)


def rows_kernel(x, dy, *refs):
    hbm, (tall, wide, turned, deep), weights, (g0, u0, z0, dz1, sems) = refs[:3], refs[3:7], refs[7:13], refs[13:]
    wg0, wu0, wd0, wg1, wu1, wd1 = weights
    first = pl.program_id(0) == 0

    def fetch(k):
        return pltpu.make_async_copy(hbm[k % 3].at[k // 3], weights[k], sems.at[k])

    @pl.when(first)
    def _():
        for k in range(2):
            fetch(k).start()

    def ready(*ks):
        @pl.when(first)
        def _():
            for k in ks:
                fetch(k).wait()
            if 0 in ks:
                for k in range(2, MATRICES):
                    fetch(k).start()

    a = (x[...].astype(F32) * scale_of(x[...].astype(F32))).astype(BF16)
    tall[1] = a.T
    deep[0] = dy[...]
    chunks = [pl.ds(j * CHUNK, CHUNK) for j in range(FF // CHUNK)]
    ready(0, 1)
    for ch in chunks:
        gate, up = dot(a, wg0[:, ch]), dot(a, wu0[:, ch])
        g0[:, ch], u0[:, ch] = gate, up
        z0[:, ch] = (gate * jax.nn.sigmoid(gate) * up).astype(BF16)
        turned[1, ch, :] = z0[:, ch].T
    ready(2, 3, 4, 5)
    for ch in chunks[:SIDE]:
        dz1[:, ch] = dot_t(dy[...], wd1[ch, :]).astype(BF16)
    h = x[...] + dot(z0[...], wd0[...]).astype(BF16)
    for ch in chunks[SIDE:]:
        dz1[:, ch] = dot_t(dy[...], wd1[ch, :]).astype(BF16)
    h = h.astype(F32)
    scale = scale_of(h)
    a = (h * scale).astype(BF16)
    tall[0] = a.T
    for ch in chunks:
        gate, up = dot(a, wg1[:, ch]), dot(a, wu1[:, ch])
        dz = dz1[:, ch].astype(F32)
        s = jax.nn.sigmoid(gate)
        silu = gate * s
        turned[0, ch, :] = (silu * up).astype(BF16).T
        wide[1, :, ch] = (dz * silu).astype(BF16)
        wide[0, :, ch] = (dz * up * (s * (1 + gate * (1 - s)))).astype(BF16)
    most, rest = pl.ds(0, FF - CHUNK), chunks[-1]
    da_gate, da_up = dot_t(wide[0, :, most], wg1[:, most]), dot_t(wide[1, :, most], wu1[:, most])
    da_gate, da_up = da_gate + dot_t(wide[0, :, rest], wg1[:, rest]), da_up + dot_t(wide[1, :, rest], wu1[:, rest])
    da = (da_gate.astype(BF16) + da_up.astype(BF16)).astype(F32)
    dwide = scale * (da - h * (scale * scale * jnp.mean(da * h, -1, keepdims=True)))
    dh = dy[...] + dwide.astype(BF16)
    deep[1] = dh
    for ch in chunks:
        dz = dot_t(dh, wd0[ch, :]).astype(BF16).astype(F32)
        gate, up = g0[:, ch], u0[:, ch]
        s = jax.nn.sigmoid(gate)
        wide[3, :, ch] = (dz * (gate * s)).astype(BF16)
        wide[2, :, ch] = (dz * up * (s * (1 + gate * (1 - s)))).astype(BF16)


def by_rows(x, dy, weights):
    state = pl.BlockSpec((ROWS, D), lambda i: (i, 0))
    return pl.pallas_call(
        rows_kernel,
        grid=(TOKENS // ROWS,),
        out_shape=tuple(jax.ShapeDtypeStruct(s, BF16) for s in ((2, D, TOKENS), (4, TOKENS, FF), (2, FF, TOKENS), (2, TOKENS, D))),
        in_specs=[state, state] + [HBM] * 3,
        out_specs=(
            pl.BlockSpec((2, D, ROWS), lambda i: (0, 0, i)),
            pl.BlockSpec((4, ROWS, FF), lambda i: (0, i, 0)),
            pl.BlockSpec((2, FF, ROWS), lambda i: (0, 0, i)),
            pl.BlockSpec((2, ROWS, D), lambda i: (0, i, 0)),
        ),
        scratch_shapes=[*[pltpu.VMEM(w.shape[1:], BF16) for w in weights * 2], pltpu.VMEM((ROWS, FF), F32), pltpu.VMEM((ROWS, FF), F32), pltpu.VMEM((ROWS, FF), BF16), pltpu.VMEM((ROWS, FF), BF16), DMA((MATRICES,))],
        compiler_params=pltpu.CompilerParams(vmem_limit_bytes=MOST_VMEM),
        name="rows",
    )(x, dy, *weights)


STARTS = (0, 48, 96, 144, 192, 232)
PART = 48


def gate_block(acc, stage, wide):
    def group(i, _):
        rows = pl.ds(pl.multiple_of(i * 56, 8), 56)
        for c in range(4):
            piece = acc[rows, pl.ds(c * LANES, LANES)]
            for z in range(4):
                wide[z, pl.ds(14 * c, 14), :] = piece[14 * z : 14 * z + 14]
        for z in range(4):
            stage[i // 4, i % 4, z] = wide[z].astype(BF16)
        return 0

    lax.fori_loop(0, 16, group, 0)


def down_block(acc, stage):
    def group(i, _):
        for t in range(5):
            rows = acc[pl.ds(pl.multiple_of(i * 40, 8) + 8 * t, 8), :]
            piece = jnp.concatenate([rows[:, c * LANES : (c + 1) * LANES] for c in range(7)], 0)
            stage[i // 4, i % 4, pl.ds(56 * t, 56)] = piece.astype(BF16)
        return 0

    lax.fori_loop(0, 16, group, 0)


def gradients_kernel(*refs):
    (tall, wide, turned, deep), (out, squares, terms), scratch = refs[:4], refs[4:7], refs[7:]
    (lhs, rhs, zs, dh, acc, acc2, stage, stage2, shift, r1, r2, r3, own, f1, f2, sums) = scratch[:16]
    (in_sem, rhs_sem, zs_sem, put_sem, send1, send2, send3, recv1, recv2, recv3, load, send4, recv4) = scratch[16:]
    at = place()

    def fetch_tall(l):
        return pltpu.make_async_copy(tall.at[l], lhs, in_sem.at[0])

    def fetch_deep(l):
        return pltpu.make_async_copy(deep.at[l], dh, in_sem.at[1])

    def fetch_wide(t):
        columns = pl.ds(pl.multiple_of(t % TILES * TILE, TILE), TILE)
        return pltpu.make_async_copy(wide.at[t // TILES, :, columns], rhs.at[t % 2], rhs_sem.at[t % 2])

    def fetch_turned(t):
        rows = pl.ds(pl.multiple_of(t % SIDE * PLANE_ROWS, LANES), PLANE_ROWS)
        return pltpu.make_async_copy(turned.at[t // SIDE, rows], zs.at[t % 2], zs_sem.at[t % 2])

    def put(m, h):
        return pltpu.make_async_copy(stage, terms.at[m, :, :, :, pl.ds(pl.multiple_of(PIECE * h, SUBLANES), PIECE)], put_sem.at[0])

    def put2(m, h):
        return pltpu.make_async_copy(stage2, terms.at[m, h], put_sem.at[1])

    fetch_tall(0).start()
    fetch_wide(0).start()
    fetch_deep(0).start()
    fetch_turned(0).start()
    enter(at)

    def split(c):
        o, s = ORDERS[c], SIGNS[c]
        return o, s, at[o[0]], at[o[1]], at[o[2]]

    def block(m, c, a, i):
        o = ORDERS[c]
        index = [slice(None)] * 3
        index[o[0]] = a
        if i is not None:
            index[o[1]] = i
        return terms.at[(m, *index, pl.ds(STARTS[c], PART))]

    def first(m, c, step, j, start=False):
        o, s, p1, p2, p3 = split(c)
        if start:
            src = block(m, c, wrap(p1 - s), wrap(p2 - s * (1 + j)))
        else:
            src = r1.at[c, m, (step + 2) % STEPS, j]
        return remote(src, r1.at[c, m, step, j], send1.at[c], recv1.at[c, m, step, j], neighbour(at, o[0], s))

    def loading(m, c, step):
        o, s, p1, p2, p3 = split(c)
        return pltpu.make_async_copy(block(m, c, wrap(p1 - s * (2 + step)), None), own.at[c, step], load.at[c, step])

    def second(m, c, step, start=False):
        o, s, p1, p2, p3 = split(c)
        src = r1.at[c, m, 2, 0] if start else r2.at[c, m, (step + 2) % STEPS]
        return remote(src, r2.at[c, m, step], send2.at[c], recv2.at[c, m, step], neighbour(at, o[1], s))

    def third(m, c, k):
        o, s, p1, p2, p3 = split(c)
        return remote(r2.at[c, m, 2, wrap(p3 + k + 1)], r3.at[c, m, k], send3.at[c], recv3.at[c, m, k], neighbour(at, o[2], k + 1))

    def launch(m):
        for c in range(WAYS):
            for j in range(SIDE):
                first(m, c, 0, j, True).start()
    def load_own(m):
        for step in range(STEPS):
            for c in range(WAYS):
                loading(m, c, step).start()

    def on_first(m, e):
        step, j = e // SIDE, e % SIDE

        @pl.when(j == 0)
        def _():
            for c in range(WAYS):
                loading(m, c, step).wait()

        for c in range(WAYS):
            o, s, p1, p2, p3 = split(c)
            first(m, c, step, j).wait_recv()
            i = wrap(p2 - s * (1 + j))
            mine = own[c, step, i] if o[1] < o[2] else own[c, step, :, i]
            both = r1[c, m, step, j].astype(F32) + mine.astype(F32)
            r1[c, m, step, j] = both.astype(BF16)

            @pl.when(step == 2)
            def _():
                f1[c, j] = both

            @pl.when(step < 2)
            def _():
                first(m, c, step + 1, j).start()

            @pl.when(e == 8)
            def _():
                second(m, c, 0, True).start()

    def on_second(m, step):
        for c in range(WAYS):
            second(m, c, step).wait_recv()
            both = r2[c, m, step].astype(F32) + f1[c, step + 1]
            r2[c, m, step] = both.astype(BF16)

            @pl.when(step == 2)
            def _():
                f2[c] = both
                for k in range(STEPS):
                    third(m, c, k).start()

            @pl.when(step < 2)
            def _():
                second(m, c, step + 1).start()

    def on_third(m):
        for c in range(WAYS):
            o, s, p1, p2, p3 = split(c)
            total = f2[c, p3]
            for k in range(STEPS):
                third(m, c, k).wait_recv()
                total = total + r3[c, m, k].astype(F32)
            out[m, pl.ds(STARTS[c], PART)] = total.astype(BF16)

    def tile(i, _):
        m, h = i // TILES, i % TILES
        kind, l = m % AXES, m // AXES

        @pl.when((h == 0) & (m > 0) & (m < MATRICES + 1))
        def _():
            @pl.when(kind > 0)
            def _():
                put(0, 0).wait()

            @pl.when(kind == 0)
            def _():
                put2(0, 0).wait()

            launch(m - 1)

        @pl.when((m < MATRICES) & (kind < 2))
        def _():
            t = (2 * l + kind) * TILES + h

            @pl.when((kind == 0) & (h == 0))
            def _():
                fetch_tall(l).wait()

                @pl.when(l == 1)
                def _():
                    fetch_deep(1).start()

            fetch_wide(t).wait()

            @pl.when(t < 19)
            def _():
                fetch_wide(t + 1).start()

            acc[...] = dot(lhs[...], rhs[t % 2])

            @pl.when(h > 0)
            def _():
                put(m, h).wait()

            gate_block(acc, stage, shift)
            put(m, h).start()

        @pl.when((m < MATRICES) & (kind == 2) & (h < SIDE))
        def _():
            t = SIDE * l + h

            @pl.when(h == 0)
            def _():
                fetch_deep(l).wait()

                @pl.when(l == 0)
                def _():
                    fetch_tall(1).start()

            fetch_turned(t).wait()

            @pl.when(t < 7)
            def _():
                fetch_turned(t + 1).start()

            acc2[...] = dot(zs[t % 2], dh[...])

            @pl.when(h > 0)
            def _():
                put2(m, h).wait()

            down_block(acc2, stage2)
            put2(m, h).start()

        @pl.when((h == 0) & (m > 2))
        def _():
            on_third(m - 3)

        @pl.when((h != 0) & (h != 3) & (m > 1) & (m < MATRICES + 2))
        def _():
            on_second(m - 2, h // 2)

        ring, turn = (i - 1) // TILES - 1, (i - 1) % TILES

        @pl.when((ring >= 0) & (ring < MATRICES))
        def _():
            lax.fori_loop(2 * turn + 1 - (SIDE - turn) // SIDE, 2 * turn + 3 + turn // SIDE, lambda e, _: (on_first(ring, e), 0)[1], 0)

        @pl.when((h == 0) & (m > 0) & (m < MATRICES + 1))
        def _():
            load_own(m - 1)

        return 0

    lax.fori_loop(0, (MATRICES + 2) * TILES + 1, tile, 0)

    total = jnp.zeros((SUBLANES, LANES), F32)
    for m in range(MATRICES):
        g = out[m].astype(F32)
        total = total + jnp.sum((g * g).reshape(-1, SUBLANES, LANES), axis=0)
    squares[...] = norm_exchange(at, sums, send4, recv4, total)
    for c in range(WAYS):
        for r, sem in ((r1, send1), (r2, send2), (r3, send3)):
            pltpu.make_async_copy(r.at[c], r.at[c], sem.at[c]).wait()
    for axis in range(STEPS):
        pltpu.make_async_copy(sums.at[axis, pl.ds(0, STEPS)], sums.at[axis, pl.ds(0, STEPS)], send4.at[axis]).wait()


def gradients(tall, wide, turned, deep):
    g, squares, _ = pl.pallas_call(
        gradients_kernel,
        out_shape=(
            jax.ShapeDtypeStruct((MATRICES, BLOCK, LANES), BF16),
            jax.ShapeDtypeStruct((SUBLANES, LANES), F32),
            jax.ShapeDtypeStruct((MATRICES, SIDE, SIDE, SIDE, BLOCK, LANES), BF16),
        ),
        in_specs=[HBM] * 4,
        out_specs=(VMEM, VMEM, HBM),
        scratch_shapes=[
            pltpu.VMEM((D, TOKENS), BF16),
            pltpu.VMEM((2, TOKENS, TILE), BF16),
            pltpu.VMEM((2, PLANE_ROWS, TOKENS), BF16),
            pltpu.VMEM((TOKENS, D), BF16),
            pltpu.VMEM((D, TILE), F32),
            pltpu.VMEM((PLANE_ROWS, D), F32),
            pltpu.VMEM((SIDE, SIDE, SIDE, PIECE, LANES), BF16),
            pltpu.VMEM((SIDE, SIDE, BLOCK, LANES), BF16),
            pltpu.VMEM((SIDE, PIECE, LANES), F32),
            pltpu.VMEM((WAYS, MATRICES, STEPS, SIDE, SIDE, PART, LANES), BF16),
            pltpu.VMEM((WAYS, MATRICES, STEPS, SIDE, PART, LANES), BF16),
            pltpu.VMEM((WAYS, MATRICES, STEPS, PART, LANES), BF16),
            pltpu.VMEM((WAYS, STEPS, SIDE, SIDE, PART, LANES), BF16),
            pltpu.VMEM((WAYS, SIDE, SIDE, PART, LANES), F32),
            pltpu.VMEM((WAYS, SIDE, PART, LANES), F32),
            pltpu.VMEM((AXES, SIDE, SUBLANES, LANES), F32),
            *[DMA((2,))] * 4,
            *[DMA((WAYS,))] * AXES,
            DMA((WAYS, MATRICES, STEPS, SIDE)), *[DMA((WAYS, MATRICES, STEPS))] * 2,
            DMA((WAYS, STEPS)),
            DMA((AXES,)), DMA((AXES, STEPS)),
        ],
        compiler_params=pltpu.CompilerParams(collective_id=0, has_side_effects=True, vmem_limit_bytes=MOST_VMEM),
        name="gradients",
    )(tall, wide, turned, deep)
    return g, squares


def solution(mesh):
    rep, dp = mesh.axis_names

    def step(x, dy, *arrays):
        weights, m, v = (arrays[i : i + 3] for i in (0, 3, 6))
        g, total = gradients(*by_rows(x[0], dy[0], weights))
        new, new_m, new_v = adam(sum(w.size for w in weights), g, total, weights, m, v)
        return (*natural(all_gather(new)), *new_m, *new_v)

    whole, rows, sequences = P(None, None, None), P(None, dp, None), P((rep, dp), None, None)
    return jax.shard_map(
        step,
        mesh=mesh,
        in_specs=(sequences, sequences, *[whole] * 3, *[rows] * 6),
        out_specs=(*[P(rep, None, None)] * 3, *[P(rep, dp, None)] * 6),
        check_vma=False,
    )
```

```python
import functools
import jax
import jax.numpy as jnp
from jax import lax
from jax.experimental import pallas as pl
from jax.experimental.pallas import tpu as pltpu
from jax.sharding import PartitionSpec as P

MESH = pl.DeviceIdType.MESH
WAYS, AXES, SIDE = 6, 3, 4
STEPS = SIDE - 1
MATRICES, LAYERS, DEVICES, PLANE = 6, 2, 64, 16
LANES, SUBLANES, BLOCK = 128, 8, 280
BF16, F32 = jnp.bfloat16, jnp.float32
HBM, VMEM = pl.BlockSpec(memory_space=pl.ANY), pl.BlockSpec(memory_space=pltpu.VMEM)
DMA = pltpu.SemaphoreType.DMA
MOST_VMEM = 62 * 1024 * 1024
ORDERS = tuple(tuple((way // 2 + i) % AXES for i in range(AXES)) for way in range(WAYS))
SIGNS = (1, -1) * AXES
TAKEN = (3, 0, 4, 1, 5, 2)


def place():
    me = lax.axis_index("dp")
    return (me // PLANE, me // SIDE % SIDE, me % SIDE)


def wrap(i):
    return (i + 3 * SIDE) % SIDE


def neighbour(at, axis, step):
    there = [c for c in at]
    there[axis] = wrap(at[axis] + step)
    return {"dp": (there[0] * SIDE + there[1]) * SIDE + there[2]}


def remote(src, dst, send, recv, to):
    return pltpu.make_async_remote_copy(src_ref=src, dst_ref=dst, send_sem=send, recv_sem=recv, device_id=to, device_id_type=MESH)


def enter(at):
    barrier = pltpu.get_barrier_semaphore()
    for axis in range(AXES):
        for step in range(STEPS):
            pl.semaphore_signal(barrier, inc=1, device_id=neighbour(at, axis, step + 1), device_id_type=MESH)
    pl.semaphore_wait(barrier, AXES * STEPS)


def norm_exchange(at, buf, send, recv, total):
    for axis in range(AXES):
        buf[axis, STEPS] = total
        copies = [
            remote(buf.at[axis, STEPS], buf.at[axis, k], send.at[axis], recv.at[axis, k], neighbour(at, axis, k + 1)) for k in range(STEPS)
        ]
        for copy in copies:
            copy.start()
        for k, copy in enumerate(copies):
            copy.wait_recv()
            total = total + buf[axis, k]
    return total


def passed_on(seen, c, phase, key):
    d1, d2, d3 = key
    if phase == 0 and d3 < STEPS:
        yield 0, (0, 0, d3 + 1)
    if phase < 2 and d2 < STEPS:
        yield 1, (0, d2 + 1, d3)
    if phase == 1 and d2 > 0:
        seen.append((c, d2))
        if seen.count((c, d2)) < SIDE:
            return
        d3 = None
    if d1 < STEPS:
        yield 2, (d1 + 1, d2, d3)


def ag_order(latency=1.8):
    import heapq

    free, out, seen, heap = {}, [], [], []

    def hold(t, c, phase, key):
        for phase, key in passed_on(seen, c, phase, key):
            link = ORDERS[c][2 - phase]
            size = SIDE if key[2] is None else 1
            free[link] = max(t, free.get(link, 0)) + size
            heapq.heappush(heap, (free[link] + latency, len(out) * WAYS + len(heap), c, phase, key))

    for c in range(0, WAYS, 2):
        hold(0, c, 0, (0, 0, 0))
    while heap:
        t, _, *arrival = heapq.heappop(heap)
        out.append(arrival)
        hold(t, *arrival)
    return out


def ag_kernel(*refs):
    mine, outs, (sends, recv1, recv2, recv3, recv4, local) = refs[0], refs[1 : 1 + WAYS], refs[1 + WAYS :]
    at = place()
    enter(at)

    def where(c, key):
        index = [None] * AXES
        for axis, d in zip(ORDERS[c], key, strict=True):
            index[axis] = slice(None) if d is None else wrap(at[axis] - SIGNS[c] * d)
        return outs[c].at[tuple(index)]

    def arrived(c, phase, key):
        d1, d2, d3 = key
        if phase == 0:
            return recv1.at[c // 2, d3 - 1]
        if phase == 1:
            return recv2.at[c // 2, d2 - 1, d3]
        if d3 is not None:
            return recv3.at[c // 2, d1 - 1, d3]
        return recv4.at[c // 2, d1 - 1, d2 - 1]

    def send_on(c, phase, key):
        d1, d2, d3 = key
        back = list(key)
        back[2 - phase] -= 1
        there = where(c, back)
        src = there if any(d != 0 for d in back) else mine.at[c]
        remote(src, there, sends.at[c, phase], arrived(c, phase, key), neighbour(at, ORDERS[c][2 - phase], SIGNS[c])).start()

    seen = []

    def hold(*held):
        for phase, key in passed_on(seen, *held):
            send_on(held[0], phase, key)

    own = [pltpu.make_async_copy(mine.at[c], where(c, (0, 0, 0)), local.at[c]) for c in range(WAYS)]
    for c in range(WAYS):
        hold(c, 0, (0, 0, 0))
    for copied in own:
        copied.start()
    for even, phase, key in ag_order():
        two = outs[even].at[0, pl.ds(0, 2)] if key[2] is None else outs[even].at[0, 0, pl.ds(0, 2)]
        pltpu.make_async_copy(two, two, arrived(even, phase, key)).wait()
        for c in (even, even + 1):
            hold(c, phase, key)
    for c in range(WAYS):
        own[c].wait()
        sent = outs[c].at[pl.ds(0, STEPS)]
        for phase in (2, 1, 0):
            pltpu.make_async_copy(sent, sent, sends.at[c, phase]).wait()
            sent = outs[c].at[(0,) * (AXES - phase) + (pl.ds(0, STEPS),)]


def all_gather(mine):
    return pl.pallas_call(
        ag_kernel,
        out_shape=(pltpu.VMEM((SIDE, SIDE, SIDE, *mine.shape[1:]), BF16),) * WAYS,
        in_specs=[VMEM],
        out_specs=(VMEM,) * WAYS,
        scratch_shapes=[DMA((WAYS, AXES)), DMA((AXES, STEPS)), *[DMA((AXES, STEPS, SIDE))] * 2, DMA((AXES, STEPS, STEPS)), DMA((WAYS,))],
        compiler_params=pltpu.CompilerParams(collective_id=1, has_side_effects=True, vmem_limit_bytes=MOST_VMEM // SUBLANES),
        name="gather",
    )(mine)


def tiles_of(t, rows, columns):
    n = columns // LANES
    if t < 2:
        return [(0, rows, j * LANES, j * rows) for j in range(n)]
    return [(8 * i, 8, j * LANES, (i * n + j) * 8) for i in range(rows // 8) for j in range(n)]


def adam_kernel(count, g, total, *refs):
    refs = list(refs)
    ws, ms, vs = (refs[AXES * k : AXES * (k + 1)] for k in range(3))
    new, *refs = refs[3 * AXES :]
    new_m, new_v, windows, owns = (refs[AXES * k : AXES * (k + 1)] for k in range(4))
    wide_g, wide_w, sems = refs[4 * AXES :]
    me = lax.axis_index("dp")
    taken = []
    for t in range(AXES):
        rows = windows[t].shape[1]
        first = pl.multiple_of((me // SIDE if t < 2 else me) * rows, SUBLANES)
        taken.append(pltpu.make_async_copy(ws[t].at[:, pl.ds(first, rows)], windows[t], sems.at[t]))
    for copy in taken:
        copy.start()
    factor = jnp.minimum(1.0, 0.5 * lax.rsqrt(jnp.full((1, 1), jnp.sum(total[...])) / count + 1e-30))
    for t in range(AXES):
        taken[t].wait()
        rows, columns = owns[t].shape[1:]
        if t < 2:
            for z in range(SIDE):

                @pl.when(me % SIDE == z)
                def _():
                    for l in range(LAYERS):
                        owns[t][l] = windows[t][l].astype(F32)[z * rows : (z + 1) * rows]

        for l in range(LAYERS):
            wide_g[...] = g[TAKEN[LAYERS * t + l]].astype(F32) * factor
            for row, n, column, at in tiles_of(t, rows, columns):
                lanes = pl.ds(column, LANES)
                here = (slice(None), l, lanes) if t < 2 else (l, pl.ds(row, n), lanes)
                grad = wide_g[pl.ds(at, n), :]
                m = 0.9 * ms[t][here] + 0.1 * grad
                v = 0.95 * vs[t][here] + 0.05 * grad * grad
                w = (owns if t < 2 else windows)[t][l, pl.ds(row, n), lanes].astype(F32)
                new_m[t][here] = m
                new_v[t][here] = v
                wide_w[pl.ds(at, n), :] = w - 0.02 * (m * lax.rsqrt(v + 1e-8) + 0.1 * w)
            new[LAYERS * t + l] = wide_w[...].astype(BF16)


def adam(count, g, total, ws, ms, vs):
    ms, vs = ([*(jnp.swapaxes(a, 0, 1) for a in arrays[:2]), arrays[2]] for arrays in (ms, vs))
    like = [jax.ShapeDtypeStruct(m.shape, F32) for m in ms]
    new, *moments = pl.pallas_call(
        functools.partial(adam_kernel, count),
        out_shape=(pltpu.VMEM(g.shape, BF16), *like, *like),
        in_specs=[VMEM] * 2 + [HBM] * AXES + [VMEM] * AXES * 2,
        out_specs=(VMEM,) * (1 + AXES * 2),
        scratch_shapes=[
            *[pltpu.VMEM((LAYERS, w.shape[1] // n, w.shape[2]), BF16) for w, n in zip(ws, (PLANE, PLANE, DEVICES), strict=True)],
            *[pltpu.VMEM((LAYERS, w.shape[1] // DEVICES, w.shape[2]), F32) for w in ws],
            *[pltpu.VMEM(g.shape[1:], F32)] * 2,
            DMA((AXES,)),
        ],
        compiler_params=pltpu.CompilerParams(vmem_limit_bytes=MOST_VMEM),
        name="adam",
    )(g, total, *ws, *ms, *vs)
    return new, *([*(jnp.swapaxes(a, 0, 1) for a in part[:2]), part[2]] for part in (moments[:AXES], moments[AXES:]))


def natural_kernel(*refs):
    gathered, outs, wide = refs[:MATRICES], refs[MATRICES:-AXES], refs[-AXES:]
    first = pl.program_id(0) * SUBLANES
    for t in range(AXES):
        for l in range(LAYERS):
            rows, columns = outs[t].shape[1:]
            for k in range(SUBLANES):
                block = gathered[LAYERS * t + l][first + k].astype(F32)
                for row, n, column, at in tiles_of(t, rows // SUBLANES, columns):
                    wide[t][pl.ds(k * rows // SUBLANES + row, n), pl.ds(column, LANES)] = block[at : at + n]
            outs[t][l] = wide[t][...].astype(BF16)


def natural(gathered):
    shapes = (GATE, GATE, DOWN)
    return pl.pallas_call(
        natural_kernel,
        grid=(SUBLANES,),
        out_shape=tuple(jax.ShapeDtypeStruct((LAYERS, *s), BF16) for s in shapes),
        in_specs=[VMEM] * MATRICES,
        out_specs=tuple(pl.BlockSpec((LAYERS, s[0] // SUBLANES, s[1]), lambda i: (0, i, 0)) for s in shapes),
        scratch_shapes=[pltpu.VMEM((s[0] // SUBLANES, s[1]), F32) for s in shapes],
        compiler_params=pltpu.CompilerParams(vmem_limit_bytes=MOST_VMEM // SIDE),
        name="natural",
    )(*[g.reshape(DEVICES, BLOCK, LANES) for g in gathered])


D, FF, TOKENS = 896, 2560, 2048
GATE, DOWN = (D, FF), (FF, D)
ROWS, CHUNK, TILE = 256, 256, 512
TILES, PIECE, PLANE_ROWS = FF // TILE, BLOCK * TILE // FF, FF // SIDE
NT = (((1,), (1,)), ((), ()))


def dot(a, b):
    return jnp.dot(a, b, preferred_element_type=F32)


def dot_t(a, b):
    return lax.dot_general(a, b, NT, preferred_element_type=F32)


def scale_of(wide):
    return lax.rsqrt(jnp.mean(wide * wide, -1, keepdims=True) + 1e-6)


def rows_kernel(x_hbm, dy_hbm, *refs):
    hbm, results, weights, rest = refs[:3], refs[3:7], refs[7:13], refs[13:]
    buffers, (xs, dys, g0, u0, z0, dz1, sems, part_sems, in_sems, out_sems) = rest[:4], rest[4:]
    wg0, wu0, wd0, wg1, wu1, wd1 = weights
    i, slot = pl.program_id(0), pl.program_id(0) % 2
    first = i == 0
    chunks = [pl.ds(j * CHUNK, CHUNK) for j in range(FF // CHUNK)]

    def fetch(k):
        return pltpu.make_async_copy(hbm[k % 3].at[k // 3], weights[k], sems.at[k])

    def fetch_part(k, j):
        return pltpu.make_async_copy(hbm[k].at[0, :, chunks[j]], weights[k].at[:, chunks[j]], part_sems.at[k, j])

    def take(i):
        rows = pl.ds(pl.multiple_of(i * ROWS, ROWS), ROWS)
        for k, (source, there) in enumerate(((x_hbm, xs), (dy_hbm, dys))):
            yield pltpu.make_async_copy(source.at[rows], there.at[i % 2], in_sems.at[i % 2, k])

    def put(k, part):
        rows = pl.ds(pl.multiple_of(i * ROWS, ROWS), ROWS)
        there = results[k].at[part, rows] if k % 2 else results[k].at[part, :, rows]
        return pltpu.make_async_copy(buffers[k].at[slot, part], there, out_sems.at[slot, k, part])

    def outs():
        return [put(k, part) for k in range(4) for part in range(results[k].shape[0])]

    @pl.when(first)
    def _():
        for copy in take(0):
            copy.start()
        for j in range(len(chunks)):
            for k in range(2):
                fetch_part(k, j).start()

    for copy in take(i):
        copy.wait()

    @pl.when(i + 1 < pl.num_programs(0))
    def _():
        for copy in take(i + 1):
            copy.start()

    @pl.when(i > 1)
    def _():
        for copy in outs():
            copy.wait()

    tall, wide, turned, deep = (b.at[slot] for b in buffers)
    x, dy = xs.at[slot], dys.at[slot]

    def forward(coming):
        a = (x[...].astype(F32) * scale_of(x[...].astype(F32))).astype(BF16)
        tall[1] = a.T
        deep[0] = dy[...]
        for j, ch in enumerate(chunks):
            if coming:
                for k in range(2):
                    fetch_part(k, j).wait()
                if 0 < j < 5:
                    fetch(j + 1).start()
            gate, up = dot(a, wg0[:, ch]), dot(a, wu0[:, ch])
            g0[:, ch], u0[:, ch] = gate, up
            z0[:, ch] = (gate * jax.nn.sigmoid(gate) * up).astype(BF16)
            turned[1, ch, :] = z0[:, ch].T

    @pl.when(first)
    def _():
        forward(True)
        for k in range(2, MATRICES):
            fetch(k).wait()

    @pl.when(i > 0)
    def _():
        forward(False)

    for k, part in ((0, 1), (3, 0), (2, 1)):
        put(k, part).start()
    for ch in chunks[:SIDE]:
        dz1[:, ch] = dot_t(dy[...], wd1[ch, :]).astype(BF16)
    h = x[...] + dot(z0[...], wd0[...]).astype(BF16)
    for ch in chunks[SIDE:]:
        dz1[:, ch] = dot_t(dy[...], wd1[ch, :]).astype(BF16)
    h = h.astype(F32)
    scale = scale_of(h)
    a = (h * scale).astype(BF16)
    tall[0] = a.T
    put(0, 0).start()
    for ch in chunks:
        gate, up = dot(a, wg1[:, ch]), dot(a, wu1[:, ch])
        dz = dz1[:, ch].astype(F32)
        s = jax.nn.sigmoid(gate)
        silu = gate * s
        turned[0, ch, :] = (silu * up).astype(BF16).T
        wide[1, :, ch] = (dz * silu).astype(BF16)
        wide[0, :, ch] = (dz * up * (s * (1 + gate * (1 - s)))).astype(BF16)
    for k, part in ((2, 0), (1, 0), (1, 1)):
        put(k, part).start()
    most, rest = pl.ds(0, FF - CHUNK), chunks[-1]
    da_gate, da_up = dot_t(wide[0, :, most], wg1[:, most]), dot_t(wide[1, :, most], wu1[:, most])
    da_gate, da_up = da_gate + dot_t(wide[0, :, rest], wg1[:, rest]), da_up + dot_t(wide[1, :, rest], wu1[:, rest])
    da = (da_gate.astype(BF16) + da_up.astype(BF16)).astype(F32)
    dwide = scale * (da - h * (scale * scale * jnp.mean(da * h, -1, keepdims=True)))
    dh = dy[...] + dwide.astype(BF16)
    deep[1] = dh
    put(3, 1).start()
    for ch in chunks:
        dz = dot_t(dh, wd0[ch, :]).astype(BF16).astype(F32)
        gate, up = g0[:, ch], u0[:, ch]
        s = jax.nn.sigmoid(gate)
        wide[3, :, ch] = (dz * (gate * s)).astype(BF16)
        wide[2, :, ch] = (dz * up * (s * (1 + gate * (1 - s)))).astype(BF16)
    put(1, 2).start()
    put(1, 3).start()

    @pl.when(i + 1 == pl.num_programs(0))
    def _():
        for copy in outs():
            copy.wait()

    @pl.when(i + 1 == pl.num_programs(0))
    def _():
        for k in range(4):
            for part in range(results[k].shape[0]):
                pltpu.make_async_copy(buffers[k].at[1 - slot, part], buffers[k].at[1 - slot, part], out_sems.at[1 - slot, k, part]).wait()


def by_rows(x, dy, weights):
    shapes = ((2, D, TOKENS), (4, TOKENS, FF), (2, FF, TOKENS), (2, TOKENS, D))
    buffers = ((2, D, ROWS), (4, ROWS, FF), (2, FF, ROWS), (2, ROWS, D))
    return pl.pallas_call(
        rows_kernel,
        grid=(TOKENS // ROWS,),
        out_shape=tuple(jax.ShapeDtypeStruct(s, BF16) for s in shapes),
        in_specs=[HBM] * 5,
        out_specs=(HBM,) * 4,
        scratch_shapes=[
            *[pltpu.VMEM(w.shape[1:], BF16) for w in weights * 2],
            *[pltpu.VMEM((2, *b), BF16) for b in buffers],
            *[pltpu.VMEM((2, ROWS, D), BF16)] * 2,
            *[pltpu.VMEM((ROWS, FF), F32)] * 2,
            *[pltpu.VMEM((ROWS, FF), BF16)] * 2,
            DMA((MATRICES,)), DMA((2, FF // CHUNK)), DMA((2, 2)), DMA((2, 4, 4)),
        ],
        compiler_params=pltpu.CompilerParams(vmem_limit_bytes=MOST_VMEM),
        name="rows",
    )(x, dy, *weights)


STARTS = (0, 48, 96, 144, 192, 232)
PART = 48


def gate_block(acc, stage, wide):
    def group(i, _):
        rows = pl.ds(pl.multiple_of(i * 56, 8), 56)
        for c in range(4):
            piece = acc[rows, pl.ds(c * LANES, LANES)]
            for z in range(4):
                wide[z, pl.ds(14 * c, 14), :] = piece[14 * z : 14 * z + 14]
        for z in range(4):
            stage[i // 4, i % 4, z] = wide[z].astype(BF16)
        return 0

    lax.fori_loop(0, 16, group, 0)


def down_block(acc, stage):
    def group(i, _):
        for t in range(5):
            rows = acc[pl.ds(pl.multiple_of(i * 40, 8) + 8 * t, 8), :]
            piece = jnp.concatenate([rows[:, c * LANES : (c + 1) * LANES] for c in range(7)], 0)
            stage[i // 4, i % 4, pl.ds(56 * t, 56)] = piece.astype(BF16)
        return 0

    lax.fori_loop(0, 16, group, 0)


def gradients_kernel(*refs):
    (tall, wide, turned, deep), (out, squares, terms), scratch = refs[:4], refs[4:7], refs[7:]
    (lhs, rhs, zs, dh, acc, acc2, stage, stage2, shift, r1, r2, r3, own, f1, f2, sums) = scratch[:16]
    (in_sem, rhs_sem, zs_sem, put_sem, send1, send2, send3, recv1, recv2, recv3, load, send4, recv4) = scratch[16:]
    at = place()

    def fetch_tall(l):
        return pltpu.make_async_copy(tall.at[l], lhs, in_sem.at[0])

    def fetch_deep(l):
        return pltpu.make_async_copy(deep.at[l], dh, in_sem.at[1])

    def fetch_wide(t):
        columns = pl.ds(pl.multiple_of(t % TILES * TILE, TILE), TILE)
        return pltpu.make_async_copy(wide.at[t // TILES, :, columns], rhs.at[t % 2], rhs_sem.at[t % 2])

    def fetch_turned(t):
        rows = pl.ds(pl.multiple_of(t % SIDE * PLANE_ROWS, LANES), PLANE_ROWS)
        return pltpu.make_async_copy(turned.at[t // SIDE, rows], zs.at[t % 2], zs_sem.at[t % 2])

    def put(m, h):
        return pltpu.make_async_copy(stage, terms.at[m, :, :, :, pl.ds(pl.multiple_of(PIECE * h, SUBLANES), PIECE)], put_sem.at[0])

    def put2(m, h):
        return pltpu.make_async_copy(stage2, terms.at[m, h], put_sem.at[1])

    fetch_tall(0).start()
    fetch_wide(0).start()
    fetch_deep(0).start()
    fetch_turned(0).start()
    enter(at)

    def split(c):
        o, s = ORDERS[c], SIGNS[c]
        return o, s, at[o[0]], at[o[1]], at[o[2]]

    def block(m, c, a, i):
        o = ORDERS[c]
        index = [slice(None)] * 3
        index[o[0]] = a
        if i is not None:
            index[o[1]] = i
        return terms.at[(m, *index, pl.ds(STARTS[c], PART))]

    def first(m, c, step, j, start=False):
        o, s, p1, p2, p3 = split(c)
        if start:
            src = block(m, c, wrap(p1 - s), wrap(p2 - s * (1 + j)))
        else:
            src = r1.at[c, m, (step + 2) % STEPS, j]
        return remote(src, r1.at[c, m, step, j], send1, recv1.at[m, step, j], neighbour(at, o[0], s))

    def loading(m, c, step):
        o, s, p1, p2, p3 = split(c)
        return pltpu.make_async_copy(block(m, c, wrap(p1 - s * (2 + step)), None), own.at[c, step], load.at[step])

    def second(m, c, step, start=False):
        o, s, p1, p2, p3 = split(c)
        src = r1.at[c, m, 2, 0] if start else r2.at[c, m, (step + 2) % STEPS]
        return remote(src, r2.at[c, m, step], send2, recv2.at[m, step], neighbour(at, o[1], s))

    def third(m, c, k):
        o, s, p1, p2, p3 = split(c)
        return remote(r2.at[c, m, 2, wrap(p3 + k + 1)], r3.at[c, m, k], send3, recv3.at[m], neighbour(at, o[2], k + 1))

    def whole(ref, sem):
        pltpu.make_async_copy(ref, ref, sem).wait()

    def launch(m):
        for c in range(WAYS):
            for j in range(SIDE):
                first(m, c, 0, j, True).start()
    def load_own(m):
        for step in range(STEPS):
            for c in range(WAYS):
                loading(m, c, step).start()

    def on_first(m, e):
        step, j = e // SIDE, e % SIDE

        @pl.when(j == 0)
        def _():
            whole(own.at[:, step], load.at[step])

        whole(r1.at[:, m, step, j], recv1.at[m, step, j])

        def both(c):
            o, s, p1, p2, p3 = split(c)
            i = wrap(p2 - s * (1 + j))
            mine = own[c, step, i] if o[1] < o[2] else own[c, step, :, i]
            return r1[c, m, step, j].astype(F32) + mine.astype(F32)

        @pl.when(step < 2)
        def _():
            for c in range(WAYS):
                r1[c, m, step, j] = both(c).astype(BF16)
                first(m, c, step + 1, j).start()

        @pl.when(step == 2)
        def _():
            for c in range(WAYS):
                total = both(c)
                f1[c, j] = total

                @pl.when(j == 0)
                def _():
                    r1[c, m, 2, 0] = total.astype(BF16)
                    second(m, c, 0, True).start()

    def on_second(m, step):
        whole(r2.at[:, m, step], recv2.at[m, step])

        def both(c):
            return r2[c, m, step].astype(F32) + f1[c, step + 1]

        @pl.when(step < 2)
        def _():
            for c in range(WAYS):
                r2[c, m, step] = both(c).astype(BF16)
                second(m, c, step + 1).start()

        @pl.when(step == 2)
        def _():
            for c in range(WAYS):
                total = both(c)
                f2[c] = total
                r2[c, m, 2] = total.astype(BF16)
                for k in range(STEPS):
                    third(m, c, k).start()

    def on_third(m):
        whole(r3.at[:, m], recv3.at[m])
        for c in range(WAYS):
            o, s, p1, p2, p3 = split(c)
            total = f2[c, p3]
            for k in range(STEPS):
                total = total + r3[c, m, k].astype(F32)
            out[m, pl.ds(STARTS[c], PART)] = total.astype(BF16)

    def tile(i, _):
        m, h = i // TILES, i % TILES
        kind, l = m % AXES, m // AXES

        @pl.when((h == 0) & (m > 0) & (m < MATRICES + 1))
        def _():
            @pl.when(kind > 0)
            def _():
                put(0, 0).wait()

            @pl.when(kind == 0)
            def _():
                put2(0, 0).wait()

            launch(m - 1)

        @pl.when((m < MATRICES) & (kind < 2))
        def _():
            t = (2 * l + kind) * TILES + h

            @pl.when((kind == 0) & (h == 0))
            def _():
                fetch_tall(l).wait()

                @pl.when(l == 1)
                def _():
                    fetch_deep(1).start()

            fetch_wide(t).wait()

            @pl.when(t < 19)
            def _():
                fetch_wide(t + 1).start()

            acc[...] = dot(lhs[...], rhs[t % 2])

            @pl.when(h > 0)
            def _():
                put(m, h).wait()

            gate_block(acc, stage, shift)
            put(m, h).start()

        @pl.when((m < MATRICES) & (kind == 2) & (h < SIDE))
        def _():
            t = SIDE * l + h

            @pl.when(h == 0)
            def _():
                fetch_deep(l).wait()

                @pl.when(l == 0)
                def _():
                    fetch_tall(1).start()

            fetch_turned(t).wait()

            @pl.when(t < 7)
            def _():
                fetch_turned(t + 1).start()

            acc2[...] = dot(zs[t % 2], dh[...])

            @pl.when(h > 0)
            def _():
                put2(m, h).wait()

            down_block(acc2, stage2)
            put2(m, h).start()

        @pl.when((h == 0) & (m > 2))
        def _():
            on_third(m - 3)

        @pl.when((h != 0) & (h != 3) & (m > 1) & (m < MATRICES + 2))
        def _():
            on_second(m - 2, h // 2)

        ring, turn = (i - 1) // TILES - 1, (i - 1) % TILES

        @pl.when((ring >= 0) & (ring < MATRICES))
        def _():
            lax.fori_loop(2 * turn + 1 - (SIDE - turn) // SIDE, 2 * turn + 3 + turn // SIDE, lambda e, _: (on_first(ring, e), 0)[1], 0)

        @pl.when((h == 0) & (m > 0) & (m < MATRICES + 1))
        def _():
            load_own(m - 1)

        return 0

    lax.fori_loop(0, (MATRICES + 2) * TILES + 1, tile, 0)

    total = jnp.zeros((SUBLANES, LANES), F32)
    for m in range(MATRICES):
        g = out[m].astype(F32)
        total = total + jnp.sum((g * g).reshape(-1, SUBLANES, LANES), axis=0)
    squares[...] = norm_exchange(at, sums, send4, recv4, total)
    for r, sem in ((r1, send1), (r2, send2), (r3, send3)):
        whole(r, sem)
    for axis in range(AXES):
        whole(sums.at[axis, pl.ds(0, STEPS)], send4.at[axis])


def gradients(tall, wide, turned, deep):
    g, squares, _ = pl.pallas_call(
        gradients_kernel,
        out_shape=(
            jax.ShapeDtypeStruct((MATRICES, BLOCK, LANES), BF16),
            jax.ShapeDtypeStruct((SUBLANES, LANES), F32),
            jax.ShapeDtypeStruct((MATRICES, SIDE, SIDE, SIDE, BLOCK, LANES), BF16),
        ),
        in_specs=[HBM] * 4,
        out_specs=(VMEM, VMEM, HBM),
        scratch_shapes=[
            pltpu.VMEM((D, TOKENS), BF16),
            pltpu.VMEM((2, TOKENS, TILE), BF16),
            pltpu.VMEM((2, PLANE_ROWS, TOKENS), BF16),
            pltpu.VMEM((TOKENS, D), BF16),
            pltpu.VMEM((D, TILE), F32),
            pltpu.VMEM((PLANE_ROWS, D), F32),
            pltpu.VMEM((SIDE, SIDE, SIDE, PIECE, LANES), BF16),
            pltpu.VMEM((SIDE, SIDE, BLOCK, LANES), BF16),
            pltpu.VMEM((SIDE, PIECE, LANES), F32),
            pltpu.VMEM((WAYS, MATRICES, STEPS, SIDE, SIDE, PART, LANES), BF16),
            pltpu.VMEM((WAYS, MATRICES, STEPS, SIDE, PART, LANES), BF16),
            pltpu.VMEM((WAYS, MATRICES, STEPS, PART, LANES), BF16),
            pltpu.VMEM((WAYS, STEPS, SIDE, SIDE, PART, LANES), BF16),
            pltpu.VMEM((WAYS, SIDE, SIDE, PART, LANES), F32),
            pltpu.VMEM((WAYS, SIDE, PART, LANES), F32),
            pltpu.VMEM((AXES, SIDE, SUBLANES, LANES), F32),
            *[DMA((2,))] * 4,
            *[DMA] * AXES,
            DMA((MATRICES, STEPS, SIDE)), DMA((MATRICES, STEPS)), DMA((MATRICES,)),
            DMA((STEPS,)),
            DMA((AXES,)), DMA((AXES, STEPS)),
        ],
        compiler_params=pltpu.CompilerParams(collective_id=0, has_side_effects=True, vmem_limit_bytes=MOST_VMEM),
        name="gradients",
    )(tall, wide, turned, deep)
    return g, squares


def solution(mesh):
    rep, dp = mesh.axis_names

    def step(x, dy, *arrays):
        weights, m, v = (arrays[i : i + 3] for i in (0, 3, 6))
        g, total = gradients(*by_rows(x[0], dy[0], weights))
        new, new_m, new_v = adam(sum(w.size for w in weights), g, total, weights, m, v)
        return (*natural(all_gather(new)), *new_m, *new_v)

    whole, rows, sequences = P(None, None, None), P(None, dp, None), P((rep, dp), None, None)
    return jax.shard_map(
        step,
        mesh=mesh,
        in_specs=(sequences, sequences, *[whole] * 3, *[rows] * 6),
        out_specs=(*[P(rep, None, None)] * 3, *[P(rep, dp, None)] * 6),
        check_vma=False,
    )
```

```python
import functools
import jax
import jax.numpy as jnp
from jax import lax
from jax.experimental import pallas as pl
from jax.experimental.pallas import tpu as pltpu
from jax.sharding import PartitionSpec as P

MESH = pl.DeviceIdType.MESH
WAYS, AXES, SIDE = 6, 3, 4
STEPS = SIDE - 1
MATRICES, LAYERS, DEVICES, PLANE = 6, 2, 64, 16
LANES, SUBLANES, BLOCK = 128, 8, 280
BF16, F32 = jnp.bfloat16, jnp.float32
HBM, VMEM = pl.BlockSpec(memory_space=pl.ANY), pl.BlockSpec(memory_space=pltpu.VMEM)
DMA = pltpu.SemaphoreType.DMA
MIB = 1 << 20
MOST_VMEM, SPARE_VMEM = 62 * MIB, 2 * MIB
ORDERS = tuple(tuple((way // 2 + i) % AXES for i in range(AXES)) for way in range(WAYS))
SIGNS = (1, -1) * AXES
TAKEN = (3, 0, 4, 1, 5, 2)


def place():
    me = lax.axis_index("dp")
    return (me // PLANE, me // SIDE % SIDE, me % SIDE)


def wrap(i):
    return (i + 3 * SIDE) % SIDE


def neighbour(at, axis, step):
    there = [c for c in at]
    there[axis] = wrap(at[axis] + step)
    return {"dp": (there[0] * SIDE + there[1]) * SIDE + there[2]}


def remote(src, dst, send, recv, to):
    return pltpu.make_async_remote_copy(src_ref=src, dst_ref=dst, send_sem=send, recv_sem=recv, device_id=to, device_id_type=MESH)


def moved(at, steps):
    x, y, z = (wrap(a + step) for a, step in zip(at, steps, strict=True))
    return {"dp": (x * SIDE + y) * SIDE + z}


LINES = tuple(tuple(k * (axis == line) for axis in range(AXES)) for line in range(AXES) for k in range(1, SIDE))
PLANE_PEERS = tuple((0, k // SIDE, k % SIDE) for k in range(1, PLANE))
LINE_PEERS = LINES[:STEPS]


def enter(at, peers):
    barrier = pltpu.get_barrier_semaphore()
    for steps in peers:
        pl.semaphore_signal(barrier, inc=1, device_id=moved(at, steps), device_id_type=MESH)
    pl.semaphore_wait(barrier, len(peers))


def norm_exchange(at, buf, send, recv, total):
    first = 0
    for stage, peers in enumerate((PLANE_PEERS, LINE_PEERS)):
        own, others = buf.at[first], buf.at[pl.ds(first + 1, len(peers))]
        own[...] = total
        for k, steps in enumerate(peers):
            remote(own, others.at[k], send.at[stage], recv.at[stage], moved(at, steps)).start()
        pltpu.make_async_copy(others, others, recv.at[stage]).wait()
        total = total + jnp.sum(others[...], axis=0)
        pltpu.make_async_copy(others, others, send.at[stage]).wait()
        first += 1 + len(peers)
    return total


def passed_on(seen, c, phase, key):
    d1, d2, d3 = key
    if phase == 0 and d3 < STEPS:
        yield 0, (0, 0, d3 + 1)
    if phase < 2 and d2 < STEPS:
        yield 1, (0, d2 + 1, d3)
    if phase == 1 and d2 > 0:
        seen.append((c, d2))
        if seen.count((c, d2)) < SIDE:
            return
        d3 = None
    if d1 < STEPS:
        yield 2, (d1 + 1, d2, d3)


def ag_order(latency=2):
    import heapq

    free, out, seen, heap = {}, [], [], []

    def hold(t, c, phase, key):
        for phase, key in passed_on(seen, c, phase, key):
            link = ORDERS[c][2 - phase]
            size = SIDE if key[2] is None else 1
            free[link] = max(t, free.get(link, 0)) + size
            heapq.heappush(heap, (free[link] + latency, len(out) * WAYS + len(heap), c, phase, key))

    for c in range(0, WAYS, 2):
        hold(0, c, 0, (0, 0, 0))
    while heap:
        t, _, *arrival = heapq.heappop(heap)
        out.append(arrival)
        hold(t, *arrival)
    return out


def ag_kernel(*refs):
    mine, outs, (sends, recv1, recv2, recv3, recv4, local) = refs[0], refs[1 : 1 + WAYS], refs[1 + WAYS :]
    at = place()
    enter(at, LINES)

    def where(c, key):
        index = [None] * AXES
        for axis, d in zip(ORDERS[c], key, strict=True):
            index[axis] = slice(None) if d is None else wrap(at[axis] - SIGNS[c] * d)
        return outs[c].at[tuple(index)]

    def arrived(c, phase, key):
        d1, d2, d3 = key
        if phase == 0:
            return recv1.at[c // 2, d3 - 1]
        if phase == 1:
            return recv2.at[c // 2, d2 - 1, d3]
        if d3 is not None:
            return recv3.at[c // 2, d1 - 1, d3]
        return recv4.at[c // 2, d1 - 1, d2 - 1]

    def send_on(c, phase, key):
        d1, d2, d3 = key
        back = list(key)
        back[2 - phase] -= 1
        there = where(c, back)
        src = there if any(d != 0 for d in back) else mine.at[c]
        remote(src, there, sends.at[c, phase], arrived(c, phase, key), neighbour(at, ORDERS[c][2 - phase], SIGNS[c])).start()

    seen = []

    def hold(*held):
        for phase, key in passed_on(seen, *held):
            send_on(held[0], phase, key)

    own = [pltpu.make_async_copy(mine.at[c], where(c, (0, 0, 0)), local.at[c]) for c in range(WAYS)]
    for c in range(WAYS):
        hold(c, 0, (0, 0, 0))
    for copied in own:
        copied.start()
    for even, phase, key in ag_order():
        two = outs[even].at[0, pl.ds(0, 2)] if key[2] is None else outs[even].at[0, 0, pl.ds(0, 2)]
        pltpu.make_async_copy(two, two, arrived(even, phase, key)).wait()
        for c in (even, even + 1):
            hold(c, phase, key)
    for c in range(WAYS):
        own[c].wait()
        sent = outs[c].at[pl.ds(0, STEPS)]
        for phase in (2, 1, 0):
            pltpu.make_async_copy(sent, sent, sends.at[c, phase]).wait()
            sent = outs[c].at[(0,) * (AXES - phase) + (pl.ds(0, STEPS),)]


def all_gather(mine):
    return pl.pallas_call(
        ag_kernel,
        out_shape=(pltpu.VMEM((SIDE, SIDE, SIDE, *mine.shape[1:]), BF16),) * WAYS,
        in_specs=[VMEM],
        out_specs=(VMEM,) * WAYS,
        scratch_shapes=[DMA((WAYS, AXES)), DMA((AXES, STEPS)), *[DMA((AXES, STEPS, SIDE))] * 2, DMA((AXES, STEPS, STEPS)), DMA((WAYS,))],
        compiler_params=pltpu.CompilerParams(collective_id=1, has_side_effects=True, vmem_limit_bytes=MOST_VMEM // SUBLANES),
        name="gather",
    )(mine)


def tiles_of(t, rows, columns):
    n = columns // LANES
    if t < 2:
        return [(0, rows, j * LANES, j * rows) for j in range(n)]
    return [(8 * i, 8, j * LANES, (i * n + j) * 8) for i in range(rows // 8) for j in range(n)]


def adam_kernel(count, g, total, *refs):
    ws, ms, vs = (refs[AXES * k : AXES * (k + 1)] for k in range(3))
    new, *refs = refs[3 * AXES :]
    *moments, wide_g, wide_w = refs
    new_m, new_v = moments[:AXES], moments[AXES:]
    factor = jnp.minimum(1.0, 0.5 * lax.rsqrt(jnp.full((1, 1), jnp.sum(total[...])) / count + 1e-30))
    for t in range(AXES):
        rows, columns = ws[t].shape[1:]
        for l in range(LAYERS):
            wide_g[...] = g[TAKEN[LAYERS * t + l]].astype(F32) * factor
            for row, n, column, at in tiles_of(t, rows, columns):
                lanes = pl.ds(column, LANES)
                here = (slice(None), l, lanes) if t < 2 else (l, pl.ds(row, n), lanes)
                grad = wide_g[pl.ds(at, n), :]
                m = 0.9 * ms[t][here] + 0.1 * grad
                v = 0.95 * vs[t][here] + 0.05 * grad * grad
                w = ws[t][l, pl.ds(row, n), lanes]
                new_m[t][here] = m
                new_v[t][here] = v
                wide_w[pl.ds(at, n), :] = w - 0.02 * (m * lax.rsqrt(v + 1e-8) + 0.1 * w)
            new[LAYERS * t + l] = wide_w[...].astype(BF16)


def adam(count, g, total, ws, ms, vs):
    ms, vs = ([*(jnp.swapaxes(a, 0, 1) for a in arrays[:2]), arrays[2]] for arrays in (ms, vs))
    like = [jax.ShapeDtypeStruct(m.shape, F32) for m in ms]
    new, *moments = pl.pallas_call(
        functools.partial(adam_kernel, count),
        out_shape=(pltpu.VMEM(g.shape, BF16), *like, *like),
        in_specs=[VMEM] * (2 + AXES * 3),
        out_specs=(VMEM,) * (1 + AXES * 2),
        scratch_shapes=[pltpu.VMEM(g.shape[1:], F32)] * 2,
        compiler_params=pltpu.CompilerParams(vmem_limit_bytes=MOST_VMEM // SIDE),
        name="adam",
    )(g, total, *ws, *ms, *vs)
    return new, *([*(jnp.swapaxes(a, 0, 1) for a in part[:2]), part[2]] for part in (moments[:AXES], moments[AXES:]))


def natural_kernel(*refs):
    gathered, outs, wide = refs[:MATRICES], refs[MATRICES:-AXES], refs[-AXES:]
    first = pl.program_id(0) * SUBLANES
    for t in range(AXES):
        for l in range(LAYERS):
            rows, columns = outs[t].shape[1:]
            for k in range(SUBLANES):
                block = gathered[LAYERS * t + l][first + k].astype(F32)
                for row, n, column, at in tiles_of(t, rows // SUBLANES, columns):
                    wide[t][pl.ds(k * rows // SUBLANES + row, n), pl.ds(column, LANES)] = block[at : at + n]
            outs[t][l] = wide[t][...].astype(BF16)


def natural(gathered):
    shapes = (GATE, GATE, DOWN)
    return pl.pallas_call(
        natural_kernel,
        grid=(SUBLANES,),
        out_shape=tuple(jax.ShapeDtypeStruct((LAYERS, *s), BF16) for s in shapes),
        in_specs=[VMEM] * MATRICES,
        out_specs=tuple(pl.BlockSpec((LAYERS, s[0] // SUBLANES, s[1]), lambda i: (0, i, 0)) for s in shapes),
        scratch_shapes=[pltpu.VMEM((s[0] // SUBLANES, s[1]), F32) for s in shapes],
        compiler_params=pltpu.CompilerParams(vmem_limit_bytes=MOST_VMEM // SIDE),
        name="natural",
    )(*[g.reshape(DEVICES, BLOCK, LANES) for g in gathered])


D, FF, TOKENS = 896, 2560, 2048
GATE, DOWN = (D, FF), (FF, D)
ROWS, CHUNK, TILE = 256, 256, 512
TILES, PIECE, PLANE_ROWS = FF // TILE, BLOCK * TILE // FF, FF // SIDE
NT = (((1,), (1,)), ((), ()))


def dot(a, b):
    return jnp.dot(a, b, preferred_element_type=F32)


def dot_t(a, b):
    return lax.dot_general(a, b, NT, preferred_element_type=F32)


def scale_of(wide):
    return lax.rsqrt(jnp.mean(wide * wide, -1, keepdims=True) + 1e-6)


def rows_kernel(x_hbm, dy_hbm, *refs):
    hbm, results, weights, rest = refs[:3], refs[3:7], refs[7:13], refs[13:]
    buffers, (xs, dys, g0, u0, z0, dz1, sems, part_sems, in_sems, out_sems) = rest[:4], rest[4:]
    wg0, wu0, wd0, wg1, wu1, wd1 = weights
    i, slot = pl.program_id(0), pl.program_id(0) % 2
    first = i == 0
    chunks = [pl.ds(j * CHUNK, CHUNK) for j in range(FF // CHUNK)]

    def fetch(k):
        return pltpu.make_async_copy(hbm[k % 3].at[k // 3], weights[k], sems.at[k])

    def fetch_part(k, j):
        return pltpu.make_async_copy(hbm[k].at[0, :, chunks[j]], weights[k].at[:, chunks[j]], part_sems.at[k, j])

    def take(i):
        rows = pl.ds(pl.multiple_of(i * ROWS, ROWS), ROWS)
        for k, (source, there) in enumerate(((x_hbm, xs), (dy_hbm, dys))):
            yield pltpu.make_async_copy(source.at[rows], there.at[i % 2], in_sems.at[i % 2, k])

    def put(k, part):
        rows = pl.ds(pl.multiple_of(i * ROWS, ROWS), ROWS)
        there = results[k].at[part, rows] if k % 2 else results[k].at[part, :, rows]
        return pltpu.make_async_copy(buffers[k].at[slot, part], there, out_sems.at[slot, k, part])

    def outs():
        return [put(k, part) for k in range(4) for part in range(results[k].shape[0])]

    @pl.when(first)
    def _():
        for copy in take(0):
            copy.start()
        for j in range(len(chunks)):
            for k in range(2):
                fetch_part(k, j).start()

    for copy in take(i):
        copy.wait()

    @pl.when(i + 1 < pl.num_programs(0))
    def _():
        for copy in take(i + 1):
            copy.start()

    @pl.when(i > 1)
    def _():
        for copy in outs():
            copy.wait()

    tall, wide, turned, deep = (b.at[slot] for b in buffers)
    x, dy = xs.at[slot], dys.at[slot]

    def forward(coming):
        a = (x[...].astype(F32) * scale_of(x[...].astype(F32))).astype(BF16)
        tall[1] = a.T
        deep[0] = dy[...]
        for j, ch in enumerate(chunks):
            if coming:
                for k in range(2):
                    fetch_part(k, j).wait()
                if 0 < j < 5:
                    fetch(j + 1).start()
            gate, up = dot(a, wg0[:, ch]), dot(a, wu0[:, ch])
            g0[:, ch], u0[:, ch] = gate, up
            z0[:, ch] = (gate * jax.nn.sigmoid(gate) * up).astype(BF16)
            turned[1, ch, :] = z0[:, ch].T

    @pl.when(first)
    def _():
        forward(True)
        for k in range(2, MATRICES):
            fetch(k).wait()

    @pl.when(i > 0)
    def _():
        forward(False)

    for k, part in ((0, 1), (3, 0), (2, 1)):
        put(k, part).start()
    for ch in chunks[:SIDE]:
        dz1[:, ch] = dot_t(dy[...], wd1[ch, :]).astype(BF16)
    h = x[...] + dot(z0[...], wd0[...]).astype(BF16)
    for ch in chunks[SIDE:]:
        dz1[:, ch] = dot_t(dy[...], wd1[ch, :]).astype(BF16)
    h = h.astype(F32)
    scale = scale_of(h)
    a = (h * scale).astype(BF16)
    tall[0] = a.T
    put(0, 0).start()
    for ch in chunks:
        gate, up = dot(a, wg1[:, ch]), dot(a, wu1[:, ch])
        dz = dz1[:, ch].astype(F32)
        s = jax.nn.sigmoid(gate)
        silu = gate * s
        turned[0, ch, :] = (silu * up).astype(BF16).T
        wide[1, :, ch] = (dz * silu).astype(BF16)
        wide[0, :, ch] = (dz * up * (s * (1 + gate * (1 - s)))).astype(BF16)
    for k, part in ((2, 0), (1, 0), (1, 1)):
        put(k, part).start()
    most, rest = pl.ds(0, FF - CHUNK), chunks[-1]
    da_gate, da_up = dot_t(wide[0, :, most], wg1[:, most]), dot_t(wide[1, :, most], wu1[:, most])
    da_gate, da_up = da_gate + dot_t(wide[0, :, rest], wg1[:, rest]), da_up + dot_t(wide[1, :, rest], wu1[:, rest])
    da = (da_gate.astype(BF16) + da_up.astype(BF16)).astype(F32)
    dwide = scale * (da - h * (scale * scale * jnp.mean(da * h, -1, keepdims=True)))
    dh = dy[...] + dwide.astype(BF16)
    deep[1] = dh
    put(3, 1).start()
    for ch in chunks:
        dz = dot_t(dh, wd0[ch, :]).astype(BF16).astype(F32)
        gate, up = g0[:, ch], u0[:, ch]
        s = jax.nn.sigmoid(gate)
        wide[3, :, ch] = (dz * (gate * s)).astype(BF16)
        wide[2, :, ch] = (dz * up * (s * (1 + gate * (1 - s)))).astype(BF16)
    put(1, 2).start()
    put(1, 3).start()

    @pl.when(i + 1 == pl.num_programs(0))
    def _():
        for copy in outs():
            copy.wait()

    @pl.when(i + 1 == pl.num_programs(0))
    def _():
        for k in range(4):
            for part in range(results[k].shape[0]):
                pltpu.make_async_copy(buffers[k].at[1 - slot, part], buffers[k].at[1 - slot, part], out_sems.at[1 - slot, k, part]).wait()


def by_rows(x, dy, weights):
    shapes = ((2, D, TOKENS), (4, TOKENS, FF), (2, FF, TOKENS), (2, TOKENS, D))
    buffers = ((2, D, ROWS), (4, ROWS, FF), (2, FF, ROWS), (2, ROWS, D))
    return pl.pallas_call(
        rows_kernel,
        grid=(TOKENS // ROWS,),
        out_shape=tuple(jax.ShapeDtypeStruct(s, BF16) for s in shapes),
        in_specs=[HBM] * 5,
        out_specs=(HBM,) * 4,
        scratch_shapes=[
            *[pltpu.VMEM(w.shape[1:], BF16) for w in weights * 2],
            *[pltpu.VMEM((2, *b), BF16) for b in buffers],
            *[pltpu.VMEM((2, ROWS, D), BF16)] * 2,
            *[pltpu.VMEM((ROWS, FF), F32)] * 2,
            *[pltpu.VMEM((ROWS, FF), BF16)] * 2,
            DMA((MATRICES,)), DMA((2, FF // CHUNK)), DMA((2, 2)), DMA((2, 4, 4)),
        ],
        compiler_params=pltpu.CompilerParams(vmem_limit_bytes=MOST_VMEM),
        name="rows",
    )(x, dy, *weights)


STARTS = (0, 48, 96, 144, 192, 232)
PART = 48


def gate_block(acc, stage, wide):
    def group(i, _):
        rows = pl.ds(pl.multiple_of(i * 56, 8), 56)
        for c in range(4):
            piece = acc[rows, pl.ds(c * LANES, LANES)]
            for z in range(4):
                wide[z, pl.ds(14 * c, 14), :] = piece[14 * z : 14 * z + 14]
        for z in range(4):
            stage[i // 4, i % 4, z] = wide[z].astype(BF16)
        return 0

    lax.fori_loop(0, 16, group, 0)


def down_block(acc, stage):
    def group(i, _):
        for t in range(5):
            rows = acc[pl.ds(pl.multiple_of(i * 40, 8) + 8 * t, 8), :]
            piece = jnp.concatenate([rows[:, c * LANES : (c + 1) * LANES] for c in range(7)], 0)
            stage[i // 4, i % 4, pl.ds(56 * t, 56)] = piece.astype(BF16)
        return 0

    lax.fori_loop(0, 16, group, 0)


def own_rows(ws, windows, owns, sems):
    me = lax.axis_index("dp")
    taken = []
    for t in range(AXES):
        rows = windows[t].shape[1]
        first = pl.multiple_of((me // SIDE if t < 2 else me) * rows, SUBLANES)
        taken.append(pltpu.make_async_copy(ws[t].at[:, pl.ds(first, rows)], windows[t], sems.at[t]))
        taken[t].start()
    for t in range(AXES):
        taken[t].wait()
        rows = owns[t].shape[1]
        if t == 2:
            owns[t][...] = windows[t][...].astype(F32)
        for z in range(SIDE if t < 2 else 0):

            @pl.when(me % SIDE == z)
            def _():
                for l in range(LAYERS):
                    owns[t][l] = windows[t][l].astype(F32)[z * rows : (z + 1) * rows]


def gradients_kernel(*refs):
    (tall, wide, turned, deep), ws, (out, squares, terms), owns, scratch = refs[:4], refs[4:7], refs[7:10], refs[10:13], refs[13:]
    (lhs, rhs, zs, dh, acc, acc2, stage, stage2, shift, r1, r2, r3, own, f1, f2, sums) = scratch[:16]
    *windows, window_sem = scratch[16:20]
    (in_sem, rhs_sem, zs_sem, put_sem, send1, send2, send3, recv1, recv2, recv3, load, send4, recv4) = scratch[20:]
    at = place()

    def fetch_tall(l):
        return pltpu.make_async_copy(tall.at[l], lhs, in_sem.at[0])

    def fetch_deep(l):
        return pltpu.make_async_copy(deep.at[l], dh, in_sem.at[1])

    def fetch_wide(t):
        columns = pl.ds(pl.multiple_of(t % TILES * TILE, TILE), TILE)
        return pltpu.make_async_copy(wide.at[t // TILES, :, columns], rhs.at[t % 2], rhs_sem.at[t % 2])

    def fetch_turned(t):
        rows = pl.ds(pl.multiple_of(t % SIDE * PLANE_ROWS, LANES), PLANE_ROWS)
        return pltpu.make_async_copy(turned.at[t // SIDE, rows], zs.at[t % 2], zs_sem.at[t % 2])

    def put(m, h):
        return pltpu.make_async_copy(stage, terms.at[m, :, :, :, pl.ds(pl.multiple_of(PIECE * h, SUBLANES), PIECE)], put_sem.at[0])

    def put2(m, h):
        return pltpu.make_async_copy(stage2, terms.at[m, h], put_sem.at[1])

    fetch_tall(0).start()
    fetch_wide(0).start()
    fetch_deep(0).start()
    fetch_turned(0).start()
    enter(at, sorted({*LINES, *PLANE_PEERS}))

    def split(c):
        o, s = ORDERS[c], SIGNS[c]
        return o, s, at[o[0]], at[o[1]], at[o[2]]

    def block(m, c, a, i):
        o = ORDERS[c]
        index = [slice(None)] * 3
        index[o[0]] = a
        if i is not None:
            index[o[1]] = i
        return terms.at[(m, *index, pl.ds(STARTS[c], PART))]

    def first(m, c, step, j, start=False):
        o, s, p1, p2, p3 = split(c)
        if start:
            src = block(m, c, wrap(p1 - s), wrap(p2 - s * (1 + j)))
        else:
            src = r1.at[c, m, (step + 2) % STEPS, j]
        return remote(src, r1.at[c, m, step, j], send1, recv1.at[m, step, j], neighbour(at, o[0], s))

    def loading(m, c, step):
        o, s, p1, p2, p3 = split(c)
        return pltpu.make_async_copy(block(m, c, wrap(p1 - s * (2 + step)), None), own.at[c, step], load.at[step])

    def second(m, c, step, start=False):
        o, s, p1, p2, p3 = split(c)
        src = r1.at[c, m, 2, 0] if start else r2.at[c, m, (step + 2) % STEPS]
        return remote(src, r2.at[c, m, step], send2, recv2.at[m, step], neighbour(at, o[1], s))

    def third(m, c, k):
        o, s, p1, p2, p3 = split(c)
        return remote(r2.at[c, m, 2, wrap(p3 + k + 1)], r3.at[c, m, k], send3, recv3.at[m], neighbour(at, o[2], k + 1))

    def whole(ref, sem):
        pltpu.make_async_copy(ref, ref, sem).wait()

    def launch(m):
        for c in range(WAYS):
            for j in range(SIDE):
                first(m, c, 0, j, True).start()
    def load_own(m):
        for step in range(STEPS):
            for c in range(WAYS):
                loading(m, c, step).start()

    def on_first(m, e):
        step, j = e // SIDE, e % SIDE

        @pl.when(j == 0)
        def _():
            whole(own.at[:, step], load.at[step])

        whole(r1.at[:, m, step, j], recv1.at[m, step, j])

        def both(c):
            o, s, p1, p2, p3 = split(c)
            i = wrap(p2 - s * (1 + j))
            mine = own[c, step, i] if o[1] < o[2] else own[c, step, :, i]
            return r1[c, m, step, j].astype(F32) + mine.astype(F32)

        @pl.when(step < 2)
        def _():
            for c in range(WAYS):
                r1[c, m, step, j] = both(c).astype(BF16)
                first(m, c, step + 1, j).start()

        @pl.when(step == 2)
        def _():
            for c in range(WAYS):
                total = both(c)
                f1[c, j] = total

                @pl.when(j == 0)
                def _():
                    r1[c, m, 2, 0] = total.astype(BF16)
                    second(m, c, 0, True).start()

    def on_second(m, step):
        whole(r2.at[:, m, step], recv2.at[m, step])

        def both(c):
            return r2[c, m, step].astype(F32) + f1[c, step + 1]

        @pl.when(step < 2)
        def _():
            for c in range(WAYS):
                r2[c, m, step] = both(c).astype(BF16)
                second(m, c, step + 1).start()

        @pl.when(step == 2)
        def _():
            for c in range(WAYS):
                total = both(c)
                f2[c] = total
                r2[c, m, 2] = total.astype(BF16)
                for k in range(STEPS):
                    third(m, c, k).start()

    def on_third(m):
        whole(r3.at[:, m], recv3.at[m])
        for c in range(WAYS):
            o, s, p1, p2, p3 = split(c)
            total = f2[c, p3]
            for k in range(STEPS):
                total = total + r3[c, m, k].astype(F32)
            out[m, pl.ds(STARTS[c], PART)] = total.astype(BF16)

    def tile(i, _):
        m, h = i // TILES, i % TILES
        kind, l = m % AXES, m // AXES

        @pl.when((h == 0) & (m > 0) & (m < MATRICES + 1))
        def _():
            @pl.when(kind > 0)
            def _():
                put(0, 0).wait()

            @pl.when(kind == 0)
            def _():
                put2(0, 0).wait()

            launch(m - 1)

        @pl.when((m < MATRICES) & (kind < 2))
        def _():
            t = (2 * l + kind) * TILES + h

            @pl.when((kind == 0) & (h == 0))
            def _():
                fetch_tall(l).wait()

                @pl.when(l == 1)
                def _():
                    fetch_deep(1).start()

            fetch_wide(t).wait()

            @pl.when(t < 19)
            def _():
                fetch_wide(t + 1).start()

            acc[...] = dot(lhs[...], rhs[t % 2])

            @pl.when(h > 0)
            def _():
                put(m, h).wait()

            gate_block(acc, stage, shift)
            put(m, h).start()

        @pl.when((m < MATRICES) & (kind == 2) & (h < SIDE))
        def _():
            t = SIDE * l + h

            @pl.when(h == 0)
            def _():
                fetch_deep(l).wait()

                @pl.when(l == 0)
                def _():
                    fetch_tall(1).start()

            fetch_turned(t).wait()

            @pl.when(t < 7)
            def _():
                fetch_turned(t + 1).start()

            acc2[...] = dot(zs[t % 2], dh[...])

            @pl.when(h > 0)
            def _():
                put2(m, h).wait()

            down_block(acc2, stage2)
            put2(m, h).start()

        @pl.when((h == 0) & (m > 2))
        def _():
            on_third(m - AXES)

        @pl.when((h != 0) & (h != 3) & (m > 1) & (m < MATRICES + 2))
        def _():
            on_second(m - 2, h // 2)

        ring, turn = (i - 1) // TILES - 1, (i - 1) % TILES

        @pl.when((ring >= 0) & (ring < MATRICES))
        def _():
            lax.fori_loop(2 * turn + 1 - (SIDE - turn) // SIDE, 2 * turn + 3 + turn // SIDE, lambda e, _: (on_first(ring, e), 0)[1], 0)

        @pl.when((h == 0) & (m > 0) & (m < MATRICES + 1))
        def _():
            load_own(m - 1)

        return 0

    lax.fori_loop(0, (MATRICES + 2) * TILES, tile, 0)
    own_rows(ws, windows, owns, window_sem)
    on_third(MATRICES - 1)

    total = jnp.zeros((SUBLANES, LANES), F32)
    for m in range(MATRICES):
        g = out[m].astype(F32)
        total = total + jnp.sum((g * g).reshape(-1, SUBLANES, LANES), axis=0)
    squares[...] = norm_exchange(at, sums, send4, recv4, total)
    for r, sem in ((r1, send1), (r2, send2), (r3, send3)):
        whole(r, sem)


def gradients(tall, wide, turned, deep, weights):
    g, squares, _, *owns = pl.pallas_call(
        gradients_kernel,
        out_shape=(
            pltpu.VMEM((MATRICES, BLOCK, LANES), BF16),
            pltpu.VMEM((SUBLANES, LANES), F32),
            jax.ShapeDtypeStruct((MATRICES, SIDE, SIDE, SIDE, BLOCK, LANES), BF16),
            *[pltpu.VMEM((LAYERS, w.shape[1] // DEVICES, w.shape[2]), F32) for w in weights],
        ),
        in_specs=[HBM] * (4 + AXES),
        out_specs=(VMEM, VMEM, HBM, *[VMEM] * AXES),
        scratch_shapes=[
            pltpu.VMEM((D, TOKENS), BF16),
            pltpu.VMEM((2, TOKENS, TILE), BF16),
            pltpu.VMEM((2, PLANE_ROWS, TOKENS), BF16),
            pltpu.VMEM((TOKENS, D), BF16),
            pltpu.VMEM((D, TILE), F32),
            pltpu.VMEM((PLANE_ROWS, D), F32),
            pltpu.VMEM((SIDE, SIDE, SIDE, PIECE, LANES), BF16),
            pltpu.VMEM((SIDE, SIDE, BLOCK, LANES), BF16),
            pltpu.VMEM((SIDE, PIECE, LANES), F32),
            pltpu.VMEM((WAYS, MATRICES, STEPS, SIDE, SIDE, PART, LANES), BF16),
            pltpu.VMEM((WAYS, MATRICES, STEPS, SIDE, PART, LANES), BF16),
            pltpu.VMEM((WAYS, MATRICES, STEPS, PART, LANES), BF16),
            pltpu.VMEM((WAYS, STEPS, SIDE, SIDE, PART, LANES), BF16),
            pltpu.VMEM((WAYS, SIDE, SIDE, PART, LANES), F32),
            pltpu.VMEM((WAYS, SIDE, PART, LANES), F32),
            pltpu.VMEM((PLANE + SIDE, SUBLANES, LANES), F32),
            *[pltpu.VMEM((LAYERS, w.shape[1] // n, w.shape[2]), BF16) for w, n in zip(weights, (PLANE, PLANE, DEVICES), strict=True)],
            DMA((AXES,)),
            *[DMA((2,))] * 4,
            *[DMA] * AXES,
            DMA((MATRICES, STEPS, SIDE)), DMA((MATRICES, STEPS)), DMA((MATRICES,)),
            DMA((STEPS,)),
            DMA((2,)), DMA((2,)),
        ],
        compiler_params=pltpu.CompilerParams(collective_id=0, has_side_effects=True, vmem_limit_bytes=MOST_VMEM - SPARE_VMEM),
        name="gradients",
    )(tall, wide, turned, deep, *weights)
    return g, squares, owns


def solution(mesh):
    rep, dp = mesh.axis_names

    def step(x, dy, *arrays):
        weights, m, v = (arrays[i : i + 3] for i in (0, 3, 6))
        g, total, owns = gradients(*by_rows(x[0], dy[0], weights), weights)
        new, new_m, new_v = adam(MATRICES * D * FF, g, total, owns, m, v)
        return (*natural(all_gather(new)), *new_m, *new_v)

    whole, rows, sequences = P(None, None, None), P(None, dp, None), P((rep, dp), None, None)
    return jax.shard_map(
        step,
        mesh=mesh,
        in_specs=(sequences, sequences, *[whole] * 3, *[rows] * 6),
        out_specs=(*[P(rep, None, None)] * 3, *[P(rep, dp, None)] * 6),
        check_vma=False,
    )
```

```python
import functools
import jax
import jax.numpy as jnp
from jax import lax
from jax.experimental import pallas as pl
from jax.experimental.pallas import tpu as pltpu
from jax.sharding import PartitionSpec as P

MESH = pl.DeviceIdType.MESH
WAYS, AXES, SIDE = 6, 3, 4
STEPS = SIDE - 1
MATRICES, LAYERS, DEVICES, PLANE = 6, 2, 64, 16
LANES, SUBLANES, BLOCK = 128, 8, 280
BF16, F32 = jnp.bfloat16, jnp.float32
HBM, VMEM = pl.BlockSpec(memory_space=pl.ANY), pl.BlockSpec(memory_space=pltpu.VMEM)
DMA = pltpu.SemaphoreType.DMA
MIB = 1 << 20
MOST_VMEM, SPARE_VMEM = 62 * MIB, 2 * MIB
ORDERS = tuple(tuple((way // 2 + i) % AXES for i in range(AXES)) for way in range(WAYS))
SIGNS = (1, -1) * AXES
TAKEN = (3, 0, 4, 1, 5, 2)


def place():
    me = lax.axis_index("dp")
    return (me // PLANE, me // SIDE % SIDE, me % SIDE)


def wrap(i):
    return (i + 3 * SIDE) % SIDE


def neighbour(at, axis, step):
    there = [c for c in at]
    there[axis] = wrap(at[axis] + step)
    return {"dp": (there[0] * SIDE + there[1]) * SIDE + there[2]}


def remote(src, dst, send, recv, to):
    return pltpu.make_async_remote_copy(src_ref=src, dst_ref=dst, send_sem=send, recv_sem=recv, device_id=to, device_id_type=MESH)


def moved(at, steps):
    x, y, z = (wrap(a + step) for a, step in zip(at, steps, strict=True))
    return {"dp": (x * SIDE + y) * SIDE + z}


LINES = tuple(tuple(k * (axis == line) for axis in range(AXES)) for line in range(AXES) for k in range(1, SIDE))
PLANE_PEERS = tuple((0, k // SIDE, k % SIDE) for k in range(1, PLANE))
LINE_PEERS = LINES[:STEPS]


def enter(at, peers):
    barrier = pltpu.get_barrier_semaphore()
    for steps in peers:
        pl.semaphore_signal(barrier, inc=1, device_id=moved(at, steps), device_id_type=MESH)
    pl.semaphore_wait(barrier, len(peers))


def norm_exchange(at, buf, send, recv, total):
    first = 0
    for stage, peers in enumerate((PLANE_PEERS, LINE_PEERS)):
        own, others = buf.at[first], buf.at[pl.ds(first + 1, len(peers))]
        own[...] = total
        for k, steps in enumerate(peers):
            remote(own, others.at[k], send.at[stage], recv.at[stage], moved(at, steps)).start()
        pltpu.make_async_copy(others, others, recv.at[stage]).wait()
        total = total + jnp.sum(others[...], axis=0)
        pltpu.make_async_copy(others, others, send.at[stage]).wait()
        first += 1 + len(peers)
    return total


def passed_on(seen, c, phase, key):
    d1, d2, d3 = key
    if phase == 0 and d3 < STEPS:
        yield 0, (0, 0, d3 + 1)
    if phase < 2 and d2 < STEPS:
        yield 1, (0, d2 + 1, d3)
    if phase == 1 and d2 > 0:
        seen.append((c, d2))
        if seen.count((c, d2)) < SIDE:
            return
        d3 = None
    if d1 < STEPS:
        yield 2, (d1 + 1, d2, d3)


def ag_order(latency=2):
    import heapq

    free, out, seen, heap = {}, [], [], []

    def hold(t, c, phase, key):
        for phase, key in passed_on(seen, c, phase, key):
            link = ORDERS[c][2 - phase]
            size = SIDE if key[2] is None else 1
            free[link] = max(t, free.get(link, 0)) + size
            heapq.heappush(heap, (free[link] + latency, len(out) * WAYS + len(heap), c, phase, key))

    for c in range(0, WAYS, 2):
        hold(0, c, 0, (0, 0, 0))
    while heap:
        t, _, *arrival = heapq.heappop(heap)
        out.append(arrival)
        hold(t, *arrival)
    return out


def ag_kernel(*refs):
    mine, outs, (sends, recv1, recv2, recv3, recv4, local) = refs[0], refs[1 : 1 + WAYS], refs[1 + WAYS :]
    at = place()
    enter(at, LINES)

    def where(c, key):
        index = [None] * AXES
        for axis, d in zip(ORDERS[c], key, strict=True):
            index[axis] = slice(None) if d is None else wrap(at[axis] - SIGNS[c] * d)
        return outs[c].at[tuple(index)]

    def arrived(c, phase, key):
        d1, d2, d3 = key
        if phase == 0:
            return recv1.at[c // 2, d3 - 1]
        if phase == 1:
            return recv2.at[c // 2, d2 - 1, d3]
        if d3 is not None:
            return recv3.at[c // 2, d1 - 1, d3]
        return recv4.at[c // 2, d1 - 1, d2 - 1]

    def send_on(c, phase, key):
        d1, d2, d3 = key
        back = list(key)
        back[2 - phase] -= 1
        there = where(c, back)
        src = there if any(d != 0 for d in back) else mine.at[c]
        remote(src, there, sends.at[c, phase], arrived(c, phase, key), neighbour(at, ORDERS[c][2 - phase], SIGNS[c])).start()

    seen = []

    def hold(*held):
        for phase, key in passed_on(seen, *held):
            send_on(held[0], phase, key)

    own = [pltpu.make_async_copy(mine.at[c], where(c, (0, 0, 0)), local.at[c]) for c in range(WAYS)]
    for c in range(WAYS):
        hold(c, 0, (0, 0, 0))
    for copied in own:
        copied.start()
    for even, phase, key in ag_order():
        two = outs[even].at[0, pl.ds(0, 2)] if key[2] is None else outs[even].at[0, 0, pl.ds(0, 2)]
        pltpu.make_async_copy(two, two, arrived(even, phase, key)).wait()
        for c in (even, even + 1):
            hold(c, phase, key)
    for c in range(WAYS):
        own[c].wait()
        sent = outs[c].at[pl.ds(0, STEPS)]
        for phase in (2, 1, 0):
            pltpu.make_async_copy(sent, sent, sends.at[c, phase]).wait()
            sent = outs[c].at[(0,) * (AXES - phase) + (pl.ds(0, STEPS),)]


def all_gather(mine):
    return pl.pallas_call(
        ag_kernel,
        out_shape=(pltpu.VMEM((SIDE, SIDE, SIDE, *mine.shape[1:]), BF16),) * WAYS,
        in_specs=[VMEM],
        out_specs=(VMEM,) * WAYS,
        scratch_shapes=[DMA((WAYS, AXES)), DMA((AXES, STEPS)), *[DMA((AXES, STEPS, SIDE))] * 2, DMA((AXES, STEPS, STEPS)), DMA((WAYS,))],
        compiler_params=pltpu.CompilerParams(collective_id=1, has_side_effects=True, vmem_limit_bytes=MOST_VMEM // SUBLANES),
        name="gather",
    )(mine)


def tiles_of(t, rows, columns):
    n = columns // LANES
    if t < 2:
        return [(0, rows, j * LANES, j * rows) for j in range(n)]
    return [(8 * i, 8, j * LANES, (i * n + j) * 8) for i in range(rows // 8) for j in range(n)]


def adam_kernel(count, g, total, *refs):
    ws, ms, vs = (refs[AXES * k : AXES * (k + 1)] for k in range(3))
    new, *refs = refs[3 * AXES :]
    *moments, wide_g, wide_w = refs
    new_m, new_v = moments[:AXES], moments[AXES:]
    factor = jnp.minimum(1.0, 0.5 * lax.rsqrt(jnp.full((1, 1), jnp.sum(total[...])) / count + 1e-30))
    for t in range(AXES):
        rows, columns = ws[t].shape[1:]
        for l in range(LAYERS):
            wide_g[...] = g[TAKEN[LAYERS * t + l]].astype(F32) * factor
            for row, n, column, at in tiles_of(t, rows, columns):
                lanes = pl.ds(column, LANES)
                here = (slice(None), l, lanes) if t < 2 else (l, pl.ds(row, n), lanes)
                grad = wide_g[pl.ds(at, n), :]
                m = 0.9 * ms[t][here] + 0.1 * grad
                v = 0.95 * vs[t][here] + 0.05 * grad * grad
                w = ws[t][l, pl.ds(row, n), lanes]
                new_m[t][here] = m
                new_v[t][here] = v
                wide_w[pl.ds(at, n), :] = w - 0.02 * (m * lax.rsqrt(v + 1e-8) + 0.1 * w)
            new[LAYERS * t + l] = wide_w[...].astype(BF16)


def adam(count, g, total, ws, ms, vs):
    ms, vs = ([*(jnp.swapaxes(a, 0, 1) for a in arrays[:2]), arrays[2]] for arrays in (ms, vs))
    like = [jax.ShapeDtypeStruct(m.shape, F32) for m in ms]
    new, *moments = pl.pallas_call(
        functools.partial(adam_kernel, count),
        out_shape=(pltpu.VMEM(g.shape, BF16), *like, *like),
        in_specs=[VMEM] * (2 + AXES * 3),
        out_specs=(VMEM,) * (1 + AXES * 2),
        scratch_shapes=[pltpu.VMEM(g.shape[1:], F32)] * 2,
        compiler_params=pltpu.CompilerParams(vmem_limit_bytes=MOST_VMEM // SIDE),
        name="adam",
    )(g, total, *ws, *ms, *vs)
    return new, *([*(jnp.swapaxes(a, 0, 1) for a in part[:2]), part[2]] for part in (moments[:AXES], moments[AXES:]))


def natural_kernel(*refs):
    gathered, outs, wide = refs[:MATRICES], refs[MATRICES:-AXES], refs[-AXES:]
    first = pl.program_id(0) * SUBLANES
    for t in range(AXES):
        for l in range(LAYERS):
            rows, columns = outs[t].shape[1:]
            for k in range(SUBLANES):
                block = gathered[LAYERS * t + l][first + k].astype(F32)
                for row, n, column, at in tiles_of(t, rows // SUBLANES, columns):
                    wide[t][pl.ds(k * rows // SUBLANES + row, n), pl.ds(column, LANES)] = block[at : at + n]
            outs[t][l] = wide[t][...].astype(BF16)


def natural(gathered):
    shapes = (GATE, GATE, DOWN)
    return pl.pallas_call(
        natural_kernel,
        grid=(SUBLANES,),
        out_shape=tuple(jax.ShapeDtypeStruct((LAYERS, *s), BF16) for s in shapes),
        in_specs=[VMEM] * MATRICES,
        out_specs=tuple(pl.BlockSpec((LAYERS, s[0] // SUBLANES, s[1]), lambda i: (0, i, 0)) for s in shapes),
        scratch_shapes=[pltpu.VMEM((s[0] // SUBLANES, s[1]), F32) for s in shapes],
        compiler_params=pltpu.CompilerParams(vmem_limit_bytes=MOST_VMEM // SIDE),
        name="natural",
    )(*[g.reshape(DEVICES, BLOCK, LANES) for g in gathered])


D, FF, TOKENS = 896, 2560, 2048
GATE, DOWN = (D, FF), (FF, D)
ROWS, CHUNK, TILE = 256, 256, 512
TILES, PIECE, PLANE_ROWS = FF // TILE, BLOCK * TILE // FF, FF // SIDE
NT = (((1,), (1,)), ((), ()))


def dot(a, b):
    return jnp.dot(a, b, preferred_element_type=F32)


def dot_t(a, b):
    return lax.dot_general(a, b, NT, preferred_element_type=F32)


def scale_of(wide):
    return lax.rsqrt(jnp.mean(wide * wide, -1, keepdims=True) + 1e-6)


def rows_kernel(x_hbm, dy_hbm, *refs):
    hbm, results, weights, rest = refs[:3], refs[3:7], refs[7:13], refs[13:]
    buffers, (xs, dys, g0, u0, z0, dz1, sems, part_sems, in_sems, out_sems) = rest[:4], rest[4:]
    wg0, wu0, wd0, wg1, wu1, wd1 = weights
    i, slot = pl.program_id(0), pl.program_id(0) % 2
    first = i == 0
    chunks = [pl.ds(j * CHUNK, CHUNK) for j in range(FF // CHUNK)]

    def fetch(k):
        return pltpu.make_async_copy(hbm[k % 3].at[k // 3], weights[k], sems.at[k])

    def fetch_part(k, j):
        return pltpu.make_async_copy(hbm[k].at[0, :, chunks[j]], weights[k].at[:, chunks[j]], part_sems.at[k, j])

    def take(i):
        rows = pl.ds(pl.multiple_of(i * ROWS, ROWS), ROWS)
        for k, (source, there) in enumerate(((x_hbm, xs), (dy_hbm, dys))):
            yield pltpu.make_async_copy(source.at[rows], there.at[i % 2], in_sems.at[i % 2, k])

    def put(k, part):
        rows = pl.ds(pl.multiple_of(i * ROWS, ROWS), ROWS)
        there = results[k].at[part, rows] if k % 2 else results[k].at[part, :, rows]
        return pltpu.make_async_copy(buffers[k].at[slot, part], there, out_sems.at[slot, k, part])

    def outs():
        return [put(k, part) for k in range(4) for part in range(results[k].shape[0])]

    @pl.when(first)
    def _():
        for copy in take(0):
            copy.start()
        for j in range(len(chunks)):
            for k in range(2):
                fetch_part(k, j).start()

    for copy in take(i):
        copy.wait()

    @pl.when(i + 1 < pl.num_programs(0))
    def _():
        for copy in take(i + 1):
            copy.start()

    @pl.when(i > 1)
    def _():
        for copy in outs():
            copy.wait()

    tall, wide, turned, deep = (b.at[slot] for b in buffers)
    x, dy = xs.at[slot], dys.at[slot]

    def forward(coming):
        a = (x[...].astype(F32) * scale_of(x[...].astype(F32))).astype(BF16)
        tall[1] = a.T
        deep[0] = dy[...]
        for j, ch in enumerate(chunks):
            if coming:
                for k in range(2):
                    fetch_part(k, j).wait()
                if 0 < j < 5:
                    fetch(j + 1).start()
            gate, up = dot(a, wg0[:, ch]), dot(a, wu0[:, ch])
            g0[:, ch], u0[:, ch] = gate, up
            z0[:, ch] = (gate * jax.nn.sigmoid(gate) * up).astype(BF16)
            turned[1, ch, :] = z0[:, ch].T

    @pl.when(first)
    def _():
        forward(True)
        for k in range(2, MATRICES):
            fetch(k).wait()

    @pl.when(i > 0)
    def _():
        forward(False)

    for k, part in ((0, 1), (3, 0), (2, 1)):
        put(k, part).start()
    for ch in chunks[:SIDE]:
        dz1[:, ch] = dot_t(dy[...], wd1[ch, :]).astype(BF16)
    h = x[...] + dot(z0[...], wd0[...]).astype(BF16)
    for ch in chunks[SIDE:]:
        dz1[:, ch] = dot_t(dy[...], wd1[ch, :]).astype(BF16)
    h = h.astype(F32)
    scale = scale_of(h)
    a = (h * scale).astype(BF16)
    tall[0] = a.T
    put(0, 0).start()
    for ch in chunks:
        gate, up = dot(a, wg1[:, ch]), dot(a, wu1[:, ch])
        dz = dz1[:, ch].astype(F32)
        s = jax.nn.sigmoid(gate)
        silu = gate * s
        turned[0, ch, :] = (silu * up).astype(BF16).T
        wide[1, :, ch] = (dz * silu).astype(BF16)
        wide[0, :, ch] = (dz * up * (s * (1 + gate * (1 - s)))).astype(BF16)
    for k, part in ((2, 0), (1, 0), (1, 1)):
        put(k, part).start()
    most, rest = pl.ds(0, FF - CHUNK), chunks[-1]
    da_gate, da_up = dot_t(wide[0, :, most], wg1[:, most]), dot_t(wide[1, :, most], wu1[:, most])
    da_gate, da_up = da_gate + dot_t(wide[0, :, rest], wg1[:, rest]), da_up + dot_t(wide[1, :, rest], wu1[:, rest])
    da = (da_gate.astype(BF16) + da_up.astype(BF16)).astype(F32)
    dwide = scale * (da - h * (scale * scale * jnp.mean(da * h, -1, keepdims=True)))
    dh = dy[...] + dwide.astype(BF16)
    deep[1] = dh
    put(3, 1).start()
    for ch in chunks:
        dz = dot_t(dh, wd0[ch, :]).astype(BF16).astype(F32)
        gate, up = g0[:, ch], u0[:, ch]
        s = jax.nn.sigmoid(gate)
        wide[3, :, ch] = (dz * (gate * s)).astype(BF16)
        wide[2, :, ch] = (dz * up * (s * (1 + gate * (1 - s)))).astype(BF16)
    put(1, 2).start()
    put(1, 3).start()

    @pl.when(i + 1 == pl.num_programs(0))
    def _():
        for copy in outs():
            copy.wait()

    @pl.when(i + 1 == pl.num_programs(0))
    def _():
        for k in range(4):
            for part in range(results[k].shape[0]):
                pltpu.make_async_copy(buffers[k].at[1 - slot, part], buffers[k].at[1 - slot, part], out_sems.at[1 - slot, k, part]).wait()


def by_rows(x, dy, weights):
    shapes = ((2, D, TOKENS), (4, TOKENS, FF), (2, FF, TOKENS), (2, TOKENS, D))
    buffers = ((2, D, ROWS), (4, ROWS, FF), (2, FF, ROWS), (2, ROWS, D))
    return pl.pallas_call(
        rows_kernel,
        grid=(TOKENS // ROWS,),
        out_shape=tuple(jax.ShapeDtypeStruct(s, BF16) for s in shapes),
        in_specs=[HBM] * 5,
        out_specs=(HBM,) * 4,
        scratch_shapes=[
            *[pltpu.VMEM(w.shape[1:], BF16) for w in weights * 2],
            *[pltpu.VMEM((2, *b), BF16) for b in buffers],
            *[pltpu.VMEM((2, ROWS, D), BF16)] * 2,
            *[pltpu.VMEM((ROWS, FF), F32)] * 2,
            *[pltpu.VMEM((ROWS, FF), BF16)] * 2,
            DMA((MATRICES,)), DMA((2, FF // CHUNK)), DMA((2, 2)), DMA((2, 4, 4)),
        ],
        compiler_params=pltpu.CompilerParams(vmem_limit_bytes=MOST_VMEM),
        name="rows",
    )(x, dy, *weights)


GATE_ROWS, DOWN_ROWS = D // DEVICES, FF // DEVICES
STARTS = (0, 48, 96, 144, 192, 232)
PART = 48


def gate_block(acc, stage, wide):
    def group(i, _):
        rows = pl.ds(pl.multiple_of(i * PIECE, SUBLANES), PIECE)
        for c in range(SIDE):
            piece = acc[rows, pl.ds(c * LANES, LANES)]
            for z in range(SIDE):
                wide[z, pl.ds(GATE_ROWS * c, GATE_ROWS), :] = piece[GATE_ROWS * z : GATE_ROWS * (z + 1)]
        for z in range(SIDE):
            stage[i // SIDE, i % SIDE, z] = wide[z].astype(BF16)
        return 0

    lax.fori_loop(0, PLANE, group, 0)


def down_block(acc, stage):
    def group(i, _):
        for t in range(DOWN_ROWS // SUBLANES):
            rows = acc[pl.ds(pl.multiple_of(i * DOWN_ROWS, SUBLANES) + SUBLANES * t, SUBLANES), :]
            piece = jnp.concatenate([rows[:, c * LANES : (c + 1) * LANES] for c in range(D // LANES)], 0)
            stage[i // SIDE, i % SIDE, pl.ds(PIECE * t, PIECE)] = piece.astype(BF16)
        return 0

    lax.fori_loop(0, PLANE, group, 0)


def own_rows(ws, windows, owns, sems):
    me = lax.axis_index("dp")
    taken = []
    for t in range(AXES):
        rows = windows[t].shape[1]
        first = pl.multiple_of((me // SIDE if t < 2 else me) * rows, SUBLANES)
        taken.append(pltpu.make_async_copy(ws[t].at[:, pl.ds(first, rows)], windows[t], sems.at[t]))
        taken[t].start()
    for t in range(AXES):
        taken[t].wait()
        rows = owns[t].shape[1]
        if t == 2:
            owns[t][...] = windows[t][...].astype(F32)
        for z in range(SIDE if t < 2 else 0):

            @pl.when(me % SIDE == z)
            def _():
                for l in range(LAYERS):
                    owns[t][l] = windows[t][l].astype(F32)[z * rows : (z + 1) * rows]


def gradients_kernel(*refs):
    (tall, wide, turned, deep), ws, (out, squares, terms), owns, scratch = refs[:4], refs[4:7], refs[7:10], refs[10:13], refs[13:]
    (lhs, rhs, zs, dh, acc, acc2, stage, stage2, shift, ra, rf, qa, qf, r3, own, f1, f2, sums) = scratch[:18]
    *windows, window_sem = scratch[18:22]
    (in_sem, rhs_sem, zs_sem, put_sem, sent, first_a, first_f, second_a, second_f, recv3, load, send4, recv4) = scratch[22:]
    at = place()

    def fetch_tall(l):
        return pltpu.make_async_copy(tall.at[l], lhs, in_sem.at[0])

    def fetch_deep(l):
        return pltpu.make_async_copy(deep.at[l], dh, in_sem.at[1])

    def fetch_wide(t):
        columns = pl.ds(pl.multiple_of(t % TILES * TILE, TILE), TILE)
        return pltpu.make_async_copy(wide.at[t // TILES, :, columns], rhs.at[t % 2], rhs_sem.at[t % 2])

    def fetch_turned(t):
        rows = pl.ds(pl.multiple_of(t % SIDE * PLANE_ROWS, LANES), PLANE_ROWS)
        return pltpu.make_async_copy(turned.at[t // SIDE, rows], zs.at[t % 2], zs_sem.at[t % 2])

    def put(m, h):
        return pltpu.make_async_copy(stage, terms.at[m, :, :, :, pl.ds(pl.multiple_of(PIECE * h, SUBLANES), PIECE)], put_sem.at[0])

    def put2(m, h):
        return pltpu.make_async_copy(stage2, terms.at[m, h], put_sem.at[1])

    fetch_tall(0).start()
    fetch_wide(0).start()
    fetch_deep(0).start()
    fetch_turned(0).start()
    enter(at, sorted({*LINES, *PLANE_PEERS}))

    def split(c):
        o, s = ORDERS[c], SIGNS[c]
        return o, s, at[o[0]], at[o[1]], at[o[2]]

    def block(m, c, a, i):
        o = ORDERS[c]
        index = [slice(None)] * 3
        index[o[0]] = a
        if i is not None:
            index[o[1]] = i
        return terms.at[(m, *index, pl.ds(STARTS[c], PART))]

    def piece(c, j):
        return wrap(split(c)[3] + SIGNS[c] * (2 + j - j // 2 * (2 * j - 1)))

    def along(c, axis, src, there, sem, recv, steps=1):
        return remote(src, there, sent.at[sem], recv, neighbour(at, ORDERS[c][axis], SIGNS[c] * steps))

    def launch(m):
        for j in range(SIDE):
            for c in range(WAYS):
                src = block(m, c, wrap(split(c)[2] + 2 * SIGNS[c]), piece(c, j))
                along(c, 0, src, ra.at[c, m, j], 0, first_a.at[m, j]).start()
        for j in range(SIDE):
            for c in range(WAYS):
                src = block(m, c, wrap(split(c)[2] - SIGNS[c]), piece(c, j))
                along(c, 0, src, rf.at[c, m, 1, j], 1, first_f.at[m, j], -1).start()

    def load_own(m):
        for k in range(2):
            for c in range(WAYS):
                mine = block(m, c, wrap(split(c)[2] + SIGNS[c] * (1 - k)), None)
                pltpu.make_async_copy(mine, own.at[c, k], load.at[k]).start()

    def whole(ref, sem):
        pltpu.make_async_copy(ref, ref, sem).wait()

    def term(c, k, j):
        i = piece(c, j)
        mine = own[c, k, i] if ORDERS[c][1] < ORDERS[c][2] else own[c, k, :, i]
        return mine.astype(F32)

    def on_first_a(m, j):
        whole(ra.at[:, m, j], first_a.at[m, j])
        for c in range(WAYS):
            ra[c, m, j] = (ra[c, m, j].astype(F32) + term(c, 0, j)).astype(BF16)
            along(c, 0, ra.at[c, m, j], rf.at[c, m, 0, j], 1, first_f.at[m, j]).start()

    def on_first_f(m, j):
        whole(rf.at[:, m, :, j], first_f.at[m, j])
        for c in range(WAYS):
            total = rf[c, m, 0, j].astype(F32) + rf[c, m, 1, j].astype(F32) + term(c, 1, j)
            if j < 2:
                rf[c, m, 1, j] = total.astype(BF16)
            else:
                f1[c, j - 2] = total
            if j == 0:
                along(c, 1, rf.at[c, m, 1, j], qa.at[c, m], 2, second_a.at[m]).start()
            if j == 1:
                along(c, 1, rf.at[c, m, 1, j], qf.at[c, m, 1], 3, second_f.at[m], -1).start()

    def on_second_a(m):
        whole(qa.at[:, m], second_a.at[m])
        for c in range(WAYS):
            qa[c, m] = (qa[c, m].astype(F32) + f1[c, 0]).astype(BF16)
            along(c, 1, qa.at[c, m], qf.at[c, m, 0], 3, second_f.at[m]).start()

    def third(m, c, k):
        src = qf.at[c, m, 1, wrap(split(c)[4] + k + 1)]
        return remote(src, r3.at[c, m, k], sent.at[4], recv3.at[m], neighbour(at, ORDERS[c][2], k + 1))

    def on_second_f(m):
        whole(qf.at[:, m], second_f.at[m])
        for c in range(WAYS):
            total = qf[c, m, 0].astype(F32) + qf[c, m, 1].astype(F32) + f1[c, 1]
            f2[c] = total
            qf[c, m, 1] = total.astype(BF16)
            for k in range(STEPS):
                third(m, c, k).start()

    def on_third(m):
        whole(r3.at[:, m], recv3.at[m])
        for c in range(WAYS):
            o, s, p1, p2, p3 = split(c)
            total = f2[c, p3]
            for k in range(STEPS):
                total = total + r3[c, m, k].astype(F32)
            out[m, pl.ds(STARTS[c], PART)] = total.astype(BF16)

    def tile(i, _):
        m, h = i // TILES, i % TILES
        kind, l = m % AXES, m // AXES

        @pl.when((h == 0) & (m > 0) & (m < MATRICES + 1))
        def _():
            @pl.when(kind > 0)
            def _():
                put(0, 0).wait()

            @pl.when(kind == 0)
            def _():
                put2(0, 0).wait()

            launch(m - 1)

        @pl.when((m < MATRICES) & (kind < 2))
        def _():
            t = (2 * l + kind) * TILES + h

            @pl.when((kind == 0) & (h == 0))
            def _():
                fetch_tall(l).wait()

                @pl.when(l == 1)
                def _():
                    fetch_deep(1).start()

            fetch_wide(t).wait()

            @pl.when(t < 19)
            def _():
                fetch_wide(t + 1).start()

            acc[...] = dot(lhs[...], rhs[t % 2])

            @pl.when(h > 0)
            def _():
                put(m, h).wait()

            gate_block(acc, stage, shift)
            put(m, h).start()

        @pl.when((m < MATRICES) & (kind == 2) & (h < SIDE))
        def _():
            t = SIDE * l + h

            @pl.when(h == 0)
            def _():
                fetch_deep(l).wait()

                @pl.when(l == 0)
                def _():
                    fetch_tall(1).start()

            fetch_turned(t).wait()

            @pl.when(t < 7)
            def _():
                fetch_turned(t + 1).start()

            acc2[...] = dot(zs[t % 2], dh[...])

            @pl.when(h > 0)
            def _():
                put2(m, h).wait()

            down_block(acc2, stage2)
            put2(m, h).start()

        @pl.when((h == 0) & (m > 2))
        def _():
            on_third(m - AXES)

        @pl.when((h == 2) & (m > 1))
        def _():
            on_second_a(m - 2)

        @pl.when((h == SIDE) & (m > 1))
        def _():
            on_second_f(m - 2)

        @pl.when((h == SIDE) & (m > 0) & (m < MATRICES + 1))
        def _():
            whole(own.at[:, 1], load.at[1])
            for j in range(2):
                on_first_f(m - 1, j)

        @pl.when((h == 0) & (m > 1))
        def _():
            for j in range(2, SIDE):
                on_first_f(m - 2, j)

        @pl.when(((h == 1) | (h == 2)) & (m > 0) & (m < MATRICES + 1))
        def _():
            @pl.when(h == 1)
            def _():
                whole(own.at[:, 0], load.at[0])

            lax.fori_loop(h - 1, AXES * h - 2, lambda j, _: (on_first_a(m - 1, j), 0)[1], 0)

        @pl.when((h == 0) & (m > 0) & (m < MATRICES + 1))
        def _():
            load_own(m - 1)

        return 0

    lax.fori_loop(0, (MATRICES + 2) * TILES, tile, 0)
    own_rows(ws, windows, owns, window_sem)
    on_third(MATRICES - 1)

    total = jnp.zeros((SUBLANES, LANES), F32)
    for m in range(MATRICES):
        g = out[m].astype(F32)
        total = total + jnp.sum((g * g).reshape(-1, SUBLANES, LANES), axis=0)
    squares[...] = norm_exchange(at, sums, send4, recv4, total)
    for k, buffer in enumerate((ra, rf, qa, qf, r3)):
        whole(buffer, sent.at[k])


def gradients(tall, wide, turned, deep, weights):
    g, squares, _, *owns = pl.pallas_call(
        gradients_kernel,
        out_shape=(
            pltpu.VMEM((MATRICES, BLOCK, LANES), BF16),
            pltpu.VMEM((SUBLANES, LANES), F32),
            jax.ShapeDtypeStruct((MATRICES, SIDE, SIDE, SIDE, BLOCK, LANES), BF16),
            *[pltpu.VMEM((LAYERS, w.shape[1] // DEVICES, w.shape[2]), F32) for w in weights],
        ),
        in_specs=[HBM] * (4 + AXES),
        out_specs=(VMEM, VMEM, HBM, *[VMEM] * AXES),
        scratch_shapes=[
            pltpu.VMEM((D, TOKENS), BF16),
            pltpu.VMEM((2, TOKENS, TILE), BF16),
            pltpu.VMEM((2, PLANE_ROWS, TOKENS), BF16),
            pltpu.VMEM((TOKENS, D), BF16),
            pltpu.VMEM((D, TILE), F32),
            pltpu.VMEM((PLANE_ROWS, D), F32),
            pltpu.VMEM((SIDE, SIDE, SIDE, PIECE, LANES), BF16),
            pltpu.VMEM((SIDE, SIDE, BLOCK, LANES), BF16),
            pltpu.VMEM((SIDE, PIECE, LANES), F32),
            pltpu.VMEM((WAYS, MATRICES, SIDE, SIDE, PART, LANES), BF16),
            pltpu.VMEM((WAYS, MATRICES, 2, SIDE, SIDE, PART, LANES), BF16),
            pltpu.VMEM((WAYS, MATRICES, SIDE, PART, LANES), BF16),
            pltpu.VMEM((WAYS, MATRICES, 2, SIDE, PART, LANES), BF16),
            pltpu.VMEM((WAYS, MATRICES, STEPS, PART, LANES), BF16),
            pltpu.VMEM((WAYS, 2, SIDE, SIDE, PART, LANES), BF16),
            pltpu.VMEM((WAYS, 2, SIDE, PART, LANES), F32),
            pltpu.VMEM((WAYS, SIDE, PART, LANES), F32),
            pltpu.VMEM((PLANE + SIDE, SUBLANES, LANES), F32),
            *[pltpu.VMEM((LAYERS, w.shape[1] // n, w.shape[2]), BF16) for w, n in zip(weights, (PLANE, PLANE, DEVICES), strict=True)],
            DMA((AXES,)),
            *[DMA((2,))] * 4,
            DMA((TILES,)),
            *[DMA((MATRICES, SIDE))] * 2, *[DMA((MATRICES,))] * 3,
            DMA((2,)),
            DMA((2,)), DMA((2,)),
        ],
        compiler_params=pltpu.CompilerParams(collective_id=0, has_side_effects=True, vmem_limit_bytes=MOST_VMEM - SPARE_VMEM),
        name="gradients",
    )(tall, wide, turned, deep, *weights)
    return g, squares, owns


def solution(mesh):
    rep, dp = mesh.axis_names

    def step(x, dy, *arrays):
        weights, m, v = (arrays[i : i + 3] for i in (0, 3, 6))
        g, total, owns = gradients(*by_rows(x[0], dy[0], weights), weights)
        new, new_m, new_v = adam(MATRICES * D * FF, g, total, owns, m, v)
        return (*natural(all_gather(new)), *new_m, *new_v)

    whole, rows, sequences = P(), P(None, dp), P((rep, dp))
    return jax.shard_map(
        step,
        mesh=mesh,
        in_specs=(sequences, sequences, *[whole] * AXES, *[rows] * MATRICES),
        out_specs=(*[P(rep)] * AXES, *[P(rep, dp)] * MATRICES),
        check_vma=False,
    )
```

```python
import functools
import jax
import jax.numpy as jnp
from jax import lax
from jax.experimental import pallas as pl
from jax.experimental.pallas import tpu as pltpu
from jax.sharding import PartitionSpec as P

MESH = pl.DeviceIdType.MESH
WAYS, AXES, SIDE = 6, 3, 4
STEPS = SIDE - 1
MATRICES, LAYERS, DEVICES, PLANE = 6, 2, 64, 16
LANES, SUBLANES, BLOCK = 128, 8, 280
BF16, F32 = jnp.bfloat16, jnp.float32
HBM, VMEM = pl.BlockSpec(memory_space=pl.ANY), pl.BlockSpec(memory_space=pltpu.VMEM)
DMA = pltpu.SemaphoreType.DMA
MIB = 1 << 20
MOST_VMEM, SPARE_VMEM = 62 * MIB, 2 * MIB
ORDERS = tuple(tuple((way // 2 + i) % AXES for i in range(AXES)) for way in range(WAYS))
SIGNS = (1, -1) * AXES
TAKEN = (3, 0, 4, 1, 5, 2)


def place():
    me = lax.axis_index("dp")
    return (me // PLANE, me // SIDE % SIDE, me % SIDE)


def wrap(i):
    return (i + 3 * SIDE) % SIDE


def neighbour(at, axis, step):
    there = [c for c in at]
    there[axis] = wrap(at[axis] + step)
    return {"dp": (there[0] * SIDE + there[1]) * SIDE + there[2]}


def remote(src, dst, send, recv, to):
    return pltpu.make_async_remote_copy(src_ref=src, dst_ref=dst, send_sem=send, recv_sem=recv, device_id=to, device_id_type=MESH)


def moved(at, steps):
    x, y, z = (wrap(a + step) for a, step in zip(at, steps, strict=True))
    return {"dp": (x * SIDE + y) * SIDE + z}


LINES = tuple(tuple(k * (axis == line) for axis in range(AXES)) for line in range(AXES) for k in range(1, SIDE))
PLANE_PEERS = tuple((0, k // SIDE, k % SIDE) for k in range(1, PLANE))
LINE_PEERS = LINES[:STEPS]


def enter(at, peers):
    barrier = pltpu.get_barrier_semaphore()
    for steps in peers:
        pl.semaphore_signal(barrier, inc=1, device_id=moved(at, steps), device_id_type=MESH)
    pl.semaphore_wait(barrier, len(peers))


def norm_exchange(at, buf, send, recv, total):
    first = 0
    for stage, peers in enumerate((PLANE_PEERS, LINE_PEERS)):
        own, others = buf.at[first], buf.at[pl.ds(first + 1, len(peers))]
        own[...] = total
        for k, steps in enumerate(peers):
            remote(own, others.at[k], send.at[stage], recv.at[stage], moved(at, steps)).start()
        pltpu.make_async_copy(others, others, recv.at[stage]).wait()
        total = total + jnp.sum(others[...], axis=0)
        pltpu.make_async_copy(others, others, send.at[stage]).wait()
        first += 1 + len(peers)
    return total


def passed_on(seen, c, phase, key):
    d1, d2, d3 = key
    if phase == 0 and d3 < STEPS:
        yield 0, (0, 0, d3 + 1)
    if phase < 2 and d2 < STEPS:
        yield 1, (0, d2 + 1, d3)
    if phase == 1 and d2 > 0:
        seen.append((c, d2))
        if seen.count((c, d2)) < SIDE:
            return
        d3 = None
    if d1 < STEPS:
        yield 2, (d1 + 1, d2, d3)


def ag_order(latency=2):
    import heapq

    free, out, seen, heap = {}, [], [], []

    def hold(t, c, phase, key):
        for phase, key in passed_on(seen, c, phase, key):
            link = ORDERS[c][2 - phase]
            size = SIDE if key[2] is None else 1
            free[link] = max(t, free.get(link, 0)) + size
            heapq.heappush(heap, (free[link] + latency, len(out) * WAYS + len(heap), c, phase, key))

    for c in range(0, WAYS, 2):
        hold(0, c, 0, (0, 0, 0))
    while heap:
        t, _, *arrival = heapq.heappop(heap)
        out.append(arrival)
        hold(t, *arrival)
    return out


def ag_kernel(*refs):
    mine, outs, (sends, recv1, recv2, recv3, recv4, local) = refs[0], refs[1 : 1 + WAYS], refs[1 + WAYS :]
    at = place()
    enter(at, LINES)

    def where(c, key):
        index = [None] * AXES
        for axis, d in zip(ORDERS[c], key, strict=True):
            index[axis] = slice(None) if d is None else wrap(at[axis] - SIGNS[c] * d)
        return outs[c].at[tuple(index)]

    def arrived(c, phase, key):
        d1, d2, d3 = key
        if phase == 0:
            return recv1.at[c // 2, d3 - 1]
        if phase == 1:
            return recv2.at[c // 2, d2 - 1, d3]
        if d3 is not None:
            return recv3.at[c // 2, d1 - 1, d3]
        return recv4.at[c // 2, d1 - 1, d2 - 1]

    def send_on(c, phase, key):
        d1, d2, d3 = key
        back = list(key)
        back[2 - phase] -= 1
        there = where(c, back)
        src = there if any(d != 0 for d in back) else mine.at[c]
        remote(src, there, sends.at[c, phase], arrived(c, phase, key), neighbour(at, ORDERS[c][2 - phase], SIGNS[c])).start()

    seen = []

    def hold(*held):
        for phase, key in passed_on(seen, *held):
            send_on(held[0], phase, key)

    own = [pltpu.make_async_copy(mine.at[c], where(c, (0, 0, 0)), local.at[c]) for c in range(WAYS)]
    for c in range(WAYS):
        hold(c, 0, (0, 0, 0))
    for copied in own:
        copied.start()
    for even, phase, key in ag_order():
        two = outs[even].at[0, pl.ds(0, 2)] if key[2] is None else outs[even].at[0, 0, pl.ds(0, 2)]
        pltpu.make_async_copy(two, two, arrived(even, phase, key)).wait()
        for c in (even, even + 1):
            hold(c, phase, key)
    for c in range(WAYS):
        own[c].wait()
        sent = outs[c].at[pl.ds(0, STEPS)]
        for phase in (2, 1, 0):
            pltpu.make_async_copy(sent, sent, sends.at[c, phase]).wait()
            sent = outs[c].at[(0,) * (AXES - phase) + (pl.ds(0, STEPS),)]


def all_gather(mine):
    return pl.pallas_call(
        ag_kernel,
        out_shape=(pltpu.VMEM((SIDE, SIDE, SIDE, *mine.shape[1:]), BF16),) * WAYS,
        in_specs=[VMEM],
        out_specs=(VMEM,) * WAYS,
        scratch_shapes=[DMA((WAYS, AXES)), DMA((AXES, STEPS)), *[DMA((AXES, STEPS, SIDE))] * 2, DMA((AXES, STEPS, STEPS)), DMA((WAYS,))],
        compiler_params=pltpu.CompilerParams(collective_id=1, has_side_effects=True, vmem_limit_bytes=MOST_VMEM // SUBLANES),
        name="gather",
    )(mine)


def tiles_of(t, rows, columns):
    n = columns // LANES
    if t < 2:
        return [(0, rows, j * LANES, j * rows) for j in range(n)]
    return [(8 * i, 8, j * LANES, (i * n + j) * 8) for i in range(rows // 8) for j in range(n)]


def adam_kernel(count, g, total, *refs):
    ws, ms, vs = (refs[AXES * k : AXES * (k + 1)] for k in range(3))
    new, *refs = refs[3 * AXES :]
    *moments, wide_g, wide_w = refs
    new_m, new_v = moments[:AXES], moments[AXES:]
    factor = jnp.minimum(1.0, 0.5 * lax.rsqrt(jnp.full((1, 1), jnp.sum(total[...])) / count + 1e-30))
    for t in range(AXES):
        rows, columns = ws[t].shape[1:]
        for l in range(LAYERS):
            wide_g[...] = g[TAKEN[LAYERS * t + l]].astype(F32) * factor
            for row, n, column, at in tiles_of(t, rows, columns):
                lanes = pl.ds(column, LANES)
                here = (slice(None), l, lanes) if t < 2 else (l, pl.ds(row, n), lanes)
                grad = wide_g[pl.ds(at, n), :]
                m = 0.9 * ms[t][here] + 0.1 * grad
                v = 0.95 * vs[t][here] + 0.05 * grad * grad
                w = ws[t][l, pl.ds(row, n), lanes]
                new_m[t][here] = m
                new_v[t][here] = v
                wide_w[pl.ds(at, n), :] = w - 0.02 * (m * lax.rsqrt(v + 1e-8) + 0.1 * w)
            new[LAYERS * t + l] = wide_w[...].astype(BF16)


def adam(count, g, total, ws, ms, vs):
    ms, vs = ([*(jnp.swapaxes(a, 0, 1) for a in arrays[:2]), arrays[2]] for arrays in (ms, vs))
    like = [jax.ShapeDtypeStruct(m.shape, F32) for m in ms]
    new, *moments = pl.pallas_call(
        functools.partial(adam_kernel, count),
        out_shape=(pltpu.VMEM(g.shape, BF16), *like, *like),
        in_specs=[VMEM] * (2 + AXES * 3),
        out_specs=(VMEM,) * (1 + AXES * 2),
        scratch_shapes=[pltpu.VMEM(g.shape[1:], F32)] * 2,
        compiler_params=pltpu.CompilerParams(vmem_limit_bytes=MOST_VMEM // SIDE),
        name="adam",
    )(g, total, *ws, *ms, *vs)
    return new, *([*(jnp.swapaxes(a, 0, 1) for a in part[:2]), part[2]] for part in (moments[:AXES], moments[AXES:]))


def natural_kernel(*refs):
    gathered, outs, wide = refs[:MATRICES], refs[MATRICES:-AXES], refs[-AXES:]
    first = pl.program_id(0) * SUBLANES
    for t in range(AXES):
        for l in range(LAYERS):
            rows, columns = outs[t].shape[1:]
            for k in range(SUBLANES):
                block = gathered[LAYERS * t + l][first + k].astype(F32)
                for row, n, column, at in tiles_of(t, rows // SUBLANES, columns):
                    wide[t][pl.ds(k * rows // SUBLANES + row, n), pl.ds(column, LANES)] = block[at : at + n]
            outs[t][l] = wide[t][...].astype(BF16)


def natural(gathered):
    shapes = (GATE, GATE, DOWN)
    return pl.pallas_call(
        natural_kernel,
        grid=(SUBLANES,),
        out_shape=tuple(jax.ShapeDtypeStruct((LAYERS, *s), BF16) for s in shapes),
        in_specs=[VMEM] * MATRICES,
        out_specs=tuple(pl.BlockSpec((LAYERS, s[0] // SUBLANES, s[1]), lambda i: (0, i, 0)) for s in shapes),
        scratch_shapes=[pltpu.VMEM((s[0] // SUBLANES, s[1]), F32) for s in shapes],
        compiler_params=pltpu.CompilerParams(vmem_limit_bytes=MOST_VMEM // SIDE),
        name="natural",
    )(*[g.reshape(DEVICES, BLOCK, LANES) for g in gathered])


D, FF, TOKENS = 896, 2560, 2048
GATE, DOWN = (D, FF), (FF, D)
ROWS, CHUNK, TILE = 256, 256, 512
SOON, AHEAD, NEXT = 4, 6, 8
TILES, PIECE, PLANE_ROWS = FF // TILE, BLOCK * TILE // FF, FF // SIDE
NT = (((1,), (1,)), ((), ()))


def dot(a, b):
    return jnp.dot(a, b, preferred_element_type=F32)


def dot_t(a, b):
    return lax.dot_general(a, b, NT, preferred_element_type=F32)


def scale_of(wide):
    return lax.rsqrt(jnp.mean(wide * wide, -1, keepdims=True) + 1e-6)


def rows_kernel(x_hbm, dy_hbm, *refs):
    hbm, results, weights, rest = refs[:3], refs[3:7], refs[7:13], refs[13:]
    buffers, (xs, dys, g0, u0, z0, dz1, sems, part_sems, in_sems, out_sems) = rest[:4], rest[4:]
    wg0, wu0, wd0, wg1, wu1, wd1 = weights
    i, slot = pl.program_id(0), pl.program_id(0) % 2
    first, blocks = i == 0, pl.num_programs(0)
    chunks = [pl.ds(j * CHUNK, CHUNK) for j in range(FF // CHUNK)]

    def fetch(k):
        return pltpu.make_async_copy(hbm[k % 3].at[k // 3], weights[k], sems.at[k])

    def fetch_part(k, j):
        return pltpu.make_async_copy(hbm[k].at[0, :, chunks[j]], weights[k].at[:, chunks[j]], part_sems.at[k, j])

    def take(source, there, i):
        rows = pl.ds(pl.multiple_of(i * ROWS, ROWS), ROWS)
        slot = i % there.shape[0]
        return pltpu.make_async_copy(source.at[rows], there.at[slot], in_sems.at[there.shape[0] - 2, slot])

    def put(k, part, slot=slot):
        rows = pl.ds(pl.multiple_of(i * ROWS, ROWS), ROWS)
        there = results[k].at[part, rows] if k % 2 else results[k].at[part, :, rows]
        return pltpu.make_async_copy(buffers[k].at[slot, part], there, out_sems.at[slot, k, part])

    def outs(slot):
        return [put(k, part, slot) for k, result in enumerate(results) for part in range(result.shape[0])]

    @pl.when(first)
    def _():
        take(x_hbm, xs, 0).start()
        take(dy_hbm, dys, 0).start()
        for j in range(len(chunks)):
            for k in range(2):
                fetch_part(k, j).start()
        take(dy_hbm, dys, 1).start()
        take(dy_hbm, dys, 0).wait()

    take(x_hbm, xs, i).wait()

    @pl.when(i + 1 < blocks)
    def _():
        take(x_hbm, xs, i + 1).start()
        take(dy_hbm, dys, i + 1).wait()

    @pl.when(i + 2 < blocks)
    def _():
        take(dy_hbm, dys, i + 2).start()

    @pl.when(i > 1)
    def _():
        for copy in outs(slot):
            copy.wait()

    tall, wide, turned, deep = (b.at[slot] for b in buffers)
    x, dy, next_dy = xs.at[slot], dys.at[i % AXES], dys.at[(i + 1) % AXES]

    def make_dz1(dy, some):
        for ch in some:
            dz1[:, ch] = dot_t(dy[...], wd1[ch, :]).astype(BF16)

    def forward(coming):
        a = (x[...].astype(F32) * scale_of(x[...].astype(F32))).astype(BF16)
        tall[1] = a.T
        deep[0] = dy[...]
        for j, ch in enumerate(chunks):
            if coming:
                for k in range(2):
                    fetch_part(k, j).wait()
                if 0 < j < 5:
                    fetch(j + 1).start()
            gate, up = dot(a, wg0[:, ch]), dot(a, wu0[:, ch])
            g0[:, ch], u0[:, ch] = gate, up
            z0[:, ch] = (gate * jax.nn.sigmoid(gate) * up).astype(BF16)
            turned[1, ch, :] = z0[:, ch].T

    @pl.when(first)
    def _():
        forward(True)
        for k in range(2, MATRICES):
            fetch(k).wait()
        make_dz1(dy, chunks[:AHEAD])

    @pl.when(i > 0)
    def _():
        forward(False)

    for k, part in ((0, 1), (3, 0), (2, 1)):
        put(k, part).start()
    make_dz1(dy, chunks[AHEAD:NEXT])
    h = x[...] + dot(z0[...], wd0[...]).astype(BF16)
    make_dz1(dy, chunks[NEXT:])
    h = h.astype(F32)
    scale = scale_of(h)
    a = (h * scale).astype(BF16)
    tall[0] = a.T
    put(0, 0).start()
    for ch in chunks:
        gate, up = dot(a, wg1[:, ch]), dot(a, wu1[:, ch])
        dz = dz1[:, ch].astype(F32)
        s = jax.nn.sigmoid(gate)
        silu = gate * s
        turned[0, ch, :] = (silu * up).astype(BF16).T
        wide[1, :, ch] = (dz * silu).astype(BF16)
        wide[0, :, ch] = (dz * up * (s + silu * (1 - s))).astype(BF16)
    for k, part in ((2, 0), (1, 0), (1, 1)):
        put(k, part).start()
    da_gate, da_up = dot_t(wg1[...], wide[0]), dot_t(wu1[...], wide[1])
    make_dz1(next_dy, chunks[:SOON])
    da = (da_gate.astype(BF16) + da_up.astype(BF16)).T.astype(F32)
    dwide = scale * (da - h * (scale * scale * jnp.mean(da * h, -1, keepdims=True)))
    dh = dy[...] + dwide.astype(BF16)
    deep[1] = dh
    put(3, 1).start()
    for ch in chunks:
        dz = dot_t(dh, wd0[ch, :]).astype(BF16).astype(F32)
        gate, up = g0[:, ch], u0[:, ch]
        s = jax.nn.sigmoid(gate)
        silu = gate * s
        wide[3, :, ch] = (dz * silu).astype(BF16)
        wide[2, :, ch] = (dz * up * (s + silu * (1 - s))).astype(BF16)
    make_dz1(next_dy, chunks[SOON:AHEAD])
    put(1, 2).start()
    put(1, 3).start()

    @pl.when(i + 1 == blocks)
    def _():
        for copy in outs(slot) + outs(1 - slot):
            copy.wait()


def by_rows(x, dy, weights):
    shapes = ((2, D, TOKENS), (4, TOKENS, FF), (2, FF, TOKENS), (2, TOKENS, D))
    buffers = ((2, D, ROWS), (4, ROWS, FF), (2, FF, ROWS), (2, ROWS, D))
    return pl.pallas_call(
        rows_kernel,
        grid=(TOKENS // ROWS,),
        out_shape=tuple(jax.ShapeDtypeStruct(s, BF16) for s in shapes),
        in_specs=[HBM] * 5,
        out_specs=(HBM,) * 4,
        scratch_shapes=[
            *[pltpu.VMEM(w.shape[1:], BF16) for w in weights * 2],
            *[pltpu.VMEM((2, *b), BF16) for b in buffers],
            *[pltpu.VMEM((n, ROWS, D), BF16) for n in (2, AXES)],
            *[pltpu.VMEM((ROWS, FF), F32)] * 2,
            *[pltpu.VMEM((ROWS, FF), BF16)] * 2,
            DMA((MATRICES,)), DMA((2, FF // CHUNK)), DMA((2, AXES)), DMA((2, 4, 4)),
        ],
        compiler_params=pltpu.CompilerParams(vmem_limit_bytes=MOST_VMEM),
        name="rows",
    )(x, dy, *weights)


GATE_ROWS, DOWN_ROWS = D // DEVICES, FF // DEVICES
STARTS = (0, 48, 96, 144, 192, 232)
PART = 48


def gate_block(acc, stage, wide):
    def group(i, _):
        rows = pl.ds(pl.multiple_of(i * PIECE, SUBLANES), PIECE)
        for c in range(SIDE):
            piece = acc[rows, pl.ds(c * LANES, LANES)]
            for z in range(SIDE):
                wide[z, pl.ds(GATE_ROWS * c, GATE_ROWS), :] = piece[GATE_ROWS * z : GATE_ROWS * (z + 1)]
        for z in range(SIDE):
            stage[i // SIDE, i % SIDE, z] = wide[z].astype(BF16)
        return 0

    lax.fori_loop(0, PLANE, group, 0)


def down_block(acc, stage):
    def group(i, _):
        for t in range(DOWN_ROWS // SUBLANES):
            rows = acc[pl.ds(pl.multiple_of(i * DOWN_ROWS, SUBLANES) + SUBLANES * t, SUBLANES), :]
            piece = jnp.concatenate([rows[:, c * LANES : (c + 1) * LANES] for c in range(D // LANES)], 0)
            stage[i // SIDE, i % SIDE, pl.ds(PIECE * t, PIECE)] = piece.astype(BF16)
        return 0

    lax.fori_loop(0, PLANE, group, 0)


def own_rows(ws, windows, owns, sems):
    me = lax.axis_index("dp")
    taken = []
    for t in range(AXES):
        rows = windows[t].shape[1]
        first = pl.multiple_of((me // SIDE if t < 2 else me) * rows, SUBLANES)
        taken.append(pltpu.make_async_copy(ws[t].at[:, pl.ds(first, rows)], windows[t], sems.at[t]))
        taken[t].start()
    for t in range(AXES):
        taken[t].wait()
        rows = owns[t].shape[1]
        if t == 2:
            owns[t][...] = windows[t][...].astype(F32)
        for z in range(SIDE if t < 2 else 0):

            @pl.when(me % SIDE == z)
            def _():
                for l in range(LAYERS):
                    owns[t][l] = windows[t][l].astype(F32)[z * rows : (z + 1) * rows]


def gradients_kernel(*refs):
    (tall, wide, turned, deep), ws, (out, squares, terms), owns, scratch = refs[:4], refs[4:7], refs[7:10], refs[10:13], refs[13:]
    (lhs, rhs, zs, dh, acc, acc2, stage, stage2, shift, ra, rf, qa, qf, r3, own, f1, f2, sums) = scratch[:18]
    *windows, window_sem = scratch[18:22]
    (in_sem, rhs_sem, zs_sem, put_sem, sent, first_a, first_f, second_a, second_f, recv3, load, send4, recv4) = scratch[22:]
    at = place()

    def fetch_tall(l):
        return pltpu.make_async_copy(tall.at[l], lhs, in_sem.at[0])

    def fetch_deep(l):
        return pltpu.make_async_copy(deep.at[l], dh, in_sem.at[1])

    def fetch_wide(t):
        columns = pl.ds(pl.multiple_of(t % TILES * TILE, TILE), TILE)
        return pltpu.make_async_copy(wide.at[t // TILES, :, columns], rhs.at[t % 2], rhs_sem.at[t % 2])

    def fetch_turned(t):
        rows = pl.ds(pl.multiple_of(t % SIDE * PLANE_ROWS, LANES), PLANE_ROWS)
        return pltpu.make_async_copy(turned.at[t // SIDE, rows], zs.at[t % 2], zs_sem.at[t % 2])

    def put(m, h):
        return pltpu.make_async_copy(stage, terms.at[m, :, :, :, pl.ds(pl.multiple_of(PIECE * h, SUBLANES), PIECE)], put_sem.at[0])

    def put2(m, h):
        return pltpu.make_async_copy(stage2, terms.at[m, h], put_sem.at[1])

    fetch_tall(0).start()
    fetch_wide(0).start()
    fetch_deep(0).start()
    fetch_turned(0).start()
    enter(at, sorted({*LINES, *PLANE_PEERS}))

    def split(c):
        o, s = ORDERS[c], SIGNS[c]
        return o, s, at[o[0]], at[o[1]], at[o[2]]

    def block(m, c, a, i):
        o = ORDERS[c]
        index = [slice(None)] * 3
        index[o[0]] = a
        if i is not None:
            index[o[1]] = i
        return terms.at[(m, *index, pl.ds(STARTS[c], PART))]

    def piece(c, j):
        return wrap(split(c)[3] + SIGNS[c] * (2 + j - j // 2 * (2 * j - 1)))

    def along(c, axis, src, there, sem, recv, steps=1):
        return remote(src, there, sent.at[sem], recv, neighbour(at, ORDERS[c][axis], SIGNS[c] * steps))

    def launch(m):
        for j in range(SIDE):
            for c in range(WAYS):
                src = block(m, c, wrap(split(c)[2] + 2 * SIGNS[c]), piece(c, j))
                along(c, 0, src, ra.at[c, m, j], 0, first_a.at[m, j]).start()
        for j in range(SIDE):
            for c in range(WAYS):
                src = block(m, c, wrap(split(c)[2] - SIGNS[c]), piece(c, j))
                along(c, 0, src, rf.at[c, m, 1, j], 1, first_f.at[m, j], -1).start()

    def load_own(m):
        for k in range(2):
            for c in range(WAYS):
                mine = block(m, c, wrap(split(c)[2] + SIGNS[c] * (1 - k)), None)
                pltpu.make_async_copy(mine, own.at[c, k], load.at[k]).start()

    def whole(ref, sem):
        pltpu.make_async_copy(ref, ref, sem).wait()

    def term(c, k, j):
        i = piece(c, j)
        mine = own[c, k, i] if ORDERS[c][1] < ORDERS[c][2] else own[c, k, :, i]
        return mine.astype(F32)

    def on_first_a(m, j):
        whole(ra.at[:, m, j], first_a.at[m, j])
        for c in range(WAYS):
            ra[c, m, j] = (ra[c, m, j].astype(F32) + term(c, 0, j)).astype(BF16)
            along(c, 0, ra.at[c, m, j], rf.at[c, m, 0, j], 1, first_f.at[m, j]).start()

    def on_first_f(m, j):
        whole(rf.at[:, m, :, j], first_f.at[m, j])
        for c in range(WAYS):
            total = rf[c, m, 0, j].astype(F32) + rf[c, m, 1, j].astype(F32) + term(c, 1, j)
            if j < 2:
                rf[c, m, 1, j] = total.astype(BF16)
            else:
                f1[c, j - 2] = total
            if j == 0:
                along(c, 1, rf.at[c, m, 1, j], qa.at[c, m], 2, second_a.at[m]).start()
            if j == 1:
                along(c, 1, rf.at[c, m, 1, j], qf.at[c, m, 1], 3, second_f.at[m], -1).start()

    def on_second_a(m):
        whole(qa.at[:, m], second_a.at[m])
        for c in range(WAYS):
            qa[c, m] = (qa[c, m].astype(F32) + f1[c, 0]).astype(BF16)
            along(c, 1, qa.at[c, m], qf.at[c, m, 0], 3, second_f.at[m]).start()

    def third(m, c, k):
        src = qf.at[c, m, 1, wrap(split(c)[4] + k + 1)]
        return remote(src, r3.at[c, m, k], sent.at[4], recv3.at[m], neighbour(at, ORDERS[c][2], k + 1))

    def on_second_f(m):
        whole(qf.at[:, m], second_f.at[m])
        for c in range(WAYS):
            total = qf[c, m, 0].astype(F32) + qf[c, m, 1].astype(F32) + f1[c, 1]
            f2[c] = total
            qf[c, m, 1] = total.astype(BF16)
            for k in range(STEPS):
                third(m, c, k).start()

    def on_third(m):
        whole(r3.at[:, m], recv3.at[m])
        for c in range(WAYS):
            o, s, p1, p2, p3 = split(c)
            total = f2[c, p3]
            for k in range(STEPS):
                total = total + r3[c, m, k].astype(F32)
            out[m, pl.ds(STARTS[c], PART)] = total.astype(BF16)

    def tile(i, _):
        m, h = i // TILES, i % TILES
        kind, l = m % AXES, m // AXES

        @pl.when((h == 0) & (m > 0) & (m < MATRICES + 1))
        def _():
            @pl.when(kind > 0)
            def _():
                put(0, 0).wait()

            @pl.when(kind == 0)
            def _():
                put2(0, 0).wait()

            launch(m - 1)

        @pl.when((m < MATRICES) & (kind < 2))
        def _():
            t = (2 * l + kind) * TILES + h

            @pl.when((kind == 0) & (h == 0))
            def _():
                fetch_tall(l).wait()

                @pl.when(l == 1)
                def _():
                    fetch_deep(1).start()

            fetch_wide(t).wait()

            @pl.when(t < 19)
            def _():
                fetch_wide(t + 1).start()

            acc[...] = dot(lhs[...], rhs[t % 2])

            @pl.when(h > 0)
            def _():
                put(m, h).wait()

            gate_block(acc, stage, shift)
            put(m, h).start()

        @pl.when((m < MATRICES) & (kind == 2) & (h < SIDE))
        def _():
            t = SIDE * l + h

            @pl.when(h == 0)
            def _():
                fetch_deep(l).wait()

                @pl.when(l == 0)
                def _():
                    fetch_tall(1).start()

            fetch_turned(t).wait()

            @pl.when(t < 7)
            def _():
                fetch_turned(t + 1).start()

            acc2[...] = dot(zs[t % 2], dh[...])

            @pl.when(h > 0)
            def _():
                put2(m, h).wait()

            down_block(acc2, stage2)
            put2(m, h).start()

        @pl.when((h == 0) & (m > 2))
        def _():
            on_third(m - AXES)

        @pl.when((h == 2) & (m > 1))
        def _():
            on_second_a(m - 2)

        @pl.when((h == SIDE) & (m > 1))
        def _():
            on_second_f(m - 2)

        @pl.when((h == SIDE) & (m > 0) & (m < MATRICES + 1))
        def _():
            whole(own.at[:, 1], load.at[1])
            for j in range(2):
                on_first_f(m - 1, j)

        @pl.when((h == 0) & (m > 1))
        def _():
            for j in range(2, SIDE):
                on_first_f(m - 2, j)

        @pl.when(((h == 1) | (h == 2)) & (m > 0) & (m < MATRICES + 1))
        def _():
            @pl.when(h == 1)
            def _():
                whole(own.at[:, 0], load.at[0])

            lax.fori_loop(h - 1, AXES * h - 2, lambda j, _: (on_first_a(m - 1, j), 0)[1], 0)

        @pl.when((h == 0) & (m > 0) & (m < MATRICES + 1))
        def _():
            load_own(m - 1)

        return 0

    lax.fori_loop(0, (MATRICES + 2) * TILES, tile, 0)
    own_rows(ws, windows, owns, window_sem)
    on_third(MATRICES - 1)

    total = jnp.zeros((SUBLANES, LANES), F32)
    for m in range(MATRICES):
        g = out[m].astype(F32)
        total = total + jnp.sum((g * g).reshape(-1, SUBLANES, LANES), axis=0)
    squares[...] = norm_exchange(at, sums, send4, recv4, total)
    for k, buffer in enumerate((ra, rf, qa, qf, r3)):
        whole(buffer, sent.at[k])


def gradients(tall, wide, turned, deep, weights):
    g, squares, _, *owns = pl.pallas_call(
        gradients_kernel,
        out_shape=(
            pltpu.VMEM((MATRICES, BLOCK, LANES), BF16),
            pltpu.VMEM((SUBLANES, LANES), F32),
            jax.ShapeDtypeStruct((MATRICES, SIDE, SIDE, SIDE, BLOCK, LANES), BF16),
            *[pltpu.VMEM((LAYERS, w.shape[1] // DEVICES, w.shape[2]), F32) for w in weights],
        ),
        in_specs=[HBM] * (4 + AXES),
        out_specs=(VMEM, VMEM, HBM, *[VMEM] * AXES),
        scratch_shapes=[
            pltpu.VMEM((D, TOKENS), BF16),
            pltpu.VMEM((2, TOKENS, TILE), BF16),
            pltpu.VMEM((2, PLANE_ROWS, TOKENS), BF16),
            pltpu.VMEM((TOKENS, D), BF16),
            pltpu.VMEM((D, TILE), F32),
            pltpu.VMEM((PLANE_ROWS, D), F32),
            pltpu.VMEM((SIDE, SIDE, SIDE, PIECE, LANES), BF16),
            pltpu.VMEM((SIDE, SIDE, BLOCK, LANES), BF16),
            pltpu.VMEM((SIDE, PIECE, LANES), F32),
            pltpu.VMEM((WAYS, MATRICES, SIDE, SIDE, PART, LANES), BF16),
            pltpu.VMEM((WAYS, MATRICES, 2, SIDE, SIDE, PART, LANES), BF16),
            pltpu.VMEM((WAYS, MATRICES, SIDE, PART, LANES), BF16),
            pltpu.VMEM((WAYS, MATRICES, 2, SIDE, PART, LANES), BF16),
            pltpu.VMEM((WAYS, MATRICES, STEPS, PART, LANES), BF16),
            pltpu.VMEM((WAYS, 2, SIDE, SIDE, PART, LANES), BF16),
            pltpu.VMEM((WAYS, 2, SIDE, PART, LANES), F32),
            pltpu.VMEM((WAYS, SIDE, PART, LANES), F32),
            pltpu.VMEM((PLANE + SIDE, SUBLANES, LANES), F32),
            *[pltpu.VMEM((LAYERS, w.shape[1] // n, w.shape[2]), BF16) for w, n in zip(weights, (PLANE, PLANE, DEVICES), strict=True)],
            DMA((AXES,)),
            *[DMA((2,))] * 4,
            DMA((TILES,)),
            *[DMA((MATRICES, SIDE))] * 2, *[DMA((MATRICES,))] * 3,
            DMA((2,)),
            DMA((2,)), DMA((2,)),
        ],
        compiler_params=pltpu.CompilerParams(collective_id=0, has_side_effects=True, vmem_limit_bytes=MOST_VMEM - SPARE_VMEM),
        name="gradients",
    )(tall, wide, turned, deep, *weights)
    return g, squares, owns


def solution(mesh):
    rep, dp = mesh.axis_names

    def step(x, dy, *arrays):
        weights, m, v = (arrays[i : i + 3] for i in (0, 3, 6))
        g, total, owns = gradients(*by_rows(x[0], dy[0], weights), weights)
        new, new_m, new_v = adam(MATRICES * D * FF, g, total, owns, m, v)
        return (*natural(all_gather(new)), *new_m, *new_v)

    whole, rows, sequences = P(), P(None, dp), P((rep, dp))
    return jax.shard_map(
        step,
        mesh=mesh,
        in_specs=(sequences, sequences, *[whole] * AXES, *[rows] * MATRICES),
        out_specs=(*[P(rep)] * AXES, *[P(rep, dp)] * MATRICES),
        check_vma=False,
    )
```

```python
import functools
import jax
import jax.numpy as jnp
from jax import lax
from jax.experimental import pallas as pl
from jax.experimental.pallas import tpu as pltpu
from jax.sharding import PartitionSpec as P

MESH = pl.DeviceIdType.MESH
WAYS, AXES, SIDE = 6, 3, 4
STEPS = SIDE - 1
MATRICES, LAYERS, DEVICES, PLANE = 6, 2, 64, 16
LANES, SUBLANES, BLOCK = 128, 8, 280
BF16, F32 = jnp.bfloat16, jnp.float32
HBM, VMEM = pl.BlockSpec(memory_space=pl.ANY), pl.BlockSpec(memory_space=pltpu.VMEM)
DMA = pltpu.SemaphoreType.DMA
MIB = 1 << 20
MOST_VMEM, SPARE_VMEM = 62 * MIB, 2 * MIB
ORDERS = tuple(tuple((way // 2 + i) % AXES for i in range(AXES)) for way in range(WAYS))
SIGNS = (1, -1) * AXES
TAKEN = (3, 0, 4, 1, 5, 2)


def place():
    me = lax.axis_index("dp")
    return (me // PLANE, me // SIDE % SIDE, me % SIDE)


def wrap(i):
    return (i + 3 * SIDE) % SIDE


def neighbour(at, axis, step):
    there = [c for c in at]
    there[axis] = wrap(at[axis] + step)
    return {"dp": (there[0] * SIDE + there[1]) * SIDE + there[2]}


def remote(src, dst, send, recv, to):
    return pltpu.make_async_remote_copy(src_ref=src, dst_ref=dst, send_sem=send, recv_sem=recv, device_id=to, device_id_type=MESH)


def moved(at, steps):
    x, y, z = (wrap(a + step) for a, step in zip(at, steps, strict=True))
    return {"dp": (x * SIDE + y) * SIDE + z}


LINES = tuple(tuple(k * (axis == line) for axis in range(AXES)) for line in range(AXES) for k in range(1, SIDE))
PLANE_PEERS = tuple((0, k // SIDE, k % SIDE) for k in range(1, PLANE))
LINE_PEERS = LINES[:STEPS]


def enter(at, peers):
    barrier = pltpu.get_barrier_semaphore()
    for steps in peers:
        pl.semaphore_signal(barrier, inc=1, device_id=moved(at, steps), device_id_type=MESH)
    pl.semaphore_wait(barrier, len(peers))


def norm_exchange(at, buf, send, recv, total):
    first = 0
    for stage, peers in enumerate((PLANE_PEERS, LINE_PEERS)):
        own, others = buf.at[first], buf.at[pl.ds(first + 1, len(peers))]
        own[...] = total
        for k, steps in enumerate(peers):
            remote(own, others.at[k], send.at[stage], recv.at[stage], moved(at, steps)).start()
        pltpu.make_async_copy(others, others, recv.at[stage]).wait()
        total = total + jnp.sum(others[...], axis=0)
        pltpu.make_async_copy(others, others, send.at[stage]).wait()
        first += 1 + len(peers)
    return total


def passed_on(seen, c, phase, key):
    d1, d2, d3 = key
    if phase == 0 and d3 < STEPS:
        yield 0, (0, 0, d3 + 1)
    if phase < 2 and d2 < STEPS:
        yield 1, (0, d2 + 1, d3)
    if phase == 1 and d2 > 0:
        seen.append((c, d2))
        if seen.count((c, d2)) < SIDE:
            return
        d3 = None
    if d1 < STEPS:
        yield 2, (d1 + 1, d2, d3)


def ag_order(latency=2):
    import heapq

    free, out, seen, heap = {}, [], [], []

    def hold(t, c, phase, key):
        for phase, key in passed_on(seen, c, phase, key):
            link = ORDERS[c][2 - phase]
            size = SIDE if key[2] is None else 1
            free[link] = max(t, free.get(link, 0)) + size
            heapq.heappush(heap, (free[link] + latency, len(out) * WAYS + len(heap), c, phase, key))

    for c in range(0, WAYS, 2):
        hold(0, c, 0, (0, 0, 0))
    while heap:
        t, _, *arrival = heapq.heappop(heap)
        out.append(arrival)
        hold(t, *arrival)
    return out


def ag_kernel(*refs):
    mine, outs, (sends, recv1, recv2, recv3, recv4, local) = refs[0], refs[1 : 1 + WAYS], refs[1 + WAYS :]
    at = place()
    enter(at, LINES)

    def where(c, key):
        index = [None] * AXES
        for axis, d in zip(ORDERS[c], key, strict=True):
            index[axis] = slice(None) if d is None else wrap(at[axis] - SIGNS[c] * d)
        return outs[c].at[tuple(index)]

    def arrived(c, phase, key):
        d1, d2, d3 = key
        if phase == 0:
            return recv1.at[c // 2, d3 - 1]
        if phase == 1:
            return recv2.at[c // 2, d2 - 1, d3]
        if d3 is not None:
            return recv3.at[c // 2, d1 - 1, d3]
        return recv4.at[c // 2, d1 - 1, d2 - 1]

    def send_on(c, phase, key):
        d1, d2, d3 = key
        back = list(key)
        back[2 - phase] -= 1
        there = where(c, back)
        src = there if any(d != 0 for d in back) else mine.at[c]
        remote(src, there, sends.at[c, phase], arrived(c, phase, key), neighbour(at, ORDERS[c][2 - phase], SIGNS[c])).start()

    seen = []

    def hold(*held):
        for phase, key in passed_on(seen, *held):
            send_on(held[0], phase, key)

    own = [pltpu.make_async_copy(mine.at[c], where(c, (0, 0, 0)), local.at[c]) for c in range(WAYS)]
    for c in range(WAYS):
        hold(c, 0, (0, 0, 0))
    for copied in own:
        copied.start()
    for even, phase, key in ag_order():
        two = outs[even].at[0, pl.ds(0, 2)] if key[2] is None else outs[even].at[0, 0, pl.ds(0, 2)]
        pltpu.make_async_copy(two, two, arrived(even, phase, key)).wait()
        for c in (even, even + 1):
            hold(c, phase, key)
    for c in range(WAYS):
        own[c].wait()
        sent = outs[c].at[pl.ds(0, STEPS)]
        for phase in (2, 1, 0):
            pltpu.make_async_copy(sent, sent, sends.at[c, phase]).wait()
            sent = outs[c].at[(0,) * (AXES - phase) + (pl.ds(0, STEPS),)]


def all_gather(mine):
    return pl.pallas_call(
        ag_kernel,
        out_shape=(pltpu.VMEM((SIDE, SIDE, SIDE, *mine.shape[1:]), BF16),) * WAYS,
        in_specs=[VMEM],
        out_specs=(VMEM,) * WAYS,
        scratch_shapes=[DMA((WAYS, AXES)), DMA((AXES, STEPS)), *[DMA((AXES, STEPS, SIDE))] * 2, DMA((AXES, STEPS, STEPS)), DMA((WAYS,))],
        compiler_params=pltpu.CompilerParams(collective_id=1, has_side_effects=True, vmem_limit_bytes=MOST_VMEM // SUBLANES),
        name="gather",
    )(mine)


def tiles_of(t, rows, columns):
    n = columns // LANES
    if t < 2:
        return [(0, rows, j * LANES, j * rows) for j in range(n)]
    return [(8 * i, 8, j * LANES, (i * n + j) * 8) for i in range(rows // 8) for j in range(n)]


def adam_kernel(count, g, total, *refs):
    ws, ms, vs = (refs[AXES * k : AXES * (k + 1)] for k in range(3))
    new, *refs = refs[3 * AXES :]
    *moments, wide_g, wide_w = refs
    new_m, new_v = moments[:AXES], moments[AXES:]
    factor = jnp.minimum(1.0, 0.5 * lax.rsqrt(jnp.full((1, 1), jnp.sum(total[...])) / count + 1e-30))
    for t in range(AXES):
        rows, columns = ws[t].shape[1:]
        for l in range(LAYERS):
            wide_g[...] = g[TAKEN[LAYERS * t + l]].astype(F32) * factor
            for row, n, column, at in tiles_of(t, rows, columns):
                lanes = pl.ds(column, LANES)
                here = (slice(None), l, lanes) if t < 2 else (l, pl.ds(row, n), lanes)
                grad = wide_g[pl.ds(at, n), :]
                m = 0.9 * ms[t][here] + 0.1 * grad
                v = 0.95 * vs[t][here] + 0.05 * grad * grad
                w = ws[t][l, pl.ds(row, n), lanes]
                new_m[t][here] = m
                new_v[t][here] = v
                wide_w[pl.ds(at, n), :] = w - 0.02 * (m * lax.rsqrt(v + 1e-8) + 0.1 * w)
            new[LAYERS * t + l] = wide_w[...].astype(BF16)


def adam(count, g, total, ws, ms, vs):
    ms, vs = ([*(jnp.swapaxes(a, 0, 1) for a in arrays[:2]), arrays[2]] for arrays in (ms, vs))
    like = [jax.ShapeDtypeStruct(m.shape, F32) for m in ms]
    new, *moments = pl.pallas_call(
        functools.partial(adam_kernel, count),
        out_shape=(pltpu.VMEM(g.shape, BF16), *like, *like),
        in_specs=[VMEM] * (2 + AXES * 3),
        out_specs=(VMEM,) * (1 + AXES * 2),
        scratch_shapes=[pltpu.VMEM(g.shape[1:], F32)] * 2,
        compiler_params=pltpu.CompilerParams(vmem_limit_bytes=MOST_VMEM // SIDE),
        name="adam",
    )(g, total, *ws, *ms, *vs)
    return new, *([*(jnp.swapaxes(a, 0, 1) for a in part[:2]), part[2]] for part in (moments[:AXES], moments[AXES:]))


def natural_kernel(*refs):
    gathered, outs, wide = refs[:MATRICES], refs[MATRICES:-AXES], refs[-AXES:]
    first = pl.program_id(0) * SUBLANES
    for t in range(AXES):
        for l in range(LAYERS):
            rows, columns = outs[t].shape[1:]
            for k in range(SUBLANES):
                block = gathered[LAYERS * t + l][first + k].astype(F32)
                for row, n, column, at in tiles_of(t, rows // SUBLANES, columns):
                    wide[t][pl.ds(k * rows // SUBLANES + row, n), pl.ds(column, LANES)] = block[at : at + n]
            outs[t][l] = wide[t][...].astype(BF16)


def natural(gathered):
    shapes = (GATE, GATE, DOWN)
    return pl.pallas_call(
        natural_kernel,
        grid=(SUBLANES,),
        out_shape=tuple(jax.ShapeDtypeStruct((LAYERS, *s), BF16) for s in shapes),
        in_specs=[VMEM] * MATRICES,
        out_specs=tuple(pl.BlockSpec((LAYERS, s[0] // SUBLANES, s[1]), lambda i: (0, i, 0)) for s in shapes),
        scratch_shapes=[pltpu.VMEM((s[0] // SUBLANES, s[1]), F32) for s in shapes],
        compiler_params=pltpu.CompilerParams(vmem_limit_bytes=MOST_VMEM // SIDE),
        name="natural",
    )(*[g.reshape(DEVICES, BLOCK, LANES) for g in gathered])


D, FF, TOKENS = 896, 2560, 2048
GATE, DOWN = (D, FF), (FF, D)
ROWS, CHUNK, TILE = 256, 256, 512
TALL, WIDE, TURNED, DEEP = range(4)
SOON, AHEAD, NEXT = 4, 6, 8
TILES, PIECE, PLANE_ROWS = FF // TILE, BLOCK * TILE // FF, FF // SIDE
NT = (((1,), (1,)), ((), ()))


def dot(a, b):
    return jnp.dot(a, b, preferred_element_type=F32)


def dot_t(a, b):
    return lax.dot_general(a, b, NT, preferred_element_type=F32)


def scale_of(wide):
    return lax.rsqrt(jnp.mean(wide * wide, -1, keepdims=True) + 1e-6)


def rows_kernel(x_hbm, dy_hbm, *refs):
    hbm, results, weights, rest = refs[:3], refs[3:7], refs[7:13], refs[13:]
    buffers, (xs, dys, g0, u0, z0, dz1, sems, part_sems, in_sems, out_sems) = rest[:4], rest[4:]
    wg0, wu0, wd0, wg1, wu1, wd1 = weights
    i, slot = pl.program_id(0), pl.program_id(0) % 2
    first, blocks = i == 0, pl.num_programs(0)
    chunks = [pl.ds(j * CHUNK, CHUNK) for j in range(FF // CHUNK)]

    def fetch(k):
        return pltpu.make_async_copy(hbm[k % 3].at[k // 3], weights[k], sems.at[k])

    def fetch_part(k, j):
        return pltpu.make_async_copy(hbm[k].at[0, :, chunks[j]], weights[k].at[:, chunks[j]], part_sems.at[k, j])

    def take(source, there, i):
        rows = pl.ds(pl.multiple_of(i * ROWS, ROWS), ROWS)
        slot = i % there.shape[0]
        return pltpu.make_async_copy(source.at[rows], there.at[slot], in_sems.at[there.shape[0] - 2, slot])

    def put(k, part, slot=slot):
        rows = pl.ds(pl.multiple_of(i * ROWS, ROWS), ROWS)
        there = results[k].at[part, rows] if k % 2 else results[k].at[part, :, rows]
        return pltpu.make_async_copy(buffers[k].at[slot, part], there, out_sems.at[slot, k, part])

    def outs(slot):
        return [put(k, part, slot) for k, result in enumerate(results) for part in range(result.shape[0])]

    @pl.when(first)
    def _():
        take(x_hbm, xs, 0).start()
        take(dy_hbm, dys, 0).start()
        for j in range(len(chunks)):
            for k in range(2):
                fetch_part(k, j).start()
        take(dy_hbm, dys, 1).start()
        take(dy_hbm, dys, 0).wait()

    take(x_hbm, xs, i).wait()

    @pl.when(i + 1 < blocks)
    def _():
        take(x_hbm, xs, i + 1).start()
        take(dy_hbm, dys, i + 1).wait()

    @pl.when(i + 2 < blocks)
    def _():
        take(dy_hbm, dys, i + 2).start()

    @pl.when(i > 1)
    def _():
        for copy in outs(slot):
            copy.wait()

    tall, wide, turned, deep = (b.at[slot] for b in buffers)
    x, dy, next_dy = xs.at[slot], dys.at[i % AXES], dys.at[(i + 1) % AXES]

    def make_dz1(dy, some):
        for ch in some:
            dz1[:, ch] = dot_t(dy[...], wd1[ch, :]).astype(BF16)

    def forward(coming):
        a = (x[...].astype(F32) * scale_of(x[...].astype(F32))).astype(BF16)
        tall[1] = a.T
        deep[0] = dy[...]
        for j, ch in enumerate(chunks):
            if coming:
                for k in range(2):
                    fetch_part(k, j).wait()
                if 0 < j < 5:
                    fetch(j + 1).start()
            gate, up = dot(a, wg0[:, ch]), dot(a, wu0[:, ch])
            g0[:, ch], u0[:, ch] = gate, up
            z0[:, ch] = (gate * jax.nn.sigmoid(gate) * up).astype(BF16)
            turned[1, ch, :] = z0[:, ch].T

    @pl.when(first)
    def _():
        forward(True)
        for k in range(2, MATRICES):
            fetch(k).wait()
        make_dz1(dy, chunks[:AHEAD])

    @pl.when(i > 0)
    def _():
        forward(False)

    for k, part in ((TALL, 1), (DEEP, 0), (TURNED, 1)):
        put(k, part).start()
    make_dz1(dy, chunks[AHEAD:NEXT])
    h = x[...] + dot(z0[...], wd0[...]).astype(BF16)
    make_dz1(dy, chunks[NEXT:])
    h = h.astype(F32)
    scale = scale_of(h)
    a = (h * scale).astype(BF16)
    tall[0] = a.T
    put(TALL, 0).start()
    for ch in chunks:
        gate, up = dot(a, wg1[:, ch]), dot(a, wu1[:, ch])
        dz = dz1[:, ch].astype(F32)
        s = jax.nn.sigmoid(gate)
        silu = gate * s
        turned[0, ch, :] = (silu * up).astype(BF16).T
        wide[1, :, ch] = (dz * silu).astype(BF16)
        wide[0, :, ch] = (dz * up * (s + silu * (1 - s))).astype(BF16)
    for k, part in ((TURNED, 0), (WIDE, 0), (WIDE, 1)):
        put(k, part).start()
    da_gate, da_up = dot_t(wg1[...], wide[0]), dot_t(wu1[...], wide[1])
    make_dz1(next_dy, chunks[:SOON])
    da = (da_gate.astype(BF16) + da_up.astype(BF16)).T.astype(F32)
    dwide = scale * (da - h * (scale * scale * jnp.mean(da * h, -1, keepdims=True)))
    dh = dy[...] + dwide.astype(BF16)
    deep[1] = dh
    put(DEEP, 1).start()
    for ch in chunks:
        dz = dot_t(dh, wd0[ch, :]).astype(BF16).astype(F32)
        gate, up = g0[:, ch], u0[:, ch]
        s = jax.nn.sigmoid(gate)
        silu = gate * s
        wide[3, :, ch] = (dz * silu).astype(BF16)
        wide[2, :, ch] = (dz * up * (s + silu * (1 - s))).astype(BF16)
    make_dz1(next_dy, chunks[SOON:AHEAD])
    put(WIDE, 2).start()
    put(WIDE, 3).start()

    @pl.when(i + 1 == blocks)
    def _():
        for copy in outs(slot) + outs(1 - slot):
            copy.wait()


def by_rows(x, dy, weights):
    shapes = ((2, D, TOKENS), (4, TOKENS, FF), (2, FF, TOKENS), (2, TOKENS, D))
    buffers = ((2, D, ROWS), (4, ROWS, FF), (2, FF, ROWS), (2, ROWS, D))
    return pl.pallas_call(
        rows_kernel,
        grid=(TOKENS // ROWS,),
        out_shape=tuple(jax.ShapeDtypeStruct(s, BF16) for s in shapes),
        in_specs=[HBM] * 5,
        out_specs=(HBM,) * 4,
        scratch_shapes=[
            *[pltpu.VMEM(w.shape[1:], BF16) for w in weights * 2],
            *[pltpu.VMEM((2, *b), BF16) for b in buffers],
            *[pltpu.VMEM((n, ROWS, D), BF16) for n in (2, AXES)],
            *[pltpu.VMEM((ROWS, FF), F32)] * 2,
            *[pltpu.VMEM((ROWS, FF), BF16)] * 2,
            DMA((MATRICES,)), DMA((2, FF // CHUNK)), DMA((2, AXES)), DMA((2, 4, 4)),
        ],
        compiler_params=pltpu.CompilerParams(vmem_limit_bytes=MOST_VMEM),
        name="rows",
    )(x, dy, *weights)


GATE_ROWS, DOWN_ROWS = D // DEVICES, FF // DEVICES
STARTS = (0, 48, 96, 144, 192, 232)
PART = 48


def gate_block(acc, stage, wide):
    for i in range(PLANE):
        part = wide.at[i % wide.shape[0]]
        for c in range(SIDE):
            piece = acc[pl.ds(i * PIECE, PIECE), pl.ds(c * LANES, LANES)]
            for z in range(SIDE):
                part[z, pl.ds(GATE_ROWS * c, GATE_ROWS), :] = piece[GATE_ROWS * z : GATE_ROWS * (z + 1)]
        for z in range(SIDE):
            stage[i // SIDE, i % SIDE, z] = part[z].astype(BF16)


def down_block(acc, stage):
    def group(i, _):
        for t in range(DOWN_ROWS // SUBLANES):
            rows = acc[pl.ds(pl.multiple_of(i * DOWN_ROWS, SUBLANES) + SUBLANES * t, SUBLANES), :]
            piece = jnp.concatenate([rows[:, c * LANES : (c + 1) * LANES] for c in range(D // LANES)], 0)
            stage[i // SIDE, i % SIDE, pl.ds(PIECE * t, PIECE)] = piece.astype(BF16)
        return 0

    lax.fori_loop(0, PLANE, group, 0)


def own_rows(ws, windows, owns, sems):
    me = lax.axis_index("dp")
    taken = []
    for t in range(AXES):
        rows = windows[t].shape[1]
        first = pl.multiple_of((me // SIDE if t < 2 else me) * rows, SUBLANES)
        taken.append(pltpu.make_async_copy(ws[t].at[:, pl.ds(first, rows)], windows[t], sems.at[t]))
        taken[t].start()
    for t in range(AXES):
        taken[t].wait()
        rows = owns[t].shape[1]
        if t == 2:
            owns[t][...] = windows[t][...].astype(F32)
        for z in range(SIDE if t < 2 else 0):

            @pl.when(me % SIDE == z)
            def _():
                for l in range(LAYERS):
                    owns[t][l] = windows[t][l].astype(F32)[z * rows : (z + 1) * rows]


def gradients_kernel(*refs):
    (tall, wide, turned, deep), ws, (out, squares, terms), owns, scratch = refs[:4], refs[4:7], refs[7:10], refs[10:13], refs[13:]
    (lhs, rhs, zs, dh, acc_a, acc_b, acc2, stage_a, stage_b, stage2, shift, ra, rf, qa, qf, r3, own, f1, f2, sums) = scratch[:20]
    accs, stages = (acc_a, acc_b), (stage_a, stage_b)
    *windows, window_sem = scratch[20:24]
    (in_sem, rhs_sem, zs_sem, put_sem, sent, first_a, first_f, second_a, second_f, recv3, load, send4, recv4) = scratch[24:]
    at = place()

    def fetch_tall(l):
        return pltpu.make_async_copy(tall.at[l], lhs, in_sem.at[0])

    def fetch_deep(l):
        return pltpu.make_async_copy(deep.at[l], dh, in_sem.at[1])

    def fetch_wide(t):
        columns = pl.ds(pl.multiple_of(t % TILES * TILE, TILE), TILE)
        return pltpu.make_async_copy(wide.at[t // TILES, :, columns], rhs.at[t % 2], rhs_sem.at[t % 2])

    def fetch_turned(t):
        rows = pl.ds(pl.multiple_of(t % SIDE * PLANE_ROWS, LANES), PLANE_ROWS)
        return pltpu.make_async_copy(turned.at[t // SIDE, rows], zs.at[t % 2], zs_sem.at[t % 2])

    def arrange(m, h, odd):
        rows = pl.ds(pl.multiple_of(PIECE * h, SUBLANES), PIECE)
        gate_block(accs[odd], stages[odd], shift)
        pltpu.make_async_copy(stages[odd], terms.at[m, :, :, :, rows], put_sem.at[odd]).start()

    def emptied(odd):
        whole(stages[odd], put_sem.at[odd])

    def put2(m, h):
        return pltpu.make_async_copy(stage2, terms.at[m, h], put_sem.at[2])

    fetch_tall(0).start()
    fetch_wide(0).start()
    fetch_deep(0).start()
    fetch_turned(0).start()
    enter(at, sorted({*LINES, *PLANE_PEERS}))

    def split(c):
        o, s = ORDERS[c], SIGNS[c]
        return o, s, at[o[0]], at[o[1]], at[o[2]]

    def block(m, c, a, i):
        o = ORDERS[c]
        index = [slice(None)] * 3
        index[o[0]] = a
        if i is not None:
            index[o[1]] = i
        return terms.at[(m, *index, pl.ds(STARTS[c], PART))]

    def piece(c, j):
        return wrap(split(c)[3] + SIGNS[c] * (2 + j - j // 2 * (2 * j - 1)))

    def along(c, axis, src, there, sem, recv, steps=1):
        return remote(src, there, sent.at[sem], recv, neighbour(at, ORDERS[c][axis], SIGNS[c] * steps))

    def launch(m):
        for j in range(SIDE):
            for c in range(WAYS):
                src = block(m, c, wrap(split(c)[2] + 2 * SIGNS[c]), piece(c, j))
                along(c, 0, src, ra.at[c, m, j], 0, first_a.at[m, j]).start()
        for j in range(SIDE):
            for c in range(WAYS):
                src = block(m, c, wrap(split(c)[2] - SIGNS[c]), piece(c, j))
                along(c, 0, src, rf.at[c, m, 1, j], 1, first_f.at[m, j], -1).start()

    def load_own(m):
        for k in range(2):
            for c in range(WAYS):
                mine = block(m, c, wrap(split(c)[2] + SIGNS[c] * (1 - k)), None)
                pltpu.make_async_copy(mine, own.at[c, k], load.at[k]).start()

    def whole(ref, sem):
        pltpu.make_async_copy(ref, ref, sem).wait()

    def term(c, k, j):
        i = piece(c, j)
        mine = own[c, k, i] if ORDERS[c][1] < ORDERS[c][2] else own[c, k, :, i]
        return mine.astype(F32)

    def on_first_a(m, j):
        whole(ra.at[:, m, j], first_a.at[m, j])
        for c in range(WAYS):
            ra[c, m, j] = (ra[c, m, j].astype(F32) + term(c, 0, j)).astype(BF16)
            along(c, 0, ra.at[c, m, j], rf.at[c, m, 0, j], 1, first_f.at[m, j]).start()

    def on_first_f(m, j):
        whole(rf.at[:, m, :, j], first_f.at[m, j])
        for c in range(WAYS):
            total = rf[c, m, 0, j].astype(F32) + rf[c, m, 1, j].astype(F32) + term(c, 1, j)
            if j < 2:
                rf[c, m, 1, j] = total.astype(BF16)
            else:
                f1[c, j - 2] = total
            if j == 0:
                along(c, 1, rf.at[c, m, 1, j], qa.at[c, m], 2, second_a.at[m]).start()
            if j == 1:
                along(c, 1, rf.at[c, m, 1, j], qf.at[c, m, 1], 3, second_f.at[m], -1).start()

    def on_second_a(m):
        whole(qa.at[:, m], second_a.at[m])
        for c in range(WAYS):
            qa[c, m] = (qa[c, m].astype(F32) + f1[c, 0]).astype(BF16)
            along(c, 1, qa.at[c, m], qf.at[c, m, 0], 3, second_f.at[m]).start()

    def third(m, c, k):
        src = qf.at[c, m, 1, wrap(split(c)[4] + k + 1)]
        return remote(src, r3.at[c, m, k], sent.at[4], recv3.at[m], neighbour(at, ORDERS[c][2], k + 1))

    def on_second_f(m):
        whole(qf.at[:, m], second_f.at[m])
        for c in range(WAYS):
            total = qf[c, m, 0].astype(F32) + qf[c, m, 1].astype(F32) + f1[c, 1]
            f2[c] = total
            qf[c, m, 1] = total.astype(BF16)
            for k in range(STEPS):
                third(m, c, k).start()

    def on_third(m):
        whole(r3.at[:, m], recv3.at[m])
        for c in range(WAYS):
            o, s, p1, p2, p3 = split(c)
            total = f2[c, p3]
            for k in range(STEPS):
                total = total + r3[c, m, k].astype(F32)
            out[m, pl.ds(STARTS[c], PART)] = total.astype(BF16)

    def tile(i, _):
        m, h = i // TILES, i % TILES
        kind, l = m % AXES, m // AXES
        launched = (m > 0) & (m < MATRICES + 1)

        @pl.when((h == 0) & launched)
        def _():
            @pl.when(kind > 0)
            def _():
                for odd in range(2):
                    emptied(odd)

            @pl.when(kind == 0)
            def _():
                put2(0, 0).wait()

            launch(m - 1)

        @pl.when((m < MATRICES) & (kind < 2))
        def _():
            t = (2 * l + kind) * TILES + h

            @pl.when((kind == 0) & (h == 0))
            def _():
                fetch_tall(l).wait()

                @pl.when(l == 1)
                def _():
                    fetch_deep(1).start()

            fetch_wide(t).wait()

            @pl.when(t < 19)
            def _():
                fetch_wide(t + 1).start()

            @pl.when(h == 0)
            def _():
                accs[0][...] = dot(lhs[...], rhs[t % 2])

            @pl.when(h == AXES)
            def _():
                emptied(0)

            @pl.when(h == SIDE)
            def _():
                emptied(1)

            for odd in range(2):

                @pl.when((h > 0) & (h % 2 == odd))
                def _():
                    accs[odd][...] = dot(lhs[...], rhs[t % 2])
                    arrange(m, h - 1, 1 - odd)

            @pl.when(h == SIDE)
            def _():
                emptied(0)
                arrange(m, h, 0)

        @pl.when((m < MATRICES) & (kind == 2) & (h < SIDE))
        def _():
            t = SIDE * l + h

            @pl.when(h == 0)
            def _():
                fetch_deep(l).wait()

                @pl.when(l == 0)
                def _():
                    fetch_tall(1).start()

            fetch_turned(t).wait()

            @pl.when(t < 7)
            def _():
                fetch_turned(t + 1).start()

            acc2[...] = dot(zs[t % 2], dh[...])

            @pl.when(h > 0)
            def _():
                put2(m, h).wait()

            down_block(acc2, stage2)
            put2(m, h).start()

        @pl.when((h == 0) & (m > 2))
        def _():
            on_third(m - AXES)

        @pl.when((h == 2) & (m > 1))
        def _():
            on_second_a(m - 2)

        @pl.when((h == SIDE) & (m > 1))
        def _():
            on_second_f(m - 2)

        @pl.when((h == SIDE) & launched)
        def _():
            whole(own.at[:, 1], load.at[1])
            for j in range(2):
                on_first_f(m - 1, j)

        @pl.when((h == 0) & (m > 1))
        def _():
            for j in range(2, SIDE):
                on_first_f(m - 2, j)

        @pl.when(((h == 1) | (h == 2)) & launched)
        def _():
            @pl.when(h == 1)
            def _():
                whole(own.at[:, 0], load.at[0])

            lax.fori_loop(h - 1, AXES * h - 2, lambda j, _: (on_first_a(m - 1, j), 0)[1], 0)

        @pl.when((h == 0) & launched)
        def _():
            load_own(m - 1)

        return 0

    lax.fori_loop(0, (MATRICES + 2) * TILES, tile, 0)
    own_rows(ws, windows, owns, window_sem)
    on_third(MATRICES - 1)

    total = jnp.zeros((SUBLANES, LANES), F32)
    for m in range(MATRICES):
        g = out[m].astype(F32)
        total = total + jnp.sum((g * g).reshape(-1, SUBLANES, LANES), axis=0)
    squares[...] = norm_exchange(at, sums, send4, recv4, total)
    for k, buffer in enumerate((ra, rf, qa, qf, r3)):
        whole(buffer, sent.at[k])


def gradients(tall, wide, turned, deep, weights):
    g, squares, _, *owns = pl.pallas_call(
        gradients_kernel,
        out_shape=(
            pltpu.VMEM((MATRICES, BLOCK, LANES), BF16),
            pltpu.VMEM((SUBLANES, LANES), F32),
            jax.ShapeDtypeStruct((MATRICES, SIDE, SIDE, SIDE, BLOCK, LANES), BF16),
            *[pltpu.VMEM((LAYERS, w.shape[1] // DEVICES, w.shape[2]), F32) for w in weights],
        ),
        in_specs=[HBM] * (4 + AXES),
        out_specs=(VMEM, VMEM, HBM, *[VMEM] * AXES),
        scratch_shapes=[
            pltpu.VMEM((D, TOKENS), BF16),
            pltpu.VMEM((2, TOKENS, TILE), BF16),
            pltpu.VMEM((2, PLANE_ROWS, TOKENS), BF16),
            pltpu.VMEM((TOKENS, D), BF16),
            *[pltpu.VMEM((D, TILE), F32)] * 2,
            pltpu.VMEM((PLANE_ROWS, D), F32),
            *[pltpu.VMEM((SIDE, SIDE, SIDE, PIECE, LANES), BF16)] * 2,
            pltpu.VMEM((SIDE, SIDE, BLOCK, LANES), BF16),
            pltpu.VMEM((SIDE, SIDE, PIECE, LANES), F32),
            pltpu.VMEM((WAYS, MATRICES, SIDE, SIDE, PART, LANES), BF16),
            pltpu.VMEM((WAYS, MATRICES, 2, SIDE, SIDE, PART, LANES), BF16),
            pltpu.VMEM((WAYS, MATRICES, SIDE, PART, LANES), BF16),
            pltpu.VMEM((WAYS, MATRICES, 2, SIDE, PART, LANES), BF16),
            pltpu.VMEM((WAYS, MATRICES, STEPS, PART, LANES), BF16),
            pltpu.VMEM((WAYS, 2, SIDE, SIDE, PART, LANES), BF16),
            pltpu.VMEM((WAYS, 2, SIDE, PART, LANES), F32),
            pltpu.VMEM((WAYS, SIDE, PART, LANES), F32),
            pltpu.VMEM((PLANE + SIDE, SUBLANES, LANES), F32),
            *[pltpu.VMEM((LAYERS, w.shape[1] // n, w.shape[2]), BF16) for w, n in zip(weights, (PLANE, PLANE, DEVICES), strict=True)],
            DMA((AXES,)),
            *[DMA((2,))] * AXES, DMA((AXES,)),
            DMA((TILES,)),
            *[DMA((MATRICES, SIDE))] * 2, *[DMA((MATRICES,))] * 3,
            DMA((2,)),
            DMA((2,)), DMA((2,)),
        ],
        compiler_params=pltpu.CompilerParams(collective_id=0, has_side_effects=True, vmem_limit_bytes=MOST_VMEM - SPARE_VMEM),
        name="gradients",
    )(tall, wide, turned, deep, *weights)
    return g, squares, owns


def solution(mesh):
    rep, dp = mesh.axis_names

    def step(x, dy, *arrays):
        weights, m, v = (arrays[i : i + 3] for i in (0, 3, 6))
        g, total, owns = gradients(*by_rows(x[0], dy[0], weights), weights)
        new, new_m, new_v = adam(MATRICES * D * FF, g, total, owns, m, v)
        return (*natural(all_gather(new)), *new_m, *new_v)

    whole, rows, sequences = P(), P(None, dp), P((rep, dp))
    return jax.shard_map(
        step,
        mesh=mesh,
        in_specs=(sequences, sequences, *[whole] * AXES, *[rows] * MATRICES),
        out_specs=(*[P(rep)] * AXES, *[P(rep, dp)] * MATRICES),
        check_vma=False,
    )
```

```python
import functools
import jax
import jax.numpy as jnp
from jax import lax
from jax.experimental import pallas as pl
from jax.experimental.pallas import tpu as pltpu
from jax.sharding import PartitionSpec as P

MESH = pl.DeviceIdType.MESH
WAYS, AXES, SIDE = 6, 3, 4
STEPS = SIDE - 1
MATRICES, LAYERS, DEVICES, PLANE = 6, 2, 64, 16
LANES, SUBLANES, BLOCK = 128, 8, 280
BF16, F32 = jnp.bfloat16, jnp.float32
HBM, VMEM = pl.BlockSpec(memory_space=pl.ANY), pl.BlockSpec(memory_space=pltpu.VMEM)
DMA = pltpu.SemaphoreType.DMA
MIB = 1 << 20
MOST_VMEM, SPARE_VMEM = 62 * MIB, 2 * MIB
ORDERS = tuple(tuple((way // 2 + i) % AXES for i in range(AXES)) for way in range(WAYS))
SIGNS = (1, -1) * AXES
TURNS = tuple(tuple((way + i) % AXES for i in range(AXES)) for way in range(WAYS))
SENSES = (1,) * AXES + (-1,) * AXES
TAKEN = (3, 0, 4, 1, 5, 2)


def place():
    me = lax.axis_index("dp")
    return (me // PLANE, me // SIDE % SIDE, me % SIDE)


def wrap(i):
    return (i + 3 * SIDE) % SIDE


def neighbour(at, axis, step):
    there = [c for c in at]
    there[axis] = wrap(at[axis] + step)
    return {"dp": (there[0] * SIDE + there[1]) * SIDE + there[2]}


def remote(src, dst, send, recv, to):
    return pltpu.make_async_remote_copy(src_ref=src, dst_ref=dst, send_sem=send, recv_sem=recv, device_id=to, device_id_type=MESH)


def moved(at, steps):
    x, y, z = (wrap(a + step) for a, step in zip(at, steps, strict=True))
    return {"dp": (x * SIDE + y) * SIDE + z}


LINES = tuple(tuple(k * (axis == line) for axis in range(AXES)) for line in range(AXES) for k in range(1, SIDE))
PLANE_PEERS = tuple((0, k // SIDE, k % SIDE) for k in range(1, PLANE))
LINE_PEERS = LINES[:STEPS]


def enter(at, peers):
    barrier = pltpu.get_barrier_semaphore()
    for steps in peers:
        pl.semaphore_signal(barrier, inc=1, device_id=moved(at, steps), device_id_type=MESH)
    pl.semaphore_wait(barrier, len(peers))


def norm_exchange(at, buf, send, recv, total):
    first = 0
    for stage, peers in enumerate((PLANE_PEERS, LINE_PEERS)):
        own, others = buf.at[first], buf.at[pl.ds(first + 1, len(peers))]
        own[...] = total
        for k, steps in enumerate(peers):
            remote(own, others.at[k], send.at[stage], recv.at[stage], moved(at, steps)).start()
        pltpu.make_async_copy(others, others, recv.at[stage]).wait()
        total = total + jnp.sum(others[...], axis=0)
        pltpu.make_async_copy(others, others, send.at[stage]).wait()
        first += 1 + len(peers)
    return total


def passed_on(seen, c, phase, key):
    d1, d2, d3 = key
    if phase == 0 and d3 < STEPS:
        yield 0, (0, 0, d3 + 1)
    if phase < 2 and d2 < STEPS:
        yield 1, (0, d2 + 1, d3)
    if phase == 1 and d2 > 0:
        seen.append((c, d2))
        if seen.count((c, d2)) < SIDE:
            return
        d3 = None
    if d1 < STEPS:
        yield 2, (d1 + 1, d2, d3)


def ag_order(latency=2):
    import heapq

    free, out, seen, heap = {}, [], [], []

    def hold(t, c, phase, key):
        for phase, key in passed_on(seen, c, phase, key):
            link = ORDERS[c][2 - phase]
            size = SIDE if key[2] is None else 1
            free[link] = max(t, free.get(link, 0)) + size
            heapq.heappush(heap, (free[link] + latency, len(out) * WAYS + len(heap), c, phase, key))

    for c in range(0, WAYS, 2):
        hold(0, c, 0, (0, 0, 0))
    while heap:
        t, _, *arrival = heapq.heappop(heap)
        out.append(arrival)
        hold(t, *arrival)
    return out


def ag_kernel(*refs):
    mine, outs, (sends, recv1, recv2, recv3, recv4, local) = refs[0], refs[1 : 1 + WAYS], refs[1 + WAYS :]
    at = place()
    enter(at, LINES)

    def where(c, key):
        index = [None] * AXES
        for axis, d in zip(ORDERS[c], key, strict=True):
            index[axis] = slice(None) if d is None else wrap(at[axis] - SIGNS[c] * d)
        return outs[c].at[tuple(index)]

    def arrived(c, phase, key):
        d1, d2, d3 = key
        if phase == 0:
            return recv1.at[c // 2, d3 - 1]
        if phase == 1:
            return recv2.at[c // 2, d2 - 1, d3]
        if d3 is not None:
            return recv3.at[c // 2, d1 - 1, d3]
        return recv4.at[c // 2, d1 - 1, d2 - 1]

    def send_on(c, phase, key):
        d1, d2, d3 = key
        back = list(key)
        back[2 - phase] -= 1
        there = where(c, back)
        src = there if any(d != 0 for d in back) else mine.at[c]
        remote(src, there, sends.at[c, phase], arrived(c, phase, key), neighbour(at, ORDERS[c][2 - phase], SIGNS[c])).start()

    seen = []

    def hold(*held):
        for phase, key in passed_on(seen, *held):
            send_on(held[0], phase, key)

    own = [pltpu.make_async_copy(mine.at[c], where(c, (0, 0, 0)), local.at[c]) for c in range(WAYS)]
    for c in range(WAYS):
        hold(c, 0, (0, 0, 0))
    for copied in own:
        copied.start()
    for even, phase, key in ag_order():
        two = outs[even].at[0, pl.ds(0, 2)] if key[2] is None else outs[even].at[0, 0, pl.ds(0, 2)]
        pltpu.make_async_copy(two, two, arrived(even, phase, key)).wait()
        for c in (even, even + 1):
            hold(c, phase, key)
    for c in range(WAYS):
        own[c].wait()
        sent = outs[c].at[pl.ds(0, STEPS)]
        for phase in (2, 1, 0):
            pltpu.make_async_copy(sent, sent, sends.at[c, phase]).wait()
            sent = outs[c].at[(0,) * (AXES - phase) + (pl.ds(0, STEPS),)]


def all_gather(mine):
    return pl.pallas_call(
        ag_kernel,
        out_shape=(pltpu.VMEM((SIDE, SIDE, SIDE, *mine.shape[1:]), BF16),) * WAYS,
        in_specs=[VMEM],
        out_specs=(VMEM,) * WAYS,
        scratch_shapes=[DMA((WAYS, AXES)), DMA((AXES, STEPS)), *[DMA((AXES, STEPS, SIDE))] * 2, DMA((AXES, STEPS, STEPS)), DMA((WAYS,))],
        compiler_params=pltpu.CompilerParams(collective_id=1, has_side_effects=True, vmem_limit_bytes=MOST_VMEM // SUBLANES),
        name="gather",
    )(mine)


def tiles_of(t, rows, columns):
    n = columns // LANES
    if t < 2:
        return [(0, rows, j * LANES, j * rows) for j in range(n)]
    return [(8 * i, 8, j * LANES, (i * n + j) * 8) for i in range(rows // 8) for j in range(n)]


def adam_kernel(count, g, total, *refs):
    ws, ms, vs = (refs[AXES * k : AXES * (k + 1)] for k in range(3))
    new, *refs = refs[3 * AXES :]
    *moments, wide_g, wide_w = refs
    new_m, new_v = moments[:AXES], moments[AXES:]
    factor = jnp.minimum(1.0, 0.5 * lax.rsqrt(jnp.full((1, 1), jnp.sum(total[...])) / count + 1e-30))
    for t in range(AXES):
        rows, columns = ws[t].shape[1:]
        for l in range(LAYERS):
            wide_g[...] = g[TAKEN[LAYERS * t + l]].astype(F32) * factor
            for row, n, column, at in tiles_of(t, rows, columns):
                lanes = pl.ds(column, LANES)
                here = (slice(None), l, lanes) if t < 2 else (l, pl.ds(row, n), lanes)
                grad = wide_g[pl.ds(at, n), :]
                m = 0.9 * ms[t][here] + 0.1 * grad
                v = 0.95 * vs[t][here] + 0.05 * grad * grad
                w = ws[t][l, pl.ds(row, n), lanes]
                new_m[t][here] = m
                new_v[t][here] = v
                wide_w[pl.ds(at, n), :] = w - 0.02 * (m * lax.rsqrt(v + 1e-8) + 0.1 * w)
            new[LAYERS * t + l] = wide_w[...].astype(BF16)


def adam(count, g, total, ws, ms, vs):
    ms, vs = ([*(jnp.swapaxes(a, 0, 1) for a in arrays[:2]), arrays[2]] for arrays in (ms, vs))
    like = [jax.ShapeDtypeStruct(m.shape, F32) for m in ms]
    new, *moments = pl.pallas_call(
        functools.partial(adam_kernel, count),
        out_shape=(pltpu.VMEM(g.shape, BF16), *like, *like),
        in_specs=[VMEM] * (2 + AXES * 3),
        out_specs=(VMEM,) * (1 + AXES * 2),
        scratch_shapes=[pltpu.VMEM(g.shape[1:], F32)] * 2,
        compiler_params=pltpu.CompilerParams(vmem_limit_bytes=MOST_VMEM // SIDE),
        name="adam",
    )(g, total, *ws, *ms, *vs)
    return new, *([*(jnp.swapaxes(a, 0, 1) for a in part[:2]), part[2]] for part in (moments[:AXES], moments[AXES:]))


def natural_kernel(*refs):
    gathered, outs, wide = refs[:MATRICES], refs[MATRICES:-AXES], refs[-AXES:]
    first = pl.program_id(0) * SUBLANES
    for t in range(AXES):
        for l in range(LAYERS):
            rows, columns = outs[t].shape[1:]
            for k in range(SUBLANES):
                block = gathered[LAYERS * t + l][first + k].astype(F32)
                for row, n, column, at in tiles_of(t, rows // SUBLANES, columns):
                    wide[t][pl.ds(k * rows // SUBLANES + row, n), pl.ds(column, LANES)] = block[at : at + n]
            outs[t][l] = wide[t][...].astype(BF16)


def natural(gathered):
    shapes = (GATE, GATE, DOWN)
    return pl.pallas_call(
        natural_kernel,
        grid=(SUBLANES,),
        out_shape=tuple(jax.ShapeDtypeStruct((LAYERS, *s), BF16) for s in shapes),
        in_specs=[VMEM] * MATRICES,
        out_specs=tuple(pl.BlockSpec((LAYERS, s[0] // SUBLANES, s[1]), lambda i: (0, i, 0)) for s in shapes),
        scratch_shapes=[pltpu.VMEM((s[0] // SUBLANES, s[1]), F32) for s in shapes],
        compiler_params=pltpu.CompilerParams(vmem_limit_bytes=MOST_VMEM // SIDE),
        name="natural",
    )(*[g.reshape(DEVICES, BLOCK, LANES) for g in gathered])


D, FF, TOKENS = 896, 2560, 2048
GATE, DOWN = (D, FF), (FF, D)
ROWS, CHUNK, TILE = 256, 256, 512
TALL, WIDE, TURNED, DEEP = range(4)
SOON, AHEAD, NEXT = 4, 6, 8
TILES, PIECE, PLANE_ROWS = FF // TILE, BLOCK * TILE // FF, FF // SIDE
NT = (((1,), (1,)), ((), ()))


def dot(a, b):
    return jnp.dot(a, b, preferred_element_type=F32)


def dot_t(a, b):
    return lax.dot_general(a, b, NT, preferred_element_type=F32)


def scale_of(wide):
    return lax.rsqrt(jnp.mean(wide * wide, -1, keepdims=True) + 1e-6)


def rows_kernel(x_hbm, dy_hbm, *refs):
    hbm, results, weights, rest = refs[:3], refs[3:7], refs[7:13], refs[13:]
    buffers, (xs, dys, g0, u0, z0, dz1, sems, part_sems, in_sems, out_sems) = rest[:4], rest[4:]
    wg0, wu0, wd0, wg1, wu1, wd1 = weights
    i, slot = pl.program_id(0), pl.program_id(0) % 2
    first, blocks = i == 0, pl.num_programs(0)
    chunks = [pl.ds(j * CHUNK, CHUNK) for j in range(FF // CHUNK)]

    def fetch(k):
        return pltpu.make_async_copy(hbm[k % 3].at[k // 3], weights[k], sems.at[k])

    def fetch_part(k, j):
        return pltpu.make_async_copy(hbm[k].at[0, :, chunks[j]], weights[k].at[:, chunks[j]], part_sems.at[k, j])

    def take(source, there, i):
        rows = pl.ds(pl.multiple_of(i * ROWS, ROWS), ROWS)
        slot = i % there.shape[0]
        return pltpu.make_async_copy(source.at[rows], there.at[slot], in_sems.at[there.shape[0] - 2, slot])

    def put(k, part, slot=slot):
        rows = pl.ds(pl.multiple_of(i * ROWS, ROWS), ROWS)
        there = results[k].at[part, rows] if k % 2 else results[k].at[part, :, rows]
        return pltpu.make_async_copy(buffers[k].at[slot, part], there, out_sems.at[slot, k, part])

    def outs(slot):
        return [put(k, part, slot) for k, result in enumerate(results) for part in range(result.shape[0])]

    @pl.when(first)
    def _():
        take(x_hbm, xs, 0).start()
        take(dy_hbm, dys, 0).start()
        for j in range(len(chunks)):
            for k in range(2):
                fetch_part(k, j).start()
        take(dy_hbm, dys, 1).start()
        take(dy_hbm, dys, 0).wait()

    take(x_hbm, xs, i).wait()

    @pl.when(i + 1 < blocks)
    def _():
        take(x_hbm, xs, i + 1).start()
        take(dy_hbm, dys, i + 1).wait()

    @pl.when(i + 2 < blocks)
    def _():
        take(dy_hbm, dys, i + 2).start()

    @pl.when(i > 1)
    def _():
        for copy in outs(slot):
            copy.wait()

    tall, wide, turned, deep = (b.at[slot] for b in buffers)
    x, dy, next_dy = xs.at[slot], dys.at[i % AXES], dys.at[(i + 1) % AXES]

    def make_dz1(dy, some):
        for ch in some:
            dz1[:, ch] = dot_t(dy[...], wd1[ch, :]).astype(BF16)

    def forward(coming):
        a = (x[...].astype(F32) * scale_of(x[...].astype(F32))).astype(BF16)
        tall[1] = a.T
        deep[0] = dy[...]
        for j, ch in enumerate(chunks):
            if coming:
                for k in range(2):
                    fetch_part(k, j).wait()
                if 0 < j < 5:
                    fetch(j + 1).start()
            gate, up = dot(a, wg0[:, ch]), dot(a, wu0[:, ch])
            g0[:, ch], u0[:, ch] = gate, up
            z0[:, ch] = (gate * jax.nn.sigmoid(gate) * up).astype(BF16)
            turned[1, ch, :] = z0[:, ch].T

    @pl.when(first)
    def _():
        forward(True)
        for k in range(2, MATRICES):
            fetch(k).wait()
        make_dz1(dy, chunks[:AHEAD])

    @pl.when(i > 0)
    def _():
        forward(False)

    for k, part in ((TALL, 1), (DEEP, 0), (TURNED, 1)):
        put(k, part).start()
    make_dz1(dy, chunks[AHEAD:NEXT])
    h = x[...] + dot(z0[...], wd0[...]).astype(BF16)
    make_dz1(dy, chunks[NEXT:])
    h = h.astype(F32)
    scale = scale_of(h)
    a = (h * scale).astype(BF16)
    tall[0] = a.T
    put(TALL, 0).start()
    for ch in chunks:
        gate, up = dot(a, wg1[:, ch]), dot(a, wu1[:, ch])
        dz = dz1[:, ch].astype(F32)
        s = jax.nn.sigmoid(gate)
        silu = gate * s
        turned[0, ch, :] = (silu * up).astype(BF16).T
        wide[1, :, ch] = (dz * silu).astype(BF16)
        wide[0, :, ch] = (dz * up * (s + silu * (1 - s))).astype(BF16)
    for k, part in ((TURNED, 0), (WIDE, 0), (WIDE, 1)):
        put(k, part).start()
    da_gate, da_up = dot_t(wg1[...], wide[0]), dot_t(wu1[...], wide[1])
    make_dz1(next_dy, chunks[:SOON])
    da = (da_gate.astype(BF16) + da_up.astype(BF16)).T.astype(F32)
    dwide = scale * (da - h * (scale * scale * jnp.mean(da * h, -1, keepdims=True)))
    dh = dy[...] + dwide.astype(BF16)
    deep[1] = dh
    put(DEEP, 1).start()
    for ch in chunks:
        dz = dot_t(dh, wd0[ch, :]).astype(BF16).astype(F32)
        gate, up = g0[:, ch], u0[:, ch]
        s = jax.nn.sigmoid(gate)
        silu = gate * s
        wide[3, :, ch] = (dz * silu).astype(BF16)
        wide[2, :, ch] = (dz * up * (s + silu * (1 - s))).astype(BF16)
    make_dz1(next_dy, chunks[SOON:AHEAD])
    put(WIDE, 2).start()
    put(WIDE, 3).start()

    @pl.when(i + 1 == blocks)
    def _():
        for copy in outs(slot) + outs(1 - slot):
            copy.wait()


def by_rows(x, dy, weights):
    shapes = ((2, D, TOKENS), (4, TOKENS, FF), (2, FF, TOKENS), (2, TOKENS, D))
    buffers = ((2, D, ROWS), (4, ROWS, FF), (2, FF, ROWS), (2, ROWS, D))
    return pl.pallas_call(
        rows_kernel,
        grid=(TOKENS // ROWS,),
        out_shape=tuple(jax.ShapeDtypeStruct(s, BF16) for s in shapes),
        in_specs=[HBM] * 5,
        out_specs=(HBM,) * 4,
        scratch_shapes=[
            *[pltpu.VMEM(w.shape[1:], BF16) for w in weights * 2],
            *[pltpu.VMEM((2, *b), BF16) for b in buffers],
            *[pltpu.VMEM((n, ROWS, D), BF16) for n in (2, AXES)],
            *[pltpu.VMEM((ROWS, FF), F32)] * 2,
            *[pltpu.VMEM((ROWS, FF), BF16)] * 2,
            DMA((MATRICES,)), DMA((2, FF // CHUNK)), DMA((2, AXES)), DMA((2, 4, 4)),
        ],
        compiler_params=pltpu.CompilerParams(vmem_limit_bytes=MOST_VMEM),
        name="rows",
    )(x, dy, *weights)


GATE_ROWS, DOWN_ROWS = D // DEVICES, FF // DEVICES
STARTS = (0, 48, 96, 144, 192, 232)
PART = 48


def gate_block(acc, stage, wide):
    for i in range(PLANE):
        part = wide.at[i % wide.shape[0]]
        for c in range(SIDE):
            piece = acc[pl.ds(i * PIECE, PIECE), pl.ds(c * LANES, LANES)]
            for z in range(SIDE):
                part[z, pl.ds(GATE_ROWS * c, GATE_ROWS), :] = piece[GATE_ROWS * z : GATE_ROWS * (z + 1)]
        for z in range(SIDE):
            stage[i // SIDE, i % SIDE, z] = part[z].astype(BF16)


def down_block(acc, stage):
    def group(i, _):
        for t in range(DOWN_ROWS // SUBLANES):
            rows = acc[pl.ds(pl.multiple_of(i * DOWN_ROWS, SUBLANES) + SUBLANES * t, SUBLANES), :]
            piece = jnp.concatenate([rows[:, c * LANES : (c + 1) * LANES] for c in range(D // LANES)], 0)
            stage[i // SIDE, i % SIDE, pl.ds(PIECE * t, PIECE)] = piece.astype(BF16)
        return 0

    lax.fori_loop(0, PLANE, group, 0)


def own_rows(ws, windows, owns, sems):
    me = lax.axis_index("dp")
    taken = []
    for t in range(AXES):
        rows = windows[t].shape[1]
        first = pl.multiple_of((me // SIDE if t < 2 else me) * rows, SUBLANES)
        taken.append(pltpu.make_async_copy(ws[t].at[:, pl.ds(first, rows)], windows[t], sems.at[t]))
        taken[t].start()
    for t in range(AXES):
        taken[t].wait()
        rows = owns[t].shape[1]
        if t == 2:
            owns[t][...] = windows[t][...].astype(F32)
        for z in range(SIDE if t < 2 else 0):

            @pl.when(me % SIDE == z)
            def _():
                for l in range(LAYERS):
                    owns[t][l] = windows[t][l].astype(F32)[z * rows : (z + 1) * rows]


def gradients_kernel(*refs):
    (tall, wide, turned, deep), ws, (out, squares, terms), owns, scratch = refs[:4], refs[4:7], refs[7:10], refs[10:13], refs[13:]
    (lhs, rhs, zs, dh, acc_a, acc_b, acc2, stage_a, stage_b, stage2, shift, ra, rf, qa, qf, r3, own, f1, f2, sums) = scratch[:20]
    accs, stages = (acc_a, acc_b), (stage_a, stage_b)
    *windows, window_sem = scratch[20:24]
    (in_sem, rhs_sem, zs_sem, put_sem, sent, first_a, first_f, second_a, second_f, recv3, load, send4, recv4) = scratch[24:]
    at = place()

    def fetch_tall(l):
        return pltpu.make_async_copy(tall.at[l], lhs, in_sem.at[0])

    def fetch_deep(l):
        return pltpu.make_async_copy(deep.at[l], dh, in_sem.at[1])

    def fetch_wide(t):
        columns = pl.ds(pl.multiple_of(t % TILES * TILE, TILE), TILE)
        return pltpu.make_async_copy(wide.at[t // TILES, :, columns], rhs.at[t % 2], rhs_sem.at[t % 2])

    def fetch_turned(t):
        rows = pl.ds(pl.multiple_of(t % SIDE * PLANE_ROWS, LANES), PLANE_ROWS)
        return pltpu.make_async_copy(turned.at[t // SIDE, rows], zs.at[t % 2], zs_sem.at[t % 2])

    def arrange(m, h, odd):
        rows = pl.ds(pl.multiple_of(PIECE * h, SUBLANES), PIECE)
        gate_block(accs[odd], stages[odd], shift)
        pltpu.make_async_copy(stages[odd], terms.at[m, :, :, :, rows], put_sem.at[odd]).start()

    def emptied(odd):
        whole(stages[odd], put_sem.at[odd])

    def put2(m, h):
        return pltpu.make_async_copy(stage2, terms.at[m, h], put_sem.at[2])

    fetch_tall(0).start()
    fetch_wide(0).start()
    fetch_deep(0).start()
    fetch_turned(0).start()
    enter(at, sorted({*LINES, *PLANE_PEERS}))

    def split(c):
        o, s = TURNS[c], SENSES[c]
        return o, s, at[o[0]], at[o[1]], at[o[2]]

    def block(m, c, a, i):
        o = TURNS[c]
        index = [slice(None)] * 3
        index[o[0]] = a
        if i is not None:
            index[o[1]] = i
        return terms.at[(m, *index, pl.ds(STARTS[c], PART))]

    def piece(c, j):
        return wrap(split(c)[3] + SENSES[c] * (2 + j - j // 2 * (2 * j - 1)))

    def along(c, axis, src, there, sem, recv, steps=1):
        return remote(src, there, sent.at[sem], recv, neighbour(at, TURNS[c][axis], SENSES[c] * steps))

    def launch_a(m, ways):
        for j in range(SIDE):
            for c in ways:
                src = block(m, c, wrap(split(c)[2] + 2 * SENSES[c]), piece(c, j))
                along(c, 0, src, ra.at[c, m, j], 0, first_a.at[m, j]).start()

    def launch_d(m, ways):
        for j in range(SIDE):
            for c in ways:
                src = block(m, c, wrap(split(c)[2] - SENSES[c]), piece(c, j))
                along(c, 0, src, rf.at[c, m, 1, j], 1, first_f.at[m, j], -1).start()

    def load_own(m):
        for k in range(2):
            for c in range(WAYS):
                mine = block(m, c, wrap(split(c)[2] + SENSES[c] * (1 - k)), None)
                pltpu.make_async_copy(mine, own.at[c, k], load.at[k]).start()

    def whole(ref, sem):
        pltpu.make_async_copy(ref, ref, sem).wait()

    def term(c, k, j):
        i = piece(c, j)
        mine = own[c, k, i] if TURNS[c][1] < TURNS[c][2] else own[c, k, :, i]
        return mine.astype(F32)

    def on_first_a(m, j):
        whole(ra.at[:, m, j], first_a.at[m, j])
        for c in range(WAYS):
            ra[c, m, j] = (ra[c, m, j].astype(F32) + term(c, 0, j)).astype(BF16)
            along(c, 0, ra.at[c, m, j], rf.at[c, m, 0, j], 1, first_f.at[m, j]).start()

    def on_first_f(m, j):
        whole(rf.at[:, m, :, j], first_f.at[m, j])
        for c in range(WAYS):
            total = rf[c, m, 0, j].astype(F32) + rf[c, m, 1, j].astype(F32) + term(c, 1, j)
            if j < 2:
                rf[c, m, 1, j] = total.astype(BF16)
            else:
                f1[c, j - 2] = total
            if j == 0:
                along(c, 1, rf.at[c, m, 1, j], qa.at[c, m], 2, second_a.at[m]).start()
            if j == 1:
                along(c, 1, rf.at[c, m, 1, j], qf.at[c, m, 1], 3, second_f.at[m], -1).start()

    def on_second_a(m):
        whole(qa.at[:, m], second_a.at[m])
        for c in range(WAYS):
            qa[c, m] = (qa[c, m].astype(F32) + f1[c, 0]).astype(BF16)
            along(c, 1, qa.at[c, m], qf.at[c, m, 0], 3, second_f.at[m]).start()

    def third(m, c, k):
        src = qf.at[c, m, 1, wrap(split(c)[4] + k + 1)]
        return remote(src, r3.at[c, m, k], sent.at[4], recv3.at[m], neighbour(at, TURNS[c][2], k + 1))

    def on_second_f(m):
        whole(qf.at[:, m], second_f.at[m])
        for c in range(WAYS):
            total = qf[c, m, 0].astype(F32) + qf[c, m, 1].astype(F32) + f1[c, 1]
            f2[c] = total
            qf[c, m, 1] = total.astype(BF16)
            for k in range(STEPS):
                third(m, c, k).start()

    def on_third(m):
        whole(r3.at[:, m], recv3.at[m])
        for c in range(WAYS):
            o, s, p1, p2, p3 = split(c)
            total = f2[c, p3]
            for k in range(STEPS):
                total = total + r3[c, m, k].astype(F32)
            out[m, pl.ds(STARTS[c], PART)] = total.astype(BF16)

    def tile(i, _):
        m, h = i // TILES, i % TILES
        kind, l = m % AXES, m // AXES
        launched = (m > 0) & (m < MATRICES + 1)

        early = i == SIDE
        halves = (early | ((h == 0) & launched & (m > 1)), range(AXES)), ((h == 0) & launched, range(AXES, WAYS))

        @pl.when(early)
        def _():
            for odd in range(2):
                emptied(odd)

        @pl.when((h == 0) & launched)
        def _():
            @pl.when(kind > 0)
            def _():
                for odd in range(2):
                    emptied(odd)

            @pl.when(kind == 0)
            def _():
                put2(0, 0).wait()

        for send in (launch_a, launch_d):
            for now, ways in halves:

                @pl.when(now)
                def _():
                    send(jnp.where(early, m, m - 1), ways)

        @pl.when((m < MATRICES) & (kind < 2))
        def _():
            t = (2 * l + kind) * TILES + h

            @pl.when((kind == 0) & (h == 0))
            def _():
                fetch_tall(l).wait()

                @pl.when(l == 1)
                def _():
                    fetch_deep(1).start()

            fetch_wide(t).wait()

            @pl.when(t < 19)
            def _():
                fetch_wide(t + 1).start()

            @pl.when(h == 0)
            def _():
                accs[0][...] = dot(lhs[...], rhs[t % 2])

            @pl.when(h == AXES)
            def _():
                emptied(0)

            @pl.when((h == SIDE) & (m > 0))
            def _():
                emptied(1)

            for odd in range(2):

                @pl.when((h > 0) & (h % 2 == odd))
                def _():
                    accs[odd][...] = dot(lhs[...], rhs[t % 2])
                    arrange(m, h - 1, 1 - odd)

            @pl.when((h == SIDE) & (m > 0))
            def _():
                emptied(0)

            @pl.when(h == SIDE)
            def _():
                arrange(m, h, 0)

        @pl.when((m < MATRICES) & (kind == 2) & (h < SIDE))
        def _():
            t = SIDE * l + h

            @pl.when(h == 0)
            def _():
                fetch_deep(l).wait()

                @pl.when(l == 0)
                def _():
                    fetch_tall(1).start()

            fetch_turned(t).wait()

            @pl.when(t < 7)
            def _():
                fetch_turned(t + 1).start()

            acc2[...] = dot(zs[t % 2], dh[...])

            @pl.when(h > 0)
            def _():
                put2(m, h).wait()

            down_block(acc2, stage2)
            put2(m, h).start()

        @pl.when((h == 0) & (m > 2))
        def _():
            on_third(m - AXES)

        @pl.when((h == 2) & (m > 1))
        def _():
            on_second_a(m - 2)

        @pl.when((h == SIDE) & (m > 1))
        def _():
            on_second_f(m - 2)

        @pl.when((h == SIDE) & launched)
        def _():
            whole(own.at[:, 1], load.at[1])
            for j in range(2):
                on_first_f(m - 1, j)

        @pl.when((h == 0) & (m > 1))
        def _():
            for j in range(2, SIDE):
                on_first_f(m - 2, j)

        @pl.when(((h == 1) | (h == 2)) & launched)
        def _():
            @pl.when(h == 1)
            def _():
                whole(own.at[:, 0], load.at[0])

            lax.fori_loop(h - 1, AXES * h - 2, lambda j, _: (on_first_a(m - 1, j), 0)[1], 0)

        @pl.when((h == 0) & launched)
        def _():
            load_own(m - 1)

        return 0

    lax.fori_loop(0, (MATRICES + 2) * TILES, tile, 0)
    own_rows(ws, windows, owns, window_sem)
    on_third(MATRICES - 1)

    total = jnp.zeros((SUBLANES, LANES), F32)
    for m in range(MATRICES):
        g = out[m].astype(F32)
        total = total + jnp.sum((g * g).reshape(-1, SUBLANES, LANES), axis=0)
    squares[...] = norm_exchange(at, sums, send4, recv4, total)
    for k, buffer in enumerate((ra, rf, qa, qf, r3)):
        whole(buffer, sent.at[k])


def gradients(tall, wide, turned, deep, weights):
    g, squares, _, *owns = pl.pallas_call(
        gradients_kernel,
        out_shape=(
            pltpu.VMEM((MATRICES, BLOCK, LANES), BF16),
            pltpu.VMEM((SUBLANES, LANES), F32),
            jax.ShapeDtypeStruct((MATRICES, SIDE, SIDE, SIDE, BLOCK, LANES), BF16),
            *[pltpu.VMEM((LAYERS, w.shape[1] // DEVICES, w.shape[2]), F32) for w in weights],
        ),
        in_specs=[HBM] * (4 + AXES),
        out_specs=(VMEM, VMEM, HBM, *[VMEM] * AXES),
        scratch_shapes=[
            pltpu.VMEM((D, TOKENS), BF16),
            pltpu.VMEM((2, TOKENS, TILE), BF16),
            pltpu.VMEM((2, PLANE_ROWS, TOKENS), BF16),
            pltpu.VMEM((TOKENS, D), BF16),
            *[pltpu.VMEM((D, TILE), F32)] * 2,
            pltpu.VMEM((PLANE_ROWS, D), F32),
            *[pltpu.VMEM((SIDE, SIDE, SIDE, PIECE, LANES), BF16)] * 2,
            pltpu.VMEM((SIDE, SIDE, BLOCK, LANES), BF16),
            pltpu.VMEM((SIDE, SIDE, PIECE, LANES), F32),
            pltpu.VMEM((WAYS, MATRICES, SIDE, SIDE, PART, LANES), BF16),
            pltpu.VMEM((WAYS, MATRICES, 2, SIDE, SIDE, PART, LANES), BF16),
            pltpu.VMEM((WAYS, MATRICES, SIDE, PART, LANES), BF16),
            pltpu.VMEM((WAYS, MATRICES, 2, SIDE, PART, LANES), BF16),
            pltpu.VMEM((WAYS, MATRICES, STEPS, PART, LANES), BF16),
            pltpu.VMEM((WAYS, 2, SIDE, SIDE, PART, LANES), BF16),
            pltpu.VMEM((WAYS, 2, SIDE, PART, LANES), F32),
            pltpu.VMEM((WAYS, SIDE, PART, LANES), F32),
            pltpu.VMEM((PLANE + SIDE, SUBLANES, LANES), F32),
            *[pltpu.VMEM((LAYERS, w.shape[1] // n, w.shape[2]), BF16) for w, n in zip(weights, (PLANE, PLANE, DEVICES), strict=True)],
            DMA((AXES,)),
            *[DMA((2,))] * AXES, DMA((AXES,)),
            DMA((TILES,)),
            *[DMA((MATRICES, SIDE))] * 2, *[DMA((MATRICES,))] * 3,
            DMA((2,)),
            DMA((2,)), DMA((2,)),
        ],
        compiler_params=pltpu.CompilerParams(collective_id=0, has_side_effects=True, vmem_limit_bytes=MOST_VMEM - SPARE_VMEM),
        name="gradients",
    )(tall, wide, turned, deep, *weights)
    return g, squares, owns


def solution(mesh):
    rep, dp = mesh.axis_names

    def step(x, dy, *arrays):
        weights, m, v = (arrays[i : i + 3] for i in (0, 3, 6))
        g, total, owns = gradients(*by_rows(x[0], dy[0], weights), weights)
        new, new_m, new_v = adam(MATRICES * D * FF, g, total, owns, m, v)
        return (*natural(all_gather(new)), *new_m, *new_v)

    whole, rows, sequences = P(), P(None, dp), P((rep, dp))
    return jax.shard_map(
        step,
        mesh=mesh,
        in_specs=(sequences, sequences, *[whole] * AXES, *[rows] * MATRICES),
        out_specs=(*[P(rep)] * AXES, *[P(rep, dp)] * MATRICES),
        check_vma=False,
    )
```

```python
import functools
import jax
import jax.numpy as jnp
from jax import lax
from jax.experimental import pallas as pl
from jax.experimental.pallas import tpu as pltpu
from jax.sharding import PartitionSpec as P

MESH = pl.DeviceIdType.MESH
WAYS, AXES, SIDE = 6, 3, 4
STEPS = SIDE - 1
MATRICES, LAYERS, DEVICES, PLANE = 6, 2, 64, 16
LANES, SUBLANES, BLOCK = 128, 8, 280
BF16, F32 = jnp.bfloat16, jnp.float32
HBM, VMEM = pl.BlockSpec(memory_space=pl.ANY), pl.BlockSpec(memory_space=pltpu.VMEM)
DMA = pltpu.SemaphoreType.DMA
MIB = 1 << 20
MOST_VMEM, SPARE_VMEM = 62 * MIB, 2 * MIB
ORDERS = tuple(tuple((way // 2 + i) % AXES for i in range(AXES)) for way in range(WAYS))
SIGNS = (1, -1) * AXES
TAKEN = (3, 0, 4, 1, 5, 2)


def place():
    me = lax.axis_index("dp")
    return (me // PLANE, me // SIDE % SIDE, me % SIDE)


def wrap(i):
    return (i + 3 * SIDE) % SIDE


def neighbour(at, axis, step):
    there = [c for c in at]
    there[axis] = wrap(at[axis] + step)
    return {"dp": (there[0] * SIDE + there[1]) * SIDE + there[2]}


def remote(src, dst, send, recv, to):
    return pltpu.make_async_remote_copy(src_ref=src, dst_ref=dst, send_sem=send, recv_sem=recv, device_id=to, device_id_type=MESH)


def moved(at, steps):
    x, y, z = (wrap(a + step) for a, step in zip(at, steps, strict=True))
    return {"dp": (x * SIDE + y) * SIDE + z}


LINES = tuple(tuple(k * (axis == line) for axis in range(AXES)) for line in range(AXES) for k in range(1, SIDE))
PLANE_PEERS = tuple((0, k // SIDE, k % SIDE) for k in range(1, PLANE))
LINE_PEERS = LINES[:STEPS]
NEIGHBOURS = tuple(steps for steps in LINES if 2 not in steps)


def enter(at, peers):
    barrier = pltpu.get_barrier_semaphore()
    for steps in peers:
        pl.semaphore_signal(barrier, inc=1, device_id=moved(at, steps), device_id_type=MESH)
    pl.semaphore_wait(barrier, len(peers))


def norm_exchange(at, buf, send, recv, total):
    first = 0
    for stage, peers in enumerate((PLANE_PEERS, LINE_PEERS)):
        own, others = buf.at[first], buf.at[pl.ds(first + 1, len(peers))]
        own[...] = total
        for k, steps in enumerate(peers):
            remote(own, others.at[k], send.at[stage], recv.at[stage], moved(at, steps)).start()
        pltpu.make_async_copy(others, others, recv.at[stage]).wait()
        total = total + jnp.sum(others[...], axis=0)
        pltpu.make_async_copy(others, others, send.at[stage]).wait()
        first += 1 + len(peers)
    return total


def passed_on(seen, c, phase, key):
    d1, d2, d3 = key
    if phase == 0 and d3 < STEPS:
        yield 0, (0, 0, d3 + 1)
    if phase < 2 and d2 < STEPS:
        yield 1, (0, d2 + 1, d3)
    if phase == 1 and d2 > 0:
        seen.append((c, d2))
        if seen.count((c, d2)) < SIDE:
            return
        d3 = None
    if d1 < STEPS:
        yield 2, (d1 + 1, d2, d3)


def ag_order(latency=2):
    import heapq

    free, out, seen, heap = {}, [], [], []

    def hold(t, c, phase, key):
        for phase, key in passed_on(seen, c, phase, key):
            link = ORDERS[c][2 - phase]
            size = SIDE if key[2] is None else 1
            free[link] = max(t, free.get(link, 0)) + size
            heapq.heappush(heap, (free[link] + latency, len(out) * WAYS + len(heap), c, phase, key))

    for c in range(0, WAYS, 2):
        hold(0, c, 0, (0, 0, 0))
    while heap:
        t, _, *arrival = heapq.heappop(heap)
        out.append(arrival)
        hold(t, *arrival)
    return out


def ag_kernel(*refs):
    mine, outs, (sends, recv1, recv2, recv3, recv4, local) = refs[0], refs[1 : 1 + WAYS], refs[1 + WAYS :]
    at = place()
    enter(at, NEIGHBOURS)

    def where(c, key):
        index = [None] * AXES
        for axis, d in zip(ORDERS[c], key, strict=True):
            index[axis] = slice(None) if d is None else wrap(at[axis] - SIGNS[c] * d)
        return outs[c].at[tuple(index)]

    def arrived(c, phase, key):
        d1, d2, d3 = key
        if phase == 0:
            return recv1.at[c // 2, d3 - 1]
        if phase == 1:
            return recv2.at[c // 2, d2 - 1, d3]
        if d3 is not None:
            return recv3.at[c // 2, d1 - 1, d3]
        return recv4.at[c // 2, d1 - 1, d2 - 1]

    def send_on(c, phase, key):
        d1, d2, d3 = key
        back = list(key)
        back[2 - phase] -= 1
        there = where(c, back)
        src = there if any(d != 0 for d in back) else mine.at[c]
        remote(src, there, sends.at[c, phase], arrived(c, phase, key), neighbour(at, ORDERS[c][2 - phase], SIGNS[c])).start()

    seen = []

    def hold(*held):
        for phase, key in passed_on(seen, *held):
            send_on(held[0], phase, key)

    own = [pltpu.make_async_copy(mine.at[c], where(c, (0, 0, 0)), local.at[c]) for c in range(WAYS)]
    for c in range(WAYS):
        hold(c, 0, (0, 0, 0))
    for copied in own:
        copied.start()
    for even, phase, key in ag_order():
        two = outs[even].at[0, pl.ds(0, 2)] if key[2] is None else outs[even].at[0, 0, pl.ds(0, 2)]
        pltpu.make_async_copy(two, two, arrived(even, phase, key)).wait()
        for c in (even, even + 1):
            hold(c, phase, key)
    for c in range(WAYS):
        own[c].wait()
        sent = outs[c].at[pl.ds(0, STEPS)]
        for phase in (2, 1, 0):
            pltpu.make_async_copy(sent, sent, sends.at[c, phase]).wait()
            sent = outs[c].at[(0,) * (AXES - phase) + (pl.ds(0, STEPS),)]


def all_gather(mine):
    return pl.pallas_call(
        ag_kernel,
        out_shape=(pltpu.VMEM((SIDE, SIDE, SIDE, *mine.shape[1:]), BF16),) * WAYS,
        in_specs=[VMEM],
        out_specs=(VMEM,) * WAYS,
        scratch_shapes=[DMA((WAYS, AXES)), DMA((AXES, STEPS)), *[DMA((AXES, STEPS, SIDE))] * 2, DMA((AXES, STEPS, STEPS)), DMA((WAYS,))],
        compiler_params=pltpu.CompilerParams(collective_id=1, has_side_effects=True, vmem_limit_bytes=MOST_VMEM // SUBLANES),
        name="gather",
    )(mine)


def tiles_of(t, rows, columns):
    n = columns // LANES
    if t < 2:
        return [(0, rows, j * LANES, j * rows) for j in range(n)]
    return [(8 * i, 8, j * LANES, (i * n + j) * 8) for i in range(rows // 8) for j in range(n)]


def adam_kernel(count, g, total, *refs):
    ws, ms, vs = (refs[AXES * k : AXES * (k + 1)] for k in range(3))
    new, *refs = refs[3 * AXES :]
    *moments, wide_g, wide_w = refs
    new_m, new_v = moments[:AXES], moments[AXES:]
    factor = jnp.minimum(1.0, 0.5 * lax.rsqrt(jnp.full((1, 1), jnp.sum(total[...])) / count + 1e-30))
    for t in range(AXES):
        rows, columns = ws[t].shape[1:]
        for l in range(LAYERS):
            wide_g[...] = g[TAKEN[LAYERS * t + l]].astype(F32) * factor
            for row, n, column, at in tiles_of(t, rows, columns):
                lanes = pl.ds(column, LANES)
                here = (slice(None), l, lanes) if t < 2 else (l, pl.ds(row, n), lanes)
                grad = wide_g[pl.ds(at, n), :]
                m = 0.9 * ms[t][here] + 0.1 * grad
                v = 0.95 * vs[t][here] + 0.05 * grad * grad
                w = ws[t][l, pl.ds(row, n), lanes]
                new_m[t][here] = m
                new_v[t][here] = v
                wide_w[pl.ds(at, n), :] = w - 0.02 * (m * lax.rsqrt(v + 1e-8) + 0.1 * w)
            new[LAYERS * t + l] = wide_w[...].astype(BF16)


def adam(count, g, total, ws, ms, vs):
    ms, vs = ([*(jnp.swapaxes(a, 0, 1) for a in arrays[:2]), arrays[2]] for arrays in (ms, vs))
    like = [jax.ShapeDtypeStruct(m.shape, F32) for m in ms]
    new, *moments = pl.pallas_call(
        functools.partial(adam_kernel, count),
        out_shape=(pltpu.VMEM(g.shape, BF16), *like, *like),
        in_specs=[VMEM] * (2 + AXES * 3),
        out_specs=(VMEM,) * (1 + AXES * 2),
        scratch_shapes=[pltpu.VMEM(g.shape[1:], F32)] * 2,
        compiler_params=pltpu.CompilerParams(vmem_limit_bytes=MOST_VMEM // SIDE),
        name="adam",
    )(g, total, *ws, *ms, *vs)
    return new, *([*(jnp.swapaxes(a, 0, 1) for a in part[:2]), part[2]] for part in (moments[:AXES], moments[AXES:]))


def natural_kernel(*refs):
    gathered, outs, wide = refs[:MATRICES], refs[MATRICES:-AXES], refs[-AXES:]
    first = pl.program_id(0) * SUBLANES
    for t in range(AXES):
        for l in range(LAYERS):
            rows, columns = outs[t].shape[1:]
            for k in range(SUBLANES):
                block = gathered[LAYERS * t + l][first + k].astype(F32)
                for row, n, column, at in tiles_of(t, rows // SUBLANES, columns):
                    wide[t][pl.ds(k * rows // SUBLANES + row, n), pl.ds(column, LANES)] = block[at : at + n]
            outs[t][l] = wide[t][...].astype(BF16)


def natural(gathered):
    shapes = (GATE, GATE, DOWN)
    return pl.pallas_call(
        natural_kernel,
        grid=(SUBLANES,),
        out_shape=tuple(jax.ShapeDtypeStruct((LAYERS, *s), BF16) for s in shapes),
        in_specs=[VMEM] * MATRICES,
        out_specs=tuple(pl.BlockSpec((LAYERS, s[0] // SUBLANES, s[1]), lambda i: (0, i, 0)) for s in shapes),
        scratch_shapes=[pltpu.VMEM((s[0] // SUBLANES, s[1]), F32) for s in shapes],
        compiler_params=pltpu.CompilerParams(vmem_limit_bytes=MOST_VMEM // SIDE),
        name="natural",
    )(*[g.reshape(DEVICES, BLOCK, LANES) for g in gathered])


D, FF, TOKENS = 896, 2560, 2048
GATE, DOWN = (D, FF), (FF, D)
ROWS, CHUNK, TILE = 256, 256, 512
TALL, WIDE, TURNED, DEEP = range(4)
SOON, AHEAD, NEXT = 4, 6, 8
TILES, PIECE, PLANE_ROWS = FF // TILE, BLOCK * TILE // FF, FF // SIDE
NT = (((1,), (1,)), ((), ()))


def dot(a, b):
    return jnp.dot(a, b, preferred_element_type=F32)


def dot_t(a, b):
    return lax.dot_general(a, b, NT, preferred_element_type=F32)


def scale_of(wide):
    return lax.rsqrt(jnp.mean(wide * wide, -1, keepdims=True) + 1e-6)


def rows_kernel(x_hbm, dy_hbm, *refs):
    hbm, results, weights, rest = refs[:3], refs[3:7], refs[7:13], refs[13:]
    buffers, (xs, dys, g0, u0, z0, dz1, sems, part_sems, in_sems, out_sems) = rest[:4], rest[4:]
    wg0, wu0, wd0, wg1, wu1, wd1 = weights
    i, slot = pl.program_id(0), pl.program_id(0) % 2
    first, blocks = i == 0, pl.num_programs(0)
    chunks = [pl.ds(j * CHUNK, CHUNK) for j in range(FF // CHUNK)]

    def fetch(k):
        return pltpu.make_async_copy(hbm[k % 3].at[k // 3], weights[k], sems.at[k])

    def fetch_part(k, j):
        return pltpu.make_async_copy(hbm[k].at[0, :, chunks[j]], weights[k].at[:, chunks[j]], part_sems.at[k, j])

    def take(source, there, i):
        rows = pl.ds(pl.multiple_of(i * ROWS, ROWS), ROWS)
        slot = i % there.shape[0]
        return pltpu.make_async_copy(source.at[rows], there.at[slot], in_sems.at[there.shape[0] - 2, slot])

    def put(k, part, slot=slot):
        rows = pl.ds(pl.multiple_of(i * ROWS, ROWS), ROWS)
        there = results[k].at[part, rows] if k % 2 else results[k].at[part, :, rows]
        return pltpu.make_async_copy(buffers[k].at[slot, part], there, out_sems.at[slot, k, part])

    def outs(slot):
        return [put(k, part, slot) for k, result in enumerate(results) for part in range(result.shape[0])]

    @pl.when(first)
    def _():
        take(x_hbm, xs, 0).start()
        take(dy_hbm, dys, 0).start()
        for j in range(len(chunks)):
            for k in range(2):
                fetch_part(k, j).start()
        take(dy_hbm, dys, 1).start()
        take(dy_hbm, dys, 0).wait()

    take(x_hbm, xs, i).wait()

    @pl.when(i + 1 < blocks)
    def _():
        take(x_hbm, xs, i + 1).start()
        take(dy_hbm, dys, i + 1).wait()

    @pl.when(i + 2 < blocks)
    def _():
        take(dy_hbm, dys, i + 2).start()

    @pl.when(i > 1)
    def _():
        for copy in outs(slot):
            copy.wait()

    tall, wide, turned, deep = (b.at[slot] for b in buffers)
    x, dy, next_dy = xs.at[slot], dys.at[i % AXES], dys.at[(i + 1) % AXES]

    def make_dz1(dy, some):
        for ch in some:
            dz1[:, ch] = dot_t(dy[...], wd1[ch, :]).astype(BF16)

    def forward(coming):
        a = (x[...].astype(F32) * scale_of(x[...].astype(F32))).astype(BF16)
        tall[1] = a.T
        deep[0] = dy[...]
        for j, ch in enumerate(chunks):
            if coming:
                for k in range(2):
                    fetch_part(k, j).wait()
                if 0 < j < 5:
                    fetch(j + 1).start()
            gate, up = dot(a, wg0[:, ch]), dot(a, wu0[:, ch])
            g0[:, ch], u0[:, ch] = gate, up
            z0[:, ch] = (gate * jax.nn.sigmoid(gate) * up).astype(BF16)
            turned[1, ch, :] = z0[:, ch].T

    @pl.when(first)
    def _():
        forward(True)
        for k in range(2, MATRICES):
            fetch(k).wait()
        make_dz1(dy, chunks[:AHEAD])

    @pl.when(i > 0)
    def _():
        forward(False)

    for k, part in ((TALL, 1), (DEEP, 0), (TURNED, 1)):
        put(k, part).start()
    make_dz1(dy, chunks[AHEAD:NEXT])
    h = x[...] + dot(z0[...], wd0[...]).astype(BF16)
    make_dz1(dy, chunks[NEXT:])
    h = h.astype(F32)
    scale = scale_of(h)
    a = (h * scale).astype(BF16)
    tall[0] = a.T
    put(TALL, 0).start()
    for ch in chunks:
        gate, up = dot(a, wg1[:, ch]), dot(a, wu1[:, ch])
        dz = dz1[:, ch].astype(F32)
        s = jax.nn.sigmoid(gate)
        silu = gate * s
        turned[0, ch, :] = (silu * up).astype(BF16).T
        wide[1, :, ch] = (dz * silu).astype(BF16)
        wide[0, :, ch] = (dz * up * (s + silu * (1 - s))).astype(BF16)
    for k, part in ((TURNED, 0), (WIDE, 0), (WIDE, 1)):
        put(k, part).start()
    da_gate, da_up = dot_t(wg1[...], wide[0]), dot_t(wu1[...], wide[1])
    make_dz1(next_dy, chunks[:SOON])
    da = (da_gate.astype(BF16) + da_up.astype(BF16)).T.astype(F32)
    dwide = scale * (da - h * (scale * scale * jnp.mean(da * h, -1, keepdims=True)))
    dh = dy[...] + dwide.astype(BF16)
    deep[1] = dh
    put(DEEP, 1).start()
    for ch in chunks:
        dz = dot_t(dh, wd0[ch, :]).astype(BF16).astype(F32)
        gate, up = g0[:, ch], u0[:, ch]
        s = jax.nn.sigmoid(gate)
        silu = gate * s
        wide[3, :, ch] = (dz * silu).astype(BF16)
        wide[2, :, ch] = (dz * up * (s + silu * (1 - s))).astype(BF16)
    make_dz1(next_dy, chunks[SOON:AHEAD])
    put(WIDE, 2).start()
    put(WIDE, 3).start()

    @pl.when(i + 1 == blocks)
    def _():
        for copy in outs(slot) + outs(1 - slot):
            copy.wait()


def by_rows(x, dy, weights):
    shapes = ((2, D, TOKENS), (4, TOKENS, FF), (2, FF, TOKENS), (2, TOKENS, D))
    buffers = ((2, D, ROWS), (4, ROWS, FF), (2, FF, ROWS), (2, ROWS, D))
    return pl.pallas_call(
        rows_kernel,
        grid=(TOKENS // ROWS,),
        out_shape=tuple(jax.ShapeDtypeStruct(s, BF16) for s in shapes),
        in_specs=[HBM] * 5,
        out_specs=(HBM,) * 4,
        scratch_shapes=[
            *[pltpu.VMEM(w.shape[1:], BF16) for w in weights * 2],
            *[pltpu.VMEM((2, *b), BF16) for b in buffers],
            *[pltpu.VMEM((n, ROWS, D), BF16) for n in (2, AXES)],
            *[pltpu.VMEM((ROWS, FF), F32)] * 2,
            *[pltpu.VMEM((ROWS, FF), BF16)] * 2,
            DMA((MATRICES,)), DMA((2, FF // CHUNK)), DMA((2, AXES)), DMA((2, 4, 4)),
        ],
        compiler_params=pltpu.CompilerParams(vmem_limit_bytes=MOST_VMEM),
        name="rows",
    )(x, dy, *weights)


GATE_ROWS, DOWN_ROWS = D // DEVICES, FF // DEVICES
STARTS = (0, 48, 96, 144, 192, 232)
PART = 48


def gate_block(acc, stage, wide):
    for i in range(PLANE):
        part = wide.at[i % wide.shape[0]]
        for c in range(SIDE):
            piece = acc[pl.ds(i * PIECE, PIECE), pl.ds(c * LANES, LANES)]
            for z in range(SIDE):
                part[z, pl.ds(GATE_ROWS * c, GATE_ROWS), :] = piece[GATE_ROWS * z : GATE_ROWS * (z + 1)]
        for z in range(SIDE):
            stage[i // SIDE, i % SIDE, z] = part[z].astype(BF16)


def down_block(acc, stage):
    def group(i, _):
        for t in range(DOWN_ROWS // SUBLANES):
            rows = acc[pl.ds(pl.multiple_of(i * DOWN_ROWS, SUBLANES) + SUBLANES * t, SUBLANES), :]
            piece = jnp.concatenate([rows[:, c * LANES : (c + 1) * LANES] for c in range(D // LANES)], 0)
            stage[i // SIDE, i % SIDE, pl.ds(PIECE * t, PIECE)] = piece.astype(BF16)
        return 0

    lax.fori_loop(0, PLANE, group, 0)


def own_rows(ws, windows, owns, sems):
    me = lax.axis_index("dp")
    taken = []
    for t in range(AXES):
        rows = windows[t].shape[1]
        first = pl.multiple_of((me // SIDE if t < 2 else me) * rows, SUBLANES)
        taken.append(pltpu.make_async_copy(ws[t].at[:, pl.ds(first, rows)], windows[t], sems.at[t]))
        taken[t].start()
    for t in range(AXES):
        taken[t].wait()
        rows = owns[t].shape[1]
        if t == 2:
            owns[t][...] = windows[t][...].astype(F32)
        for z in range(SIDE if t < 2 else 0):

            @pl.when(me % SIDE == z)
            def _():
                for l in range(LAYERS):
                    owns[t][l] = windows[t][l].astype(F32)[z * rows : (z + 1) * rows]


def gradients_kernel(*refs):
    (tall, wide, turned, deep), ws, (out, squares, terms), owns, scratch = refs[:4], refs[4:7], refs[7:10], refs[10:13], refs[13:]
    (lhs, rhs, zs, dh, acc_a, acc_b, acc2, stage_a, stage_b, stage2, shift, ra, rf, qa, qf, r3, own, f1, f2, sums) = scratch[:20]
    accs, stages = (acc_a, acc_b), (stage_a, stage_b)
    *windows, window_sem = scratch[20:24]
    (in_sem, rhs_sem, zs_sem, put_sem, sent, first_a, first_f, second_a, second_f, recv3, load, send4, recv4) = scratch[24:]
    at = place()

    def fetch_tall(l):
        return pltpu.make_async_copy(tall.at[l], lhs, in_sem.at[0])

    def fetch_deep(l):
        return pltpu.make_async_copy(deep.at[l], dh, in_sem.at[1])

    def fetch_wide(t):
        columns = pl.ds(pl.multiple_of(t % TILES * TILE, TILE), TILE)
        return pltpu.make_async_copy(wide.at[t // TILES, :, columns], rhs.at[t % 2], rhs_sem.at[t % 2])

    def fetch_turned(t):
        rows = pl.ds(pl.multiple_of(t % SIDE * PLANE_ROWS, LANES), PLANE_ROWS)
        return pltpu.make_async_copy(turned.at[t // SIDE, rows], zs.at[t % 2], zs_sem.at[t % 2])

    def arrange(m, h, odd):
        rows = pl.ds(pl.multiple_of(PIECE * h, SUBLANES), PIECE)
        gate_block(accs[odd], stages[odd], shift)
        pltpu.make_async_copy(stages[odd], terms.at[m, :, :, :, rows], put_sem.at[odd]).start()

    def emptied(odd):
        whole(stages[odd], put_sem.at[odd])

    def put2(m, h):
        return pltpu.make_async_copy(stage2, terms.at[m, h], put_sem.at[2])

    fetch_tall(0).start()
    fetch_wide(0).start()
    fetch_deep(0).start()
    fetch_turned(0).start()
    enter(at, sorted({*LINES, *PLANE_PEERS}))

    def split(c):
        o, s = ORDERS[c], SIGNS[c]
        return o, s, at[o[0]], at[o[1]], at[o[2]]

    def block(m, c, a, i):
        o = ORDERS[c]
        index = [slice(None)] * 3
        index[o[0]] = a
        if i is not None:
            index[o[1]] = i
        return terms.at[(m, *index, pl.ds(STARTS[c], PART))]

    def piece(c, j):
        return wrap(split(c)[3] + SIGNS[c] * (2 + j - j // 2 * (2 * j - 1)))

    def along(c, axis, src, there, sem, recv, steps=1):
        return remote(src, there, sent.at[sem], recv, neighbour(at, ORDERS[c][axis], SIGNS[c] * steps))

    def launch(m):
        for j in range(SIDE):
            for c in range(WAYS):
                src = block(m, c, wrap(split(c)[2] + 2 * SIGNS[c]), piece(c, j))
                along(c, 0, src, ra.at[c, m, j], 0, first_a.at[m, j]).start()
        for j in range(SIDE):
            for c in range(WAYS):
                src = block(m, c, wrap(split(c)[2] - SIGNS[c]), piece(c, j))
                along(c, 0, src, rf.at[c, m, 1, j], 1, first_f.at[m, j], -1).start()

    def load_own(m):
        for k in range(2):
            for c in range(WAYS):
                mine = block(m, c, wrap(split(c)[2] + SIGNS[c] * (1 - k)), None)
                pltpu.make_async_copy(mine, own.at[c, k], load.at[k]).start()

    def whole(ref, sem):
        pltpu.make_async_copy(ref, ref, sem).wait()

    def term(c, k, j):
        i = piece(c, j)
        mine = own[c, k, i] if ORDERS[c][1] < ORDERS[c][2] else own[c, k, :, i]
        return mine.astype(F32)

    def on_first_a(m, j):
        whole(ra.at[:, m, j], first_a.at[m, j])
        for c in range(WAYS):
            ra[c, m, j] = (ra[c, m, j].astype(F32) + term(c, 0, j)).astype(BF16)
            along(c, 0, ra.at[c, m, j], rf.at[c, m, 0, j], 1, first_f.at[m, j]).start()

    def on_first_f(m, j):
        whole(rf.at[:, m, :, j], first_f.at[m, j])
        for c in range(WAYS):
            total = rf[c, m, 0, j].astype(F32) + rf[c, m, 1, j].astype(F32) + term(c, 1, j)
            if j < 2:
                rf[c, m, 1, j] = total.astype(BF16)
            else:
                f1[c, j - 2] = total
            if j == 0:
                along(c, 1, rf.at[c, m, 1, j], qa.at[c, m], 2, second_a.at[m]).start()
            if j == 1:
                along(c, 1, rf.at[c, m, 1, j], qf.at[c, m, 1], 3, second_f.at[m], -1).start()

    def on_second_a(m):
        whole(qa.at[:, m], second_a.at[m])
        for c in range(WAYS):
            qa[c, m] = (qa[c, m].astype(F32) + f1[c, 0]).astype(BF16)
            along(c, 1, qa.at[c, m], qf.at[c, m, 0], 3, second_f.at[m]).start()

    def third(m, c, k):
        src = qf.at[c, m, 1, wrap(split(c)[4] + k + 1)]
        return remote(src, r3.at[c, m, k], sent.at[4], recv3.at[m], neighbour(at, ORDERS[c][2], k + 1))

    def on_second_f(m):
        whole(qf.at[:, m], second_f.at[m])
        for c in range(WAYS):
            total = qf[c, m, 0].astype(F32) + qf[c, m, 1].astype(F32) + f1[c, 1]
            f2[c] = total
            qf[c, m, 1] = total.astype(BF16)
            for k in range(STEPS):
                third(m, c, k).start()

    def on_third(m):
        whole(r3.at[:, m], recv3.at[m])
        for c in range(WAYS):
            o, s, p1, p2, p3 = split(c)
            total = f2[c, p3]
            for k in range(STEPS):
                total = total + r3[c, m, k].astype(F32)
            out[m, pl.ds(STARTS[c], PART)] = total.astype(BF16)

    def tile(i, _):
        m, h = i // TILES, i % TILES
        kind, l = m % AXES, m // AXES
        launched = (m > 0) & (m < MATRICES + 1)

        @pl.when((h == 0) & launched)
        def _():
            @pl.when(kind > 0)
            def _():
                for odd in range(2):
                    emptied(odd)

            @pl.when(kind == 0)
            def _():
                put2(0, 0).wait()

            launch(m - 1)

        @pl.when((m < MATRICES) & (kind < 2))
        def _():
            t = (2 * l + kind) * TILES + h

            @pl.when((kind == 0) & (h == 0))
            def _():
                fetch_tall(l).wait()

                @pl.when(l == 1)
                def _():
                    fetch_deep(1).start()

            fetch_wide(t).wait()

            @pl.when(t < 19)
            def _():
                fetch_wide(t + 1).start()

            @pl.when(h == 0)
            def _():
                accs[0][...] = dot(lhs[...], rhs[t % 2])

            @pl.when(h == AXES)
            def _():
                emptied(0)

            @pl.when(h == SIDE)
            def _():
                emptied(1)

            for odd in range(2):

                @pl.when((h > 0) & (h % 2 == odd))
                def _():
                    accs[odd][...] = dot(lhs[...], rhs[t % 2])
                    arrange(m, h - 1, 1 - odd)

            @pl.when(h == SIDE)
            def _():
                emptied(0)
                arrange(m, h, 0)

        @pl.when((m < MATRICES) & (kind == 2) & (h < SIDE))
        def _():
            t = SIDE * l + h

            @pl.when(h == 0)
            def _():
                fetch_deep(l).wait()

                @pl.when(l == 0)
                def _():
                    fetch_tall(1).start()

            fetch_turned(t).wait()

            @pl.when(t < 7)
            def _():
                fetch_turned(t + 1).start()

            acc2[...] = dot(zs[t % 2], dh[...])

            @pl.when(h > 0)
            def _():
                put2(m, h).wait()

            down_block(acc2, stage2)
            put2(m, h).start()

        @pl.when((h == 0) & (m > 2))
        def _():
            on_third(m - AXES)

        @pl.when((h == 2) & (m > 1))
        def _():
            on_second_a(m - 2)

        @pl.when((h == SIDE) & (m > 1))
        def _():
            on_second_f(m - 2)

        @pl.when((h == SIDE) & launched)
        def _():
            whole(own.at[:, 1], load.at[1])
            for j in range(2):
                on_first_f(m - 1, j)

        @pl.when((h == 0) & (m > 1))
        def _():
            for j in range(2, SIDE):
                on_first_f(m - 2, j)

        @pl.when(((h == 1) | (h == 2)) & launched)
        def _():
            @pl.when(h == 1)
            def _():
                whole(own.at[:, 0], load.at[0])

            lax.fori_loop(h - 1, AXES * h - 2, lambda j, _: (on_first_a(m - 1, j), 0)[1], 0)

        @pl.when((h == 0) & launched)
        def _():
            load_own(m - 1)

        return 0

    lax.fori_loop(0, (MATRICES + 2) * TILES, tile, 0)
    own_rows(ws, windows, owns, window_sem)
    on_third(MATRICES - 1)

    total = jnp.zeros((SUBLANES, LANES), F32)
    for m in range(MATRICES):
        g = out[m].astype(F32)
        total = total + jnp.sum((g * g).reshape(-1, SUBLANES, LANES), axis=0)
    squares[...] = norm_exchange(at, sums, send4, recv4, total)
    for k, buffer in enumerate((ra, rf, qa, qf, r3)):
        whole(buffer, sent.at[k])


def gradients(tall, wide, turned, deep, weights):
    g, squares, _, *owns = pl.pallas_call(
        gradients_kernel,
        out_shape=(
            pltpu.VMEM((MATRICES, BLOCK, LANES), BF16),
            pltpu.VMEM((SUBLANES, LANES), F32),
            jax.ShapeDtypeStruct((MATRICES, SIDE, SIDE, SIDE, BLOCK, LANES), BF16),
            *[pltpu.VMEM((LAYERS, w.shape[1] // DEVICES, w.shape[2]), F32) for w in weights],
        ),
        in_specs=[HBM] * (4 + AXES),
        out_specs=(VMEM, VMEM, HBM, *[VMEM] * AXES),
        scratch_shapes=[
            pltpu.VMEM((D, TOKENS), BF16),
            pltpu.VMEM((2, TOKENS, TILE), BF16),
            pltpu.VMEM((2, PLANE_ROWS, TOKENS), BF16),
            pltpu.VMEM((TOKENS, D), BF16),
            *[pltpu.VMEM((D, TILE), F32)] * 2,
            pltpu.VMEM((PLANE_ROWS, D), F32),
            *[pltpu.VMEM((SIDE, SIDE, SIDE, PIECE, LANES), BF16)] * 2,
            pltpu.VMEM((SIDE, SIDE, BLOCK, LANES), BF16),
            pltpu.VMEM((SIDE, SIDE, PIECE, LANES), F32),
            pltpu.VMEM((WAYS, MATRICES, SIDE, SIDE, PART, LANES), BF16),
            pltpu.VMEM((WAYS, MATRICES, 2, SIDE, SIDE, PART, LANES), BF16),
            pltpu.VMEM((WAYS, MATRICES, SIDE, PART, LANES), BF16),
            pltpu.VMEM((WAYS, MATRICES, 2, SIDE, PART, LANES), BF16),
            pltpu.VMEM((WAYS, MATRICES, STEPS, PART, LANES), BF16),
            pltpu.VMEM((WAYS, 2, SIDE, SIDE, PART, LANES), BF16),
            pltpu.VMEM((WAYS, 2, SIDE, PART, LANES), F32),
            pltpu.VMEM((WAYS, SIDE, PART, LANES), F32),
            pltpu.VMEM((PLANE + SIDE, SUBLANES, LANES), F32),
            *[pltpu.VMEM((LAYERS, w.shape[1] // n, w.shape[2]), BF16) for w, n in zip(weights, (PLANE, PLANE, DEVICES), strict=True)],
            DMA((AXES,)),
            *[DMA((2,))] * AXES, DMA((AXES,)),
            DMA((TILES,)),
            *[DMA((MATRICES, SIDE))] * 2, *[DMA((MATRICES,))] * 3,
            DMA((2,)),
            DMA((2,)), DMA((2,)),
        ],
        compiler_params=pltpu.CompilerParams(collective_id=0, has_side_effects=True, vmem_limit_bytes=MOST_VMEM - SPARE_VMEM),
        name="gradients",
    )(tall, wide, turned, deep, *weights)
    return g, squares, owns


def solution(mesh):
    rep, dp = mesh.axis_names

    def step(x, dy, *arrays):
        weights, m, v = (arrays[i : i + 3] for i in (0, 3, 6))
        g, total, owns = gradients(*by_rows(x[0], dy[0], weights), weights)
        new, new_m, new_v = adam(MATRICES * D * FF, g, total, owns, m, v)
        return (*natural(all_gather(new)), *new_m, *new_v)

    whole, rows, sequences = P(), P(None, dp), P((rep, dp))
    return jax.shard_map(
        step,
        mesh=mesh,
        in_specs=(sequences, sequences, *[whole] * AXES, *[rows] * MATRICES),
        out_specs=(*[P(rep)] * AXES, *[P(rep, dp)] * MATRICES),
        check_vma=False,
    )
```

```python
import functools
import jax
import jax.numpy as jnp
from jax import lax
from jax.experimental import pallas as pl
from jax.experimental.pallas import tpu as pltpu
from jax.sharding import PartitionSpec as P

MESH = pl.DeviceIdType.MESH
WAYS, AXES, SIDE = 6, 3, 4
STEPS = SIDE - 1
MATRICES, LAYERS, DEVICES, PLANE = 6, 2, 64, 16
LANES, SUBLANES, BLOCK = 128, 8, 280
BF16, F32 = jnp.bfloat16, jnp.float32
HBM, VMEM = pl.BlockSpec(memory_space=pl.ANY), pl.BlockSpec(memory_space=pltpu.VMEM)
DMA = pltpu.SemaphoreType.DMA
MIB = 1 << 20
MOST_VMEM, SPARE_VMEM = 62 * MIB, 2 * MIB
ORDERS = tuple(tuple((way // 2 + i) % AXES for i in range(AXES)) for way in range(WAYS))
SIGNS = (1, -1) * AXES
TAKEN = (3, 0, 4, 1, 5, 2)


def place():
    me = lax.axis_index("dp")
    return (me // PLANE, me // SIDE % SIDE, me % SIDE)


def wrap(i):
    return (i + 3 * SIDE) % SIDE


def neighbour(at, axis, step):
    there = [c for c in at]
    there[axis] = wrap(at[axis] + step)
    return {"dp": (there[0] * SIDE + there[1]) * SIDE + there[2]}


def remote(src, dst, send, recv, to):
    return pltpu.make_async_remote_copy(src_ref=src, dst_ref=dst, send_sem=send, recv_sem=recv, device_id=to, device_id_type=MESH)


def moved(at, steps):
    x, y, z = (wrap(a + step) for a, step in zip(at, steps, strict=True))
    return {"dp": (x * SIDE + y) * SIDE + z}


LINES = tuple(tuple(k * (axis == line) for axis in range(AXES)) for line in range(AXES) for k in range(1, SIDE))
PLANE_PEERS = tuple((0, k // SIDE, k % SIDE) for k in range(1, PLANE))
LINE_PEERS = LINES[:STEPS]
NEIGHBOURS = tuple(steps for steps in LINES if 2 not in steps)


def enter(at, peers):
    barrier = pltpu.get_barrier_semaphore()
    for steps in peers:
        pl.semaphore_signal(barrier, inc=1, device_id=moved(at, steps), device_id_type=MESH)
    pl.semaphore_wait(barrier, len(peers))


def norm_exchange(at, buf, send, recv, total):
    first = 0
    for stage, peers in enumerate((PLANE_PEERS, LINE_PEERS)):
        own, others = buf.at[first], buf.at[pl.ds(first + 1, len(peers))]
        own[...] = total
        for k, steps in enumerate(peers):
            remote(own, others.at[k], send.at[stage], recv.at[stage], moved(at, steps)).start()
        pltpu.make_async_copy(others, others, recv.at[stage]).wait()
        total = total + jnp.sum(others[...], axis=0)
        pltpu.make_async_copy(others, others, send.at[stage]).wait()
        first += 1 + len(peers)
    return total


def passed_on(seen, c, phase, key):
    d1, d2, d3 = key
    if phase == 0 and d3 < STEPS:
        yield 0, (0, 0, d3 + 1)
    if phase < 2 and d2 < STEPS:
        yield 1, (0, d2 + 1, d3)
    if phase == 1 and d2 > 0:
        seen.append((c, d2))
        if seen.count((c, d2)) < SIDE:
            return
        d3 = None
    if d1 < STEPS:
        yield 2, (d1 + 1, d2, d3)


def ag_order(latency=2):
    import heapq

    free, out, seen, heap = {}, [], [], []

    def hold(t, c, phase, key):
        for phase, key in passed_on(seen, c, phase, key):
            link = ORDERS[c][2 - phase]
            size = SIDE if key[2] is None else 1
            free[link] = max(t, free.get(link, 0)) + size
            heapq.heappush(heap, (free[link] + latency, len(out) * WAYS + len(heap), c, phase, key))

    for c in range(0, WAYS, 2):
        hold(0, c, 0, (0, 0, 0))
    while heap:
        t, _, *arrival = heapq.heappop(heap)
        out.append(arrival)
        hold(t, *arrival)
    return out


def ag_kernel(*refs):
    mine, outs, (sends, recv1, recv2, recv3, recv4, local) = refs[0], refs[1 : 1 + WAYS], refs[1 + WAYS :]
    at = place()
    enter(at, NEIGHBOURS)

    def where(c, key):
        index = [None] * AXES
        for axis, d in zip(ORDERS[c], key, strict=True):
            index[axis] = slice(None) if d is None else wrap(at[axis] - SIGNS[c] * d)
        return outs[c].at[tuple(index)]

    def arrived(c, phase, key):
        d1, d2, d3 = key
        if phase == 0:
            return recv1.at[c // 2, d3 - 1]
        if phase == 1:
            return recv2.at[c // 2, d2 - 1, d3]
        if d3 is not None:
            return recv3.at[c // 2, d1 - 1, d3]
        return recv4.at[c // 2, d1 - 1, d2 - 1]

    def send_on(c, phase, key):
        d1, d2, d3 = key
        back = list(key)
        back[2 - phase] -= 1
        there = where(c, back)
        src = there if any(d != 0 for d in back) else mine.at[c]
        remote(src, there, sends.at[c, phase], arrived(c, phase, key), neighbour(at, ORDERS[c][2 - phase], SIGNS[c])).start()

    seen = []

    def hold(*held):
        for phase, key in passed_on(seen, *held):
            send_on(held[0], phase, key)

    own = [pltpu.make_async_copy(mine.at[c], where(c, (0, 0, 0)), local.at[c]) for c in range(WAYS)]
    for c in range(WAYS):
        hold(c, 0, (0, 0, 0))
    for copied in own:
        copied.start()
    for even, phase, key in ag_order():
        two = outs[even].at[0, pl.ds(0, 2)] if key[2] is None else outs[even].at[0, 0, pl.ds(0, 2)]
        pltpu.make_async_copy(two, two, arrived(even, phase, key)).wait()
        for c in (even, even + 1):
            hold(c, phase, key)
    for c in range(WAYS):
        own[c].wait()
        sent = outs[c].at[pl.ds(0, STEPS)]
        for phase in (2, 1, 0):
            pltpu.make_async_copy(sent, sent, sends.at[c, phase]).wait()
            sent = outs[c].at[(0,) * (AXES - phase) + (pl.ds(0, STEPS),)]


def all_gather(mine):
    return pl.pallas_call(
        ag_kernel,
        out_shape=(pltpu.VMEM((SIDE, SIDE, SIDE, *mine.shape[1:]), BF16),) * WAYS,
        in_specs=[VMEM],
        out_specs=(VMEM,) * WAYS,
        scratch_shapes=[DMA((WAYS, AXES)), DMA((AXES, STEPS)), *[DMA((AXES, STEPS, SIDE))] * 2, DMA((AXES, STEPS, STEPS)), DMA((WAYS,))],
        compiler_params=pltpu.CompilerParams(collective_id=1, has_side_effects=True, vmem_limit_bytes=MOST_VMEM // SUBLANES),
        name="gather",
    )(mine)


def tiles_of(t, rows, columns):
    n = columns // LANES
    if t < 2:
        return [(0, rows, j * LANES, j * rows) for j in range(n)]
    return [(8 * i, 8, j * LANES, (i * n + j) * 8) for i in range(rows // 8) for j in range(n)]


def adam_kernel(count, g, total, *refs):
    ws, ms, vs = (refs[AXES * k : AXES * (k + 1)] for k in range(3))
    new, *refs = refs[3 * AXES :]
    *moments, wide_g, wide_w = refs
    new_m, new_v = moments[:AXES], moments[AXES:]
    factor = jnp.minimum(1.0, 0.5 * lax.rsqrt(jnp.full((1, 1), jnp.sum(total[...])) / count + 1e-30))
    for t in range(AXES):
        rows, columns = ws[t].shape[1:]
        for l in range(LAYERS):
            wide_g[...] = g[TAKEN[LAYERS * t + l]].astype(F32) * factor
            for row, n, column, at in tiles_of(t, rows, columns):
                lanes = pl.ds(column, LANES)
                here = (slice(None), l, lanes) if t < 2 else (l, pl.ds(row, n), lanes)
                grad = wide_g[pl.ds(at, n), :]
                m = 0.9 * ms[t][here] + 0.1 * grad
                v = 0.95 * vs[t][here] + 0.05 * grad * grad
                w = ws[t][l, pl.ds(row, n), lanes]
                new_m[t][here] = m
                new_v[t][here] = v
                wide_w[pl.ds(at, n), :] = w - 0.02 * (m * lax.rsqrt(v + 1e-8) + 0.1 * w)
            new[LAYERS * t + l] = wide_w[...].astype(BF16)


def adam(count, g, total, ws, ms, vs):
    ms, vs = ([*(jnp.swapaxes(a, 0, 1) for a in arrays[:2]), arrays[2]] for arrays in (ms, vs))
    like = [jax.ShapeDtypeStruct(m.shape, F32) for m in ms]
    new, *moments = pl.pallas_call(
        functools.partial(adam_kernel, count),
        out_shape=(pltpu.VMEM(g.shape, BF16), *like, *like),
        in_specs=[VMEM] * (2 + AXES * 3),
        out_specs=(VMEM,) * (1 + AXES * 2),
        scratch_shapes=[pltpu.VMEM(g.shape[1:], F32)] * 2,
        compiler_params=pltpu.CompilerParams(vmem_limit_bytes=MOST_VMEM // SIDE),
        name="adam",
    )(g, total, *ws, *ms, *vs)
    return new, *([*(jnp.swapaxes(a, 0, 1) for a in part[:2]), part[2]] for part in (moments[:AXES], moments[AXES:]))


def natural_kernel(*refs):
    gathered, outs, wide = refs[:MATRICES], refs[MATRICES:-AXES], refs[-AXES:]
    first = pl.program_id(0) * SUBLANES
    for t in range(AXES):
        for l in range(LAYERS):
            rows, columns = outs[t].shape[1:]
            for k in range(SUBLANES):
                block = gathered[LAYERS * t + l][first + k].astype(F32)
                for row, n, column, at in tiles_of(t, rows // SUBLANES, columns):
                    wide[t][pl.ds(k * rows // SUBLANES + row, n), pl.ds(column, LANES)] = block[at : at + n]
            outs[t][l] = wide[t][...].astype(BF16)


def natural(gathered):
    shapes = (GATE, GATE, DOWN)
    return pl.pallas_call(
        natural_kernel,
        grid=(SUBLANES,),
        out_shape=tuple(jax.ShapeDtypeStruct((LAYERS, *s), BF16) for s in shapes),
        in_specs=[VMEM] * MATRICES,
        out_specs=tuple(pl.BlockSpec((LAYERS, s[0] // SUBLANES, s[1]), lambda i: (0, i, 0)) for s in shapes),
        scratch_shapes=[pltpu.VMEM((s[0] // SUBLANES, s[1]), F32) for s in shapes],
        compiler_params=pltpu.CompilerParams(vmem_limit_bytes=MOST_VMEM // SIDE),
        name="natural",
    )(*[g.reshape(DEVICES, BLOCK, LANES) for g in gathered])


D, FF, TOKENS = 896, 2560, 2048
GATE, DOWN = (D, FF), (FF, D)
ROWS, CHUNK, TILE = 256, 256, 512
TALL, WIDE, TURNED, DEEP = range(4)
SOON, AHEAD, NEXT = 4, 6, 8
TILES, PIECE, PLANE_ROWS = FF // TILE, BLOCK * TILE // FF, FF // SIDE
NT = (((1,), (1,)), ((), ()))


def dot(a, b):
    return jnp.dot(a, b, preferred_element_type=F32)


def dot_t(a, b):
    return lax.dot_general(a, b, NT, preferred_element_type=F32)


def scale_of(wide):
    return lax.rsqrt(jnp.mean(wide * wide, -1, keepdims=True) + 1e-6)


def rows_kernel(x_hbm, dy_hbm, *refs):
    hbm, results, weights, rest = refs[:3], refs[3:7], refs[7:13], refs[13:]
    buffers, (xs, dys, g0, u0, z0, dz1, sems, part_sems, in_sems, out_sems) = rest[:4], rest[4:]
    wg0, wu0, wd0, wg1, wu1, wd1 = weights
    i, slot = pl.program_id(0), pl.program_id(0) % 2
    first, blocks = i == 0, pl.num_programs(0)
    chunks = [pl.ds(j * CHUNK, CHUNK) for j in range(FF // CHUNK)]

    def fetch(k):
        return pltpu.make_async_copy(hbm[k % 3].at[k // 3], weights[k], sems.at[k])

    def fetch_part(k, j):
        return pltpu.make_async_copy(hbm[k].at[0, :, chunks[j]], weights[k].at[:, chunks[j]], part_sems.at[k, j])

    def take(source, there, i):
        rows = pl.ds(pl.multiple_of(i * ROWS, ROWS), ROWS)
        slot = i % there.shape[0]
        return pltpu.make_async_copy(source.at[rows], there.at[slot], in_sems.at[there.shape[0] - 2, slot])

    def put(k, part, slot=slot):
        rows = pl.ds(pl.multiple_of(i * ROWS, ROWS), ROWS)
        there = results[k].at[part, rows] if k % 2 else results[k].at[part, :, rows]
        return pltpu.make_async_copy(buffers[k].at[slot, part], there, out_sems.at[slot, k, part])

    def outs(slot):
        return [put(k, part, slot) for k, result in enumerate(results) for part in range(result.shape[0])]

    @pl.when(first)
    def _():
        take(x_hbm, xs, 0).start()
        take(dy_hbm, dys, 0).start()
        for j in range(len(chunks)):
            for k in range(2):
                fetch_part(k, j).start()
        take(dy_hbm, dys, 1).start()
        take(dy_hbm, dys, 0).wait()

    take(x_hbm, xs, i).wait()

    @pl.when(i + 1 < blocks)
    def _():
        take(x_hbm, xs, i + 1).start()
        take(dy_hbm, dys, i + 1).wait()

    @pl.when(i + 2 < blocks)
    def _():
        take(dy_hbm, dys, i + 2).start()

    @pl.when(i > 1)
    def _():
        for copy in outs(slot):
            copy.wait()

    tall, wide, turned, deep = (b.at[slot] for b in buffers)
    x, dy, next_dy = xs.at[slot], dys.at[i % AXES], dys.at[(i + 1) % AXES]

    def make_dz1(dy, some):
        for ch in some:
            dz1[:, ch] = dot_t(dy[...], wd1[ch, :]).astype(BF16)

    def forward(coming):
        a = (x[...].astype(F32) * scale_of(x[...].astype(F32))).astype(BF16)
        tall[1] = a.T
        deep[0] = dy[...]
        for j, ch in enumerate(chunks):
            if coming:
                for k in range(2):
                    fetch_part(k, j).wait()
                if 0 < j < 5:
                    fetch(j + 1).start()
            gate, up = dot(a, wg0[:, ch]), dot(a, wu0[:, ch])
            g0[:, ch], u0[:, ch] = gate, up
            z0[:, ch] = (gate * jax.nn.sigmoid(gate) * up).astype(BF16)
            turned[1, ch, :] = z0[:, ch].T

    @pl.when(first)
    def _():
        forward(True)
        for k in range(2, MATRICES):
            fetch(k).wait()
        make_dz1(dy, chunks[:AHEAD])

    @pl.when(i > 0)
    def _():
        forward(False)

    for k, part in ((TALL, 1), (DEEP, 0), (TURNED, 1)):
        put(k, part).start()
    make_dz1(dy, chunks[AHEAD:NEXT])
    h = x[...] + dot(z0[...], wd0[...]).astype(BF16)
    make_dz1(dy, chunks[NEXT:])
    h = h.astype(F32)
    scale = scale_of(h)
    a = (h * scale).astype(BF16)
    tall[0] = a.T
    put(TALL, 0).start()
    for ch in chunks:
        gate, up = dot(a, wg1[:, ch]), dot(a, wu1[:, ch])
        dz = dz1[:, ch].astype(F32)
        s = jax.nn.sigmoid(gate)
        silu = gate * s
        turned[0, ch, :] = (silu * up).astype(BF16).T
        wide[1, :, ch] = (dz * silu).astype(BF16)
        wide[0, :, ch] = (dz * up * (s + silu * (1 - s))).astype(BF16)
    for k, part in ((TURNED, 0), (WIDE, 0), (WIDE, 1)):
        put(k, part).start()
    da_gate, da_up = dot_t(wg1[...], wide[0]), dot_t(wu1[...], wide[1])
    make_dz1(next_dy, chunks[:SOON])
    da = (da_gate.astype(BF16) + da_up.astype(BF16)).T.astype(F32)
    dwide = scale * (da - h * (scale * scale * jnp.mean(da * h, -1, keepdims=True)))
    dh = dy[...] + dwide.astype(BF16)
    deep[1] = dh
    put(DEEP, 1).start()
    for ch in chunks:
        dz = dot_t(dh, wd0[ch, :]).astype(BF16).astype(F32)
        gate, up = g0[:, ch], u0[:, ch]
        s = jax.nn.sigmoid(gate)
        silu = gate * s
        wide[3, :, ch] = (dz * silu).astype(BF16)
        wide[2, :, ch] = (dz * up * (s + silu * (1 - s))).astype(BF16)
    make_dz1(next_dy, chunks[SOON:AHEAD])
    put(WIDE, 2).start()
    put(WIDE, 3).start()

    @pl.when(i + 1 == blocks)
    def _():
        for copy in outs(slot) + outs(1 - slot):
            copy.wait()


def by_rows(x, dy, weights):
    shapes = ((2, D, TOKENS), (4, TOKENS, FF), (2, FF, TOKENS), (2, TOKENS, D))
    buffers = ((2, D, ROWS), (4, ROWS, FF), (2, FF, ROWS), (2, ROWS, D))
    return pl.pallas_call(
        rows_kernel,
        grid=(TOKENS // ROWS,),
        out_shape=tuple(jax.ShapeDtypeStruct(s, BF16) for s in shapes),
        in_specs=[HBM] * 5,
        out_specs=(HBM,) * 4,
        scratch_shapes=[
            *[pltpu.VMEM(w.shape[1:], BF16) for w in weights * 2],
            *[pltpu.VMEM((2, *b), BF16) for b in buffers],
            *[pltpu.VMEM((n, ROWS, D), BF16) for n in (2, AXES)],
            *[pltpu.VMEM((ROWS, FF), F32)] * 2,
            *[pltpu.VMEM((ROWS, FF), BF16)] * 2,
            DMA((MATRICES,)), DMA((2, FF // CHUNK)), DMA((2, AXES)), DMA((2, 4, 4)),
        ],
        compiler_params=pltpu.CompilerParams(vmem_limit_bytes=MOST_VMEM),
        name="rows",
    )(x, dy, *weights)


GATE_ROWS, DOWN_ROWS = D // DEVICES, FF // DEVICES
STARTS = (0, 48, 96, 144, 192, 232)
PART = 48


def gate_block(acc, stage, wide):
    for i in range(PLANE):
        part = wide.at[i % wide.shape[0]]
        for c in range(SIDE):
            piece = acc[pl.ds(i * PIECE, PIECE), pl.ds(c * LANES, LANES)]
            for z in range(SIDE):
                part[z, pl.ds(GATE_ROWS * c, GATE_ROWS), :] = piece[GATE_ROWS * z : GATE_ROWS * (z + 1)]
        for z in range(SIDE):
            stage[i // SIDE, i % SIDE, z] = part[z].astype(BF16)


def down_block(acc, stage):
    def group(i, _):
        for t in range(DOWN_ROWS // SUBLANES):
            rows = acc[pl.ds(pl.multiple_of(i * DOWN_ROWS, SUBLANES) + SUBLANES * t, SUBLANES), :]
            piece = jnp.concatenate([rows[:, c * LANES : (c + 1) * LANES] for c in range(D // LANES)], 0)
            stage[i // SIDE, i % SIDE, pl.ds(PIECE * t, PIECE)] = piece.astype(BF16)
        return 0

    lax.fori_loop(0, PLANE, group, 0)


def own_rows(ws, windows, owns, sems):
    me = lax.axis_index("dp")
    taken = []
    for t in range(AXES):
        rows = windows[t].shape[1]
        first = pl.multiple_of((me // SIDE if t < 2 else me) * rows, SUBLANES)
        taken.append(pltpu.make_async_copy(ws[t].at[:, pl.ds(first, rows)], windows[t], sems.at[t]))
        taken[t].start()
    for t in range(AXES):
        taken[t].wait()
        rows = owns[t].shape[1]
        if t == 2:
            owns[t][...] = windows[t][...].astype(F32)
        for z in range(SIDE if t < 2 else 0):

            @pl.when(me % SIDE == z)
            def _():
                for l in range(LAYERS):
                    owns[t][l] = windows[t][l].astype(F32)[z * rows : (z + 1) * rows]


def gradients_kernel(*refs):
    (tall, wide, turned, deep), ws, (out, squares, terms), owns, scratch = refs[:4], refs[4:7], refs[7:10], refs[10:13], refs[13:]
    (lhs, rhs, zs, dh, acc_a, acc_b, acc2, stage_a, stage_b, stage2, shift, ra, rf, qa, qf, r3, own, f1, f2, sums) = scratch[:20]
    accs, stages = (acc_a, acc_b), (stage_a, stage_b)
    *windows, window_sem = scratch[20:24]
    (in_sem, rhs_sem, zs_sem, put_sem, sent, first_a, first_f, second_a, second_f, recv3, load, send4, recv4) = scratch[24:]
    at = place()

    def fetch_tall(l):
        return pltpu.make_async_copy(tall.at[l], lhs, in_sem.at[0])

    def fetch_deep(l):
        return pltpu.make_async_copy(deep.at[l], dh, in_sem.at[1])

    def fetch_wide(t):
        columns = pl.ds(pl.multiple_of(t % TILES * TILE, TILE), TILE)
        return pltpu.make_async_copy(wide.at[t // TILES, :, columns], rhs.at[t % 2], rhs_sem.at[t % 2])

    def fetch_turned(t):
        rows = pl.ds(pl.multiple_of(t % SIDE * PLANE_ROWS, LANES), PLANE_ROWS)
        return pltpu.make_async_copy(turned.at[t // SIDE, rows], zs.at[t % 2], zs_sem.at[t % 2])

    def arrange(m, h, odd):
        rows = pl.ds(pl.multiple_of(PIECE * h, SUBLANES), PIECE)
        gate_block(accs[odd], stages[odd], shift)
        pltpu.make_async_copy(stages[odd], terms.at[m, :, :, :, rows], put_sem.at[odd]).start()

    def emptied(odd):
        whole(stages[odd], put_sem.at[odd])

    def put2(m, h):
        return pltpu.make_async_copy(stage2, terms.at[m, h], put_sem.at[2])

    fetch_tall(0).start()
    fetch_wide(0).start()
    fetch_deep(0).start()
    fetch_turned(0).start()
    enter(at, sorted({*LINES, *PLANE_PEERS}))

    def split(c):
        o, s = ORDERS[c], SIGNS[c]
        return o, s, at[o[0]], at[o[1]], at[o[2]]

    def block(m, c, a, i):
        o = ORDERS[c]
        index = [slice(None)] * 3
        index[o[0]] = a
        if i is not None:
            index[o[1]] = i
        return terms.at[(m, *index, pl.ds(STARTS[c], PART))]

    def piece(c, j):
        return wrap(split(c)[3] + SIGNS[c] * (2 + j - j // 2 * (2 * j - 1)))

    def along(c, axis, src, there, sem, recv, steps=1):
        return remote(src, there, sent.at[sem], recv, neighbour(at, ORDERS[c][axis], SIGNS[c] * steps))

    def launch(m):
        for j in range(SIDE):
            for c in range(WAYS):
                src = block(m, c, wrap(split(c)[2] + 2 * SIGNS[c]), piece(c, j))
                along(c, 0, src, ra.at[c, m, j], 0, first_a.at[m, j]).start()
        for j in range(SIDE):
            for c in range(WAYS):
                src = block(m, c, wrap(split(c)[2] - SIGNS[c]), piece(c, j))
                along(c, 0, src, rf.at[c, m, 1, j], 1, first_f.at[m, j], -1).start()

    def load_own(m):
        for k in range(2):
            for c in range(WAYS):
                mine = block(m, c, wrap(split(c)[2] + SIGNS[c] * (1 - k)), None)
                pltpu.make_async_copy(mine, own.at[c, k], load.at[k]).start()

    def whole(ref, sem):
        pltpu.make_async_copy(ref, ref, sem).wait()

    def term(c, k, j):
        i = piece(c, j)
        mine = own[c, k, i] if ORDERS[c][1] < ORDERS[c][2] else own[c, k, :, i]
        return mine.astype(F32)

    def on_first_a(m, j):
        whole(ra.at[:, m, j], first_a.at[m, j])
        for c in range(WAYS):
            ra[c, m, j] = (ra[c, m, j].astype(F32) + term(c, 0, j)).astype(BF16)
            along(c, 0, ra.at[c, m, j], rf.at[c, m, 0, j], 1, first_f.at[m, j]).start()

    def on_first_f(m, j):
        whole(rf.at[:, m, :, j], first_f.at[m, j])
        for c in range(WAYS):
            total = rf[c, m, 0, j].astype(F32) + rf[c, m, 1, j].astype(F32) + term(c, 1, j)
            if j < 2:
                rf[c, m, 1, j] = total.astype(BF16)
            else:
                f1[c, j - 2] = total
            if j == 0:
                along(c, 1, rf.at[c, m, 1, j], qa.at[c, m], 2, second_a.at[m]).start()
            if j == 1:
                along(c, 1, rf.at[c, m, 1, j], qf.at[c, m, 1], 3, second_f.at[m], -1).start()

    def on_second_a(m):
        whole(qa.at[:, m], second_a.at[m])
        for c in range(WAYS):
            qa[c, m] = (qa[c, m].astype(F32) + f1[c, 0]).astype(BF16)
            along(c, 1, qa.at[c, m], qf.at[c, m, 0], 3, second_f.at[m]).start()

    def third(m, c, k):
        src = qf.at[c, m, 1, wrap(split(c)[4] + k + 1)]
        return remote(src, r3.at[c, m, k], sent.at[4], recv3.at[m], neighbour(at, ORDERS[c][2], k + 1))

    def on_second_f(m):
        whole(qf.at[:, m], second_f.at[m])
        for c in range(WAYS):
            total = qf[c, m, 0].astype(F32) + qf[c, m, 1].astype(F32) + f1[c, 1]
            f2[c] = total
            qf[c, m, 1] = total.astype(BF16)
            for k in range(STEPS):
                third(m, c, k).start()

    def on_third(m):
        whole(r3.at[:, m], recv3.at[m])
        for c in range(WAYS):
            o, s, p1, p2, p3 = split(c)
            total = f2[c, p3]
            for k in range(STEPS):
                total = total + r3[c, m, k].astype(F32)
            out[m, pl.ds(STARTS[c], PART)] = total.astype(BF16)

    def tile(i, _):
        m, h = i // TILES, i % TILES
        kind, l = m % AXES, m // AXES
        launched = (m > 0) & (m < MATRICES + 1)

        @pl.when((h == 0) & launched)
        def _():
            @pl.when(kind > 0)
            def _():
                for odd in range(2):
                    emptied(odd)

            @pl.when(kind == 0)
            def _():
                put2(0, 0).wait()

            launch(m - 1)

        @pl.when((m < MATRICES) & (kind < 2))
        def _():
            t = (2 * l + kind) * TILES + h

            @pl.when((kind == 0) & (h == 0))
            def _():
                fetch_tall(l).wait()

                @pl.when(l == 1)
                def _():
                    fetch_deep(1).start()

            fetch_wide(t).wait()

            @pl.when(t < 19)
            def _():
                fetch_wide(t + 1).start()

            @pl.when(h == 0)
            def _():
                accs[0][...] = dot(lhs[...], rhs[t % 2])

            @pl.when(h == AXES)
            def _():
                emptied(0)

            @pl.when(h == SIDE)
            def _():
                emptied(1)

            for odd in range(2):

                @pl.when((h > 0) & (h % 2 == odd))
                def _():
                    accs[odd][...] = dot(lhs[...], rhs[t % 2])
                    arrange(m, h - 1, 1 - odd)

            @pl.when(h == SIDE)
            def _():
                emptied(0)
                arrange(m, h, 0)

        @pl.when((m < MATRICES) & (kind == 2) & (h < SIDE))
        def _():
            t = SIDE * l + h

            @pl.when(h == 0)
            def _():
                fetch_deep(l).wait()

                @pl.when(l == 0)
                def _():
                    fetch_tall(1).start()

            fetch_turned(t).wait()

            @pl.when(t < 7)
            def _():
                fetch_turned(t + 1).start()

            acc2[...] = dot(zs[t % 2], dh[...])

            @pl.when(h > 0)
            def _():
                put2(m, h).wait()

            down_block(acc2, stage2)
            put2(m, h).start()

        @pl.when((h == 1) & (m > 2))
        def _():
            on_third(m - AXES)

        @pl.when((h == 1) & (m > 1))
        def _():
            on_second_a(m - 2)

        @pl.when((h == SIDE) & (m > 1))
        def _():
            on_second_f(m - 2)

        @pl.when((h == SIDE) & launched)
        def _():
            whole(own.at[:, 1], load.at[1])
            on_first_f(m - 1, 0)

        @pl.when((h == 0) & (m > 1))
        def _():
            for j in range(1, SIDE):
                on_first_f(m - 2, j)

        @pl.when(((h == 1) | (h == 2)) & launched)
        def _():
            @pl.when(h == 1)
            def _():
                whole(own.at[:, 0], load.at[0])

            lax.fori_loop(h - 1, AXES * h - 2, lambda j, _: (on_first_a(m - 1, j), 0)[1], 0)

        @pl.when((h == 0) & launched)
        def _():
            load_own(m - 1)

        return 0

    lax.fori_loop(0, (MATRICES + 2) * TILES, tile, 0)
    own_rows(ws, windows, owns, window_sem)
    on_third(MATRICES - 1)

    total = jnp.zeros((SUBLANES, LANES), F32)
    for m in range(MATRICES):
        g = out[m].astype(F32)
        total = total + jnp.sum((g * g).reshape(-1, SUBLANES, LANES), axis=0)
    squares[...] = norm_exchange(at, sums, send4, recv4, total)
    for k, buffer in enumerate((ra, rf, qa, qf, r3)):
        whole(buffer, sent.at[k])


def gradients(tall, wide, turned, deep, weights):
    g, squares, _, *owns = pl.pallas_call(
        gradients_kernel,
        out_shape=(
            pltpu.VMEM((MATRICES, BLOCK, LANES), BF16),
            pltpu.VMEM((SUBLANES, LANES), F32),
            jax.ShapeDtypeStruct((MATRICES, SIDE, SIDE, SIDE, BLOCK, LANES), BF16),
            *[pltpu.VMEM((LAYERS, w.shape[1] // DEVICES, w.shape[2]), F32) for w in weights],
        ),
        in_specs=[HBM] * (4 + AXES),
        out_specs=(VMEM, VMEM, HBM, *[VMEM] * AXES),
        scratch_shapes=[
            pltpu.VMEM((D, TOKENS), BF16),
            pltpu.VMEM((2, TOKENS, TILE), BF16),
            pltpu.VMEM((2, PLANE_ROWS, TOKENS), BF16),
            pltpu.VMEM((TOKENS, D), BF16),
            *[pltpu.VMEM((D, TILE), F32)] * 2,
            pltpu.VMEM((PLANE_ROWS, D), F32),
            *[pltpu.VMEM((SIDE, SIDE, SIDE, PIECE, LANES), BF16)] * 2,
            pltpu.VMEM((SIDE, SIDE, BLOCK, LANES), BF16),
            pltpu.VMEM((SIDE, SIDE, PIECE, LANES), F32),
            pltpu.VMEM((WAYS, MATRICES, SIDE, SIDE, PART, LANES), BF16),
            pltpu.VMEM((WAYS, MATRICES, 2, SIDE, SIDE, PART, LANES), BF16),
            pltpu.VMEM((WAYS, MATRICES, SIDE, PART, LANES), BF16),
            pltpu.VMEM((WAYS, MATRICES, 2, SIDE, PART, LANES), BF16),
            pltpu.VMEM((WAYS, MATRICES, STEPS, PART, LANES), BF16),
            pltpu.VMEM((WAYS, 2, SIDE, SIDE, PART, LANES), BF16),
            pltpu.VMEM((WAYS, 2, SIDE, PART, LANES), F32),
            pltpu.VMEM((WAYS, SIDE, PART, LANES), F32),
            pltpu.VMEM((PLANE + SIDE, SUBLANES, LANES), F32),
            *[pltpu.VMEM((LAYERS, w.shape[1] // n, w.shape[2]), BF16) for w, n in zip(weights, (PLANE, PLANE, DEVICES), strict=True)],
            DMA((AXES,)),
            *[DMA((2,))] * AXES, DMA((AXES,)),
            DMA((TILES,)),
            *[DMA((MATRICES, SIDE))] * 2, *[DMA((MATRICES,))] * 3,
            DMA((2,)),
            DMA((2,)), DMA((2,)),
        ],
        compiler_params=pltpu.CompilerParams(collective_id=0, has_side_effects=True, vmem_limit_bytes=MOST_VMEM - SPARE_VMEM),
        name="gradients",
    )(tall, wide, turned, deep, *weights)
    return g, squares, owns


def solution(mesh):
    rep, dp = mesh.axis_names

    def step(x, dy, *arrays):
        weights, m, v = (arrays[i : i + 3] for i in (0, 3, 6))
        g, total, owns = gradients(*by_rows(x[0], dy[0], weights), weights)
        new, new_m, new_v = adam(MATRICES * D * FF, g, total, owns, m, v)
        return (*natural(all_gather(new)), *new_m, *new_v)

    whole, rows, sequences = P(), P(None, dp), P((rep, dp))
    return jax.shard_map(
        step,
        mesh=mesh,
        in_specs=(sequences, sequences, *[whole] * AXES, *[rows] * MATRICES),
        out_specs=(*[P(rep)] * AXES, *[P(rep, dp)] * MATRICES),
        check_vma=False,
    )
```
